32 devices in a mesh: fsdp: 32 (over z, y, x, core).
Axes of the slice: x: 2, y: 2, z: 4, core: 2. Of those that a mesh axis runs over, the one named last changes fastest.
Arguments:
- block_input: bfloat16 [12288, 1152], P('fsdp'), may hold values from -6 to 6
- params: bfloat16 [1, 15241216], P(None, 'fsdp'), may hold values from -4 to 4, as said below
- cotangent: bfloat16 [12288, 1152], P('fsdp'), may hold values from -6 to 6
- segment_ids: int32 [12288], replicated, may hold values from 0 to 17, never falling along the last dimension, each value on 1 to 729 neighbouring positions
Outputs:
- activations: bfloat16 [12288, 1152], P('fsdp')
- input_grad: bfloat16 [12288, 1152], P('fsdp')
- param_grads: float32 [1, 15241216], P(None, 'fsdp')
The draws below stay inside these ranges and needn't reach their ends.
Inputs may be any that keep to these rules, and one draw needn't show every extreme that they name: `segment_ids`: image ids never fall along the tokens; each image holds 1 to 729 tokens, one exactly 729. `params`: gains lie around one, biases and weights around zero.
All inputs are finite; a program needn't handle non-finite values.
Results may differ from the reference program's by a relative error of at most 0.012.
Values may be sent and summed in bfloat16 or wider, within the bound.
A program may use at most 320 MiB of HBM per device.

```python
import math
import jax
import jax.numpy as jnp
import numpy as np
from jax import lax

D = 1152
HEADS = 16
HEAD_DIM = 72
FF = 4304
LAYERS = 1
IMG = 729
TOK_DEV = 384
REACH = 2
TOKENS = 12288
IMAGES = 18
PARAMS = 15238352
PPAD = 15241216


def draw_params(key, part):
    square = D * D
    ragged = D * FF
    wide_out = 0.5 * math.sqrt(IMG) / math.sqrt(D)
    table = [(D, 1.0, 0.25), (D, 0.0, 0.5), (square, 0.0, D ** (-0.5)), (square, 0.0, D ** (-0.5)), (square, 0.0, D ** (-0.5)), (D, 0.0, 0.5), (D, 0.0, 0.5), (square, 0.0, wide_out), (D, 0.0, 0.3), (D, 1.0, 0.25), (D, 0.0, 0.5), (ragged, 0.0, D ** (-0.5)), (FF, 0.0, 0.5), (ragged, 0.0, FF ** (-0.5)), (D, 0.0, 0.3), (PPAD - PARAMS, 0.0, 1.0)]
    centre = jnp.concatenate([jnp.full((entry[0],), entry[1], jnp.float32) for entry in table])
    spread = jnp.concatenate([jnp.full((entry[0],), entry[2], jnp.float32) for entry in table])
    noise = jnp.clip(jax.random.normal(key, (LAYERS, PPAD), jnp.float32), -4.0, 4.0)
    drawn = centre[None, :] + spread[None, :] * noise
    return drawn.astype(jnp.bfloat16)


def level_of(key, shape, split, smallest, largest):
    factor_of, own = 1.0, jax.random.fold_in(key, 6)
    for dim, blocks in split:
        steps = jnp.exp(jax.random.uniform(jax.random.fold_in(own, dim), (blocks,), jnp.float32, smallest / len(split), largest / len(split)))
        factor_of = factor_of * jnp.repeat(steps, shape[dim] // blocks).reshape([-1 if axis == dim else 1 for axis in range(len(shape))])
    return factor_of


def split_up(count, total, reach, slope):
    loads = [(1 << 20) // math.isqrt(rank ** slope) + 1 for rank in range(2, count + 1)]
    rest, holding = total - reach - (count - 1), [1] * (count - 1)
    while rest > 0:
        free = [i for i in range(count - 1) if holding[i] < reach]
        pool, budget = sum([loads[i] for i in free]), rest
        for i in free:
            extra = min(reach - holding[i], max(1, budget * loads[i] // pool), rest)
            holding[i] = holding[i] + extra
            rest = rest - extra
    return np.array([reach] + holding)


def uneven(own_key, number_of, total, most, slope):
    if number_of == 2:
        one = jax.random.randint(own_key, (), max(1, total - most), min(most, total - 1) + 1)
        return jnp.stack([one, total - one])
    lengths = jnp.asarray(split_up(number_of, total, most, slope), jnp.int32)
    couples = (number_of - 1) // 2
    giver, sink = lengths[1:1 + 2 * couples:2], lengths[2:2 + 2 * couples:2]
    slack = jnp.minimum(giver - 1, most - sink)
    passed = jax.random.randint(jax.random.fold_in(own_key, 1), (couples,), 0, 1 << 20) % (slack + 1)
    lengths = lengths.at[1:1 + 2 * couples:2].set(giver - passed).at[2:2 + 2 * couples:2].set(sink + passed)
    return lengths[jax.random.permutation(jax.random.fold_in(own_key, 2), number_of)]


def normal_values(key, dims, scale, bound, split=(), kind=jnp.bfloat16):
    factor_of = level_of(key, dims, split, -0.22, 0.18) if split else 1.0
    values = jax.random.normal(key, dims, jnp.float32) * scale * factor_of
    return jnp.minimum(jnp.maximum(values, -bound), bound).astype(kind)


def setup_inputs(seed: int = 0) -> dict:
    key_list = jax.random.split(jax.random.key(seed), 5)
    block_input = normal_values(key_list[0], (TOKENS, D), 1.0, 6.0, ((0, 32),))
    params = draw_params(jax.random.fold_in(key_list[4], 71), 0)
    cotangent = normal_values(key_list[2], (TOKENS, D), 1.0, 6.0, ((0, 32),))
    segment_ids = jnp.searchsorted(jnp.cumsum(uneven(key_list[3], IMAGES, TOKENS, IMG, 1)), jnp.arange(TOKENS), side="right").astype(jnp.int32)
    return dict(block_input=block_input, params=params, cotangent=cotangent, segment_ids=segment_ids)


EPS = 1e-06
NEG = -1e+30

def to_bf16(tensor):
    return lax.optimization_barrier(tensor.astype(jnp.bfloat16))

def layout():
    return [('ln1_gain', (D,)), ('ln1_bias', (D,)), ('w_query', (D, D)), ('w_key', (D, D)), ('w_value', (D, D)), ('b_query', (D,)), ('b_value', (D,)), ('w_out', (D, D)), ('b_out', (D,)), ('ln2_gain', (D,)), ('ln2_bias', (D,)), ('w_up', (D, FF)), ('b_up', (FF,)), ('w_down', (FF, D)), ('b_down', (D,))]

def unpack(flat_vec):
    pieces = {}
    offset = 0
    for param_name, param_shape in layout():
        length = math.prod(param_shape)
        pieces[param_name] = flat_vec[offset:offset + length].reshape(param_shape)
        offset += length
    return pieces

def pack_grads(grad_map, total_len):
    pieces = [grad_map[param_name].astype(jnp.float32).reshape(-1) for param_name, param_shape in layout()]
    used_len = sum((math.prod(param_shape) for param_name, param_shape in layout()))
    pieces.append(jnp.zeros((total_len - used_len,), jnp.float32))
    return jnp.concatenate(pieces)

def layer_norm(values, gain_vec, bias_vec):
    centre = values - lax.optimization_barrier(jnp.mean(values, axis=-1, keepdims=True))
    inverse = lax.rsqrt(lax.optimization_barrier(jnp.mean(centre * centre, axis=-1, keepdims=True)) + EPS)
    normed = centre * inverse
    return (normed, inverse, normed * gain_vec.astype(jnp.float32) + bias_vec.astype(jnp.float32))

def norm_back(grad_out, normed, inverse, gain_vec):
    gain_grad = lax.optimization_barrier(jnp.sum(grad_out * normed, axis=0))
    bias_grad = lax.optimization_barrier(jnp.sum(grad_out, axis=0))
    scaled = grad_out * gain_vec.astype(jnp.float32)
    grad_in = inverse * (scaled - lax.optimization_barrier(jnp.mean(scaled, axis=-1, keepdims=True)) - normed * lax.optimization_barrier(jnp.mean(scaled * normed, axis=-1, keepdims=True)))
    return (grad_in, gain_grad, bias_grad)

def gelu_tanh(values):
    return jax.nn.gelu(values, approximate=True)

def mat(left, right):
    return jnp.dot(left, right, preferred_element_type=jnp.float32)

def block_scores(queries, key_rows, allowed):
    rows = queries.shape[0]
    width = key_rows.shape[0]
    q_heads = queries.astype(jnp.float32).reshape(rows, HEADS, HEAD_DIM)
    k_heads = key_rows.astype(jnp.float32).reshape(width, HEADS, HEAD_DIM)
    scores = jnp.einsum('bhd,khd->hbk', q_heads, k_heads) * HEAD_DIM ** (-0.5)
    return (jnp.where(allowed[None], scores, NEG), q_heads, k_heads)

def attend_block(queries, key_rows, value_rows, allowed):
    rows = queries.shape[0]
    width = key_rows.shape[0]
    scores, q_heads, k_heads = block_scores(queries, key_rows, allowed)
    top_score = lax.optimization_barrier(jnp.max(scores, axis=-1, keepdims=True))
    logsum = top_score + jnp.log(lax.optimization_barrier(jnp.sum(jnp.exp(scores - top_score), axis=-1, keepdims=True)))
    probs = to_bf16(jnp.exp(scores - logsum))
    v_heads = value_rows.astype(jnp.float32).reshape(width, HEADS, HEAD_DIM)
    output = jnp.einsum('hbk,khd->bhd', probs.astype(jnp.float32), v_heads).reshape(rows, D)
    return (to_bf16(output), logsum[..., 0])

def attend_block_back(queries, key_rows, value_rows, allowed, logsum, grad_attn):
    rows = queries.shape[0]
    width = key_rows.shape[0]
    scores, q_heads, k_heads = block_scores(queries, key_rows, allowed)
    v_heads = value_rows.astype(jnp.float32).reshape(width, HEADS, HEAD_DIM)
    g_heads = grad_attn.astype(jnp.float32).reshape(rows, HEADS, HEAD_DIM)
    probs = jnp.exp(scores - logsum[..., None])
    probs_b = to_bf16(probs).astype(jnp.float32)
    prob_grad = jnp.einsum('bhd,khd->hbk', g_heads, v_heads)
    row_total = lax.optimization_barrier(jnp.sum(probs * prob_grad, axis=-1, keepdims=True))
    score_b = to_bf16(probs * (prob_grad - row_total)).astype(jnp.float32)
    scale = HEAD_DIM ** (-0.5)
    grad_q = jnp.einsum('hbk,khd->bhd', score_b, k_heads).reshape(rows, D) * scale
    grad_k = jnp.einsum('hbk,bhd->khd', score_b, q_heads).reshape(width, D) * scale
    grad_v = jnp.einsum('hbk,bhd->khd', probs_b, g_heads).reshape(width, D)
    return (grad_q, grad_k, grad_v)

def padded_windows(key_rows, value_rows, segment_ids):
    margin = REACH * TOK_DEV
    key_pad = jnp.pad(key_rows, ((margin, margin), (0, 0)))
    value_pad = jnp.pad(value_rows, ((margin, margin), (0, 0)))
    seg_pad = jnp.pad(segment_ids, (margin, margin), constant_values=-1)
    return (key_pad, value_pad, seg_pad)

def attention(queries, key_rows, value_rows, segment_ids):
    span_len = (2 * REACH + 1) * TOK_DEV
    key_pad, value_pad, seg_pad = padded_windows(key_rows, value_rows, segment_ids)

    def one_block(block_idx):
        start = block_idx * TOK_DEV
        q_blk = lax.dynamic_slice_in_dim(queries, start, TOK_DEV, 0)
        k_blk = lax.dynamic_slice_in_dim(key_pad, start, span_len, 0)
        v_blk = lax.dynamic_slice_in_dim(value_pad, start, span_len, 0)
        seg_q = lax.dynamic_slice_in_dim(segment_ids, start, TOK_DEV, 0)
        seg_k = lax.dynamic_slice_in_dim(seg_pad, start, span_len, 0)
        return attend_block(q_blk, k_blk, v_blk, seg_q[:, None] == seg_k[None, :])
    outputs, logsums = lax.map(one_block, jnp.arange(TOKENS // TOK_DEV, dtype=jnp.int32))
    return (outputs.reshape(TOKENS, D), logsums)

def attention_back(queries, key_rows, value_rows, segment_ids, logsums, grad_attn):
    margin = REACH * TOK_DEV
    span_len = (2 * REACH + 1) * TOK_DEV
    key_pad, value_pad, seg_pad = padded_windows(key_rows, value_rows, segment_ids)

    def visit(carry, inputs):
        key_acc, value_acc = carry
        block_idx, block_logs = inputs
        start = block_idx * TOK_DEV
        q_blk = lax.dynamic_slice_in_dim(queries, start, TOK_DEV, 0)
        k_blk = lax.dynamic_slice_in_dim(key_pad, start, span_len, 0)
        v_blk = lax.dynamic_slice_in_dim(value_pad, start, span_len, 0)
        g_blk = lax.dynamic_slice_in_dim(grad_attn, start, TOK_DEV, 0)
        seg_q = lax.dynamic_slice_in_dim(segment_ids, start, TOK_DEV, 0)
        seg_k = lax.dynamic_slice_in_dim(seg_pad, start, span_len, 0)
        grad_q, grad_k, grad_v = attend_block_back(q_blk, k_blk, v_blk, seg_q[:, None] == seg_k[None, :], block_logs, g_blk)
        key_acc = lax.dynamic_update_slice_in_dim(key_acc, lax.dynamic_slice_in_dim(key_acc, start, span_len, 0) + grad_k, start, 0)
        value_acc = lax.dynamic_update_slice_in_dim(value_acc, lax.dynamic_slice_in_dim(value_acc, start, span_len, 0) + grad_v, start, 0)
        return ((key_acc, value_acc), grad_q)
    zeros_acc = jnp.zeros((TOKENS + 2 * margin, D), jnp.float32)
    (key_acc, value_acc), grad_qs = lax.scan(visit, (zeros_acc, zeros_acc), (jnp.arange(TOKENS // TOK_DEV, dtype=jnp.int32), logsums))
    return (grad_qs.reshape(TOKENS, D), key_acc[margin:margin + TOKENS], value_acc[margin:margin + TOKENS])

def mlp_forward(normed_mid, weights):
    block_rows = math.gcd(TOKENS, 4096)

    def one_block(rows_in):
        pre_act = mat(rows_in, weights['w_up']) + weights['b_up'].astype(jnp.float32)
        hidden = to_bf16(gelu_tanh(pre_act))
        return mat(hidden, weights['w_down']) + weights['b_down'].astype(jnp.float32)
    return lax.map(one_block, normed_mid.reshape(TOKENS // block_rows, block_rows, D)).reshape(TOKENS, D)

def mlp_back(normed_mid, grad_out, weights):
    block_rows = math.gcd(TOKENS, 4096)

    def visit(carry, inputs):
        acc_up, acc_bup, acc_down, acc_bdown = carry
        rows_in, grad_rows = inputs
        pre_act = mat(rows_in, weights['w_up']) + weights['b_up'].astype(jnp.float32)
        hidden = to_bf16(gelu_tanh(pre_act))
        grad_b = to_bf16(grad_rows)
        acc_down = acc_down + mat(hidden.T, grad_b)
        acc_bdown = acc_bdown + lax.optimization_barrier(jnp.sum(grad_rows, axis=0))
        hidden_grad = mat(grad_b, weights['w_down'].T)
        pre_grad = jax.vjp(gelu_tanh, pre_act)[1](hidden_grad)[0]
        pre_b = to_bf16(pre_grad)
        acc_up = acc_up + mat(rows_in.T, pre_b)
        acc_bup = acc_bup + lax.optimization_barrier(jnp.sum(pre_grad, axis=0))
        return ((acc_up, acc_bup, acc_down, acc_bdown), mat(pre_b, weights['w_up'].T))
    start_acc = (jnp.zeros((D, FF), jnp.float32), jnp.zeros((FF,), jnp.float32), jnp.zeros((FF, D), jnp.float32), jnp.zeros((D,), jnp.float32))
    (acc_up, acc_bup, acc_down, acc_bdown), norm_grads = lax.scan(visit, start_acc, (normed_mid.reshape(-1, block_rows, D), grad_out.reshape(-1, block_rows, D)))
    return (norm_grads.reshape(TOKENS, D), acc_up, acc_bup, acc_down, acc_bdown)

def layer_forward(state, weights, segment_ids):
    normed1, inverse1, pre1 = layer_norm(state, weights['ln1_gain'], weights['ln1_bias'])
    normed_in = to_bf16(pre1)
    queries = to_bf16(mat(normed_in, weights['w_query']) + weights['b_query'].astype(jnp.float32))
    key_rows = to_bf16(mat(normed_in, weights['w_key']))
    value_rows = to_bf16(mat(normed_in, weights['w_value']) + weights['b_value'].astype(jnp.float32))
    attended, logsums = attention(queries, key_rows, value_rows, segment_ids)
    mid = state + (mat(attended, weights['w_out']) + weights['b_out'].astype(jnp.float32))
    normed2, inverse2, pre2 = layer_norm(mid, weights['ln2_gain'], weights['ln2_bias'])
    normed_mid = to_bf16(pre2)
    out_state = mid + mlp_forward(normed_mid, weights)
    saved = (normed1, inverse1, normed_in, queries, key_rows, value_rows, attended, logsums, normed2, inverse2, normed_mid)
    return (out_state, saved)

def layer_backward(grad_out, weights, saved, segment_ids):
    normed1, inverse1, normed_in, queries, key_rows, value_rows, attended, logsums, normed2, inverse2, normed_mid = saved
    grads = {}
    norm_grad, grads['w_up'], grads['b_up'], grads['w_down'], grads['b_down'] = mlp_back(normed_mid, grad_out, weights)
    mid_part, grads['ln2_gain'], grads['ln2_bias'] = norm_back(norm_grad, normed2, inverse2, weights['ln2_gain'])
    mid_grad = grad_out + mid_part
    mid_b = to_bf16(mid_grad)
    grads['w_out'] = mat(attended.T, mid_b)
    grads['b_out'] = lax.optimization_barrier(jnp.sum(mid_grad, axis=0))
    attended_grad = to_bf16(mat(mid_b, weights['w_out'].T))
    grad_q, grad_k, grad_v = attention_back(queries, key_rows, value_rows, segment_ids, logsums, attended_grad)
    query_b, key_b, value_b = (to_bf16(grad_q), to_bf16(grad_k), to_bf16(grad_v))
    grads['w_query'] = mat(normed_in.T, query_b)
    grads['w_key'] = mat(normed_in.T, key_b)
    grads['w_value'] = mat(normed_in.T, value_b)
    grads['b_query'] = lax.optimization_barrier(jnp.sum(grad_q, axis=0))
    grads['b_value'] = lax.optimization_barrier(jnp.sum(grad_v, axis=0))
    in_grad = mat(query_b, weights['w_query'].T) + mat(key_b, weights['w_key'].T) + mat(value_b, weights['w_value'].T)
    in_part, grads['ln1_gain'], grads['ln1_bias'] = norm_back(in_grad, normed1, inverse1, weights['ln1_gain'])
    return (mid_grad + in_part, grads)

def reference(block_input, params, cotangent, segment_ids):
    state = block_input.astype(jnp.float32)
    saved_list = []
    for layer_idx in range(LAYERS):
        state, saved = layer_forward(state, unpack(params[layer_idx]), segment_ids)
        saved_list.append(saved)
    activations = state.astype(jnp.bfloat16)
    grad = cotangent.astype(jnp.float32)
    flat_list = [None] * LAYERS
    for layer_idx in reversed(range(LAYERS)):
        grad, grad_map = layer_backward(grad, unpack(params[layer_idx]), saved_list[layer_idx], segment_ids)
        flat_list[layer_idx] = pack_grads(grad_map, PPAD)
    return (activations, grad.astype(jnp.bfloat16), jnp.stack(flat_list))
```

```python
import functools
import math

import jax
import jax.numpy as jnp
import numpy as np
from jax import lax
from jax.experimental import pallas as pl
from jax.experimental.pallas import tpu as pltpu
from jax.sharding import PartitionSpec as P

D = 1152
HEADS = 16
HEAD_DIM = 72
FF = 4304
REACH = 2


EPS = 1e-06
NEG = -1e30
LANES = 128
ROWS = 16
DC = D // LANES
FC = -(-FF // LANES)
WIDE = FF * ROWS // LANES
HEAD = 544
KIND_A, KIND_D, KIND_L2, KIND_L3, KIND_B = 1, 2, 3, 4, 5
MESH = pl.DeviceIdType.MESH


def units():
    found = []
    offset = 0

    def matrix(name, kind, rows, width, tiles):
        nonlocal offset
        for row in range(0, rows, ROWS):
            found.append((name, kind, offset + row * width, tiles))
        offset += rows * width

    def vectors(name, kind, length, tiles):
        nonlocal offset
        found.append((name, kind, offset, tiles))
        offset += length

    vectors("vec1", KIND_L2, 2 * D, 2)
    matrix("w_query", KIND_A, D, D, DC)
    matrix("w_key", KIND_A, D, D, DC)
    matrix("w_value", KIND_A, D, D, DC)
    vectors("vec2", KIND_L2, 2 * D, 2)
    matrix("w_out", KIND_A, D, D, DC)
    vectors("vec3", KIND_L2, 3 * D, 2)
    matrix("w_up", KIND_B, D, FF, FC)
    vectors("vec4", KIND_L3, FF, 3)
    matrix("w_down", KIND_D, FF, D, DC)
    vectors("vec5", KIND_D, D, DC)
    return found


def unit_width(name):
    return {"vec1": 2 * D, "vec2": 2 * D, "vec3": 3 * D, "vec4": FF, "vec5": D, "w_up": ROWS * FF}.get(
        name, ROWS * D
    )


def wire_plan(count, shard):
    blocks = [[] for _ in range(count)]
    where = {}
    used = [0] * count
    tails = [0] * count
    for name, kind, first, tiles in units():
        owner = first // shard
        where.setdefault(name, []).append((owner, used[owner], tiles))
        blocks[owner].append((kind, (first - owner * shard) // LANES, used[owner]))
        used[owner] += tiles
        tails[owner] = max(0, first + unit_width(name) - (owner + 1) * shard)
    block = max(used)
    block += block % 2
    most = max(len(b) for b in blocks)
    table = np.zeros((count, 3 * most), np.int32)
    for owner, entries in enumerate(blocks):
        for i, entry in enumerate(entries):
            table[owner, 3 * i : 3 * i + 3] = entry
    return where, block, table, np.array(tails, np.int32)


def lane_iota(rows):
    return lax.broadcasted_iota(jnp.int32, (rows, LANES), 1)


def wide_rows():
    return [divmod(row * FF, LANES) for row in range(ROWS)]


SKEW = (D * 0 + 80) % LANES


def rows_from_line(line_ref, flat_ref, first, rows):
    step = 8 * LANES

    @pl.loop(0, rows // 8)
    def _(i):
        part = line_ref[:, pl.ds(pl.multiple_of(i * step, step), step)].astype(jnp.float32)
        flat_ref[pl.ds(first + i * 8, 8)] = part.reshape(8, LANES)

    for row in range(rows // 8 * 8, rows):
        flat_ref[pl.ds(first + row, 1)] = line_ref[:, row * LANES : (row + 1) * LANES].astype(jnp.float32)


def line_from_rows(flat_ref, line_ref, first, rows):
    step = 8 * LANES

    @pl.loop(0, rows // 8)
    def _(i):
        part = flat_ref[pl.ds(first + i * 8, 8)]
        line_ref[:, pl.ds(pl.multiple_of(i * step, step), step)] = part.reshape(1, step)

    for row in range(rows // 8 * 8, rows):
        line_ref[:, row * LANES : (row + 1) * LANES] = flat_ref[pl.ds(first + row, 1)]


def to_tiles_kernel(entries, table_ref, line_ref, head_ref, tile_ref, stage_ref, flat_ref):
    rows = line_ref.shape[1] // LANES
    rows_from_line(line_ref, flat_ref, 0, rows)
    rows_from_line(head_ref, flat_ref, rows, HEAD)

    def unit(i, _):
        kind, src, dst = (table_ref[3 * i + j] for j in range(3))

        @pl.when(kind == KIND_A)
        def _():
            for c in range(DC):
                tile_ref[dst + c] = flat_ref[pl.ds(src + c, ROWS, stride=DC), :].astype(jnp.bfloat16)

        @pl.when(kind == KIND_D)
        def _():
            lane = lane_iota(ROWS)
            for c in range(DC):
                here = flat_ref[pl.ds(src + c, ROWS, stride=DC), :]
                after = flat_ref[pl.ds(src + c + 1, ROWS, stride=DC), :]
                both = jnp.where(lane >= SKEW, here, after)
                tile_ref[dst + c] = pltpu.roll(both, LANES - SKEW, 1).astype(jnp.bfloat16)

        for code, tiles in ((KIND_L2, 2), (KIND_L3, 3)):

            @pl.when(kind == code)
            def _():
                for j in range(tiles):
                    tile_ref[dst + j] = flat_ref[pl.ds(src + ROWS * j, ROWS), :].astype(jnp.bfloat16)

        @pl.when(kind == KIND_B)
        def _():
            tall = 8 * pl.cdiv(FC, 8)
            lane = lane_iota(tall)
            row = lax.broadcasted_iota(jnp.int32, (tall, LANES), 0)
            keep = (row < FC - 1) | (lane < FF % LANES)
            for r, (base, skew) in enumerate(wide_rows()):
                part = flat_ref[pl.ds(src + base, tall), :]
                if skew:
                    after = flat_ref[pl.ds(src + base + 1, tall), :]
                    part = pltpu.roll(jnp.where(lane >= skew, part, after), LANES - skew, 1)
                stage_ref[pl.ds(r, tall, stride=ROWS), :] = jnp.where(keep, part, 0.0)
            for c in range(FC):
                tile_ref[dst + c] = stage_ref[pl.ds(ROWS * c, ROWS), :].astype(jnp.bfloat16)

        return 0

    lax.fori_loop(0, entries, unit, 0)


def to_flat_kernel(entries, table_ref, tile_ref, line_ref, tail_ref, stage_ref, flat_ref):
    flat_ref[...] = jnp.zeros_like(flat_ref)

    def unit(i, _):
        kind, src, dst = (table_ref[3 * i + j] for j in range(3))

        @pl.when(kind == KIND_A)
        def _():
            for c in range(DC):
                flat_ref[pl.ds(src + c, ROWS, stride=DC), :] = tile_ref[dst + c]

        @pl.when(kind == KIND_D)
        def _():
            lane = lane_iota(ROWS)
            for c in range(DC):
                turned = pltpu.roll(tile_ref[dst + c], SKEW, 1)
                for step, keep in ((0, lane >= SKEW), (1, lane < SKEW)):
                    at = pl.ds(src + c + step, ROWS, stride=DC)
                    flat_ref[at, :] = jnp.where(keep, turned, flat_ref[at, :])

        for code, tiles in ((KIND_L2, 2), (KIND_L3, 3)):

            @pl.when(kind == code)
            def _():
                for j in range(tiles):
                    flat_ref[pl.ds(src + ROWS * j, ROWS), :] = tile_ref[dst + j]

        @pl.when(kind == KIND_B)
        def _():
            tall = 8 * pl.cdiv(FC, 8)
            lane = lane_iota(tall)
            row = lax.broadcasted_iota(jnp.int32, (tall, LANES), 0)
            for c in range(FC):
                stage_ref[pl.ds(ROWS * c, ROWS), :] = tile_ref[dst + c]
            for r, (base, skew) in enumerate(wide_rows()):
                turned = stage_ref[pl.ds(r, tall, stride=ROWS), :]
                if skew:
                    turned = pltpu.roll(turned, skew, 1)
                for step in range(2 if skew else 1):
                    entry = row * LANES + lane + (step * LANES - skew)
                    keep = (lane < skew if step else lane >= skew) & (entry < FF)
                    at = pl.ds(src + base + step, tall)
                    flat_ref[at, :] = jnp.where(keep, turned, flat_ref[at, :])

        return 0

    lax.fori_loop(0, entries, unit, 0)
    rows = line_ref.shape[1] // LANES
    line_from_rows(flat_ref, line_ref, 0, rows)
    line_from_rows(flat_ref, tail_ref, rows, HEAD)


def my_row(table):
    return lax.dynamic_index_in_dim(jnp.asarray(table), lax.axis_index("fsdp"), 0, keepdims=False)


def relayout_scratch(rows):
    return [
        pltpu.VMEM((ROWS * 8 * pl.cdiv(FC, 8), LANES), jnp.float32),
        pltpu.VMEM((8 * pl.cdiv(rows + HEAD + 8, 8), LANES), jnp.float32),
    ]


def to_tiles(line, plan):
    where, block, table, tails = plan
    count = lax.axis_size("fsdp")
    head = lax.ppermute(line[:, : HEAD * LANES], "fsdp", [(i, (i - 1) % count) for i in range(count)])
    vmem = pl.BlockSpec(memory_space=pltpu.VMEM)
    return pl.pallas_call(
        functools.partial(to_tiles_kernel, table.shape[1] // 3),
        out_shape=jax.ShapeDtypeStruct((block, ROWS, LANES), jnp.bfloat16),
        grid_spec=pltpu.PrefetchScalarGridSpec(
            num_scalar_prefetch=1, grid=(1,), in_specs=[vmem, vmem], out_specs=vmem,
            scratch_shapes=relayout_scratch(line.shape[1] // LANES),
        ),
        name="to_tiles",
    )(my_row(table), line, head)


def to_flat(tiles, plan, length):
    where, block, table, tails = plan
    count = lax.axis_size("fsdp")
    vmem = pl.BlockSpec(memory_space=pltpu.VMEM)
    line, tail = pl.pallas_call(
        functools.partial(to_flat_kernel, table.shape[1] // 3),
        out_shape=(jax.ShapeDtypeStruct((1, length), jnp.float32), jax.ShapeDtypeStruct((1, HEAD * LANES), jnp.float32)),
        grid_spec=pltpu.PrefetchScalarGridSpec(
            num_scalar_prefetch=1, grid=(1,), in_specs=[vmem], out_specs=[vmem, vmem],
            scratch_shapes=relayout_scratch(length // LANES),
        ),
        name="to_flat",
    )(my_row(table), tiles)
    tail = lax.ppermute(tail, "fsdp", [(i, (i + 1) % count) for i in range(count)])
    entry = lax.broadcasted_iota(jnp.int32, tail.shape, 1)
    first = jnp.where(entry < my_row(np.roll(tails, 1)), tail, line[:, : HEAD * LANES])
    return lax.dynamic_update_slice(line, first, (0, 0))


def place(me):
    return lax.rem(me, 2), lax.rem(me // 2, 2), lax.rem(me // 4, 2), me // 8


def index_of(core, x, y, z):
    return ((z * 2 + y) * 2 + x) * 2 + core


def greet(devices_and_conditions):
    barrier = pltpu.get_barrier_semaphore()
    for device, present in devices_and_conditions:
        if present is None:
            pl.semaphore_signal(barrier, inc=1, device_id=(device,), device_id_type=MESH)
        else:

            @pl.when(present)
            def _():
                pl.semaphore_signal(barrier, inc=1, device_id=(device,), device_id_type=MESH)

    present = [1 if p is None else p.astype(jnp.int32) for _, p in devices_and_conditions]
    pl.semaphore_wait(barrier, sum(present))


def scatter_kernel(
    depth, part_ref, out_ref, held, mates, halfs, fulls, lines, load_sem, mate_send, mate_recv, half_send, half_recv, full_send, full_recv, line_send, line_recv
):
    me = lax.axis_index("fsdp")
    core, x, y, z = place(me)
    mate, x_near, y_near = index_of(1 - core, x, y, z), index_of(core, 1 - x, y, z), index_of(core, x, 1 - y, z)
    half = part_ref.shape[1] // 2
    halves = (pl.ds(0, half), pl.ds(half, half))
    greet(
        [(mate, None), (x_near, None), (y_near, None), (me - 8, z > 0), (me + 8, z < depth - 1)]
    )

    def remote(source, target, send, recv, device):
        return pltpu.make_async_remote_copy(
            src_ref=source, dst_ref=target, send_sem=send, recv_sem=recv, device_id=(device,), device_id_type=MESH
        )

    def level_at(step):
        low, high = jnp.minimum(z, depth - 1 - z), jnp.maximum(z, depth - 1 - z)
        side_up = depth - 1 - z >= z
        single = high - low
        distance_single = high - step
        pair = (step - single) // 2
        distance_pair = low - pair
        first_of_pair = lax.rem(step - single, 2) == 0
        distance = jnp.where(step < single, distance_single, distance_pair)
        up = jnp.where(step < single, side_up, first_of_pair)
        return jnp.where(up, z + distance, z - distance)

    order = [level_at(step) for step in range(depth)]
    def owner(level, slot, which_core):
        return index_of(which_core, 1 - x if slot in (1, 3) else x, 1 - y if slot in (2, 3) else y, level)

    def to_mate(step, slot):
        return remote(
            part_ref.at[owner(order[step], slot, 1 - core)],
            mates.at[step, slot],
            mate_send.at[step, slot],
            mate_recv.at[step, slot],
            mate,
        )

    def load(step, slot):
        return pltpu.make_async_copy(part_ref.at[owner(order[step], slot, core)], held.at[step, slot], load_sem.at[step, slot])

    slots = (3, 1, 2, 0)
    for step in range(depth):
        for slot in slots:
            to_mate(step, slot).start()
            load(step, slot).start()

    tiles = max(t for t in range(1, 17) if half % t == 0)

    def add(target, sources, first, count):
        @pl.loop(0, count // tiles)
        def _(i):
            at = pl.ds(first + i * tiles, tiles)
            total = target[at].astype(jnp.float32)
            for source, shift in sources:
                total = total + source[pl.ds(first - shift + i * tiles, tiles)].astype(jnp.float32)
            target[at] = total.astype(target.dtype)

    def corner_out(step):
        return (
            remote(held.at[step, 3, halves[0]], halfs.at[step, 0], half_send.at[step, 0], half_recv.at[step, 0], y_near),
            remote(held.at[step, 3, halves[1]], halfs.at[step, 1], half_send.at[step, 1], half_recv.at[step, 1], x_near),
        )

    def full_out(step):
        return (
            remote(held.at[step, 1], fulls.at[step, 0], full_send.at[step, 0], full_recv.at[step, 0], x_near),
            remote(held.at[step, 2], fulls.at[step, 1], full_send.at[step, 1], full_recv.at[step, 1], y_near),
        )

    def line_out(step, up):
        level = order[step]
        if up:
            return remote(held.at[step, 0], lines.at[level], line_send.at[step], line_recv.at[level], me + 8)
        slot = jnp.where(level == z - 1, depth, level)
        return remote(held.at[step, 0], lines.at[slot], line_send.at[step], line_recv.at[slot], me - 8)

    def line_in(slot):
        remote(held.at[0, 0], lines.at[slot], line_send.at[0], line_recv.at[slot], me).wait_recv()

    def chip_sum(step, slot):
        to_mate(step, slot).wait_recv()
        load(step, slot).wait()
        add(held.at[step, slot], [(mates.at[step, slot], 0)], 0, 2 * half)

    def begin(step):
        chip_sum(step, 3)
        for c in corner_out(step):
            c.start()
        chip_sum(step, 1)
        chip_sum(step, 2)
        chip_sum(step, 0)

    def middle(step):
        by_y, by_x = corner_out(step)
        by_y.wait_recv()
        add(held.at[step, 1], [(halfs.at[step, 0], 0)], 0, half)
        to_x, to_y = full_out(step)
        to_x.start()
        by_x.wait_recv()
        add(held.at[step, 2], [(halfs.at[step, 1], half)], half, half)
        to_y.start()

    def end(step):
        level = order[step]
        to_x, to_y = full_out(step)
        to_x.wait_recv()
        to_y.wait_recv()
        if step < depth - 1:
            near = [(fulls.at[step, 0], 0), (fulls.at[step, 1], 0)]

            @pl.when(level > z)
            def _():
                @pl.when(z > 0)
                def _():
                    line_in(level)
                    add(held.at[step, 0], near + [(lines.at[level], 0)], 0, 2 * half)

                @pl.when(z == 0)
                def _():
                    add(held.at[step, 0], near, 0, 2 * half)

                line_out(step, True).start()

            @pl.when(level < z)
            def _():
                @pl.when(z < depth - 1)
                def _():
                    line_in(level)
                    add(held.at[step, 0], near + [(lines.at[level], 0)], 0, 2 * half)

                @pl.when(z == depth - 1)
                def _():
                    add(held.at[step, 0], near, 0, 2 * half)

                line_out(step, False).start()

    def total():
        step = depth - 1

        def write(sources):
            @pl.loop(0, 2 * half // tiles)
            def _(i):
                at = pl.ds(i * tiles, tiles)
                value = held[step, 0, at].astype(jnp.float32)
                for source in sources:
                    value = value + source[at].astype(jnp.float32)
                out_ref[at] = value

        near = [fulls.at[step, 0], fulls.at[step, 1]]

        @pl.when(z > 0)
        def _():
            line_in(z)

        @pl.when(z < depth - 1)
        def _():
            line_in(depth)

        @pl.when((z > 0) & (z < depth - 1))
        def _():
            write(near + [lines.at[z], lines.at[depth]])

        @pl.when(z == 0)
        def _():
            write(near + [lines.at[depth]])

        @pl.when(z == depth - 1)
        def _():
            write(near + [lines.at[z]])

    for step in range(depth):
        begin(step)
        if step >= 1:
            middle(step - 1)
        if step >= 2:
            end(step - 2)
    middle(depth - 1)
    end(depth - 2)
    end(depth - 1)
    total()
    for step in range(depth):
        for slot in slots:
            to_mate(step, slot).wait_send()
        for c in corner_out(step) + full_out(step):
            c.wait_send()
        if step < depth - 1:
            line_out(step, True).wait_send()


def scatter_blocks(parts, kernels):
    count, block = parts.shape[:2]
    if not kernels:
        received = lax.all_to_all(parts, "fsdp", split_axis=0, concat_axis=0, tiled=True)
        return jnp.sum(received.astype(jnp.float32), axis=0)
    depth = count // 8
    dma = pltpu.SemaphoreType.DMA
    full, part = (block, ROWS, LANES), (block // 2, ROWS, LANES)
    vmem = lambda lead, shape: pltpu.VMEM((*lead, *shape), parts.dtype)
    return pl.pallas_call(
        functools.partial(scatter_kernel, depth),
        out_shape=jax.ShapeDtypeStruct(full, jnp.float32),
        in_specs=[pl.BlockSpec(memory_space=pl.ANY)],
        out_specs=pl.BlockSpec(memory_space=pltpu.VMEM),
        scratch_shapes=[
            vmem((depth, 4), full), vmem((depth, 4), full), vmem((depth, 2), part), vmem((depth, 2), full), vmem((depth + 1,), full),
            dma((depth, 4)), dma((depth, 4)), dma((depth, 4)), dma((depth, 2)), dma((depth, 2)), dma((depth, 2)), dma((depth, 2)),
            dma((depth,)), dma((depth + 1,)),
        ],
        compiler_params=pltpu.CompilerParams(collective_id=1, has_side_effects=True, vmem_limit_bytes=62 << 20),
        name="scatter_blocks",
    )(parts)


BF = jnp.bfloat16
F32 = jnp.float32
PAIR = 2 * LANES
SCALE = HEAD_DIM**-0.5
GELU_A = math.sqrt(2.0 / math.pi)
GELU_B = 0.044715
ANY = pl.BlockSpec(memory_space=pl.ANY)
VM = pl.BlockSpec(memory_space=pltpu.VMEM)
VMEM_LIMIT = 63 << 20


def nn(left, right):
    return lax.dot_general(left, right, (((1,), (0,)), ((), ())), preferred_element_type=F32)


def nt(left, right):
    return lax.dot_general(left, right, (((1,), (1,)), ((), ())), preferred_element_type=F32)


def runs_of(where, name):
    runs, done = [], 0
    for owner, at, tiles in where[name]:
        if runs and runs[-1][0] == owner and runs[-1][1] + runs[-1][2] == at:
            runs[-1][2] += tiles
        else:
            runs.append([owner, at, tiles, done])
        done += tiles
    return runs


def copies(where, name, blocks_ref, tiles_ref, sem, out=False):
    made = []
    flat_tiles = tiles_ref if len(tiles_ref.shape) == 3 else tiles_ref.reshape(-1, ROWS, LANES)
    for owner, at, tiles, done in runs_of(where, name):
        there, here = blocks_ref.at[owner, pl.ds(at, tiles)], flat_tiles.at[pl.ds(done, tiles)]
        made.append(pltpu.make_async_copy(here, there, sem) if out else pltpu.make_async_copy(there, here, sem))
    return made


def start(made):
    for copy in made:
        copy.start()


def wait(made):
    for copy in made:
        copy.wait()


def panel(tiles_ref, c, units, first=0):
    return tiles_ref[pl.ds(first, units), pl.ds(c, 1)].reshape(units * ROWS, LANES)


def panels(tiles_ref, c, many, units, first=0):
    return jnp.concatenate([panel(tiles_ref, c + i, units, first) for i in range(many)], axis=1)


def put_panel(tiles_ref, c, value, first=0):
    units = value.shape[0] // ROWS
    tiles_ref[pl.ds(first, units), pl.ds(c, 1)] = value.astype(BF).reshape(units, 1, ROWS, LANES)


def put_panels(tiles_ref, c, value, first=0):
    for i in range(value.shape[1] // LANES):
        put_panel(tiles_ref, c + i, value[:, i * LANES : (i + 1) * LANES], first)


def vector_rows(tiles_ref):
    return jnp.concatenate([tiles_ref[i].astype(F32) for i in range(tiles_ref.shape[0])], axis=0)


def as_row(rows, first, many):
    return jnp.concatenate([rows[first + i : first + i + 1] for i in range(many)], axis=1)


def put_vectors(tiles_ref, rows_list):
    parts = [row[:, i * LANES : (i + 1) * LANES] for row in rows_list for i in range(row.shape[1] // LANES)]
    missing = tiles_ref.shape[0] * ROWS - len(parts)
    whole = jnp.concatenate(parts + [jnp.zeros((missing, LANES), F32)] if missing else parts, axis=0)
    for i in range(tiles_ref.shape[0]):
        tiles_ref[i] = whole[i * ROWS : (i + 1) * ROWS].astype(BF)


def norm_rows(values):
    centre = values - jnp.mean(values, axis=-1, keepdims=True)
    inverse = lax.rsqrt(jnp.mean(centre * centre, axis=-1, keepdims=True) + EPS)
    return centre * inverse, inverse


def norm_rows_back(grad, normed, inverse, gain):
    scaled = grad * gain
    return inverse * (
        scaled - jnp.mean(scaled, axis=-1, keepdims=True) - normed * jnp.mean(scaled * normed, axis=-1, keepdims=True)
    )


def column_sums(values):
    return jnp.sum(values, axis=0, keepdims=True)


def head_window(h):
    block = jnp.minimum((h * HEAD_DIM) // LANES, DC - 2)
    lane = pl.multiple_of(block * LANES, LANES)
    return lane, h * HEAD_DIM - lane


def head_mask(rows, offset):
    lane = lax.broadcasted_iota(jnp.int32, (rows, PAIR), 1)
    return (lane >= offset) & (lane < offset + HEAD_DIM)


def front_kernel(
    where, x_ref, segq_ref, segk_ref, blocks_ref, q_ref, k_ref, v_ref, attended_ref, logs_ref,
    normed_ref, w_ref, vec1_ref, vec2_ref, bias_ref, score_ref, prob_ref, sem, vec_sem,
):
    window, rows = x_ref.shape[0], q_ref.shape[0]
    margin = (window - rows) // 2
    loads = [copies(where, name, blocks_ref, w_ref.at[i], sem.at[i]) for i, name in enumerate(("w_query", "w_key", "w_value"))]
    vecs = copies(where, "vec1", blocks_ref, vec1_ref, vec_sem) + copies(where, "vec2", blocks_ref, vec2_ref, vec_sem)
    start(vecs)
    for made in loads:
        start(made)
    wait(vecs)
    vec = vector_rows(vec1_ref)
    gain, shift = as_row(vec, 0, DC), as_row(vec, DC, DC)
    step = rows // 3

    @pl.loop(0, window // step)
    def _(i):
        at = pl.ds(i * step, step)
        normed, _ = norm_rows(x_ref[at].astype(F32))
        normed_ref[at] = (normed * gain + shift).astype(BF)

    @pl.loop(0, rows // 8)
    def _(i):
        at = pl.ds(i * 8, 8)
        bias_ref[at] = jnp.where(segq_ref[at] == segk_ref[...], 0.0, NEG)

    biases = vector_rows(vec2_ref)
    zero = jnp.zeros((1, D), F32)
    for made in loads:
        wait(made)
    for i, (out, add) in enumerate(((q_ref, as_row(biases, 0, DC)), (k_ref, zero), (v_ref, as_row(biases, DC, DC)))):
        for c in range(0, DC, 2):
            many = min(2, DC - c)
            lanes = slice(c * LANES, (c + many) * LANES)
            weights = panels(w_ref.at[i], c, many, D // ROWS)
            if i == 0:
                out[:, lanes] = (nn(normed_ref[pl.ds(margin, rows)], weights) + add[:, lanes]).astype(BF)
            else:

                @pl.loop(0, window // rows)
                def _(b):
                    at = pl.ds(b * rows, rows)
                    out[at, lanes] = (nn(normed_ref[at], weights) + add[:, lanes]).astype(BF)

    attended_ref[...] = jnp.zeros_like(attended_ref)
    logs_ref[...] = jnp.zeros_like(logs_ref)
    lane_l = lax.broadcasted_iota(jnp.int32, logs_ref.shape, 1)

    @pl.loop(0, HEADS)
    def _(h):
        lane, offset = head_window(h)
        mask = head_mask(rows, offset)
        lanes = pl.ds(lane, PAIR)
        query = jnp.where(mask, q_ref[:, lanes], jnp.zeros((), BF))
        score_ref[...] = nt(query, k_ref[:, lanes]) * SCALE + bias_ref[...]
        top = jnp.max(score_ref[...], axis=-1, keepdims=True)
        powers = jnp.exp(score_ref[...] - top)
        total = jnp.sum(powers, axis=-1, keepdims=True)
        prob_ref[...] = powers.astype(BF)
        out = nn(prob_ref[...], v_ref[:, lanes]) / total
        attended_ref[:, lanes] = jnp.where(mask, out.astype(BF), attended_ref[:, lanes])
        logs_ref[...] = jnp.where(lane_l == h, top + jnp.log(total), logs_ref[...])


def front(x_win, seg_query, seg_keys, gathered, where, rows):
    window = x_win.shape[0]
    shape = lambda n, d=D, t=BF: jax.ShapeDtypeStruct((n, d), t)
    dma = pltpu.SemaphoreType.DMA
    units = D // ROWS
    return pl.pallas_call(
        functools.partial(front_kernel, where),
        out_shape=(shape(rows), shape(window), shape(window), shape(rows), shape(rows, LANES, F32)),
        in_specs=[VM, VM, VM, ANY],
        out_specs=[VM] * 5,
        scratch_shapes=[
            pltpu.VMEM((window, D), BF),
            pltpu.VMEM((3, units, DC, ROWS, LANES), BF), pltpu.VMEM((2, ROWS, LANES), BF), pltpu.VMEM((2, ROWS, LANES), BF),
            pltpu.VMEM((rows, window), F32), pltpu.VMEM((rows, window), F32), pltpu.VMEM((rows, window), BF), dma((3,)), dma,
        ],
        compiler_params=pltpu.CompilerParams(vmem_limit_bytes=VMEM_LIMIT),
        name="front",
    )(x_win, seg_query, seg_keys, gathered)


def middle_kernel(
    where, x_ref, cot_ref, attended_ref, blocks_ref, act_ref, mid_grad_ref, att_grad_ref, parts_ref,
    wo_ref, wu_ref, wd_ref, vec3_ref, vec4_ref, vec5_ref, b_up_ref, hidden_ref, slope_ref, pre_ref, normed_ref, normed_b_ref,
    mid_ref, g_up_ref, sem, out_sem,
):
    rows = x_ref.shape[0]
    units, f_units = D // ROWS, FF // ROWS
    names = ("w_out", "w_up", "w_down", "vec3", "vec4", "vec5")
    refs = (wo_ref, wu_ref, wd_ref, vec3_ref, vec4_ref, vec5_ref)
    loads = {n: copies(where, n, blocks_ref, r, sem.at[i]) for i, (n, r) in enumerate(zip(names, refs))}
    saves = {n: copies(where, n, parts_ref, r, out_sem, out=True) for n, r in zip(names, refs)}
    for n in ("vec3", "vec4", "vec5", "w_out", "w_up", "w_down"):
        start(loads[n])
    f_wide = FC * LANES
    pads = f_wide // ROWS - f_units
    wd_ref[pl.ds(f_units, pads)] = jnp.zeros((pads, DC, ROWS, LANES), BF)
    for n in ("vec3", "vec4", "vec5", "w_out"):
        wait(loads[n])
    vec = vector_rows(vec3_ref)
    b_out, gain, shift = (as_row(vec, i * DC, DC) for i in range(3))
    vec = vector_rows(vec4_ref)
    entry = lax.broadcasted_iota(jnp.int32, vec.shape, 0) * LANES + lax.broadcasted_iota(jnp.int32, vec.shape, 1)
    b_up_ref[...] = jnp.where(entry < FF, vec, 0.0)
    b_down = jnp.concatenate([vec5_ref[c].astype(F32)[0:1] for c in range(DC)], axis=1)

    for c in range(0, DC, 2):
        many = min(2, DC - c)
        lanes = slice(c * LANES, (c + many) * LANES)
        mid_ref[:, lanes] = (
            x_ref[:, lanes].astype(F32) + nn(attended_ref[...], panels(wo_ref, c, many, units)) + b_out[:, lanes]
        )
    normed, inverse = norm_rows(mid_ref[...])
    normed_ref[...] = normed
    normed_b_ref[...] = (normed * gain + shift).astype(BF)

    wait(loads["w_up"])

    @pl.loop(0, FC // 2)
    def _(p):
        at = pl.ds(pl.multiple_of(p * PAIR, PAIR), PAIR)
        bias = jnp.concatenate([b_up_ref[pl.ds(2 * p, 1)], b_up_ref[pl.ds(2 * p + 1, 1)]], axis=1)
        v = nn(normed_b_ref[...], panels(wu_ref, 2 * p, 2, units)) + bias
        square = v * v
        bent = jnp.tanh(GELU_A * v * (1.0 + GELU_B * square))
        hidden_ref[:, at] = (0.5 * v * (1.0 + bent)).astype(BF)
        slope_ref[:, at] = 0.5 * (1.0 + bent) + 0.5 * v * (1.0 - bent * bent) * (
            GELU_A * (1.0 + 3.0 * GELU_B * square)
        )

    wait(loads["w_down"])
    for c in range(0, DC, 2):
        many = min(2, DC - c)
        lanes = slice(c * LANES, (c + many) * LANES)
        act_ref[:, lanes] = (
            mid_ref[:, lanes] + nn(hidden_ref[...], panels(wd_ref, c, many, f_wide // ROWS)) + b_down[:, lanes]
        ).astype(BF)

    @pl.loop(0, FC // 2)
    def _(p):
        at = pl.ds(pl.multiple_of(p * PAIR, PAIR), PAIR)
        first = p * (PAIR // ROWS)
        grad = nt(cot_ref[...], panels(wd_ref, 0, DC, PAIR // ROWS, first)) * slope_ref[:, at]
        pre_ref[:, at] = grad.astype(BF)
        sums = column_sums(grad)
        g_up_ref[pl.ds(2 * p, 1)] = sums[:, :LANES]
        g_up_ref[pl.ds(2 * p + 1, 1)] = sums[:, LANES:]
        put_panels(wd_ref, 0, nn(hidden_ref[:, at].T, cot_ref[...]), first)

    start(saves["w_down"])
    put_vectors(vec4_ref, [b_up_row for b_up_row in [g_up_ref[i : i + 1] for i in range(FC)]])
    start(saves["vec4"])
    cot = cot_ref[...].astype(F32)
    sums = column_sums(cot)
    row0 = lax.broadcasted_iota(jnp.int32, (ROWS, LANES), 0) == 0
    for c in range(DC):
        vec5_ref[c] = jnp.where(row0, sums[:, c * LANES : (c + 1) * LANES], 0.0).astype(BF)
    start(saves["vec5"])

    for c in range(0, DC, 2):
        many = min(2, DC - c)
        weights = panels(wu_ref, 0, FC, many * LANES // ROWS, c * LANES // ROWS)
        mid_ref[:, c * LANES : (c + many) * LANES] = nt(pre_ref[...], weights)
    e = mid_ref[...]
    normed = normed_ref[...]
    g_gain, g_shift = column_sums(e * normed), column_sums(e)
    mid_grad = cot + norm_rows_back(e, normed, inverse, gain)
    mid_grad_ref[...] = mid_grad
    put_vectors(vec3_ref, [column_sums(mid_grad), g_gain, g_shift])
    start(saves["vec3"])
    mid_b = mid_grad.astype(BF)
    for c in range(0, DC, 2):
        many = min(2, DC - c)
        lanes = slice(c * LANES, (c + many) * LANES)
        weights = panels(wo_ref, 0, DC, many * LANES // ROWS, c * LANES // ROWS)
        att_grad_ref[:, lanes] = nt(mid_b, weights).astype(BF)
    turned = attended_ref[...].T
    for c in range(0, DC, 2):
        many = min(2, DC - c)
        put_panels(wo_ref, c, nn(turned, mid_b[:, c * LANES : (c + many) * LANES]))
    start(saves["w_out"])
    turned_b = normed_b_ref[...].T

    @pl.loop(0, FC // 2)
    def _(p):
        at = pl.ds(pl.multiple_of(p * PAIR, PAIR), PAIR)
        put_panels(wu_ref, 2 * p, nn(turned_b, pre_ref[:, at]))

    start(saves["w_up"])
    for n in names:
        wait(saves[n])


def middle(block_input, cotangent, attended, gathered, where):
    rows = block_input.shape[0]
    shape = lambda t: jax.ShapeDtypeStruct((rows, D), t)
    dma = pltpu.SemaphoreType.DMA
    tiles = lambda *n: pltpu.VMEM((*n, ROWS, LANES), BF)
    units, f_wide = D // ROWS, FC * LANES
    return pl.pallas_call(
        functools.partial(middle_kernel, where),
        out_shape=(shape(BF), shape(F32), shape(BF), jax.ShapeDtypeStruct(gathered.shape, BF)),
        in_specs=[VM, VM, VM, ANY],
        out_specs=[VM, VM, VM, ANY],
        scratch_shapes=[
            tiles(units, DC), tiles(units, FC), tiles(f_wide // ROWS, DC), tiles(2), tiles(3), tiles(DC),
            pltpu.VMEM((3 * ROWS, LANES), F32), pltpu.VMEM((rows, f_wide), BF), pltpu.VMEM((rows, f_wide), F32),
            pltpu.VMEM((rows, f_wide), BF), pltpu.VMEM((rows, D), F32), pltpu.VMEM((rows, D), BF), pltpu.VMEM((rows, D), F32),
            pltpu.VMEM((3 * ROWS, LANES), F32), dma((6,)), dma,
        ],
        compiler_params=pltpu.CompilerParams(vmem_limit_bytes=VMEM_LIMIT),
        name="middle",
    )(block_input, cotangent, attended, gathered)


def back_kernel(
    where, x_hbm_ref, segq_ref, segk_ref, blocks_ref, q_ref, k_ref, v_ref, grad_ref, logs_ref, parts_in_ref,
    near_ref, own_ref, parts_ref,
    w_ref, vec1_ref, vec2_ref, bias_ref, score_ref, prob_ref, turned_ref, dk_ref, dv_ref, dq_ref, part_ref, logs_t_ref, x_ref,
    sem, vec_sem, out_sem, x_sem,
):
    window, rows = x_ref.shape[0], q_ref.shape[0]
    margin = (window - rows) // 2
    units = D // ROWS
    names = ("w_query", "w_key", "w_value")
    loads = [copies(where, name, blocks_ref, w_ref.at[i], sem.at[i]) for i, name in enumerate(names)]
    vecs = copies(where, "vec1", blocks_ref, vec1_ref, vec_sem)
    start(vecs)
    for made in loads:
        start(made)
    x_load = pltpu.make_async_copy(x_hbm_ref, x_ref, x_sem)
    x_load.start()

    @pl.loop(0, window // LANES)
    def _(i):
        at = pl.ds(pl.multiple_of(i * LANES, LANES), LANES)
        bias_ref[at] = jnp.where(segk_ref[at] == segq_ref[...], 0.0, NEG)
        turned_ref[:, at] = k_ref[at].T
        dk_ref[at] = jnp.zeros((LANES, D), F32)
        dv_ref[at] = jnp.zeros((LANES, D), F32)

    logs_t_ref[...] = logs_ref[...].T

    @pl.loop(0, HEADS)
    def _(h):
        lane, offset = head_window(h)
        mask = head_mask(rows, offset)
        lanes = pl.ds(lane, PAIR)
        query = jnp.where(mask, q_ref[:, lanes], jnp.zeros((), BF))
        grad = jnp.where(mask, grad_ref[:, lanes], jnp.zeros((), BF))
        probs = jnp.exp(nt(k_ref[:, lanes], query) * SCALE + bias_ref[...] - logs_t_ref[pl.ds(h, 1)])
        score_ref[...] = probs
        prob_ref[...] = probs.astype(BF)
        prob_grad = nt(v_ref[:, lanes], grad)
        row_total = jnp.sum(score_ref[...] * prob_grad, axis=0, keepdims=True)
        dv_ref[:, lanes] += nn(prob_ref[...], grad)
        prob_ref[...] = (score_ref[...] * (prob_grad - row_total)).astype(BF)
        dk_ref[:, lanes] += nn(prob_ref[...], query)
        part_ref[...] = nn(turned_ref[lanes], prob_ref[...])
        at = pl.ds(pl.multiple_of(h * HEAD_DIM, 8), HEAD_DIM)
        dq_ref[at] = part_ref[pl.ds(pl.multiple_of(offset, 8), HEAD_DIM)]

    dq = dq_ref[...].T * SCALE
    g_query = column_sums(dq)
    dq_b = dq.astype(BF)
    wait(vecs)
    vec = vector_rows(vec1_ref)
    gain, shift = as_row(vec, 0, DC), as_row(vec, DC, DC)
    dk_b_ref, dv_b_ref = k_ref, v_ref
    x_load.wait()
    g_value = jnp.zeros((1, D), F32)
    step = rows // 3

    def rounded(i, total):
        at = pl.ds(pl.multiple_of(i * step, step), step)
        dk_b_ref[at] = (dk_ref[at] * SCALE).astype(BF)
        dv = dv_ref[at]
        dv_b_ref[at] = dv.astype(BF)
        normed, _ = norm_rows(x_ref[at].astype(F32))
        turned_ref[:, at] = (normed * gain + shift).astype(BF).T
        return total + column_sums(dv)

    g_value = lax.fori_loop(0, window // step, rounded, g_value)
    put_vectors(vec2_ref, [g_query, g_value])
    save = copies(where, "vec2", parts_ref, vec2_ref, out_sem, out=True)
    for made in loads:
        wait(made)
    for c in range(0, DC, 2):
        many = min(2, DC - c)
        lanes = slice(c * LANES, (c + many) * LANES)
        part = [panels(w_ref.at[i], 0, DC, many * LANES // ROWS, c * LANES // ROWS) for i in range(3)]

        @pl.loop(0, window // rows)
        def _(b):
            at = pl.ds(b * rows, rows)
            dk_ref[at, lanes] = nt(dk_b_ref[at], part[1]) + nt(dv_b_ref[at], part[2])

        dk_ref[pl.ds(margin, rows), lanes] += nt(dq_b, part[0])
    turned_own = turned_ref[:, pl.ds(margin, rows)]
    for c in range(0, DC, 2):
        many = min(2, DC - c)
        lanes = slice(c * LANES, (c + many) * LANES)
        put_panels(w_ref.at[0], c, nn(turned_own, dq_b[:, lanes]))
        put_panels(w_ref.at[1], c, nn(turned_ref[...], dk_b_ref[:, lanes]))
        put_panels(w_ref.at[2], c, nn(turned_ref[...], dv_b_ref[:, lanes]))
    for i, name in enumerate(names):
        save = save + copies(where, name, parts_ref, w_ref.at[i], out_sem, out=True)
    start(save)

    def norm_block(i, totals):
        at = pl.ds(pl.multiple_of(i * step, step), step)
        normed, inverse = norm_rows(x_ref[at].astype(F32))
        e = dk_ref[at]
        part = norm_rows_back(e, normed, inverse, gain)
        x_ref[at] = part.astype(BF)

        @pl.when((i >= margin // step) & (i < (margin + rows) // step))
        def _():
            own_ref[pl.ds(pl.multiple_of(i * step - margin, step), step)] = part

        return totals[0] + column_sums(e * normed), totals[1] + column_sums(e)

    zero = jnp.zeros((1, D), F32)
    g_gain, g_shift = lax.fori_loop(0, window // step, norm_block, (zero, zero))
    put_vectors(vec1_ref, [g_gain, g_shift])
    last = copies(where, "vec1", parts_ref, vec1_ref, out_sem, out=True)
    last = last + [pltpu.make_async_copy(x_ref, near_ref, x_sem)]
    start(last)
    wait(save + last)


def back(x_win, seg_query, seg_keys, gathered, queries, key_win, value_win, att_grad, logs, parts, where):
    window, rows = x_win.shape[0], queries.shape[0]
    dma = pltpu.SemaphoreType.DMA
    tiles = lambda *n: pltpu.VMEM((*n, ROWS, LANES), BF)
    vm = lambda a, b, t: pltpu.VMEM((a, b), t)
    return pl.pallas_call(
        functools.partial(back_kernel, where),
        out_shape=(
            jax.ShapeDtypeStruct((window, D), BF), jax.ShapeDtypeStruct((rows, D), F32), jax.ShapeDtypeStruct(parts.shape, BF),
        ),
        in_specs=[ANY, VM, VM, ANY, VM, VM, VM, VM, VM, ANY],
        out_specs=[ANY, VM, ANY],
        scratch_shapes=[
            tiles(3, D // ROWS, DC), tiles(2), tiles(2), vm(window, rows, F32), vm(window, rows, F32), vm(window, rows, BF),
            vm(D, window, BF), vm(window, D, F32), vm(window, D, F32), vm(D, rows, F32), vm(PAIR, rows, F32), vm(LANES, rows, F32),
            vm(window, D, BF), dma((3,)), dma, dma, dma,
        ],
        input_output_aliases={9: 2},
        compiler_params=pltpu.CompilerParams(vmem_limit_bytes=VMEM_LIMIT),
        name="back",
    )(x_win, seg_query, seg_keys, gathered, queries, key_win, value_win, att_grad, logs, parts)


HOT_NAMES = ("vec1", "w_query", "w_key", "w_value", "vec2")


def transfer_pieces(plan, depth):
    where, block = plan[:2]
    count = plan[2].shape[0]
    hot = [0] * depth
    for name in HOT_NAMES:
        for owner, at, tiles in where[name]:
            level = owner * depth // count
            hot[level] = max(hot[level], at + tiles)
    hot = [min(block, h + h % 2) for h in hot]
    early = [(level, 0, h) for level, h in enumerate(hot) if h]
    late = [(level, h, block - h) for level, h in enumerate(hot) if h < block]
    return early, late


def cut(piece, many):
    level, first, tiles = piece
    edges = [tiles // 2 * i // (many // 2) if i <= many // 2 else 0 for i in range(many // 2 + 1)]
    half = tiles // 2
    edges = [half * i // (many // 2) for i in range(many // 2)] + [
        half + (tiles - half) * i // (many // 2) for i in range(many // 2 + 1)
    ]
    return [(level, first + a, b - a) for a, b in zip(edges[:-1], edges[1:])]


def gather_front_kernel(
    depth, where, early, late,
    block_ref, x_in_ref, segq_ref, segk_ref,
    out_ref, x_out_ref, x_got_ref, q_ref, k_ref, v_ref, attended_ref, logs_ref,
    z_send, z_recv, x_send, x_recv, y_send, y_recv, corner_send, corner_recv, mate_send, mate_recv, w_send, w_recv,
    local_sem, stage_ref, x_ref, normed_ref, w_ref, vec1_ref, vec2_ref, bias_ref, score_ref, prob_ref, sem, vec_sem,
):
    me = lax.axis_index("fsdp")
    count = 8 * depth
    core, x, y, z = place(me)
    mate, x_near, y_near = index_of(1 - core, x, y, z), index_of(core, 1 - x, y, z), index_of(core, x, 1 - y, z)
    up, down = me + 8, me - 8
    after, before = me + 2, me - 2
    has_after, has_before = after < count, before >= 0
    greet(
        [(mate, None), (x_near, None), (y_near, None), (down, z > 0), (up, z < depth - 1), (after, has_after), (before, has_before)]
    )
    pieces = early + late
    chunks = {p: cut(piece, 4) if piece[0] == 0 and p < len(early) else [piece] for p, piece in enumerate(pieces)}
    chunk_list = [(p, chunk) for p in chunks for chunk in chunks[p]]
    ids = {p: [i for i, (q, _) in enumerate(chunk_list) if q == p] for p in chunks}
    hot, cold = range(len(early)), range(len(early), len(pieces))

    def remote(source, target, send, recv, device):
        return pltpu.make_async_remote_copy(
            src_ref=source, dst_ref=target, send_sem=send, recv_sem=recv, device_id=(device,), device_id_type=MESH
        )

    def span(piece):
        return pl.ds(piece[1], piece[2])

    def halves(p):
        level, first, tiles = pieces[p]
        return (level, first, tiles // 2), (level, first + tiles // 2, tiles - tiles // 2)

    def column(level):
        return index_of(core, x, y, level)

    def from_x(level):
        return index_of(core, 1 - x, y, level)

    def from_y(level):
        return index_of(core, x, 1 - y, level)

    def across(level):
        return index_of(core, 1 - x, 1 - y, level)

    def pass_on(block, piece, send, recv, device, own=False):
        there = out_ref.at[block, span(piece)]
        return remote(block_ref.at[span(piece)] if own else there, there, send, recv, device)

    def z_copy(i, upward, own=False):
        piece = chunk_list[i][1]
        return pass_on(column(piece[0]), piece, z_send.at[i, 0 if upward else 1], z_recv.at[i], up if upward else down, own)

    def plane_copies(i, own=False):
        piece = chunk_list[i][1]
        block = column(piece[0])
        return (
            pass_on(block, piece, x_send.at[i], x_recv.at[i], x_near, own),
            pass_on(block, piece, y_send.at[i], y_recv.at[i], y_near, own),
            pass_on(block, piece, mate_send.at[0, i], mate_recv.at[0, i], mate, own),
        )

    def got(block, i, recv):
        piece = chunk_list[i][1]
        pass_on(block, piece, x_send.at[i], recv, me).wait_recv()

    def spread(i, own=False):
        for copy in plane_copies(i, own):
            copy.start()

    def take(i):
        def run(zv):
            level = chunk_list[i][1][0]
            got(column(level), i, z_recv.at[i])
            if level < zv < depth - 1:
                z_copy(i, True).start()
            if 0 < zv < level:
                z_copy(i, False).start()
            spread(i)

        return run

    def corner_copies(p):
        level = pieces[p][0]
        first, second = halves(p)
        return (
            pass_on(from_x(level), first, corner_send.at[p, 0], corner_recv.at[p, 0], y_near),
            pass_on(from_y(level), second, corner_send.at[p, 1], corner_recv.at[p, 1], x_near),
        )

    def mate_copies(p):
        level = pieces[p][0]
        first, second = halves(p)
        return (
            pass_on(from_x(level), pieces[p], mate_send.at[1, p], mate_recv.at[1, p], mate),
            pass_on(from_y(level), pieces[p], mate_send.at[2, p], mate_recv.at[2, p], mate),
            pass_on(across(level), first, mate_send.at[3, p], mate_recv.at[3, p], mate),
            pass_on(across(level), second, mate_send.at[4, p], mate_recv.at[4, p], mate),
        )

    def beside(p):
        def run(zv):
            level = pieces[p][0]
            for i in ids[p]:
                got(from_x(level), i, x_recv.at[i])
            corner_copies(p)[0].start()
            mate_copies(p)[0].start()
            for i in ids[p]:
                got(from_y(level), i, y_recv.at[i])
            corner_copies(p)[1].start()
            mate_copies(p)[1].start()

        return run

    def corner(p):
        def run(zv):
            level = pieces[p][0]
            for side, half in enumerate(halves(p)):
                pass_on(across(level), half, corner_send.at[p, side], corner_recv.at[p, side], me).wait_recv()
                mate_copies(p)[2 + side].start()

        return run

    def from_mate(p):
        def run(zv):
            level = pieces[p][0]
            other = 1 - 2 * core
            for i in ids[p]:
                pass_on(column(level) + other, chunk_list[i][1], mate_send.at[0, i], mate_recv.at[0, i], me).wait_recv()
            first, second = halves(p)
            for slot, (block, piece) in enumerate(
                ((from_x(level), pieces[p]), (from_y(level), pieces[p]), (across(level), first), (across(level), second))
            ):
                pass_on(block + other, piece, mate_send.at[slot + 1, p], mate_recv.at[slot + 1, p], me).wait_recv()

        return run

    def own_spread(i):
        return lambda zv: spread(i, True)

    def own_up(i):
        return lambda zv: z_copy(i, True, True).start() if zv < depth - 1 else None

    def own_down(i):
        return lambda zv: z_copy(i, False, True).start() if zv > 0 else None

    def w_copy(slot, which, device, source=None):
        return remote(x_in_ref if source is None else source, x_got_ref.at[slot], w_send.at[which], w_recv.at[slot], device)

    def w_start():
        w_copy(1 + 2 * core, 0, mate).start()

        @pl.when(has_after)
        def _():
            w_copy(0, 1, after).start()

        @pl.when(has_before)
        def _():
            w_copy(4, 2, before).start()

    def w_forward(core_index):
        slot = 0 if core_index else 4
        return w_copy(1 if core_index else 3, 3, mate, x_got_ref.at[slot])

    def w_wait(slot):
        w_copy(slot, 0, me).wait_recv()

    def w_middle(zv):
        @pl.when(has_before)
        def _():
            w_wait(0)

        @pl.when(has_after)
        def _():
            w_wait(4)

        @pl.when((core == 1) & has_before)
        def _():
            w_forward(1).start()

        @pl.when((core == 0) & has_after)
        def _():
            w_forward(0).start()

    first_cold = {0: 0, 1: 0, 2: 1, 3: 2}
    levels = [pieces[p][0] for p in cold]

    def lists(zv):
        own_hot = [p for p in hot if pieces[p][0] == zv]
        own_cold = [p for p in cold if pieces[p][0] == zv]
        far_hot = sorted((p for p in hot if pieces[p][0] != zv), key=lambda p: abs(pieces[p][0] - zv))
        far_cold = sorted((p for p in cold if pieces[p][0] != zv), key=lambda p: (abs(pieces[p][0] - zv), -pieces[p][0]))
        start = []
        for p in own_hot:
            for i in ids[p]:
                start += [own_up(i), own_down(i), own_spread(i)]
        for p in own_cold:
            start += [own_down(i) for i in ids[p]]
        for p in far_hot:
            start += [take(i) for i in ids[p]]
        for p in own_cold:
            start += [own_up(i) for i in ids[p]]
        start.append(w_middle)
        order_hot = own_hot + far_hot
        start += [beside(p) for p in order_hot]
        for p in own_cold:
            start += [own_spread(i) for i in ids[p]]
        near = [p for p in far_cold if abs(pieces[p][0] - zv) == 1]
        rest = [p for p in far_cold if p not in near]
        for p in near:
            start += [take(i) for i in ids[p]]
        start += [corner(p) for p in order_hot]
        start += [from_mate(p) for p in order_hot]
        return start, [[take(i) for p in rest for i in ids[p]], own_cold + near + rest]

    plans = [lists(zv) for zv in range(depth)]

    def each_plane(events_of):
        for zv in range(depth):
            events = events_of(zv)
            if events:

                @pl.when(z == zv)
                def _():
                    for event in events:
                        event(zv)

    w_start()
    fill = pltpu.make_async_copy(block_ref, stage_ref, local_sem)
    fill.start()
    fill.wait()
    keep = pltpu.make_async_copy(stage_ref, out_ref.at[me], local_sem)
    keep.start()
    each_plane(lambda zv: plans[zv][0])
    keep.wait()

    def cold_step(k, step):
        return lambda zv: [step(plans[zv][1][1][k])] if k < len(plans[zv][1][1]) else []

    services = {
        "takes": lambda zv: plans[zv][1][0],
        **{("beside", k): cold_step(k, beside) for k in range(len(cold))},
        **{("corner", k): cold_step(k, corner) for k in range(len(cold))},
    }

    def service(name):
        each_plane(services[name])

    rows = q_ref.shape[0]
    window = k_ref.shape[0]
    margin = (window - rows) // 2
    w_wait(3 - 2 * core)

    @pl.when((core == 0) & has_before)
    def _():
        w_wait(1)

    @pl.when((core == 1) & has_after)
    def _():
        w_wait(3)

    near_sem = vec_sem
    present = (before >= 0, (core == 1) | has_before, None, (core == 0) | has_after, after < count)
    for slot, there in enumerate(present):
        at = x_ref.at[pl.ds(slot * rows, rows)]
        if there is None:
            pltpu.make_async_copy(x_in_ref, at, near_sem).start()
            continue

        @pl.when(there)
        def _():
            pltpu.make_async_copy(x_got_ref.at[slot], at, near_sem).start()

        @pl.when(jnp.logical_not(there))
        def _():
            pltpu.make_async_copy(x_in_ref, at, near_sem).start()

    for slot in range(5):
        pltpu.make_async_copy(x_in_ref, x_ref.at[pl.ds(slot * rows, rows)], near_sem).wait()
    x_save = pltpu.make_async_copy(x_ref, x_out_ref, local_sem)
    x_save.start()
    loads = [copies(where, name, out_ref, w_ref.at[i], sem.at[i]) for i, name in enumerate(("w_query", "w_key", "w_value"))]
    vecs = copies(where, "vec1", out_ref, vec1_ref, vec_sem) + copies(where, "vec2", out_ref, vec2_ref, vec_sem)
    start(vecs)
    for made in loads:
        start(made)
    wait(vecs)
    vec = vector_rows(vec1_ref)
    gain, shift = as_row(vec, 0, DC), as_row(vec, DC, DC)
    step = rows // 3

    @pl.loop(0, window // step)
    def _(i):
        at = pl.ds(i * step, step)
        normed, _ = norm_rows(x_ref[at].astype(F32))
        normed_ref[at] = (normed * gain + shift).astype(BF)

    @pl.loop(0, rows // 8)
    def _(i):
        at = pl.ds(i * 8, 8)
        bias_ref[at] = jnp.where(segq_ref[at] == segk_ref[...], 0.0, NEG)

    biases = vector_rows(vec2_ref)
    zero = jnp.zeros((1, D), F32)
    for made in loads:
        wait(made)
    for i, (out, add) in enumerate(((q_ref, as_row(biases, 0, DC)), (k_ref, zero), (v_ref, as_row(biases, DC, DC)))):
        for c in range(0, DC, 2):
            many = min(2, DC - c)
            lanes = slice(c * LANES, (c + many) * LANES)
            weights = panels(w_ref.at[i], c, many, D // ROWS)
            if i == 0:
                out[:, lanes] = (nn(normed_ref[pl.ds(margin, rows)], weights) + add[:, lanes]).astype(BF)
            else:

                @pl.loop(0, window // rows)
                def _(b):
                    at = pl.ds(b * rows, rows)
                    out[at, lanes] = (nn(normed_ref[at], weights) + add[:, lanes]).astype(BF)

        if i == 1:
            service("takes")
    attended_ref[...] = jnp.zeros_like(attended_ref)
    logs_ref[...] = jnp.zeros_like(logs_ref)
    lane_l = lax.broadcasted_iota(jnp.int32, logs_ref.shape, 1)
    when = {("beside", k): (0, 4, 10)[min(k, 2)] for k in range(len(cold))}
    when |= {("corner", k): (12, 15, 16)[min(k, 2)] for k in range(len(cold))}

    @pl.loop(0, HEADS)
    def _(h):
        for name, at_head in when.items():
            if at_head < HEADS:

                @pl.when(h == at_head)
                def _():
                    service(name)

        lane, offset = head_window(h)
        mask = head_mask(rows, offset)
        lanes = pl.ds(lane, PAIR)
        query = jnp.where(mask, q_ref[:, lanes], jnp.zeros((), BF))
        score_ref[...] = nt(query, k_ref[:, lanes]) * SCALE + bias_ref[...]
        top = jnp.max(score_ref[...], axis=-1, keepdims=True)
        powers = jnp.exp(score_ref[...] - top)
        total = jnp.sum(powers, axis=-1, keepdims=True)
        prob_ref[...] = powers.astype(BF)
        out = nn(prob_ref[...], v_ref[:, lanes]) / total
        attended_ref[:, lanes] = jnp.where(mask, out.astype(BF), attended_ref[:, lanes])
        logs_ref[...] = jnp.where(lane_l == h, top + jnp.log(total), logs_ref[...])

    for name, at_head in when.items():
        if at_head >= HEADS:
            service(name)
    each_plane(lambda zv: [from_mate(p) for p in plans[zv][1][1]])

    def sent(zv):
        for i, (p, piece) in enumerate(chunk_list):
            for copy in plane_copies(i):
                copy.wait_send()
            level = piece[0]
            if zv < depth - 1 and level <= zv:
                z_copy(i, True).wait_send()
            if zv > 0 and level >= zv:
                z_copy(i, False).wait_send()
        for p in range(len(pieces)):
            for copy in corner_copies(p) + mate_copies(p):
                copy.wait_send()

    each_plane(lambda zv: [sent])
    w_copy(0, 0, mate).wait_send()

    @pl.when(has_after)
    def _():
        w_copy(0, 1, after).wait_send()

    @pl.when(has_before)
    def _():
        w_copy(4, 2, before).wait_send()

    @pl.when(jnp.where(core == 1, has_before, has_after))
    def _():
        w_forward(0).wait_send()

    x_save.wait()


def gather_front(block, block_input, seg_query, seg_keys, plan):
    where = plan[0]
    count = lax.axis_size("fsdp")
    depth = count // 8
    rows, window = block_input.shape[0], seg_keys.shape[1]
    early, late = transfer_pieces(plan, depth)
    shape = lambda n, d=D, t=BF: jax.ShapeDtypeStruct((n, d), t)
    dma = pltpu.SemaphoreType.DMA
    units = D // ROWS
    many = len(early) + len(late)
    chunks = many + 3 * sum(1 for piece in early if piece[0] == 0)
    got = jax.ShapeDtypeStruct((5, rows, D), BF)
    return pl.pallas_call(
        functools.partial(gather_front_kernel, depth, where, early, late),
        out_shape=(
            jax.ShapeDtypeStruct((count, *block.shape), BF), shape(window), got,
            shape(rows), shape(window), shape(window), shape(rows), shape(rows, LANES, F32),
        ),
        in_specs=[ANY, ANY, VM, VM],
        out_specs=[ANY] * 3 + [VM] * 5,
        scratch_shapes=[
            dma((chunks, 2)), dma((chunks,)), dma((chunks,)), dma((chunks,)), dma((chunks,)), dma((chunks,)),
            dma((many, 2)), dma((many, 2)), dma((5, chunks)), dma((5, chunks)), dma((4,)), dma((5,)),
            dma, pltpu.VMEM(block.shape, BF), pltpu.VMEM((window, D), BF), pltpu.VMEM((window, D), BF),
            pltpu.VMEM((3, units, DC, ROWS, LANES), BF), pltpu.VMEM((2, ROWS, LANES), BF), pltpu.VMEM((2, ROWS, LANES), BF),
            pltpu.VMEM((rows, window), F32), pltpu.VMEM((rows, window), F32), pltpu.VMEM((rows, window), BF), dma((3,)), dma,
        ],
        compiler_params=pltpu.CompilerParams(collective_id=0, has_side_effects=True, vmem_limit_bytes=VMEM_LIMIT),
        name="gather_front",
    )(block, block_input, seg_query, seg_keys)


def passed_along(value, steps):
    count = lax.axis_size("fsdp")
    first, last = (max(0, -steps), min(count, count - steps))
    return lax.ppermute(value, "fsdp", [(source, source + steps) for source in range(first, last)])


def window_of(rows):
    near = [rows if k == 0 else passed_along(rows, -k) for k in range(-REACH, REACH + 1)]
    return jnp.concatenate(near, axis=0)


def shards(kernels, block_input, params, cotangent, segment_ids):
    count = lax.axis_size("fsdp")
    me = lax.axis_index("fsdp")
    rows = block_input.shape[0]
    margin = REACH * rows
    seg_pad = jnp.pad(segment_ids, (margin, margin), constant_values=-1)
    seg_query = lax.dynamic_slice_in_dim(segment_ids, me * rows, rows, 0)
    seg_keys = lax.dynamic_slice_in_dim(seg_pad, me * rows, 2 * margin + rows, 0)
    plan = wire_plan(count, params.shape[1])
    where = plan[0]
    block = to_tiles(params, plan)
    if kernels:
        gathered, x_win, _, queries, key_win, value_win, attended, logs = gather_front(
            block, block_input, seg_query[:, None], seg_keys[None, :], plan
        )
    else:
        x_win = window_of(block_input)
        gathered = lax.all_gather(block, "fsdp", axis=0, tiled=False)
        queries, key_win, value_win, attended, logs = front(
            x_win, seg_query[:, None], seg_keys[None, :], gathered, where, rows
        )
    activations, mid_grad, att_grad, parts = middle(block_input, cotangent, attended, gathered, where)
    near, own, parts = back(
        x_win, seg_query[None, :], seg_keys[:, None], gathered, queries, key_win, value_win, att_grad, logs, parts, where
    )
    input_grad = mid_grad + own
    for k in range(-REACH, REACH + 1):
        if k != 0:
            part = near[(k + REACH) * rows : (k + REACH + 1) * rows]
            input_grad = input_grad + passed_along(part, k).astype(jnp.float32)
    summed = scatter_blocks(parts, kernels)
    param_grads = to_flat(summed, plan, params.shape[1])
    return (activations, input_grad.astype(jnp.bfloat16), param_grads)


def two_by_two(mesh):
    spans = np.array([device.coords for device in mesh.devices.flat])
    return tuple(spans.max(axis=0) - spans.min(axis=0))[:2] == (1, 1)


def solution(mesh):
    return jax.shard_map(
        functools.partial(shards, two_by_two(mesh)),
        mesh=mesh,
        in_specs=(P("fsdp", None), P(None, "fsdp"), P("fsdp", None), P()),
        out_specs=(P("fsdp", None), P("fsdp", None), P(None, "fsdp")),
        check_vma=False,
    )
```

```python
import functools
import math

import jax
import jax.numpy as jnp
import numpy as np
from jax import lax
from jax.experimental import pallas as pl
from jax.experimental.pallas import tpu as pltpu
from jax.sharding import PartitionSpec as P

D = 1152
HEADS = 16
HEAD_DIM = 72
FF = 4304
REACH = 2


EPS = 1e-06
NEG = -1e30
LANES = 128
ROWS = 16
DC = D // LANES
FC = -(-FF // LANES)
WIDE = FF * ROWS // LANES
HEAD = 544
KIND_A, KIND_D, KIND_L2, KIND_L3, KIND_B = 1, 2, 3, 4, 5
MESH = pl.DeviceIdType.MESH


def units():
    found = []
    offset = 0

    def matrix(name, kind, rows, width, tiles):
        nonlocal offset
        for row in range(0, rows, ROWS):
            found.append((name, kind, offset + row * width, tiles))
        offset += rows * width

    def vectors(name, kind, length, tiles):
        nonlocal offset
        found.append((name, kind, offset, tiles))
        offset += length

    vectors("vec1", KIND_L2, 2 * D, 2)
    matrix("w_query", KIND_A, D, D, DC)
    matrix("w_key", KIND_A, D, D, DC)
    matrix("w_value", KIND_A, D, D, DC)
    vectors("vec2", KIND_L2, 2 * D, 2)
    matrix("w_out", KIND_A, D, D, DC)
    vectors("vec3", KIND_L2, 3 * D, 2)
    matrix("w_up", KIND_B, D, FF, FC)
    vectors("vec4", KIND_L3, FF, 3)
    matrix("w_down", KIND_D, FF, D, DC)
    vectors("vec5", KIND_D, D, DC)
    return found


def unit_width(name):
    return {"vec1": 2 * D, "vec2": 2 * D, "vec3": 3 * D, "vec4": FF, "vec5": D, "w_up": ROWS * FF}.get(
        name, ROWS * D
    )


def wire_plan(count, shard):
    blocks = [[] for _ in range(count)]
    where = {}
    used = [0] * count
    tails = [0] * count
    for name, kind, first, tiles in units():
        owner = first // shard
        where.setdefault(name, []).append((owner, used[owner], tiles))
        blocks[owner].append((kind, (first - owner * shard) // LANES, used[owner]))
        used[owner] += tiles
        tails[owner] = max(0, first + unit_width(name) - (owner + 1) * shard)
    block = max(used)
    block += block % 2
    most = max(len(b) for b in blocks)
    table = np.zeros((count, 3 * most), np.int32)
    for owner, entries in enumerate(blocks):
        for i, entry in enumerate(entries):
            table[owner, 3 * i : 3 * i + 3] = entry
    return where, block, table, np.array(tails, np.int32)


def lane_iota(rows):
    return lax.broadcasted_iota(jnp.int32, (rows, LANES), 1)


def wide_rows():
    return [divmod(row * FF, LANES) for row in range(ROWS)]


SKEW = (D * 0 + 80) % LANES


def rows_from_line(line_ref, flat_ref, first, rows):
    step = 8 * LANES

    @pl.loop(0, rows // 8)
    def _(i):
        part = line_ref[:, pl.ds(pl.multiple_of(i * step, step), step)].astype(jnp.float32)
        flat_ref[pl.ds(first + i * 8, 8)] = part.reshape(8, LANES)

    for row in range(rows // 8 * 8, rows):
        flat_ref[pl.ds(first + row, 1)] = line_ref[:, row * LANES : (row + 1) * LANES].astype(jnp.float32)


def line_from_rows(flat_ref, line_ref, first, rows):
    step = 8 * LANES

    @pl.loop(0, rows // 8)
    def _(i):
        part = flat_ref[pl.ds(first + i * 8, 8)]
        line_ref[:, pl.ds(pl.multiple_of(i * step, step), step)] = part.reshape(1, step)

    for row in range(rows // 8 * 8, rows):
        line_ref[:, row * LANES : (row + 1) * LANES] = flat_ref[pl.ds(first + row, 1)]


def to_tiles_kernel(entries, table_ref, line_ref, head_ref, tile_ref, stage_ref, flat_ref):
    rows = line_ref.shape[1] // LANES
    rows_from_line(line_ref, flat_ref, 0, rows)
    rows_from_line(head_ref, flat_ref, rows, HEAD)

    def unit(i, _):
        kind, src, dst = (table_ref[3 * i + j] for j in range(3))

        @pl.when(kind == KIND_A)
        def _():
            for c in range(DC):
                tile_ref[dst + c] = flat_ref[pl.ds(src + c, ROWS, stride=DC), :].astype(jnp.bfloat16)

        @pl.when(kind == KIND_D)
        def _():
            lane = lane_iota(ROWS)
            for c in range(DC):
                here = flat_ref[pl.ds(src + c, ROWS, stride=DC), :]
                after = flat_ref[pl.ds(src + c + 1, ROWS, stride=DC), :]
                both = jnp.where(lane >= SKEW, here, after)
                tile_ref[dst + c] = pltpu.roll(both, LANES - SKEW, 1).astype(jnp.bfloat16)

        for code, tiles in ((KIND_L2, 2), (KIND_L3, 3)):

            @pl.when(kind == code)
            def _():
                for j in range(tiles):
                    tile_ref[dst + j] = flat_ref[pl.ds(src + ROWS * j, ROWS), :].astype(jnp.bfloat16)

        @pl.when(kind == KIND_B)
        def _():
            tall = 8 * pl.cdiv(FC, 8)
            lane = lane_iota(tall)
            row = lax.broadcasted_iota(jnp.int32, (tall, LANES), 0)
            keep = (row < FC - 1) | (lane < FF % LANES)
            for r, (base, skew) in enumerate(wide_rows()):
                part = flat_ref[pl.ds(src + base, tall), :]
                if skew:
                    after = flat_ref[pl.ds(src + base + 1, tall), :]
                    part = pltpu.roll(jnp.where(lane >= skew, part, after), LANES - skew, 1)
                stage_ref[pl.ds(r, tall, stride=ROWS), :] = jnp.where(keep, part, 0.0)
            for c in range(FC):
                tile_ref[dst + c] = stage_ref[pl.ds(ROWS * c, ROWS), :].astype(jnp.bfloat16)

        return 0

    lax.fori_loop(0, entries, unit, 0)


def to_flat_kernel(entries, table_ref, tile_ref, line_ref, tail_ref, stage_ref, flat_ref):
    flat_ref[...] = jnp.zeros_like(flat_ref)

    def unit(i, _):
        kind, src, dst = (table_ref[3 * i + j] for j in range(3))

        @pl.when(kind == KIND_A)
        def _():
            for c in range(DC):
                flat_ref[pl.ds(src + c, ROWS, stride=DC), :] = tile_ref[dst + c]

        @pl.when(kind == KIND_D)
        def _():
            lane = lane_iota(ROWS)
            for c in range(DC):
                turned = pltpu.roll(tile_ref[dst + c], SKEW, 1)
                for step, keep in ((0, lane >= SKEW), (1, lane < SKEW)):
                    at = pl.ds(src + c + step, ROWS, stride=DC)
                    flat_ref[at, :] = jnp.where(keep, turned, flat_ref[at, :])

        for code, tiles in ((KIND_L2, 2), (KIND_L3, 3)):

            @pl.when(kind == code)
            def _():
                for j in range(tiles):
                    flat_ref[pl.ds(src + ROWS * j, ROWS), :] = tile_ref[dst + j]

        @pl.when(kind == KIND_B)
        def _():
            tall = 8 * pl.cdiv(FC, 8)
            lane = lane_iota(tall)
            row = lax.broadcasted_iota(jnp.int32, (tall, LANES), 0)
            for c in range(FC):
                stage_ref[pl.ds(ROWS * c, ROWS), :] = tile_ref[dst + c]
            for r, (base, skew) in enumerate(wide_rows()):
                turned = stage_ref[pl.ds(r, tall, stride=ROWS), :]
                if skew:
                    turned = pltpu.roll(turned, skew, 1)
                for step in range(2 if skew else 1):
                    entry = row * LANES + lane + (step * LANES - skew)
                    keep = (lane < skew if step else lane >= skew) & (entry < FF)
                    at = pl.ds(src + base + step, tall)
                    flat_ref[at, :] = jnp.where(keep, turned, flat_ref[at, :])

        return 0

    lax.fori_loop(0, entries, unit, 0)
    rows = line_ref.shape[1] // LANES
    line_from_rows(flat_ref, line_ref, 0, rows)
    line_from_rows(flat_ref, tail_ref, rows, HEAD)


def my_row(table):
    return lax.dynamic_index_in_dim(jnp.asarray(table), lax.axis_index("fsdp"), 0, keepdims=False)


def relayout_scratch(rows):
    return [
        pltpu.VMEM((ROWS * 8 * pl.cdiv(FC, 8), LANES), jnp.float32),
        pltpu.VMEM((8 * pl.cdiv(rows + HEAD + 8, 8), LANES), jnp.float32),
    ]


def to_tiles(line, plan):
    where, block, table, tails = plan
    count = lax.axis_size("fsdp")
    head = lax.ppermute(line[:, : HEAD * LANES], "fsdp", [(i, (i - 1) % count) for i in range(count)])
    vmem = pl.BlockSpec(memory_space=pltpu.VMEM)
    return pl.pallas_call(
        functools.partial(to_tiles_kernel, table.shape[1] // 3),
        out_shape=jax.ShapeDtypeStruct((block, ROWS, LANES), jnp.bfloat16),
        grid_spec=pltpu.PrefetchScalarGridSpec(
            num_scalar_prefetch=1, grid=(1,), in_specs=[vmem, vmem], out_specs=vmem,
            scratch_shapes=relayout_scratch(line.shape[1] // LANES),
        ),
        name="to_tiles",
    )(my_row(table), line, head)


def to_flat(tiles, plan, length):
    where, block, table, tails = plan
    count = lax.axis_size("fsdp")
    vmem = pl.BlockSpec(memory_space=pltpu.VMEM)
    line, tail = pl.pallas_call(
        functools.partial(to_flat_kernel, table.shape[1] // 3),
        out_shape=(jax.ShapeDtypeStruct((1, length), jnp.float32), jax.ShapeDtypeStruct((1, HEAD * LANES), jnp.float32)),
        grid_spec=pltpu.PrefetchScalarGridSpec(
            num_scalar_prefetch=1, grid=(1,), in_specs=[vmem], out_specs=[vmem, vmem],
            scratch_shapes=relayout_scratch(length // LANES),
        ),
        name="to_flat",
    )(my_row(table), tiles)
    tail = lax.ppermute(tail, "fsdp", [(i, (i + 1) % count) for i in range(count)])
    entry = lax.broadcasted_iota(jnp.int32, tail.shape, 1)
    first = jnp.where(entry < my_row(np.roll(tails, 1)), tail, line[:, : HEAD * LANES])
    return lax.dynamic_update_slice(line, first, (0, 0))


def place(me):
    return lax.rem(me, 2), lax.rem(me // 2, 2), lax.rem(me // 4, 2), me // 8


def index_of(core, x, y, z):
    return ((z * 2 + y) * 2 + x) * 2 + core


def greet(devices_and_conditions):
    barrier = pltpu.get_barrier_semaphore()
    for device, present in devices_and_conditions:
        if present is None:
            pl.semaphore_signal(barrier, inc=1, device_id=(device,), device_id_type=MESH)
        else:

            @pl.when(present)
            def _():
                pl.semaphore_signal(barrier, inc=1, device_id=(device,), device_id_type=MESH)

    present = [1 if p is None else p.astype(jnp.int32) for _, p in devices_and_conditions]
    pl.semaphore_wait(barrier, sum(present))


BF = jnp.bfloat16
F32 = jnp.float32
PAIR = 2 * LANES
SCALE = HEAD_DIM**-0.5
GELU_A = math.sqrt(2.0 / math.pi)
GELU_B = 0.044715
ANY = pl.BlockSpec(memory_space=pl.ANY)
VM = pl.BlockSpec(memory_space=pltpu.VMEM)
VMEM_LIMIT = 63 << 20


def nn(left, right):
    return lax.dot_general(left, right, (((1,), (0,)), ((), ())), preferred_element_type=F32)


def nt(left, right):
    return lax.dot_general(left, right, (((1,), (1,)), ((), ())), preferred_element_type=F32)


def runs_of(where, name):
    runs, done = [], 0
    for owner, at, tiles in where[name]:
        if runs and runs[-1][0] == owner and runs[-1][1] + runs[-1][2] == at:
            runs[-1][2] += tiles
        else:
            runs.append([owner, at, tiles, done])
        done += tiles
    return runs


def copies(where, name, blocks_ref, tiles_ref, sem, out=False):
    made = []
    flat_tiles = tiles_ref if len(tiles_ref.shape) == 3 else tiles_ref.reshape(-1, ROWS, LANES)
    for owner, at, tiles, done in runs_of(where, name):
        there, here = blocks_ref.at[owner, pl.ds(at, tiles)], flat_tiles.at[pl.ds(done, tiles)]
        made.append(pltpu.make_async_copy(here, there, sem) if out else pltpu.make_async_copy(there, here, sem))
    return made


def start(made):
    for copy in made:
        copy.start()


def wait(made):
    for copy in made:
        copy.wait()


def panel(tiles_ref, c, units, first=0):
    return tiles_ref[pl.ds(first, units), pl.ds(c, 1)].reshape(units * ROWS, LANES)


def panels(tiles_ref, c, many, units, first=0):
    return jnp.concatenate([panel(tiles_ref, c + i, units, first) for i in range(many)], axis=1)


def put_panel(tiles_ref, c, value, first=0):
    units = value.shape[0] // ROWS
    tiles_ref[pl.ds(first, units), pl.ds(c, 1)] = value.astype(BF).reshape(units, 1, ROWS, LANES)


def put_panels(tiles_ref, c, value, first=0):
    for i in range(value.shape[1] // LANES):
        put_panel(tiles_ref, c + i, value[:, i * LANES : (i + 1) * LANES], first)


def vector_rows(tiles_ref):
    return jnp.concatenate([tiles_ref[i].astype(F32) for i in range(tiles_ref.shape[0])], axis=0)


def as_row(rows, first, many):
    return jnp.concatenate([rows[first + i : first + i + 1] for i in range(many)], axis=1)


def put_vectors(tiles_ref, rows_list):
    parts = [row[:, i * LANES : (i + 1) * LANES] for row in rows_list for i in range(row.shape[1] // LANES)]
    missing = tiles_ref.shape[0] * ROWS - len(parts)
    whole = jnp.concatenate(parts + [jnp.zeros((missing, LANES), F32)] if missing else parts, axis=0)
    for i in range(tiles_ref.shape[0]):
        tiles_ref[i] = whole[i * ROWS : (i + 1) * ROWS].astype(BF)


def norm_rows(values):
    centre = values - jnp.mean(values, axis=-1, keepdims=True)
    inverse = lax.rsqrt(jnp.mean(centre * centre, axis=-1, keepdims=True) + EPS)
    return centre * inverse, inverse


def norm_rows_back(grad, normed, inverse, gain):
    scaled = grad * gain
    return inverse * (
        scaled - jnp.mean(scaled, axis=-1, keepdims=True) - normed * jnp.mean(scaled * normed, axis=-1, keepdims=True)
    )


def column_sums(values):
    return jnp.sum(values, axis=0, keepdims=True)


def head_window(h):
    block = jnp.minimum((h * HEAD_DIM) // LANES, DC - 2)
    lane = pl.multiple_of(block * LANES, LANES)
    return lane, h * HEAD_DIM - lane


def head_mask(rows, offset):
    lane = lax.broadcasted_iota(jnp.int32, (rows, PAIR), 1)
    return (lane >= offset) & (lane < offset + HEAD_DIM)


def front_kernel(
    where, x_ref, segq_ref, segk_ref, blocks_ref, q_ref, k_ref, v_ref, attended_ref, rest_ref, logs_ref,
    normed_ref, w_ref, vec1_ref, vec2_ref, bias_ref, score_ref, prob_ref, sem, vec_sem,
):
    window, rows = x_ref.shape[0], q_ref.shape[0]
    margin = (window - rows) // 2
    loads = [copies(where, name, blocks_ref, w_ref.at[i], sem.at[i]) for i, name in enumerate(("w_query", "w_key", "w_value"))]
    vecs = copies(where, "vec1", blocks_ref, vec1_ref, vec_sem) + copies(where, "vec2", blocks_ref, vec2_ref, vec_sem)
    start(vecs)
    for made in loads:
        start(made)
    wait(vecs)
    vec = vector_rows(vec1_ref)
    gain, shift = as_row(vec, 0, DC), as_row(vec, DC, DC)
    step = rows // 3

    @pl.loop(0, window // step)
    def _(i):
        at = pl.ds(i * step, step)
        normed, _ = norm_rows(x_ref[at].astype(F32))
        normed_ref[at] = (normed * gain + shift).astype(BF)

    @pl.loop(0, rows // 8)
    def _(i):
        at = pl.ds(i * 8, 8)
        bias_ref[at] = jnp.where(segq_ref[at] == segk_ref[...], 0.0, NEG)

    biases = vector_rows(vec2_ref)
    zero = jnp.zeros((1, D), F32)
    for made in loads:
        wait(made)
    for i, (out, add) in enumerate(((q_ref, as_row(biases, 0, DC)), (k_ref, zero), (v_ref, as_row(biases, DC, DC)))):
        for c in range(0, DC, 2):
            many = min(2, DC - c)
            lanes = slice(c * LANES, (c + many) * LANES)
            weights = panels(w_ref.at[i], c, many, D // ROWS)
            if i == 0:
                out[:, lanes] = (nn(normed_ref[pl.ds(margin, rows)], weights) + add[:, lanes]).astype(BF)
            else:

                @pl.loop(0, window // rows)
                def _(b):
                    at = pl.ds(b * rows, rows)
                    out[at, lanes] = (nn(normed_ref[at], weights) + add[:, lanes]).astype(BF)

    attended_ref[...] = jnp.zeros_like(attended_ref)
    rest_ref[...] = jnp.zeros_like(rest_ref)
    logs_ref[...] = jnp.zeros_like(logs_ref)
    lane_l = lax.broadcasted_iota(jnp.int32, logs_ref.shape, 1)

    @pl.loop(0, HEADS)
    def _(h):
        lane, offset = head_window(h)
        mask = head_mask(rows, offset)
        lanes = pl.ds(lane, PAIR)
        query = jnp.where(mask, q_ref[:, lanes], jnp.zeros((), BF))
        score_ref[...] = nt(query, k_ref[:, lanes]) * SCALE + bias_ref[...]
        top = jnp.max(score_ref[...], axis=-1, keepdims=True)
        powers = jnp.exp(score_ref[...] - top)
        total = jnp.sum(powers, axis=-1, keepdims=True)
        prob_ref[...] = powers.astype(BF)
        out = nn(prob_ref[...], v_ref[:, lanes]) / total
        rounded = out.astype(BF)
        attended_ref[:, lanes] = jnp.where(mask, rounded, attended_ref[:, lanes])
        rest_ref[:, lanes] = jnp.where(mask, (out - rounded.astype(F32)).astype(BF), rest_ref[:, lanes])
        logs_ref[...] = jnp.where(lane_l == h, top + jnp.log(total), logs_ref[...])


def front(x_win, seg_query, seg_keys, gathered, where, rows):
    window = x_win.shape[0]
    shape = lambda n, d=D, t=BF: jax.ShapeDtypeStruct((n, d), t)
    dma = pltpu.SemaphoreType.DMA
    units = D // ROWS
    return pl.pallas_call(
        functools.partial(front_kernel, where),
        out_shape=(shape(rows), shape(window), shape(window), shape(rows), shape(rows), shape(rows, LANES, F32)),
        in_specs=[VM, VM, VM, ANY],
        out_specs=[VM] * 6,
        scratch_shapes=[
            pltpu.VMEM((window, D), BF),
            pltpu.VMEM((3, units, DC, ROWS, LANES), BF), pltpu.VMEM((2, ROWS, LANES), BF), pltpu.VMEM((2, ROWS, LANES), BF),
            pltpu.VMEM((rows, window), F32), pltpu.VMEM((rows, window), F32), pltpu.VMEM((rows, window), BF), dma((3,)), dma,
        ],
        compiler_params=pltpu.CompilerParams(vmem_limit_bytes=VMEM_LIMIT),
        name="front",
    )(x_win, seg_query, seg_keys, gathered)


def middle_kernel(
    where, x_ref, cot_ref, attended_ref, rest_ref, blocks_ref, act_ref, mid_grad_ref, att_grad_ref, delta_ref, parts_ref,
    wo_ref, wu_ref, wd_ref, vec3_ref, vec4_ref, vec5_ref, b_up_ref, hidden_ref, slope_ref, pre_ref, normed_ref, normed_b_ref,
    mid_ref, g_up_ref, sem, out_sem,
):
    rows = x_ref.shape[0]
    units, f_units = D // ROWS, FF // ROWS
    names = ("w_out", "w_up", "w_down", "vec3", "vec4", "vec5")
    refs = (wo_ref, wu_ref, wd_ref, vec3_ref, vec4_ref, vec5_ref)
    loads = {n: copies(where, n, blocks_ref, r, sem.at[i]) for i, (n, r) in enumerate(zip(names, refs))}
    saves = {n: copies(where, n, parts_ref, r, out_sem, out=True) for n, r in zip(names, refs)}
    for n in ("vec3", "vec4", "vec5", "w_out", "w_up", "w_down"):
        start(loads[n])
    f_wide = FC * LANES
    pads = f_wide // ROWS - f_units
    wd_ref[pl.ds(f_units, pads)] = jnp.zeros((pads, DC, ROWS, LANES), BF)
    for n in ("vec3", "vec4", "vec5", "w_out"):
        wait(loads[n])
    vec = vector_rows(vec3_ref)
    b_out, gain, shift = (as_row(vec, i * DC, DC) for i in range(3))
    vec = vector_rows(vec4_ref)
    entry = lax.broadcasted_iota(jnp.int32, vec.shape, 0) * LANES + lax.broadcasted_iota(jnp.int32, vec.shape, 1)
    b_up_ref[...] = jnp.where(entry < FF, vec, 0.0)
    b_down = jnp.concatenate([vec5_ref[c].astype(F32)[0:1] for c in range(DC)], axis=1)

    for c in range(0, DC, 2):
        many = min(2, DC - c)
        lanes = slice(c * LANES, (c + many) * LANES)
        mid_ref[:, lanes] = (
            x_ref[:, lanes].astype(F32) + nn(attended_ref[...], panels(wo_ref, c, many, units)) + b_out[:, lanes]
        )
    normed, inverse = norm_rows(mid_ref[...])
    normed_ref[...] = normed
    normed_b_ref[...] = (normed * gain + shift).astype(BF)

    wait(loads["w_up"])

    @pl.loop(0, FC // 2)
    def _(p):
        at = pl.ds(pl.multiple_of(p * PAIR, PAIR), PAIR)
        bias = jnp.concatenate([b_up_ref[pl.ds(2 * p, 1)], b_up_ref[pl.ds(2 * p + 1, 1)]], axis=1)
        v = nn(normed_b_ref[...], panels(wu_ref, 2 * p, 2, units)) + bias
        square = v * v
        bent = jnp.tanh(GELU_A * v * (1.0 + GELU_B * square))
        hidden_ref[:, at] = (0.5 * v * (1.0 + bent)).astype(BF)
        slope_ref[:, at] = 0.5 * (1.0 + bent) + 0.5 * v * (1.0 - bent * bent) * (
            GELU_A * (1.0 + 3.0 * GELU_B * square)
        )

    wait(loads["w_down"])
    for c in range(0, DC, 2):
        many = min(2, DC - c)
        lanes = slice(c * LANES, (c + many) * LANES)
        act_ref[:, lanes] = (
            mid_ref[:, lanes] + nn(hidden_ref[...], panels(wd_ref, c, many, f_wide // ROWS)) + b_down[:, lanes]
        ).astype(BF)

    @pl.loop(0, FC // 2)
    def _(p):
        at = pl.ds(pl.multiple_of(p * PAIR, PAIR), PAIR)
        first = p * (PAIR // ROWS)
        grad = nt(cot_ref[...], panels(wd_ref, 0, DC, PAIR // ROWS, first)) * slope_ref[:, at]
        pre_ref[:, at] = grad.astype(BF)
        sums = column_sums(grad)
        g_up_ref[pl.ds(2 * p, 1)] = sums[:, :LANES]
        g_up_ref[pl.ds(2 * p + 1, 1)] = sums[:, LANES:]
        put_panels(wd_ref, 0, nn(hidden_ref[:, at].T, cot_ref[...]), first)

    start(saves["w_down"])
    put_vectors(vec4_ref, [b_up_row for b_up_row in [g_up_ref[i : i + 1] for i in range(FC)]])
    start(saves["vec4"])
    cot = cot_ref[...].astype(F32)
    sums = column_sums(cot)
    row0 = lax.broadcasted_iota(jnp.int32, (ROWS, LANES), 0) == 0
    for c in range(DC):
        vec5_ref[c] = jnp.where(row0, sums[:, c * LANES : (c + 1) * LANES], 0.0).astype(BF)
    start(saves["vec5"])

    for c in range(0, DC, 2):
        many = min(2, DC - c)
        weights = panels(wu_ref, 0, FC, many * LANES // ROWS, c * LANES // ROWS)
        mid_ref[:, c * LANES : (c + many) * LANES] = nt(pre_ref[...], weights)
    e = mid_ref[...]
    normed = normed_ref[...]
    g_gain, g_shift = column_sums(e * normed), column_sums(e)
    mid_grad = cot + norm_rows_back(e, normed, inverse, gain)
    mid_grad_ref[...] = mid_grad
    put_vectors(vec3_ref, [column_sums(mid_grad), g_gain, g_shift])
    start(saves["vec3"])
    mid_b = mid_grad.astype(BF)
    for c in range(0, DC, 2):
        many = min(2, DC - c)
        lanes = slice(c * LANES, (c + many) * LANES)
        weights = panels(wo_ref, 0, DC, many * LANES // ROWS, c * LANES // ROWS)
        att_grad_ref[:, lanes] = nt(mid_b, weights).astype(BF)
    product = att_grad_ref[...].astype(F32) * (attended_ref[...].astype(F32) + rest_ref[...].astype(F32))
    delta_ref[...] = jnp.sum(product.T.reshape(HEADS, HEAD_DIM, rows), axis=1)
    turned = attended_ref[...].T
    for c in range(0, DC, 2):
        many = min(2, DC - c)
        put_panels(wo_ref, c, nn(turned, mid_b[:, c * LANES : (c + many) * LANES]))
    start(saves["w_out"])
    turned_b = normed_b_ref[...].T

    @pl.loop(0, FC // 2)
    def _(p):
        at = pl.ds(pl.multiple_of(p * PAIR, PAIR), PAIR)
        put_panels(wu_ref, 2 * p, nn(turned_b, pre_ref[:, at]))

    start(saves["w_up"])
    for n in names:
        wait(saves[n])


def middle(block_input, cotangent, attended, rest, gathered, where):
    rows = block_input.shape[0]
    shape = lambda t: jax.ShapeDtypeStruct((rows, D), t)
    dma = pltpu.SemaphoreType.DMA
    tiles = lambda *n: pltpu.VMEM((*n, ROWS, LANES), BF)
    units, f_wide = D // ROWS, FC * LANES
    return pl.pallas_call(
        functools.partial(middle_kernel, where),
        out_shape=(shape(BF), shape(F32), shape(BF), jax.ShapeDtypeStruct((HEADS, rows), F32), jax.ShapeDtypeStruct(gathered.shape, BF)),
        in_specs=[VM, VM, VM, VM, ANY],
        out_specs=[VM, VM, VM, VM, ANY],
        scratch_shapes=[
            tiles(units, DC), tiles(units, FC), tiles(f_wide // ROWS, DC), tiles(2), tiles(3), tiles(DC),
            pltpu.VMEM((3 * ROWS, LANES), F32), pltpu.VMEM((rows, f_wide), BF), pltpu.VMEM((rows, f_wide), F32),
            pltpu.VMEM((rows, f_wide), BF), pltpu.VMEM((rows, D), F32), pltpu.VMEM((rows, D), BF), pltpu.VMEM((rows, D), F32),
            pltpu.VMEM((3 * ROWS, LANES), F32), dma((6,)), dma,
        ],
        compiler_params=pltpu.CompilerParams(vmem_limit_bytes=VMEM_LIMIT),
        name="middle",
    )(block_input, cotangent, attended, rest, gathered)


def back_kernel(
    where, x_hbm_ref, segq_ref, segk_ref, blocks_ref, q_ref, k_ref, v_ref, grad_ref, logs_ref, parts_in_ref,
    near_ref, own_ref, parts_ref,
    w_ref, vec1_ref, vec2_ref, bias_ref, score_ref, prob_ref, turned_ref, dk_ref, dv_ref, dq_ref, part_ref, logs_t_ref, x_ref,
    sem, vec_sem, out_sem, x_sem,
):
    window, rows = x_ref.shape[0], q_ref.shape[0]
    margin = (window - rows) // 2
    units = D // ROWS
    names = ("w_query", "w_key", "w_value")
    loads = [copies(where, name, blocks_ref, w_ref.at[i], sem.at[i]) for i, name in enumerate(names)]
    vecs = copies(where, "vec1", blocks_ref, vec1_ref, vec_sem)
    start(vecs)
    for made in loads:
        start(made)
    x_load = pltpu.make_async_copy(x_hbm_ref, x_ref, x_sem)
    x_load.start()

    @pl.loop(0, window // LANES)
    def _(i):
        at = pl.ds(pl.multiple_of(i * LANES, LANES), LANES)
        bias_ref[at] = jnp.where(segk_ref[at] == segq_ref[...], 0.0, NEG)
        turned_ref[:, at] = k_ref[at].T
        dk_ref[at] = jnp.zeros((LANES, D), F32)
        dv_ref[at] = jnp.zeros((LANES, D), F32)

    logs_t_ref[...] = logs_ref[...].T

    @pl.loop(0, HEADS)
    def _(h):
        lane, offset = head_window(h)
        mask = head_mask(rows, offset)
        lanes = pl.ds(lane, PAIR)
        query = jnp.where(mask, q_ref[:, lanes], jnp.zeros((), BF))
        grad = jnp.where(mask, grad_ref[:, lanes], jnp.zeros((), BF))
        probs = jnp.exp(nt(k_ref[:, lanes], query) * SCALE + bias_ref[...] - logs_t_ref[pl.ds(h, 1)])
        score_ref[...] = probs
        prob_ref[...] = probs.astype(BF)
        prob_grad = nt(v_ref[:, lanes], grad)
        row_total = jnp.sum(score_ref[...] * prob_grad, axis=0, keepdims=True)
        dv_ref[:, lanes] += nn(prob_ref[...], grad)
        prob_ref[...] = (score_ref[...] * (prob_grad - row_total)).astype(BF)
        dk_ref[:, lanes] += nn(prob_ref[...], query)
        part_ref[...] = nn(turned_ref[lanes], prob_ref[...])
        at = pl.ds(pl.multiple_of(h * HEAD_DIM, 8), HEAD_DIM)
        dq_ref[at] = part_ref[pl.ds(pl.multiple_of(offset, 8), HEAD_DIM)]

    dq = dq_ref[...].T * SCALE
    g_query = column_sums(dq)
    dq_b = dq.astype(BF)
    wait(vecs)
    vec = vector_rows(vec1_ref)
    gain, shift = as_row(vec, 0, DC), as_row(vec, DC, DC)
    dk_b_ref, dv_b_ref = k_ref, v_ref
    x_load.wait()
    g_value = jnp.zeros((1, D), F32)
    step = rows // 3

    def rounded(i, total):
        at = pl.ds(pl.multiple_of(i * step, step), step)
        dk_b_ref[at] = (dk_ref[at] * SCALE).astype(BF)
        dv = dv_ref[at]
        dv_b_ref[at] = dv.astype(BF)
        normed, _ = norm_rows(x_ref[at].astype(F32))
        turned_ref[:, at] = (normed * gain + shift).astype(BF).T
        return total + column_sums(dv)

    g_value = lax.fori_loop(0, window // step, rounded, g_value)
    put_vectors(vec2_ref, [g_query, g_value])
    save = copies(where, "vec2", parts_ref, vec2_ref, out_sem, out=True)
    for made in loads:
        wait(made)
    for c in range(0, DC, 2):
        many = min(2, DC - c)
        lanes = slice(c * LANES, (c + many) * LANES)
        part = [panels(w_ref.at[i], 0, DC, many * LANES // ROWS, c * LANES // ROWS) for i in range(3)]

        @pl.loop(0, window // rows)
        def _(b):
            at = pl.ds(b * rows, rows)
            dk_ref[at, lanes] = nt(dk_b_ref[at], part[1]) + nt(dv_b_ref[at], part[2])

        dk_ref[pl.ds(margin, rows), lanes] += nt(dq_b, part[0])
    turned_own = turned_ref[:, pl.ds(margin, rows)]
    for c in range(0, DC, 2):
        many = min(2, DC - c)
        lanes = slice(c * LANES, (c + many) * LANES)
        put_panels(w_ref.at[0], c, nn(turned_own, dq_b[:, lanes]))
        put_panels(w_ref.at[1], c, nn(turned_ref[...], dk_b_ref[:, lanes]))
        put_panels(w_ref.at[2], c, nn(turned_ref[...], dv_b_ref[:, lanes]))
    for i, name in enumerate(names):
        save = save + copies(where, name, parts_ref, w_ref.at[i], out_sem, out=True)
    start(save)

    def norm_block(i, totals):
        at = pl.ds(pl.multiple_of(i * step, step), step)
        normed, inverse = norm_rows(x_ref[at].astype(F32))
        e = dk_ref[at]
        part = norm_rows_back(e, normed, inverse, gain)
        x_ref[at] = part.astype(BF)

        @pl.when((i >= margin // step) & (i < (margin + rows) // step))
        def _():
            own_ref[pl.ds(pl.multiple_of(i * step - margin, step), step)] = part

        return totals[0] + column_sums(e * normed), totals[1] + column_sums(e)

    zero = jnp.zeros((1, D), F32)
    g_gain, g_shift = lax.fori_loop(0, window // step, norm_block, (zero, zero))
    put_vectors(vec1_ref, [g_gain, g_shift])
    last = copies(where, "vec1", parts_ref, vec1_ref, out_sem, out=True)
    last = last + [pltpu.make_async_copy(x_ref, near_ref, x_sem)]
    start(last)
    wait(save + last)


def back(x_win, seg_query, seg_keys, gathered, queries, key_win, value_win, att_grad, logs, parts, where):
    window, rows = x_win.shape[0], queries.shape[0]
    dma = pltpu.SemaphoreType.DMA
    tiles = lambda *n: pltpu.VMEM((*n, ROWS, LANES), BF)
    vm = lambda a, b, t: pltpu.VMEM((a, b), t)
    return pl.pallas_call(
        functools.partial(back_kernel, where),
        out_shape=(
            jax.ShapeDtypeStruct((window, D), BF), jax.ShapeDtypeStruct((rows, D), F32), jax.ShapeDtypeStruct(parts.shape, BF),
        ),
        in_specs=[ANY, VM, VM, ANY, VM, VM, VM, VM, VM, ANY],
        out_specs=[ANY, VM, ANY],
        scratch_shapes=[
            tiles(3, D // ROWS, DC), tiles(2), tiles(2), vm(window, rows, F32), vm(window, rows, F32), vm(window, rows, BF),
            vm(D, window, BF), vm(window, D, F32), vm(window, D, F32), vm(D, rows, F32), vm(PAIR, rows, F32), vm(LANES, rows, F32),
            vm(window, D, BF), dma((3,)), dma, dma, dma,
        ],
        input_output_aliases={9: 2},
        compiler_params=pltpu.CompilerParams(vmem_limit_bytes=VMEM_LIMIT),
        name="back",
    )(x_win, seg_query, seg_keys, gathered, queries, key_win, value_win, att_grad, logs, parts)


HOT_NAMES = ("vec1", "w_query", "w_key", "w_value", "vec2")


def transfer_pieces(plan, depth):
    where = plan[0]
    count = plan[2].shape[0]
    hot, used = [0] * depth, [0] * depth
    for name in where:
        for owner, at, tiles in where[name]:
            level = owner * depth // count
            used[level] = max(used[level], at + tiles)
            if name in HOT_NAMES:
                hot[level] = max(hot[level], at + tiles)
    early = [(level, 0, h) for level, h in enumerate(hot) if h]
    late = [(level, h, u - h) for level, (h, u) in enumerate(zip(hot, used)) if h < u]
    return early, late


def cut(piece, many):
    level, first, tiles = piece
    half = tiles // 2
    edges = [half * i // (many // 2) for i in range(many // 2)] + [
        half + (tiles - half) * i // (many // 2) for i in range(many // 2 + 1)
    ]
    return [(level, first + a, b - a) for a, b in zip(edges[:-1], edges[1:])]


def gather_front_kernel(
    depth, where, early, late,
    block_ref, x_in_ref, segq_ref, segk_ref,
    out_ref, x_out_ref, x_got_ref, q_ref, k_ref, v_ref, attended_ref, rest_ref, logs_ref,
    z_send, z_recv, x_send, x_recv, y_send, y_recv, corner_send, corner_recv, mate_send, mate_recv, w_send, w_recv,
    local_sem, stage_ref, x_ref, normed_ref, w_ref, vec1_ref, vec2_ref, bias_ref, score_ref, prob_ref, sem, vec_sem,
):
    me = lax.axis_index("fsdp")
    count = 8 * depth
    core, x, y, z = place(me)
    mate, x_near, y_near = index_of(1 - core, x, y, z), index_of(core, 1 - x, y, z), index_of(core, x, 1 - y, z)
    up, down = me + 8, me - 8
    after, before = me + 2, me - 2
    has_after, has_before = after < count, before >= 0
    greet(
        [(mate, None), (x_near, None), (y_near, None), (down, z > 0), (up, z < depth - 1), (after, has_after), (before, has_before)]
    )
    pieces = early + late
    chunks = {p: cut(piece, 4) if piece[0] == 0 and p < len(early) else [piece] for p, piece in enumerate(pieces)}
    chunk_list = [(p, chunk) for p in chunks for chunk in chunks[p]]
    ids = {p: [i for i, (q, _) in enumerate(chunk_list) if q == p] for p in chunks}
    hot, cold = range(len(early)), range(len(early), len(pieces))

    def remote(source, target, send, recv, device):
        return pltpu.make_async_remote_copy(
            src_ref=source, dst_ref=target, send_sem=send, recv_sem=recv, device_id=(device,), device_id_type=MESH
        )

    def span(piece):
        return pl.ds(piece[1], piece[2])

    def halves(p):
        level, first, tiles = pieces[p]
        return (level, first, tiles // 2), (level, first + tiles // 2, tiles - tiles // 2)

    def column(level):
        return index_of(core, x, y, level)

    def from_x(level):
        return index_of(core, 1 - x, y, level)

    def from_y(level):
        return index_of(core, x, 1 - y, level)

    def across(level):
        return index_of(core, 1 - x, 1 - y, level)

    def pass_on(block, piece, send, recv, device, own=False):
        there = out_ref.at[block, span(piece)]
        return remote(block_ref.at[span(piece)] if own else there, there, send, recv, device)

    def z_copy(i, upward, own=False):
        piece = chunk_list[i][1]
        return pass_on(column(piece[0]), piece, z_send.at[i, 0 if upward else 1], z_recv.at[i], up if upward else down, own)

    def plane_copies(i, own=False):
        piece = chunk_list[i][1]
        block = column(piece[0])
        return (
            pass_on(block, piece, x_send.at[i], x_recv.at[i], x_near, own),
            pass_on(block, piece, y_send.at[i], y_recv.at[i], y_near, own),
            pass_on(block, piece, mate_send.at[0, i], mate_recv.at[0, i], mate, own),
        )

    def got(block, i, recv):
        piece = chunk_list[i][1]
        pass_on(block, piece, x_send.at[i], recv, me).wait_recv()

    def spread(i, own=False):
        for copy in plane_copies(i, own):
            copy.start()

    def take(i):
        def run(zv):
            level = chunk_list[i][1][0]
            got(column(level), i, z_recv.at[i])
            if level < zv < depth - 1:
                z_copy(i, True).start()
            if 0 < zv < level:
                z_copy(i, False).start()
            spread(i)

        return run

    def corner_copies(p):
        level = pieces[p][0]
        first, second = halves(p)
        return (
            pass_on(from_x(level), first, corner_send.at[p, 0], corner_recv.at[p, 0], y_near),
            pass_on(from_y(level), second, corner_send.at[p, 1], corner_recv.at[p, 1], x_near),
        )

    def mate_copies(p):
        level = pieces[p][0]
        first, second = halves(p)
        return (
            pass_on(from_x(level), pieces[p], mate_send.at[1, p], mate_recv.at[1, p], mate),
            pass_on(from_y(level), pieces[p], mate_send.at[2, p], mate_recv.at[2, p], mate),
            pass_on(across(level), first, mate_send.at[3, p], mate_recv.at[3, p], mate),
            pass_on(across(level), second, mate_send.at[4, p], mate_recv.at[4, p], mate),
        )

    def beside(p):
        def run(zv):
            level = pieces[p][0]
            for i in ids[p]:
                got(from_x(level), i, x_recv.at[i])
            corner_copies(p)[0].start()
            mate_copies(p)[0].start()
            for i in ids[p]:
                got(from_y(level), i, y_recv.at[i])
            corner_copies(p)[1].start()
            mate_copies(p)[1].start()

        return run

    def corner(p):
        def run(zv):
            level = pieces[p][0]
            for side, half in enumerate(halves(p)):
                pass_on(across(level), half, corner_send.at[p, side], corner_recv.at[p, side], me).wait_recv()
                mate_copies(p)[2 + side].start()

        return run

    def from_mate(p):
        def run(zv):
            level = pieces[p][0]
            other = 1 - 2 * core
            for i in ids[p]:
                pass_on(column(level) + other, chunk_list[i][1], mate_send.at[0, i], mate_recv.at[0, i], me).wait_recv()
            first, second = halves(p)
            for slot, (block, piece) in enumerate(
                ((from_x(level), pieces[p]), (from_y(level), pieces[p]), (across(level), first), (across(level), second))
            ):
                pass_on(block + other, piece, mate_send.at[slot + 1, p], mate_recv.at[slot + 1, p], me).wait_recv()

        return run

    def own_spread(i):
        return lambda zv: spread(i, True)

    def own_up(i):
        return lambda zv: z_copy(i, True, True).start() if zv < depth - 1 else None

    def own_down(i):
        return lambda zv: z_copy(i, False, True).start() if zv > 0 else None

    def w_copy(slot, which, device, source=None):
        return remote(x_in_ref if source is None else source, x_got_ref.at[slot], w_send.at[which], w_recv.at[slot], device)

    def w_start():
        w_copy(1 + 2 * core, 0, mate).start()

        @pl.when(has_after)
        def _():
            w_copy(0, 1, after).start()

        @pl.when(has_before)
        def _():
            w_copy(4, 2, before).start()

    def w_forward(core_index):
        slot = 0 if core_index else 4
        return w_copy(1 if core_index else 3, 3, mate, x_got_ref.at[slot])

    def w_wait(slot):
        w_copy(slot, 0, me).wait_recv()

    def w_middle(zv):
        @pl.when(has_before)
        def _():
            w_wait(0)

        @pl.when(has_after)
        def _():
            w_wait(4)

        @pl.when((core == 1) & has_before)
        def _():
            w_forward(1).start()

        @pl.when((core == 0) & has_after)
        def _():
            w_forward(0).start()

    first_cold = {0: 0, 1: 0, 2: 1, 3: 2}
    levels = [pieces[p][0] for p in cold]

    def lists(zv):
        own_hot = [p for p in hot if pieces[p][0] == zv]
        own_cold = [p for p in cold if pieces[p][0] == zv]
        far_hot = sorted((p for p in hot if pieces[p][0] != zv), key=lambda p: abs(pieces[p][0] - zv))
        far_cold = sorted((p for p in cold if pieces[p][0] != zv), key=lambda p: (abs(pieces[p][0] - zv), -pieces[p][0]))
        start = []
        for p in own_hot:
            for i in ids[p]:
                start += [own_up(i), own_down(i), own_spread(i)]
        for p in own_cold:
            start += [own_down(i) for i in ids[p]]
        for p in far_hot:
            start += [take(i) for i in ids[p]]
        for p in own_cold:
            start += [own_up(i) for i in ids[p]]
        start.append(w_middle)
        order_hot = own_hot + far_hot
        start += [beside(p) for p in order_hot]
        for p in own_cold:
            start += [own_spread(i) for i in ids[p]]
        near = [p for p in far_cold if abs(pieces[p][0] - zv) == 1]
        rest = [p for p in far_cold if p not in near]
        for p in near:
            start += [take(i) for i in ids[p]]
        start += [corner(p) for p in order_hot]
        start += [from_mate(p) for p in order_hot]
        return start, [[take(i) for p in rest for i in ids[p]], own_cold + near + rest]

    plans = [lists(zv) for zv in range(depth)]

    def each_plane(events_of):
        for zv in range(depth):
            events = events_of(zv)
            if events:

                @pl.when(z == zv)
                def _():
                    for event in events:
                        event(zv)

    w_start()
    fill = pltpu.make_async_copy(block_ref, stage_ref, local_sem)
    fill.start()
    fill.wait()
    keep = pltpu.make_async_copy(stage_ref, out_ref.at[me], local_sem)
    keep.start()
    each_plane(lambda zv: plans[zv][0])
    keep.wait()

    def cold_step(k, step):
        return lambda zv: [step(plans[zv][1][1][k])] if k < len(plans[zv][1][1]) else []

    services = {
        "takes": lambda zv: plans[zv][1][0],
        **{("beside", k): cold_step(k, beside) for k in range(len(cold))},
        **{("corner", k): cold_step(k, corner) for k in range(len(cold))},
    }

    def service(name):
        each_plane(services[name])

    rows = q_ref.shape[0]
    window = k_ref.shape[0]
    margin = (window - rows) // 2
    w_wait(3 - 2 * core)

    @pl.when((core == 0) & has_before)
    def _():
        w_wait(1)

    @pl.when((core == 1) & has_after)
    def _():
        w_wait(3)

    near_sem = vec_sem
    present = (before >= 0, (core == 1) | has_before, None, (core == 0) | has_after, after < count)
    for slot, there in enumerate(present):
        at = x_ref.at[pl.ds(slot * rows, rows)]
        if there is None:
            pltpu.make_async_copy(x_in_ref, at, near_sem).start()
            continue

        @pl.when(there)
        def _():
            pltpu.make_async_copy(x_got_ref.at[slot], at, near_sem).start()

        @pl.when(jnp.logical_not(there))
        def _():
            pltpu.make_async_copy(x_in_ref, at, near_sem).start()

    for slot in range(5):
        pltpu.make_async_copy(x_in_ref, x_ref.at[pl.ds(slot * rows, rows)], near_sem).wait()
    x_save = pltpu.make_async_copy(x_ref, x_out_ref, local_sem)
    x_save.start()
    loads = [copies(where, name, out_ref, w_ref.at[i], sem.at[i]) for i, name in enumerate(("w_query", "w_key", "w_value"))]
    vecs = copies(where, "vec1", out_ref, vec1_ref, vec_sem) + copies(where, "vec2", out_ref, vec2_ref, vec_sem)
    start(vecs)
    for made in loads:
        start(made)
    wait(vecs)
    vec = vector_rows(vec1_ref)
    gain, shift = as_row(vec, 0, DC), as_row(vec, DC, DC)
    step = rows // 3

    @pl.loop(0, window // step)
    def _(i):
        at = pl.ds(i * step, step)
        normed, _ = norm_rows(x_ref[at].astype(F32))
        normed_ref[at] = (normed * gain + shift).astype(BF)

    @pl.loop(0, rows // 8)
    def _(i):
        at = pl.ds(i * 8, 8)
        bias_ref[at] = jnp.where(segq_ref[at] == segk_ref[...], 0.0, NEG)

    biases = vector_rows(vec2_ref)
    zero = jnp.zeros((1, D), F32)
    for made in loads:
        wait(made)
    for i, (out, add) in enumerate(((q_ref, as_row(biases, 0, DC)), (k_ref, zero), (v_ref, as_row(biases, DC, DC)))):
        for c in range(0, DC, 2):
            many = min(2, DC - c)
            lanes = slice(c * LANES, (c + many) * LANES)
            weights = panels(w_ref.at[i], c, many, D // ROWS)
            if i == 0:
                out[:, lanes] = (nn(normed_ref[pl.ds(margin, rows)], weights) + add[:, lanes]).astype(BF)
            else:

                @pl.loop(0, window // rows)
                def _(b):
                    at = pl.ds(b * rows, rows)
                    out[at, lanes] = (nn(normed_ref[at], weights) + add[:, lanes]).astype(BF)

        if i == 1:
            service("takes")
    attended_ref[...] = jnp.zeros_like(attended_ref)
    rest_ref[...] = jnp.zeros_like(rest_ref)
    logs_ref[...] = jnp.zeros_like(logs_ref)
    lane_l = lax.broadcasted_iota(jnp.int32, logs_ref.shape, 1)
    when = {("beside", k): (0, 4, 10)[min(k, 2)] for k in range(len(cold))}
    when |= {("corner", k): (12, 15, 16)[min(k, 2)] for k in range(len(cold))}

    @pl.loop(0, HEADS)
    def _(h):
        for name, at_head in when.items():
            if at_head < HEADS:

                @pl.when(h == at_head)
                def _():
                    service(name)

        lane, offset = head_window(h)
        mask = head_mask(rows, offset)
        lanes = pl.ds(lane, PAIR)
        query = jnp.where(mask, q_ref[:, lanes], jnp.zeros((), BF))
        score_ref[...] = nt(query, k_ref[:, lanes]) * SCALE + bias_ref[...]
        top = jnp.max(score_ref[...], axis=-1, keepdims=True)
        powers = jnp.exp(score_ref[...] - top)
        total = jnp.sum(powers, axis=-1, keepdims=True)
        prob_ref[...] = powers.astype(BF)
        out = nn(prob_ref[...], v_ref[:, lanes]) / total
        rounded = out.astype(BF)
        attended_ref[:, lanes] = jnp.where(mask, rounded, attended_ref[:, lanes])
        rest_ref[:, lanes] = jnp.where(mask, (out - rounded.astype(F32)).astype(BF), rest_ref[:, lanes])
        logs_ref[...] = jnp.where(lane_l == h, top + jnp.log(total), logs_ref[...])

    for name, at_head in when.items():
        if at_head >= HEADS:
            service(name)
    each_plane(lambda zv: [from_mate(p) for p in plans[zv][1][1]])

    def sent(zv):
        for i, (p, piece) in enumerate(chunk_list):
            for copy in plane_copies(i):
                copy.wait_send()
            level = piece[0]
            if zv < depth - 1 and level <= zv:
                z_copy(i, True).wait_send()
            if zv > 0 and level >= zv:
                z_copy(i, False).wait_send()
        for p in range(len(pieces)):
            for copy in corner_copies(p) + mate_copies(p):
                copy.wait_send()

    each_plane(lambda zv: [sent])
    w_copy(0, 0, mate).wait_send()

    @pl.when(has_after)
    def _():
        w_copy(0, 1, after).wait_send()

    @pl.when(has_before)
    def _():
        w_copy(4, 2, before).wait_send()

    @pl.when(jnp.where(core == 1, has_before, has_after))
    def _():
        w_forward(0).wait_send()

    x_save.wait()


def gather_front(block, block_input, seg_query, seg_keys, plan):
    where = plan[0]
    count = lax.axis_size("fsdp")
    depth = count // 8
    rows, window = block_input.shape[0], seg_keys.shape[1]
    early, late = transfer_pieces(plan, depth)
    shape = lambda n, d=D, t=BF: jax.ShapeDtypeStruct((n, d), t)
    dma = pltpu.SemaphoreType.DMA
    units = D // ROWS
    many = len(early) + len(late)
    chunks = many + 3 * sum(1 for piece in early if piece[0] == 0)
    got = jax.ShapeDtypeStruct((5, rows, D), BF)
    return pl.pallas_call(
        functools.partial(gather_front_kernel, depth, where, early, late),
        out_shape=(
            jax.ShapeDtypeStruct((count, *block.shape), BF), shape(window), got,
            shape(rows), shape(window), shape(window), shape(rows), shape(rows), shape(rows, LANES, F32),
        ),
        in_specs=[ANY, ANY, VM, VM],
        out_specs=[ANY] * 3 + [VM] * 6,
        scratch_shapes=[
            dma((chunks, 2)), dma((chunks,)), dma((chunks,)), dma((chunks,)), dma((chunks,)), dma((chunks,)),
            dma((many, 2)), dma((many, 2)), dma((5, chunks)), dma((5, chunks)), dma((4,)), dma((5,)),
            dma, pltpu.VMEM(block.shape, BF), pltpu.VMEM((window, D), BF), pltpu.VMEM((window, D), BF),
            pltpu.VMEM((3, units, DC, ROWS, LANES), BF), pltpu.VMEM((2, ROWS, LANES), BF), pltpu.VMEM((2, ROWS, LANES), BF),
            pltpu.VMEM((rows, window), F32), pltpu.VMEM((rows, window), F32), pltpu.VMEM((rows, window), BF), dma((3,)), dma,
        ],
        compiler_params=pltpu.CompilerParams(collective_id=0, has_side_effects=True, vmem_limit_bytes=VMEM_LIMIT),
        name="gather_front",
    )(block, block_input, seg_query, seg_keys)


def back_scatter_kernel(
    depth, where, early, late,
    x_hbm_ref, segq_ref, segk_ref, blocks_ref, q_ref, k_hbm_ref, v_hbm_ref, grad_ref, logs_ref, delta_ref, mid_hbm_ref, parts_in_ref,
    parts_ref, out_ref, in_grad_ref, mates, sums, halfs, fulls, lines, near_ref, near_got,
    w_ref, g_ref, vec1_ref, vec2_ref, score_ref, prob_ref, turned_ref, k_ref, v_ref, dq_ref, part_ref, logs_t_ref, x_ref,
    block_ref, mid_ref, g_value_ref, gain_acc, shift_acc, stage, total,
    mate_send, mate_recv, half_send, half_recv, full_send, full_recv, line_send, line_recv, near_send, near_recv,
    load_sem, store_sem, sem, vec_sem, out_sem, x_sem,
):
    me = lax.axis_index("fsdp")
    count = 8 * depth
    core, x, y, z = place(me)
    mate, x_near, y_near = index_of(1 - core, x, y, z), index_of(core, 1 - x, y, z), index_of(core, x, 1 - y, z)
    after, before = me + 2, me - 2
    has_after, has_before = after < count, before >= 0
    greet(
        [(mate, None), (x_near, None), (y_near, None), (me - 8, z > 0), (me + 8, z < depth - 1), (after, has_after), (before, has_before)]
    )
    pieces = early + late
    early_ids, late_ids = range(len(early)), range(len(early), len(pieces))

    def remote(source, target, send, recv, device):
        return pltpu.make_async_remote_copy(
            src_ref=source, dst_ref=target, send_sem=send, recv_sem=recv, device_id=(device,), device_id_type=MESH
        )

    def owner(level, slot, which_core):
        return index_of(which_core, 1 - x if slot in (1, 3) else x, 1 - y if slot in (2, 3) else y, level)

    def at_plane(zv, run):
        @pl.when(z == zv)
        def _():
            run()

    def span(p, lo=0, many=None):
        _, first, tiles = pieces[p]
        return pl.ds(first + lo, tiles if many is None else many)

    def half_of(p):
        return pieces[p][2] // 2

    def to_mate(p, slot):
        level = pieces[p][0]
        return remote(
            parts_ref.at[owner(level, slot, 1 - core), span(p)], mates.at[level, slot, span(p)],
            mate_send.at[p, slot], mate_recv.at[p, slot], mate,
        )

    def half_out(p, side):
        level, _, tiles = pieces[p]
        part = span(p, half_of(p), tiles - half_of(p)) if side else span(p, 0, half_of(p))
        return remote(
            sums.at[level, 3, part], halfs.at[level, side, part], half_send.at[p, side], half_recv.at[p, side],
            x_near if side else y_near,
        )

    def full_out(p, side):
        level = pieces[p][0]
        return remote(
            sums.at[level, 1 + side, span(p)], fulls.at[level, side, span(p)], full_send.at[p, side], full_recv.at[p, side],
            y_near if side else x_near,
        )

    def line_out(p, zv):
        level = pieces[p][0]
        upward = level > zv
        slot = depth if not upward and level == zv - 1 else level
        side = 1 if slot == depth else 0
        return remote(
            sums.at[level, 0, span(p)], lines.at[slot, span(p)], line_send.at[p], line_recv.at[p, side],
            me + 8 if upward else me - 8,
        )

    def line_in(p, side):
        level = pieces[p][0]
        slot = depth if side else level
        return remote(sums.at[level, 0, span(p)], lines.at[slot, span(p)], line_send.at[p], line_recv.at[p, side], me)

    def line_sides(p, zv):
        level = pieces[p][0]
        if level > zv:
            return [0] if zv > 0 else []
        if level < zv:
            return [0] if zv < depth - 1 else []
        return ([0] if zv > 0 else []) + ([1] if zv < depth - 1 else [])

    def sources(kind, p, zv):
        level, _, tiles = pieces[p]
        h = half_of(p)
        found = [(parts_ref.at[owner(level, kind, core), span(p)], 0, tiles), (mates.at[level, kind, span(p)], 0, tiles)]
        if kind == 1:
            found.append((halfs.at[level, 0, span(p, 0, h)], 0, h))
        if kind == 2:
            found.append((halfs.at[level, 1, span(p, h, tiles - h)], h, tiles - h))
        if kind == 0:
            found += [(fulls.at[level, side, span(p)], 0, tiles) for side in (0, 1)]
            found += [(lines.at[depth if side else level, span(p)], 0, tiles) for side in line_sides(p, zv)]
        return found

    def loads(kind, p, zv, base):
        return [
            pltpu.make_async_copy(ref, stage.at[i, pl.ds(base + lo, many)], load_sem.at[1 if base else 0])
            for i, (ref, lo, many) in enumerate(sources(kind, p, zv))
        ]

    def store(kind, p, base):
        level, _, tiles = pieces[p]
        return pltpu.make_async_copy(
            total.at[pl.ds(base, tiles)], sums.at[level, kind, span(p)], store_sem.at[1 if base else 0]
        )

    def load(kind, p, zv, base=0):
        to_mate(p, kind).wait_recv()
        if kind in (1, 2):
            half_out(p, kind - 1).wait_recv()
        if kind == 0:
            for side in (0, 1):
                full_out(p, side).wait_recv()
            for side in line_sides(p, zv):
                line_in(p, side).wait_recv()
        start(loads(kind, p, zv, base))

    def add(base, lo, many, slots, target, shift):
        def some(first, tiles):
            value = stage[slots[0], pl.ds(first, tiles)].astype(F32)
            for slot in slots[1:]:
                value = value + stage[slot, pl.ds(first, tiles)].astype(F32)
            target[pl.ds(first + shift, tiles)] = value.astype(target.dtype)

        group = 8

        @pl.loop(0, many // group)
        def _(i):
            some(base + lo + i * group, group)

        if many % group:
            some(base + lo + many // group * group, many % group)

    def finish(kind, p, zv, base=0):
        level, first, tiles = pieces[p]
        found = sources(kind, p, zv)
        wait(loads(kind, p, zv, base))
        final = kind == 0 and level == zv
        target, shift = (out_ref, first - base) if final else (total, 0)
        edges = sorted({e for _, lo, many in found for e in (lo, lo + many)})
        for lo, hi in zip(edges[:-1], edges[1:]):
            slots = [i for i, (_, a, many) in enumerate(found) if a <= lo and hi <= a + many]
            add(base, lo, hi - lo, slots, target, shift)
        if not final:
            store(kind, p, base).start()

    def send(kind, p, zv, base=0):
        if kind == 0 and pieces[p][0] == zv:
            return
        store(kind, p, base).wait()
        if kind == 3:
            half_out(p, 0).start()
            half_out(p, 1).start()
        elif kind == 0:
            line_out(p, zv).start()
        else:
            full_out(p, kind - 1).start()

    def run(jobs, zv, ahead=False):
        bases = [(k % 2) * (stage.shape[1] // 2) if ahead else 0 for k in range(len(jobs))]
        for k, (kind, p) in enumerate(jobs):
            if k == 0 or not ahead:
                load(kind, p, zv, bases[k])
            if ahead and k + 1 < len(jobs):
                load(*jobs[k + 1], zv, bases[k + 1])
            finish(kind, p, zv, bases[k])
            send(kind, p, zv, bases[k])

    for p in early_ids:
        for slot in (3, 1, 2, 0):
            to_mate(p, slot).start()

    window, rows = k_ref.shape[0], q_ref.shape[0]
    margin = (window - rows) // 2
    names = ("w_query", "w_key", "w_value")
    k_load = [pltpu.make_async_copy(k_hbm_ref, k_ref, vec_sem), pltpu.make_async_copy(v_hbm_ref, v_ref, vec_sem)]
    start(k_load)
    weight_loads = [copies(where, name, blocks_ref, w_ref.at[i], sem.at[i]) for i, name in enumerate(names)]
    vecs = copies(where, "vec1", blocks_ref, vec1_ref, sem.at[3])
    start(vecs)
    for made in weight_loads:
        start(made)
    x_load = [pltpu.make_async_copy(x_hbm_ref, x_ref, x_sem)]
    start(x_load)
    wait(k_load)

    @pl.loop(0, window // LANES)
    def _(i):
        at = pl.ds(pl.multiple_of(i * LANES, LANES), LANES)
        turned_ref[:, at] = k_ref[at].T

    logs_t_ref[...] = logs_ref[...].T
    g_value_ref[...] = jnp.zeros_like(g_value_ref)

    by_level = {pieces[p][0]: p for p in early_ids}
    a, b, c_ = (by_level[level] for level in sorted(by_level, reverse=True)[:3])
    table = [
        (-1, 0, 3, a, None), (0, 1, 3, b, None), (3, 4, 1, a, None), (4, 5, 2, a, None), (5, 6, 3, c_, None),
        (6, 7, 1, b, None), (7, 8, 2, b, None), (11, 12, 0, a, 0), (12, 13, 1, c_, None), (13, 14, 2, c_, None),
    ]

    def beside(h, which, action):
        for entry in table:
            if entry[which] < 0:
                continue
            kind, p, zv = entry[2:]
            there = h == entry[which]
            if zv is not None:
                there = there & (z == zv)

            @pl.when(there)
            def _():
                action(kind, p, zv)

    load(3, a, None)

    @pl.loop(0, HEADS)
    def _(h):
        beside(h, 1, finish)
        lane, offset = head_window(h)
        mask = head_mask(rows, offset)
        lanes = pl.ds(lane, PAIR)
        query = jnp.where(mask, q_ref[:, lanes], jnp.zeros((), BF))
        grad = jnp.where(mask, grad_ref[:, lanes], jnp.zeros((), BF))
        log_row, delta_row = logs_t_ref[pl.ds(h, 1)], delta_ref[pl.ds(h, 1)]
        blocks = [pl.ds(n * rows, rows) for n in range(window // rows)]
        for keys in blocks:
            together = jnp.concatenate([segk_ref[keys]] * (rows // LANES), axis=1) == segq_ref[...]
            probs = jnp.exp(jnp.where(together, nt(k_ref[keys, lanes], query) * SCALE - log_row, NEG))
            prob_ref[keys] = probs.astype(BF)
            score_ref[keys] = (probs * (nt(v_ref[keys, lanes], grad) - delta_row)).astype(BF)
        beside(h, 1, send)
        beside(h, 0, load)
        side = head_mask(rows, offset)
        for keys in blocks:
            dv = nn(prob_ref[keys], grad)
            g_value_ref[:, lanes] += column_sums(dv)
            v_ref[keys, lanes] = jnp.where(side, dv.astype(BF), v_ref[keys, lanes])
            dk = nn(score_ref[keys], query) * SCALE
            k_ref[keys, lanes] = jnp.where(side, dk.astype(BF), k_ref[keys, lanes])
        part_ref[...] = nn(turned_ref[lanes], score_ref[...])
        at = pl.ds(pl.multiple_of(h * HEAD_DIM, 8), HEAD_DIM)
        dq_ref[at] = part_ref[pl.ds(pl.multiple_of(offset, 8), HEAD_DIM)]

    dq = dq_ref[...].T * SCALE
    put_vectors(vec2_ref, [column_sums(dq), g_value_ref[...]])
    saves = copies(where, "vec2", parts_ref, vec2_ref, out_sem.at[3], out=True)
    dq_b = dq.astype(BF)
    wait(vecs)
    vec = vector_rows(vec1_ref)
    gain, shift = as_row(vec, 0, DC), as_row(vec, DC, DC)
    gain_t, shift_t = (jnp.broadcast_to(v, (8, D)).T[:, :1] for v in (gain, shift))
    wait(x_load)
    step = rows // 3

    @pl.loop(0, window // step)
    def _(i):
        at = pl.ds(pl.multiple_of(i * step, step), step)
        normed, _ = norm_rows(x_ref[at].astype(F32))
        turned_ref[:, at] = normed.astype(BF).T

    for made in weight_loads:
        wait(made)
    gain_acc[...] = jnp.zeros_like(gain_acc)
    shift_acc[...] = jnp.zeros_like(shift_acc)

    later = {
        (1, 0): [("load", [(1, a), (0, b), (3, b)])], (1, 1): [("end", [(1, a), (0, b), (3, b)])],
        (2, 0): [("load", [(0, c_), (3, c_)])],
    }

    def plane_job(what, entries):
        for zv, p in entries:

            def go():
                if what == "load":
                    load(0, p, zv)
                else:
                    finish(0, p, zv)
                    send(0, p, zv)

            at_plane(zv, go)

    own = turned_ref[:, pl.ds(margin, rows)]
    made = []
    for i, (left, right_ref) in enumerate(((own, None), (turned_ref, k_ref), (turned_ref, v_ref))):
        if i == 2:
            wait(made[0])
        for pair, c in enumerate(range(0, DC, 2)):
            for what, entries in later.get((i, pair), []):
                plane_job(what, entries)
            many = min(2, DC - c)
            lanes = slice(c * LANES, (c + many) * LANES)
            right = dq_b[:, lanes] if right_ref is None else right_ref[:, lanes]
            raw = nn(left[...], right)
            summed = column_sums(right.astype(F32))
            put_panels(g_ref.at[i % 2], c, gain_t * raw + shift_t * summed)
            weights = panels(w_ref.at[i], c, many, D // ROWS).astype(F32)
            scaled, shifted = weights * raw, weights * summed
            for j in range(many):
                part = slice(j * LANES, (j + 1) * LANES)
                gain_acc[...] += scaled[:, part]
                shift_acc[...] += shifted[:, part]
        made.append(copies(where, names[i], parts_ref, g_ref.at[i % 2], out_sem.at[i], out=True))
        start(made[i])
    put_vectors(vec1_ref, [column_sums(gain_acc[...].T), column_sums(shift_acc[...].T)])
    saves = saves + copies(where, "vec1", parts_ref, vec1_ref, out_sem.at[3], out=True)
    start(saves)
    plane_job("end", [(0, c_), (3, c_)])
    wait(saves + made[1] + made[2])
    for p in late_ids:
        for slot in (3, 1, 2, 0):
            to_mate(p, slot).start()

    def row_block(n):
        first = n * rows
        own = n == window // rows // 2
        for c in range(0, DC, 2):
            many = min(2, DC - c)
            lanes = slice(c * LANES, (c + many) * LANES)
            part = lambda i: panels(w_ref.at[i], 0, DC, many * LANES // ROWS, c * LANES // ROWS)
            value = nt(k_ref[first : first + rows], part(1)) + nt(v_ref[first : first + rows], part(2))
            if own:
                value = value + nt(dq_b, part(0))
            block_ref[:, lanes] = value

        @pl.loop(0, rows // step)
        def _(i):
            here = pl.ds(pl.multiple_of(i * step, step), step)
            there = pl.ds(pl.multiple_of(first + i * step, step), step)
            normed, inverse = norm_rows(x_ref[there].astype(F32))
            result = norm_rows_back(block_ref[here], normed, inverse, gain)
            if own:
                block_ref[here] = result
            else:
                x_ref[there] = result.astype(BF)

    def near_rows(slot):
        return x_ref.at[pl.ds(slot * rows, rows)]

    def near_save(slot):
        return pltpu.make_async_copy(near_rows(slot), near_ref.at[slot], x_sem)

    def near_copy(slot, which, device):
        return remote(near_ref.at[slot], near_got.at[which], near_send.at[which], near_recv.at[which], device)

    row_block(0)
    row_block(4)
    ends = [near_save(0), near_save(4)]
    start(ends)
    at_plane(1, lambda: run([(0, b)], 1))
    at_plane(2, lambda: run([(0, a), (0, c_)], 2))
    run([(3, p) for p in late_ids], None, True)
    row_block(1)
    row_block(3)
    wait(ends)
    sides = [near_save(1), near_save(3)]
    start(sides)
    wait(sides)
    to_mate_itself, to_mate_shared = (3 - 2 * core), (1 + 2 * core)
    near_copy(to_mate_itself, 0, mate).start()
    near_copy(to_mate_shared, 1, mate).start()

    @pl.when((core == 0) & has_before)
    def _():
        near_copy(0, 2, before).start()

    @pl.when((core == 1) & has_after)
    def _():
        near_copy(4, 3, after).start()

    run([(kind, p) for p in late_ids for kind in (1, 2)], None)
    row_block(2)
    near_copy(0, 1, me).wait_recv()
    shared_slot = 4 - 4 * core
    fetch = pltpu.make_async_copy(near_got.at[1], k_ref.at[pl.ds(0, rows)], x_sem)
    fetch.start()
    fetch.wait()

    @pl.loop(0, rows // step)
    def _(i):
        here = pl.ds(pl.multiple_of(i * step, step), step)
        there = pl.ds(pl.multiple_of(shared_slot * rows + i * step, step), step)
        x_ref[there] = (x_ref[there].astype(F32) + k_ref[here].astype(F32)).astype(BF)

    shared_save = near_save(shared_slot)
    shared_save.start()
    shared_save.wait()

    @pl.when((core == 0) & has_after)
    def _():
        near_copy(4, 3, after).start()

    @pl.when((core == 1) & has_before)
    def _():
        near_copy(0, 2, before).start()

    def tail(zv):
        out = [p for p in late_ids if pieces[p][0] != zv]
        hops = lambda p: zv if pieces[p][0] > zv else depth - 1 - zv
        moving = [(0, p) for p in sorted(out, key=lambda p: (hops(p), p))]
        finals = [(0, p) for p in early_ids if pieces[p][0] == zv] + [(0, p) for p in late_ids if pieces[p][0] == zv]
        return moving + finals

    for zv in range(depth):
        at_plane(zv, lambda: run(tail(zv), zv))

    near_copy(0, 0, me).wait_recv()

    @pl.when(has_after)
    def _():
        near_copy(0, 2, me).wait_recv()

    @pl.when(has_before)
    def _():
        near_copy(0, 3, me).wait_recv()

    for i, (which, there) in enumerate(((0, None), (2, has_after), (3, has_before))):
        target = k_ref.at[pl.ds(i * rows, rows)]
        if there is None:
            pltpu.make_async_copy(near_got.at[which], target, x_sem).start()
            continue

        @pl.when(there)
        def _():
            pltpu.make_async_copy(near_got.at[which], target, x_sem).start()

        @pl.when(jnp.logical_not(there))
        def _():
            pltpu.make_async_copy(near_ref.at[0], target, x_sem).start()

    for i in range(3):
        pltpu.make_async_copy(near_got.at[0], k_ref.at[pl.ds(i * rows, rows)], x_sem).wait()
    near_after, near_before = (jnp.where(there, 1.0, 0.0) for there in (has_after, has_before))

    @pl.loop(0, rows // step)
    def _(i):
        here = pl.ds(pl.multiple_of(i * step, step), step)
        fetch_mid = pltpu.make_async_copy(mid_hbm_ref.at[here], mid_ref, x_sem)
        fetch_mid.start()
        fetch_mid.wait()
        value = mid_ref[...] + block_ref[here] + k_ref[here].astype(F32)
        value = value + near_after * k_ref[pl.ds(pl.multiple_of(rows + i * step, step), step)].astype(F32)
        value = value + near_before * k_ref[pl.ds(pl.multiple_of(2 * rows + i * step, step), step)].astype(F32)
        in_grad_ref[here] = value.astype(BF)

    for p in range(len(pieces)):
        for slot in range(4):
            to_mate(p, slot).wait_send()
        for side in (0, 1):
            half_out(p, side).wait_send()
            full_out(p, side).wait_send()
        for zv in range(depth):
            if pieces[p][0] != zv:
                at_plane(zv, lambda: line_out(p, zv).wait_send())
    near_copy(0, 0, mate).wait_send()
    near_copy(0, 1, mate).wait_send()

    @pl.when(has_before)
    def _():
        near_copy(0, 2, before).wait_send()

    @pl.when(has_after)
    def _():
        near_copy(4, 3, after).wait_send()


def back_scatter(x_win, seg_query, seg_keys, gathered, queries, key_win, value_win, att_grad, logs, delta, mid_grad, parts, plan):
    where, block = plan[:2]
    window, rows = x_win.shape[0], queries.shape[0]
    seg_keys = jnp.broadcast_to(seg_keys, (window, LANES))
    count = lax.axis_size("fsdp")
    depth = count // 8
    hot, cold = transfer_pieces(plan, depth)
    early = sorted(cold, reverse=True)
    late = []
    for piece in sorted(hot, reverse=True):
        late += cut(piece, 4) if piece[2] > block // 2 else [piece]
    many = len(early) + len(late)
    dma = pltpu.SemaphoreType.DMA
    tiles = lambda *n: pltpu.VMEM((*n, ROWS, LANES), BF)
    vm = lambda a, b, t: pltpu.VMEM((a, b), t)
    hbm = lambda *n: jax.ShapeDtypeStruct((*n, ROWS, LANES), BF)
    return pl.pallas_call(
        functools.partial(back_scatter_kernel, depth, where, early, late),
        out_shape=(
            jax.ShapeDtypeStruct(parts.shape, BF), jax.ShapeDtypeStruct((block, ROWS, LANES), F32), jax.ShapeDtypeStruct((rows, D), BF),
            hbm(depth, 4, block), hbm(depth, 4, block), hbm(depth, 2, block), hbm(depth, 2, block), hbm(depth + 1, block),
            jax.ShapeDtypeStruct((5, rows, D), BF), jax.ShapeDtypeStruct((4, rows, D), BF),
        ),
        in_specs=[ANY, VM, VM, ANY, VM, ANY, ANY, VM, VM, VM, ANY, ANY],
        out_specs=[ANY, VM, VM] + [ANY] * 7,
        scratch_shapes=[
            tiles(3, D // ROWS, DC), tiles(2, D // ROWS, DC), tiles(2), tiles(2),
            vm(window, rows, BF), vm(window, rows, BF), vm(D, window, BF), vm(window, D, BF), vm(window, D, BF),
            vm(D, rows, F32), vm(PAIR, rows, F32), vm(LANES, rows, F32), vm(window, D, BF), vm(rows, D, F32), vm(rows // 3, D, F32),
            vm(1, D, F32), vm(D, LANES, F32), vm(D, LANES, F32), tiles(6, block), tiles(block),
            dma((many, 4)), dma((many, 4)), dma((many, 2)), dma((many, 2)), dma((many, 2)), dma((many, 2)), dma((many,)), dma((many, 2)),
            dma((4,)), dma((4,)), dma((2,)), dma((2,)), dma((4,)), dma, dma((4,)), dma,
        ],
        input_output_aliases={11: 0},
        compiler_params=pltpu.CompilerParams(collective_id=1, has_side_effects=True, vmem_limit_bytes=VMEM_LIMIT),
        name="back_scatter",
    )(x_win, seg_query, seg_keys, gathered, queries, key_win, value_win, att_grad, logs, delta, mid_grad, parts)[1:3]


def passed_along(value, steps):
    count = lax.axis_size("fsdp")
    first, last = (max(0, -steps), min(count, count - steps))
    return lax.ppermute(value, "fsdp", [(source, source + steps) for source in range(first, last)])


def window_of(rows):
    near = [rows if k == 0 else passed_along(rows, -k) for k in range(-REACH, REACH + 1)]
    return jnp.concatenate(near, axis=0)


def shards(kernels, block_input, params, cotangent, segment_ids):
    count = lax.axis_size("fsdp")
    me = lax.axis_index("fsdp")
    rows = block_input.shape[0]
    margin = REACH * rows
    seg_pad = jnp.pad(segment_ids, (margin, margin), constant_values=-1)
    seg_query = lax.dynamic_slice_in_dim(segment_ids, me * rows, rows, 0)
    seg_keys = lax.dynamic_slice_in_dim(seg_pad, me * rows, 2 * margin + rows, 0)
    plan = wire_plan(count, params.shape[1])
    where = plan[0]
    block = to_tiles(params, plan)
    if kernels:
        gathered, x_win, _, queries, key_win, value_win, attended, rest, logs = gather_front(
            block, block_input, seg_query[:, None], seg_keys[None, :], plan
        )
    else:
        x_win = window_of(block_input)
        gathered = lax.all_gather(block, "fsdp", axis=0, tiled=False)
        queries, key_win, value_win, attended, rest, logs = front(
            x_win, seg_query[:, None], seg_keys[None, :], gathered, where, rows
        )
    activations, mid_grad, att_grad, delta, parts = middle(block_input, cotangent, attended, rest, gathered, where)
    sides = (x_win, seg_query[None, :], seg_keys[:, None], gathered, queries, key_win, value_win, att_grad, logs)
    if kernels:
        summed, input_grad = back_scatter(*sides, delta, mid_grad, parts, plan)
    else:
        near, own, parts = back(*sides, parts, where)
        input_grad = mid_grad + own
        for k in range(-REACH, REACH + 1):
            if k != 0:
                part = near[(k + REACH) * rows : (k + REACH + 1) * rows]
                input_grad = input_grad + passed_along(part, k).astype(jnp.float32)
        input_grad = input_grad.astype(jnp.bfloat16)
        received = lax.all_to_all(parts, "fsdp", split_axis=0, concat_axis=0, tiled=True)
        summed = jnp.sum(received.astype(jnp.float32), axis=0)
    param_grads = to_flat(summed, plan, params.shape[1])
    return (activations, input_grad, param_grads)


def two_by_two(mesh):
    spans = np.array([device.coords for device in mesh.devices.flat])
    return tuple(spans.max(axis=0) - spans.min(axis=0))[:2] == (1, 1)


def solution(mesh):
    return jax.shard_map(
        functools.partial(shards, two_by_two(mesh)),
        mesh=mesh,
        in_specs=(P("fsdp", None), P(None, "fsdp"), P("fsdp", None), P()),
        out_specs=(P("fsdp", None), P("fsdp", None), P(None, "fsdp")),
        check_vma=False,
    )
```

```python
import functools
import math

import jax
import jax.numpy as jnp
import numpy as np
from jax import lax
from jax.experimental import pallas as pl
from jax.experimental.pallas import tpu as pltpu
from jax.sharding import PartitionSpec as P

D = 1152
HEADS = 16
HEAD_DIM = 72
FF = 4304
REACH = 2


EPS = 1e-06
NEG = -1e30
LANES = 128
ROWS = 16
DC = D // LANES
FC = -(-FF // LANES)
WIDE = FF * ROWS // LANES
HEAD = 544
KIND_A, KIND_D, KIND_L2, KIND_L3, KIND_B = 1, 2, 3, 4, 5
MESH = pl.DeviceIdType.MESH


def units():
    found = []
    offset = 0

    def matrix(name, kind, rows, width, tiles):
        nonlocal offset
        for row in range(0, rows, ROWS):
            found.append((name, kind, offset + row * width, tiles))
        offset += rows * width

    def vectors(name, kind, length, tiles):
        nonlocal offset
        found.append((name, kind, offset, tiles))
        offset += length

    vectors("vec1", KIND_L2, 2 * D, 2)
    matrix("w_query", KIND_A, D, D, DC)
    matrix("w_key", KIND_A, D, D, DC)
    matrix("w_value", KIND_A, D, D, DC)
    vectors("vec2", KIND_L2, 2 * D, 2)
    matrix("w_out", KIND_A, D, D, DC)
    vectors("vec3", KIND_L2, 3 * D, 2)
    matrix("w_up", KIND_B, D, FF, FC)
    vectors("vec4", KIND_L3, FF, 3)
    matrix("w_down", KIND_D, FF, D, DC)
    vectors("vec5", KIND_D, D, DC)
    return found


def unit_width(name):
    return {"vec1": 2 * D, "vec2": 2 * D, "vec3": 3 * D, "vec4": FF, "vec5": D, "w_up": ROWS * FF}.get(
        name, ROWS * D
    )


def wire_plan(count, shard):
    blocks = [[] for _ in range(count)]
    where = {}
    used = [0] * count
    tails = [0] * count
    for name, kind, first, tiles in units():
        owner = first // shard
        where.setdefault(name, []).append((owner, used[owner], tiles))
        blocks[owner].append((kind, (first - owner * shard) // LANES, used[owner]))
        used[owner] += tiles
        tails[owner] = max(0, first + unit_width(name) - (owner + 1) * shard)
    block = max(used)
    block += block % 2
    most = max(len(b) for b in blocks)
    table = np.zeros((count, 3 * most), np.int32)
    for owner, entries in enumerate(blocks):
        for i, entry in enumerate(entries):
            table[owner, 3 * i : 3 * i + 3] = entry
    return where, block, table, np.array(tails, np.int32)


def lane_iota(rows):
    return lax.broadcasted_iota(jnp.int32, (rows, LANES), 1)


def wide_rows():
    return [divmod(row * FF, LANES) for row in range(ROWS)]


SKEW = (D * 0 + 80) % LANES


def rows_from_line(line_ref, flat_ref, first, rows):
    step = 8 * LANES

    @pl.loop(0, rows // 8)
    def _(i):
        part = line_ref[:, pl.ds(pl.multiple_of(i * step, step), step)].astype(jnp.float32)
        flat_ref[pl.ds(first + i * 8, 8)] = part.reshape(8, LANES)

    for row in range(rows // 8 * 8, rows):
        flat_ref[pl.ds(first + row, 1)] = line_ref[:, row * LANES : (row + 1) * LANES].astype(jnp.float32)


def line_from_rows(flat_ref, line_ref, first, rows):
    step = 8 * LANES

    @pl.loop(0, rows // 8)
    def _(i):
        part = flat_ref[pl.ds(first + i * 8, 8)]
        line_ref[:, pl.ds(pl.multiple_of(i * step, step), step)] = part.reshape(1, step)

    for row in range(rows // 8 * 8, rows):
        line_ref[:, row * LANES : (row + 1) * LANES] = flat_ref[pl.ds(first + row, 1)]


def to_tiles_kernel(entries, table_ref, line_ref, head_ref, tile_ref, stage_ref, flat_ref):
    rows = line_ref.shape[1] // LANES
    rows_from_line(line_ref, flat_ref, 0, rows)
    rows_from_line(head_ref, flat_ref, rows, HEAD)

    def unit(i, _):
        kind, src, dst = (table_ref[3 * i + j] for j in range(3))

        @pl.when(kind == KIND_A)
        def _():
            for c in range(DC):
                tile_ref[dst + c] = flat_ref[pl.ds(src + c, ROWS, stride=DC), :].astype(jnp.bfloat16)

        @pl.when(kind == KIND_D)
        def _():
            lane = lane_iota(ROWS)
            for c in range(DC):
                here = flat_ref[pl.ds(src + c, ROWS, stride=DC), :]
                after = flat_ref[pl.ds(src + c + 1, ROWS, stride=DC), :]
                both = jnp.where(lane >= SKEW, here, after)
                tile_ref[dst + c] = pltpu.roll(both, LANES - SKEW, 1).astype(jnp.bfloat16)

        for code, tiles in ((KIND_L2, 2), (KIND_L3, 3)):

            @pl.when(kind == code)
            def _():
                for j in range(tiles):
                    tile_ref[dst + j] = flat_ref[pl.ds(src + ROWS * j, ROWS), :].astype(jnp.bfloat16)

        @pl.when(kind == KIND_B)
        def _():
            tall = 8 * pl.cdiv(FC, 8)
            lane = lane_iota(tall)
            row = lax.broadcasted_iota(jnp.int32, (tall, LANES), 0)
            keep = (row < FC - 1) | (lane < FF % LANES)
            for r, (base, skew) in enumerate(wide_rows()):
                part = flat_ref[pl.ds(src + base, tall), :]
                if skew:
                    after = flat_ref[pl.ds(src + base + 1, tall), :]
                    part = pltpu.roll(jnp.where(lane >= skew, part, after), LANES - skew, 1)
                stage_ref[pl.ds(r, tall, stride=ROWS), :] = jnp.where(keep, part, 0.0)
            for c in range(FC):
                tile_ref[dst + c] = stage_ref[pl.ds(ROWS * c, ROWS), :].astype(jnp.bfloat16)

        return 0

    lax.fori_loop(0, entries, unit, 0)


def to_flat_kernel(entries, rows, table_ref, tile_ref, *refs):
    if len(refs) == 5:
        tail_ref, line_ref, stage_ref, flat_ref, first_ref = refs
    else:
        line_ref, stage_ref, flat_ref = refs
    if len(refs) == 5:
        flat_ref[...] = jnp.zeros_like(flat_ref)

    def unit(i, _):
        kind, src, dst = (table_ref[3 * i + j] for j in range(3))

        @pl.when(kind == KIND_A)
        def _():
            for c in range(DC):
                flat_ref[pl.ds(src + c, ROWS, stride=DC), :] = tile_ref[dst + c]

        @pl.when(kind == KIND_D)
        def _():
            lane = lane_iota(ROWS)
            for c in range(DC):
                turned = pltpu.roll(tile_ref[dst + c], SKEW, 1)
                for step, keep in ((0, lane >= SKEW), (1, lane < SKEW)):
                    at = pl.ds(src + c + step, ROWS, stride=DC)
                    flat_ref[at, :] = jnp.where(keep, turned, flat_ref[at, :])

        for code, tiles in ((KIND_L2, 2), (KIND_L3, 3)):

            @pl.when(kind == code)
            def _():
                for j in range(tiles):
                    flat_ref[pl.ds(src + ROWS * j, ROWS), :] = tile_ref[dst + j]

        @pl.when(kind == KIND_B)
        def _():
            tall = 8 * pl.cdiv(FC, 8)
            lane = lane_iota(tall)
            row = lax.broadcasted_iota(jnp.int32, (tall, LANES), 0)
            for c in range(FC):
                stage_ref[pl.ds(ROWS * c, ROWS), :] = tile_ref[dst + c]
            for r, (base, skew) in enumerate(wide_rows()):
                turned = stage_ref[pl.ds(r, tall, stride=ROWS), :]
                if skew:
                    turned = pltpu.roll(turned, skew, 1)
                for step in range(2 if skew else 1):
                    entry = row * LANES + lane + (step * LANES - skew)
                    keep = (lane < skew if step else lane >= skew) & (entry < FF)
                    at = pl.ds(src + base + step, tall)
                    flat_ref[at, :] = jnp.where(keep, turned, flat_ref[at, :])

        return 0

    lax.fori_loop(0, entries, unit, 0)
    if len(refs) == 3:
        line_from_rows(flat_ref, line_ref, rows, HEAD)
        return
    rows_from_line(tail_ref, first_ref, 0, HEAD)
    entry = lax.broadcasted_iota(jnp.int32, (HEAD, LANES), 0) * LANES + lane_iota(HEAD)
    flat_ref[:HEAD] = jnp.where(entry < table_ref[3 * entries], first_ref[...], flat_ref[:HEAD])
    line_from_rows(flat_ref, line_ref, 0, rows)


def my_row(table):
    return lax.dynamic_index_in_dim(jnp.asarray(table), lax.axis_index("fsdp"), 0, keepdims=False)


def relayout_scratch(rows):
    return [
        pltpu.VMEM((ROWS * 8 * pl.cdiv(FC, 8), LANES), jnp.float32),
        pltpu.VMEM((8 * pl.cdiv(rows + HEAD + 8, 8), LANES), jnp.float32),
    ]


def to_tiles(line, plan):
    where, block, table, tails = plan
    count = lax.axis_size("fsdp")
    head = lax.ppermute(line[:, : HEAD * LANES], "fsdp", [(i, (i - 1) % count) for i in range(count)])
    vmem = pl.BlockSpec(memory_space=pltpu.VMEM)
    return pl.pallas_call(
        functools.partial(to_tiles_kernel, table.shape[1] // 3),
        out_shape=jax.ShapeDtypeStruct((block, ROWS, LANES), jnp.bfloat16),
        grid_spec=pltpu.PrefetchScalarGridSpec(
            num_scalar_prefetch=1, grid=(1,), in_specs=[vmem, vmem], out_specs=vmem,
            scratch_shapes=relayout_scratch(line.shape[1] // LANES),
        ),
        name="to_tiles",
    )(my_row(table), line, head)


def to_flat(tiles, plan, length):
    where, block, table, tails = plan
    count = lax.axis_size("fsdp")
    rows = length // LANES
    vmem = pl.BlockSpec(memory_space=pltpu.VMEM)
    last = [max(i for i in range(table.shape[1] // 3) if row[3 * i]) for row in table]
    last = np.stack([row[3 * i : 3 * i + 3] for row, i in zip(table, last)])
    whole = np.concatenate([table, np.roll(tails, 1)[:, None]], axis=1)

    def call(entries, mine, inputs, width, scratch, name):
        return pl.pallas_call(
            functools.partial(to_flat_kernel, entries, rows),
            out_shape=jax.ShapeDtypeStruct((1, width), jnp.float32),
            grid_spec=pltpu.PrefetchScalarGridSpec(
                num_scalar_prefetch=1, grid=(1,), in_specs=[vmem] * len(inputs), out_specs=vmem,
                scratch_shapes=relayout_scratch(rows) + scratch,
            ),
            name=name,
        )(my_row(mine), *inputs)

    tail = call(1, last, (tiles,), HEAD * LANES, [], "tail")
    tail = lax.ppermute(tail, "fsdp", [(i, (i + 1) % count) for i in range(count)])
    return call(table.shape[1] // 3, whole, (tiles, tail), length, [pltpu.VMEM((HEAD, LANES), jnp.float32)], "to_flat")


def place(me):
    return lax.rem(me, 2), lax.rem(me // 2, 2), lax.rem(me // 4, 2), me // 8


def index_of(core, x, y, z):
    return ((z * 2 + y) * 2 + x) * 2 + core


def greet(devices_and_conditions):
    barrier = pltpu.get_barrier_semaphore()
    for device, present in devices_and_conditions:
        if present is None:
            pl.semaphore_signal(barrier, inc=1, device_id=(device,), device_id_type=MESH)
        else:

            @pl.when(present)
            def _():
                pl.semaphore_signal(barrier, inc=1, device_id=(device,), device_id_type=MESH)

    present = [1 if p is None else p.astype(jnp.int32) for _, p in devices_and_conditions]
    pl.semaphore_wait(barrier, sum(present))


BF = jnp.bfloat16
F32 = jnp.float32
PAIR = 2 * LANES
SCALE = HEAD_DIM**-0.5
GELU_A = math.sqrt(2.0 / math.pi)
GELU_B = 0.044715
LOG2E = math.log2(math.e)
ANY = pl.BlockSpec(memory_space=pl.ANY)
VM = pl.BlockSpec(memory_space=pltpu.VMEM)
VMEM_LIMIT = 63 << 20


def nn(left, right):
    return lax.dot_general(left, right, (((1,), (0,)), ((), ())), preferred_element_type=F32)


def nt(left, right):
    return lax.dot_general(left, right, (((1,), (1,)), ((), ())), preferred_element_type=F32)


def runs_of(where, name):
    runs, done = [], 0
    for owner, at, tiles in where[name]:
        if runs and runs[-1][0] == owner and runs[-1][1] + runs[-1][2] == at:
            runs[-1][2] += tiles
        else:
            runs.append([owner, at, tiles, done])
        done += tiles
    return runs


def copies(where, name, blocks_ref, tiles_ref, sem, out=False):
    made = []
    flat_tiles = tiles_ref if len(tiles_ref.shape) == 3 else tiles_ref.reshape(-1, ROWS, LANES)
    for owner, at, tiles, done in runs_of(where, name):
        there, here = blocks_ref.at[owner, pl.ds(at, tiles)], flat_tiles.at[pl.ds(done, tiles)]
        made.append(pltpu.make_async_copy(here, there, sem) if out else pltpu.make_async_copy(there, here, sem))
    return made


def start(made):
    for copy in made:
        copy.start()


def wait(made):
    for copy in made:
        copy.wait()


def panel(tiles_ref, c, units, first=0):
    return tiles_ref[pl.ds(first, units), pl.ds(c, 1)].reshape(units * ROWS, LANES)


def panels(tiles_ref, c, many, units, first=0):
    return jnp.concatenate([panel(tiles_ref, c + i, units, first) for i in range(many)], axis=1)


def put_panel(tiles_ref, c, value, first=0):
    units = value.shape[0] // ROWS
    tiles_ref[pl.ds(first, units), pl.ds(c, 1)] = value.astype(BF).reshape(units, 1, ROWS, LANES)


def put_panels(tiles_ref, c, value, first=0):
    for i in range(value.shape[1] // LANES):
        put_panel(tiles_ref, c + i, value[:, i * LANES : (i + 1) * LANES], first)


def vector_rows(tiles_ref):
    return jnp.concatenate([tiles_ref[i].astype(F32) for i in range(tiles_ref.shape[0])], axis=0)


def as_row(rows, first, many):
    return jnp.concatenate([rows[first + i : first + i + 1] for i in range(many)], axis=1)


def put_vectors(tiles_ref, rows_list):
    parts = [row[:, i * LANES : (i + 1) * LANES] for row in rows_list for i in range(row.shape[1] // LANES)]
    missing = tiles_ref.shape[0] * ROWS - len(parts)
    whole = jnp.concatenate(parts + [jnp.zeros((missing, LANES), F32)] if missing else parts, axis=0)
    for i in range(tiles_ref.shape[0]):
        tiles_ref[i] = whole[i * ROWS : (i + 1) * ROWS].astype(BF)


def norm_rows(values):
    centre = values - jnp.mean(values, axis=-1, keepdims=True)
    inverse = lax.rsqrt(jnp.mean(centre * centre, axis=-1, keepdims=True) + EPS)
    return centre * inverse, inverse


def norm_rows_back(grad, normed, inverse, gain):
    scaled = grad * gain
    return inverse * (
        scaled - jnp.mean(scaled, axis=-1, keepdims=True) - normed * jnp.mean(scaled * normed, axis=-1, keepdims=True)
    )


def column_sums(values):
    return jnp.sum(values, axis=0, keepdims=True)


def head_window(h):
    block = jnp.minimum((h * HEAD_DIM) // LANES, DC - 2)
    lane = pl.multiple_of(block * LANES, LANES)
    return lane, h * HEAD_DIM - lane


def head_mask(rows, offset):
    lane = lax.broadcasted_iota(jnp.int32, (rows, PAIR), 1)
    return (lane >= offset) & (lane < offset + HEAD_DIM)


def front_kernel(
    where, x_ref, segq_ref, segk_ref, blocks_ref, q_ref, k_ref, v_ref, attended_ref, rest_ref, logs_ref,
    normed_ref, w_ref, vec1_ref, vec2_ref, bias_ref, score_ref, prob_ref, sem, vec_sem,
):
    window, rows = x_ref.shape[0], q_ref.shape[0]
    margin = (window - rows) // 2
    loads = [copies(where, name, blocks_ref, w_ref.at[i], sem.at[i]) for i, name in enumerate(("w_query", "w_key", "w_value"))]
    vecs = copies(where, "vec1", blocks_ref, vec1_ref, vec_sem) + copies(where, "vec2", blocks_ref, vec2_ref, vec_sem)
    start(vecs)
    for made in loads:
        start(made)
    wait(vecs)
    vec = vector_rows(vec1_ref)
    gain, shift = as_row(vec, 0, DC), as_row(vec, DC, DC)
    step = rows // 3

    @pl.loop(0, window // step)
    def _(i):
        at = pl.ds(i * step, step)
        normed, _ = norm_rows(x_ref[at].astype(F32))
        normed_ref[at] = (normed * gain + shift).astype(BF)

    @pl.loop(0, rows // 8)
    def _(i):
        at = pl.ds(i * 8, 8)
        bias_ref[at] = jnp.where(segq_ref[at] == segk_ref[...], 0.0, NEG)

    biases = vector_rows(vec2_ref)
    zero = jnp.zeros((1, D), F32)
    for made in loads:
        wait(made)
    for i, (out, add) in enumerate(((q_ref, as_row(biases, 0, DC)), (k_ref, zero), (v_ref, as_row(biases, DC, DC)))):
        for c in range(0, DC, 2):
            many = min(2, DC - c)
            lanes = slice(c * LANES, (c + many) * LANES)
            weights = panels(w_ref.at[i], c, many, D // ROWS)
            if i == 0:
                out[:, lanes] = (nn(normed_ref[pl.ds(margin, rows)], weights) + add[:, lanes]).astype(BF)
            else:

                @pl.loop(0, window // rows)
                def _(b):
                    at = pl.ds(b * rows, rows)
                    out[at, lanes] = (nn(normed_ref[at], weights) + add[:, lanes]).astype(BF)

    attended_ref[...] = jnp.zeros_like(attended_ref)
    rest_ref[...] = jnp.zeros_like(rest_ref)
    logs_ref[...] = jnp.zeros_like(logs_ref)
    lane_l = lax.broadcasted_iota(jnp.int32, logs_ref.shape, 1)

    @pl.loop(0, HEADS)
    def _(h):
        lane, offset = head_window(h)
        mask = head_mask(rows, offset)
        lanes = pl.ds(lane, PAIR)
        query = jnp.where(mask, q_ref[:, lanes], jnp.zeros((), BF))
        score_ref[...] = nt(query, k_ref[:, lanes]) * SCALE + bias_ref[...]
        top = jnp.max(score_ref[...], axis=-1, keepdims=True)
        powers = jnp.exp(score_ref[...] - top)
        total = jnp.sum(powers, axis=-1, keepdims=True)
        prob_ref[...] = powers.astype(BF)
        out = nn(prob_ref[...], v_ref[:, lanes]) / total
        rounded = out.astype(BF)
        attended_ref[:, lanes] = jnp.where(mask, rounded, attended_ref[:, lanes])
        rest_ref[:, lanes] = jnp.where(mask, (out - rounded.astype(F32)).astype(BF), rest_ref[:, lanes])
        logs_ref[...] = jnp.where(lane_l == h, top + jnp.log(total), logs_ref[...])


def front(x_win, seg_query, seg_keys, gathered, where, rows):
    window = x_win.shape[0]
    shape = lambda n, d=D, t=BF: jax.ShapeDtypeStruct((n, d), t)
    dma = pltpu.SemaphoreType.DMA
    units = D // ROWS
    return pl.pallas_call(
        functools.partial(front_kernel, where),
        out_shape=(shape(rows), shape(window), shape(window), shape(rows), shape(rows), shape(rows, LANES, F32)),
        in_specs=[VM, VM, VM, ANY],
        out_specs=[VM] * 6,
        scratch_shapes=[
            pltpu.VMEM((window, D), BF),
            pltpu.VMEM((3, units, DC, ROWS, LANES), BF), pltpu.VMEM((2, ROWS, LANES), BF), pltpu.VMEM((2, ROWS, LANES), BF),
            pltpu.VMEM((rows, window), F32), pltpu.VMEM((rows, window), F32), pltpu.VMEM((rows, window), BF), dma((3,)), dma,
        ],
        compiler_params=pltpu.CompilerParams(vmem_limit_bytes=VMEM_LIMIT),
        name="front",
    )(x_win, seg_query, seg_keys, gathered)


def middle_kernel(
    where, x_ref, cot_ref, attended_ref, rest_ref, blocks_ref, act_ref, mid_grad_ref, att_grad_ref, delta_ref, parts_ref,
    wo_ref, wu_ref, wd_ref, vec3_ref, vec4_ref, vec5_ref, b_up_ref, hidden_ref, slope_ref, pre_ref, normed_ref, normed_b_ref,
    mid_ref, g_up_ref, sem, out_sem,
):
    rows = x_ref.shape[0]
    units, f_units = D // ROWS, FF // ROWS
    names = ("w_out", "w_up", "w_down", "vec3", "vec4", "vec5")
    refs = (wo_ref, wu_ref, wd_ref, vec3_ref, vec4_ref, vec5_ref)
    loads = {n: copies(where, n, blocks_ref, r, sem.at[i]) for i, (n, r) in enumerate(zip(names, refs))}
    saves = {n: copies(where, n, parts_ref, r, out_sem, out=True) for n, r in zip(names, refs)}
    for n in ("vec3", "vec4", "vec5", "w_out", "w_up", "w_down"):
        start(loads[n])
    f_wide = FC * LANES
    pads = f_wide // ROWS - f_units
    wd_ref[pl.ds(f_units, pads)] = jnp.zeros((pads, DC, ROWS, LANES), BF)
    for n in ("vec3", "vec4", "vec5", "w_out"):
        wait(loads[n])
    vec = vector_rows(vec3_ref)
    b_out, gain, shift = (as_row(vec, i * DC, DC) for i in range(3))
    vec = vector_rows(vec4_ref)
    entry = lax.broadcasted_iota(jnp.int32, vec.shape, 0) * LANES + lax.broadcasted_iota(jnp.int32, vec.shape, 1)
    b_up_ref[...] = jnp.where(entry < FF, vec, 0.0)
    b_down = jnp.concatenate([vec5_ref[c].astype(F32)[0:1] for c in range(DC)], axis=1)

    for c in range(0, DC, 2):
        many = min(2, DC - c)
        lanes = slice(c * LANES, (c + many) * LANES)
        mid_ref[:, lanes] = (
            x_ref[:, lanes].astype(F32) + nn(attended_ref[...], panels(wo_ref, c, many, units)) + b_out[:, lanes]
        )
    normed, inverse = norm_rows(mid_ref[...])
    normed_ref[...] = normed
    normed_b_ref[...] = (normed * gain + shift).astype(BF)

    wait(loads["w_up"])

    @pl.loop(0, FC // 2)
    def _(p):
        at = pl.ds(pl.multiple_of(p * PAIR, PAIR), PAIR)
        bias = jnp.concatenate([b_up_ref[pl.ds(2 * p, 1)], b_up_ref[pl.ds(2 * p + 1, 1)]], axis=1)
        v = nn(normed_b_ref[...], panels(wu_ref, 2 * p, 2, units)) + bias
        square = v * v
        bent = jnp.tanh(GELU_A * v * (1.0 + GELU_B * square))
        hidden_ref[:, at] = (0.5 * v * (1.0 + bent)).astype(BF)
        slope_ref[:, at] = 0.5 * (1.0 + bent) + 0.5 * v * (1.0 - bent * bent) * (
            GELU_A * (1.0 + 3.0 * GELU_B * square)
        )

    wait(loads["w_down"])
    for c in range(0, DC, 2):
        many = min(2, DC - c)
        lanes = slice(c * LANES, (c + many) * LANES)
        act_ref[:, lanes] = (
            mid_ref[:, lanes] + nn(hidden_ref[...], panels(wd_ref, c, many, f_wide // ROWS)) + b_down[:, lanes]
        ).astype(BF)

    @pl.loop(0, FC // 2)
    def _(p):
        at = pl.ds(pl.multiple_of(p * PAIR, PAIR), PAIR)
        first = p * (PAIR // ROWS)
        grad = nt(cot_ref[...], panels(wd_ref, 0, DC, PAIR // ROWS, first)) * slope_ref[:, at]
        pre_ref[:, at] = grad.astype(BF)
        sums = column_sums(grad)
        g_up_ref[pl.ds(2 * p, 1)] = sums[:, :LANES]
        g_up_ref[pl.ds(2 * p + 1, 1)] = sums[:, LANES:]
        put_panels(wd_ref, 0, nn(hidden_ref[:, at].T, cot_ref[...]), first)

    start(saves["w_down"])
    put_vectors(vec4_ref, [b_up_row for b_up_row in [g_up_ref[i : i + 1] for i in range(FC)]])
    start(saves["vec4"])
    cot = cot_ref[...].astype(F32)
    sums = column_sums(cot)
    row0 = lax.broadcasted_iota(jnp.int32, (ROWS, LANES), 0) == 0
    for c in range(DC):
        vec5_ref[c] = jnp.where(row0, sums[:, c * LANES : (c + 1) * LANES], 0.0).astype(BF)
    start(saves["vec5"])

    for c in range(0, DC, 2):
        many = min(2, DC - c)
        weights = panels(wu_ref, 0, FC, many * LANES // ROWS, c * LANES // ROWS)
        mid_ref[:, c * LANES : (c + many) * LANES] = nt(pre_ref[...], weights)
    turned_b = normed_b_ref[...].T

    @pl.loop(0, FC // 2)
    def _(p):
        at = pl.ds(pl.multiple_of(p * PAIR, PAIR), PAIR)
        put_panels(wu_ref, 2 * p, nn(turned_b, pre_ref[:, at]))

    start(saves["w_up"])
    e = mid_ref[...]
    normed = normed_ref[...]
    g_gain, g_shift = column_sums(e * normed), column_sums(e)
    mid_grad = cot + norm_rows_back(e, normed, inverse, gain)
    mid_grad_ref[...] = mid_grad
    put_vectors(vec3_ref, [column_sums(mid_grad), g_gain, g_shift])
    start(saves["vec3"])
    mid_b = mid_grad.astype(BF)
    for c in range(0, DC, 2):
        many = min(2, DC - c)
        lanes = slice(c * LANES, (c + many) * LANES)
        weights = panels(wo_ref, 0, DC, many * LANES // ROWS, c * LANES // ROWS)
        att_grad_ref[:, lanes] = nt(mid_b, weights).astype(BF)
    product = att_grad_ref[...].astype(F32) * (attended_ref[...].astype(F32) + rest_ref[...].astype(F32))
    delta_ref[...] = jnp.sum(product.T.reshape(HEADS, HEAD_DIM, rows), axis=1)
    turned = attended_ref[...].T
    for c in range(0, DC, 2):
        many = min(2, DC - c)
        put_panels(wo_ref, c, nn(turned, mid_b[:, c * LANES : (c + many) * LANES]))
    start(saves["w_out"])
    for n in names:
        wait(saves[n])


def middle(block_input, cotangent, attended, rest, gathered, where):
    rows = block_input.shape[0]
    shape = lambda t: jax.ShapeDtypeStruct((rows, D), t)
    dma = pltpu.SemaphoreType.DMA
    tiles = lambda *n: pltpu.VMEM((*n, ROWS, LANES), BF)
    units, f_wide = D // ROWS, FC * LANES
    return pl.pallas_call(
        functools.partial(middle_kernel, where),
        out_shape=(shape(BF), shape(F32), shape(BF), jax.ShapeDtypeStruct((HEADS, rows), F32), jax.ShapeDtypeStruct(gathered.shape, BF)),
        in_specs=[VM, VM, VM, VM, ANY],
        out_specs=[VM, VM, VM, VM, ANY],
        scratch_shapes=[
            tiles(units, DC), tiles(units, FC), tiles(f_wide // ROWS, DC), tiles(2), tiles(3), tiles(DC),
            pltpu.VMEM((3 * ROWS, LANES), F32), pltpu.VMEM((rows, f_wide), BF), pltpu.VMEM((rows, f_wide), F32),
            pltpu.VMEM((rows, f_wide), BF), pltpu.VMEM((rows, D), F32), pltpu.VMEM((rows, D), BF), pltpu.VMEM((rows, D), F32),
            pltpu.VMEM((3 * ROWS, LANES), F32), dma((6,)), dma,
        ],
        compiler_params=pltpu.CompilerParams(vmem_limit_bytes=VMEM_LIMIT),
        name="middle",
    )(block_input, cotangent, attended, rest, gathered)


def back_kernel(
    where, x_hbm_ref, segq_ref, segk_ref, blocks_ref, q_ref, k_ref, v_ref, grad_ref, logs_ref, parts_in_ref,
    near_ref, own_ref, parts_ref,
    w_ref, vec1_ref, vec2_ref, bias_ref, score_ref, prob_ref, turned_ref, dk_ref, dv_ref, dq_ref, part_ref, logs_t_ref, x_ref,
    sem, vec_sem, out_sem, x_sem,
):
    window, rows = x_ref.shape[0], q_ref.shape[0]
    margin = (window - rows) // 2
    units = D // ROWS
    names = ("w_query", "w_key", "w_value")
    loads = [copies(where, name, blocks_ref, w_ref.at[i], sem.at[i]) for i, name in enumerate(names)]
    vecs = copies(where, "vec1", blocks_ref, vec1_ref, vec_sem)
    start(vecs)
    for made in loads:
        start(made)
    x_load = pltpu.make_async_copy(x_hbm_ref, x_ref, x_sem)
    x_load.start()

    @pl.loop(0, window // LANES)
    def _(i):
        at = pl.ds(pl.multiple_of(i * LANES, LANES), LANES)
        bias_ref[at] = jnp.where(segk_ref[at] == segq_ref[...], 0.0, NEG)
        turned_ref[:, at] = k_ref[at].T
        dk_ref[at] = jnp.zeros((LANES, D), F32)
        dv_ref[at] = jnp.zeros((LANES, D), F32)

    logs_t_ref[...] = logs_ref[...].T

    @pl.loop(0, HEADS)
    def _(h):
        lane, offset = head_window(h)
        mask = head_mask(rows, offset)
        lanes = pl.ds(lane, PAIR)
        query = jnp.where(mask, q_ref[:, lanes], jnp.zeros((), BF))
        grad = jnp.where(mask, grad_ref[:, lanes], jnp.zeros((), BF))
        probs = jnp.exp(nt(k_ref[:, lanes], query) * SCALE + bias_ref[...] - logs_t_ref[pl.ds(h, 1)])
        score_ref[...] = probs
        prob_ref[...] = probs.astype(BF)
        prob_grad = nt(v_ref[:, lanes], grad)
        row_total = jnp.sum(score_ref[...] * prob_grad, axis=0, keepdims=True)
        dv_ref[:, lanes] += nn(prob_ref[...], grad)
        prob_ref[...] = (score_ref[...] * (prob_grad - row_total)).astype(BF)
        dk_ref[:, lanes] += nn(prob_ref[...], query)
        part_ref[...] = nn(turned_ref[lanes], prob_ref[...])
        at = pl.ds(pl.multiple_of(h * HEAD_DIM, 8), HEAD_DIM)
        dq_ref[at] = part_ref[pl.ds(pl.multiple_of(offset, 8), HEAD_DIM)]

    dq = dq_ref[...].T * SCALE
    g_query = column_sums(dq)
    dq_b = dq.astype(BF)
    wait(vecs)
    vec = vector_rows(vec1_ref)
    gain, shift = as_row(vec, 0, DC), as_row(vec, DC, DC)
    dk_b_ref, dv_b_ref = k_ref, v_ref
    x_load.wait()
    g_value = jnp.zeros((1, D), F32)
    step = rows // 3

    def rounded(i, total):
        at = pl.ds(pl.multiple_of(i * step, step), step)
        dk_b_ref[at] = (dk_ref[at] * SCALE).astype(BF)
        dv = dv_ref[at]
        dv_b_ref[at] = dv.astype(BF)
        normed, _ = norm_rows(x_ref[at].astype(F32))
        turned_ref[:, at] = (normed * gain + shift).astype(BF).T
        return total + column_sums(dv)

    g_value = lax.fori_loop(0, window // step, rounded, g_value)
    put_vectors(vec2_ref, [g_query, g_value])
    save = copies(where, "vec2", parts_ref, vec2_ref, out_sem, out=True)
    for made in loads:
        wait(made)
    for c in range(0, DC, 2):
        many = min(2, DC - c)
        lanes = slice(c * LANES, (c + many) * LANES)
        part = [panels(w_ref.at[i], 0, DC, many * LANES // ROWS, c * LANES // ROWS) for i in range(3)]

        @pl.loop(0, window // rows)
        def _(b):
            at = pl.ds(b * rows, rows)
            dk_ref[at, lanes] = nt(dk_b_ref[at], part[1]) + nt(dv_b_ref[at], part[2])

        dk_ref[pl.ds(margin, rows), lanes] += nt(dq_b, part[0])
    turned_own = turned_ref[:, pl.ds(margin, rows)]
    for c in range(0, DC, 2):
        many = min(2, DC - c)
        lanes = slice(c * LANES, (c + many) * LANES)
        put_panels(w_ref.at[0], c, nn(turned_own, dq_b[:, lanes]))
        put_panels(w_ref.at[1], c, nn(turned_ref[...], dk_b_ref[:, lanes]))
        put_panels(w_ref.at[2], c, nn(turned_ref[...], dv_b_ref[:, lanes]))
    for i, name in enumerate(names):
        save = save + copies(where, name, parts_ref, w_ref.at[i], out_sem, out=True)
    start(save)

    def norm_block(i, totals):
        at = pl.ds(pl.multiple_of(i * step, step), step)
        normed, inverse = norm_rows(x_ref[at].astype(F32))
        e = dk_ref[at]
        part = norm_rows_back(e, normed, inverse, gain)
        x_ref[at] = part.astype(BF)

        @pl.when((i >= margin // step) & (i < (margin + rows) // step))
        def _():
            own_ref[pl.ds(pl.multiple_of(i * step - margin, step), step)] = part

        return totals[0] + column_sums(e * normed), totals[1] + column_sums(e)

    zero = jnp.zeros((1, D), F32)
    g_gain, g_shift = lax.fori_loop(0, window // step, norm_block, (zero, zero))
    put_vectors(vec1_ref, [g_gain, g_shift])
    last = copies(where, "vec1", parts_ref, vec1_ref, out_sem, out=True)
    last = last + [pltpu.make_async_copy(x_ref, near_ref, x_sem)]
    start(last)
    wait(save + last)


def back(x_win, seg_query, seg_keys, gathered, queries, key_win, value_win, att_grad, logs, parts, where):
    window, rows = x_win.shape[0], queries.shape[0]
    dma = pltpu.SemaphoreType.DMA
    tiles = lambda *n: pltpu.VMEM((*n, ROWS, LANES), BF)
    vm = lambda a, b, t: pltpu.VMEM((a, b), t)
    return pl.pallas_call(
        functools.partial(back_kernel, where),
        out_shape=(
            jax.ShapeDtypeStruct((window, D), BF), jax.ShapeDtypeStruct((rows, D), F32), jax.ShapeDtypeStruct(parts.shape, BF),
        ),
        in_specs=[ANY, VM, VM, ANY, VM, VM, VM, VM, VM, ANY],
        out_specs=[ANY, VM, ANY],
        scratch_shapes=[
            tiles(3, D // ROWS, DC), tiles(2), tiles(2), vm(window, rows, F32), vm(window, rows, F32), vm(window, rows, BF),
            vm(D, window, BF), vm(window, D, F32), vm(window, D, F32), vm(D, rows, F32), vm(PAIR, rows, F32), vm(LANES, rows, F32),
            vm(window, D, BF), dma((3,)), dma, dma, dma,
        ],
        input_output_aliases={9: 2},
        compiler_params=pltpu.CompilerParams(vmem_limit_bytes=VMEM_LIMIT),
        name="back",
    )(x_win, seg_query, seg_keys, gathered, queries, key_win, value_win, att_grad, logs, parts)


HOT_NAMES = ("vec1", "w_query", "w_key", "w_value", "vec2")


def transfer_pieces(plan, depth):
    where = plan[0]
    count = plan[2].shape[0]
    hot, used = [0] * depth, [0] * depth
    for name in where:
        for owner, at, tiles in where[name]:
            level = owner * depth // count
            used[level] = max(used[level], at + tiles)
            if name in HOT_NAMES:
                hot[level] = max(hot[level], at + tiles)
    early = [(level, 0, h) for level, h in enumerate(hot) if h]
    late = [(level, h, u - h) for level, (h, u) in enumerate(zip(hot, used)) if h < u]
    return early, late


def cut(piece, many):
    level, first, tiles = piece
    half = tiles // 2
    edges = [half * i // (many // 2) for i in range(many // 2)] + [
        half + (tiles - half) * i // (many // 2) for i in range(many // 2 + 1)
    ]
    return [(level, first + a, b - a) for a, b in zip(edges[:-1], edges[1:])]


def gather_front_kernel(
    depth, where, early, late,
    block_ref, x_in_ref, segq_ref, segk_ref,
    out_ref, x_out_ref, turned_out_ref, keys_out_ref, k_out_ref, v_out_ref, x_got_ref, q_ref, attended_ref, rest_ref, logs_ref,
    z_send, z_recv, x_send, x_recv, y_send, y_recv, corner_send, corner_recv, line_send, line_recv, mate_send, mate_recv, w_send, w_recv,
    local_sem, stage_ref, k_ref, v_ref, x_ref, turned_ref, normed_ref, w_ref, vec1_ref, vec2_ref, bias_ref, score_ref, prob_ref, sem, vec_sem, x_sem, keys_sem,
):
    me = lax.axis_index("fsdp")
    count = 8 * depth
    core, x, y, z = place(me)
    mate, x_near, y_near = index_of(1 - core, x, y, z), index_of(core, 1 - x, y, z), index_of(core, x, 1 - y, z)
    up, down = me + 8, me - 8
    after, before = me + 2, me - 2
    has_after, has_before = after < count, before >= 0
    greet(
        [(mate, None), (x_near, None), (y_near, None), (down, z > 0), (up, z < depth - 1), (after, has_after), (before, has_before)]
    )
    pieces = early + late
    chunks = {p: cut(piece, 4) if piece[0] == 0 and p < len(early) else [piece] for p, piece in enumerate(pieces)}
    chunk_list = [(p, chunk) for p in chunks for chunk in chunks[p]]
    ids = {p: [i for i, (q, _) in enumerate(chunk_list) if q == p] for p in chunks}
    hot, cold = range(len(early)), range(len(early), len(pieces))
    hot_levels = {level for level, _, _ in early}

    def remote(source, target, send, recv, device):
        return pltpu.make_async_remote_copy(
            src_ref=source, dst_ref=target, send_sem=send, recv_sem=recv, device_id=(device,), device_id_type=MESH
        )

    def span(piece):
        return pl.ds(piece[1], piece[2])

    def halves(p):
        level, first, tiles = pieces[p]
        part = tiles // 2 if p in hot else tiles * 2 // 3
        return (level, first, part), (level, first + part, tiles - part)

    def column(level):
        return index_of(core, x, y, level)

    def from_x(level):
        return index_of(core, 1 - x, y, level)

    def from_y(level):
        return index_of(core, x, 1 - y, level)

    def across(level):
        return index_of(core, 1 - x, 1 - y, level)

    def pass_on(block, piece, send, recv, device, own=False):
        there = out_ref.at[block, span(piece)]
        return remote(block_ref.at[span(piece)] if own else there, there, send, recv, device)

    def z_copy(i, upward, own=False):
        piece = chunk_list[i][1]
        return pass_on(column(piece[0]), piece, z_send.at[i, 0 if upward else 1], z_recv.at[i], up if upward else down, own)

    def plane_copies(i, own=False):
        piece = chunk_list[i][1]
        block = column(piece[0])
        return (
            pass_on(block, piece, x_send.at[i], x_recv.at[i], x_near, own),
            pass_on(block, piece, y_send.at[i], y_recv.at[i], y_near, own),
            pass_on(block, piece, mate_send.at[0, i], mate_recv.at[0, i], mate, own),
        )

    def got(block, i, recv):
        piece = chunk_list[i][1]
        pass_on(block, piece, x_send.at[i], recv, me).wait_recv()

    def spread(i, own=False):
        for copy in plane_copies(i, own):
            copy.start()

    def z_pass(i):
        def run(zv):
            level = chunk_list[i][1][0]
            got(column(level), i, z_recv.at[i])
            if level < zv < depth - 1:
                z_copy(i, True).start()
            if 0 < zv < level:
                z_copy(i, False).start()

        return run

    def take(i):
        def run(zv):
            z_pass(i)(zv)
            spread(i)

        return run

    def later_spread(i):
        return lambda zv: spread(i)

    def by_plane(p, zv):
        return True

    def corner_copies(p):
        level = pieces[p][0]
        first, second = halves(p)
        return (
            pass_on(from_x(level), first, corner_send.at[p, 0], corner_recv.at[p, 0], y_near),
            pass_on(from_y(level), second, corner_send.at[p, 1], corner_recv.at[p, 1], x_near),
        )

    def corner_along_z(p, zv):
        level = pieces[p][0]
        ways = [up] * (level <= zv < depth - 1) + [down] * (0 < zv <= level)
        return [
            [
                pass_on(across(level), part, line_send.at[p, 2 * side + (way is up)], line_recv.at[p, side], way)
                for way in ways
            ]
            for side, part in enumerate(halves(p))
        ]

    def mate_copies(p):
        level = pieces[p][0]
        first, second = halves(p)
        return (
            pass_on(from_x(level), pieces[p], mate_send.at[1, p], mate_recv.at[1, p], mate),
            pass_on(from_y(level), pieces[p], mate_send.at[2, p], mate_recv.at[2, p], mate),
            pass_on(across(level), first, mate_send.at[3, p], mate_recv.at[3, p], mate),
            pass_on(across(level), second, mate_send.at[4, p], mate_recv.at[4, p], mate),
        )

    def beside(p):
        def run(zv):
            level = pieces[p][0]
            for i in ids[p]:
                got(from_x(level), i, x_recv.at[i])
            if by_plane(p, zv):
                corner_copies(p)[0].start()
            mate_copies(p)[0].start()
            for i in ids[p]:
                got(from_y(level), i, y_recv.at[i])
            if by_plane(p, zv):
                corner_copies(p)[1].start()
            mate_copies(p)[1].start()

        return run

    def corner(p):
        def run(zv):
            level = pieces[p][0]
            for side, part in enumerate(halves(p)):
                recv = corner_recv if by_plane(p, zv) else line_recv
                pass_on(across(level), part, corner_send.at[p, side], recv.at[p, side], me).wait_recv()
                if not by_plane(p, zv):
                    for copy in corner_along_z(p, zv)[side]:
                        copy.start()
                mate_copies(p)[2 + side].start()

        return run

    def from_mate(p):
        def run(zv):
            level = pieces[p][0]
            other = 1 - 2 * core
            for i in ids[p]:
                pass_on(column(level) + other, chunk_list[i][1], mate_send.at[0, i], mate_recv.at[0, i], me).wait_recv()
            first, second = halves(p)
            for slot, (block, piece) in enumerate(
                ((from_x(level), pieces[p]), (from_y(level), pieces[p]), (across(level), first), (across(level), second))
            ):
                pass_on(block + other, piece, mate_send.at[slot + 1, p], mate_recv.at[slot + 1, p], me).wait_recv()

        return run

    def own_spread(i):
        return lambda zv: spread(i, True)

    def own_up(i):
        return lambda zv: z_copy(i, True, True).start() if zv < depth - 1 else None

    def own_down(i):
        return lambda zv: z_copy(i, False, True).start() if zv > 0 else None

    def w_copy(slot, which, device, source=None):
        return remote(x_in_ref if source is None else source, x_got_ref.at[slot], w_send.at[which], w_recv.at[slot], device)

    def w_far(zv):
        @pl.when(has_after)
        def _():
            w_copy(0, 1, after).start()

        @pl.when(has_before)
        def _():
            w_copy(4, 2, before).start()

    def w_forward(core_index):
        slot = 0 if core_index else 4
        return w_copy(1 if core_index else 3, 3, mate, x_got_ref.at[slot])

    def w_wait(slot):
        w_copy(slot, 0, me).wait_recv()

    def w_middle(zv):
        @pl.when(has_before)
        def _():
            w_wait(0)

        @pl.when(has_after)
        def _():
            w_wait(4)

        @pl.when((core == 1) & has_before)
        def _():
            w_forward(1).start()

        @pl.when((core == 0) & has_after)
        def _():
            w_forward(0).start()

    stops = [61.0, 63.0, 68.0, 73.0, 95.0, 102.0, 110.0] + [110.0 + 2.7 * h for h in range(1, HEADS)]

    def lists(zv):
        own_hot = [p for p in hot if pieces[p][0] == zv]
        own_cold = [p for p in cold if pieces[p][0] == zv]
        far_hot = sorted((p for p in hot if pieces[p][0] != zv), key=lambda p: abs(pieces[p][0] - zv))
        far_cold = sorted((p for p in cold if pieces[p][0] != zv), key=lambda p: (abs(pieces[p][0] - zv), -pieces[p][0]))
        distance = {p: abs(pieces[p][0] - zv) for p in cold}
        at_once = own_cold if zv > depth // 2 else []
        after_hot = [p for p in own_cold if p not in at_once]
        first = []
        for p in own_hot:
            for i in ids[p]:
                first += [own_up(i), own_down(i), own_spread(i)]
        for p in own_cold:
            first += [own_down(i) for i in ids[p]]
        for p in at_once:
            first += [own_spread(i) for i in ids[p]]
        for p in far_hot:
            first += [take(i) for i in ids[p]]
        passed = {p for p in far_cold if distance[p] < 3 and (0 < zv < pieces[p][0] or pieces[p][0] < zv < depth - 1)}
        from_above = [p for p in far_cold if p in passed and pieces[p][0] == zv + 1]
        first += [z_pass(i) for p in from_above for i in ids[p]]
        for p in own_cold:
            first += [own_up(i) for i in ids[p]]
        order_hot = own_hot + far_hot
        first += [beside(p) for p in order_hot]
        first += [z_pass(i) for p in far_cold if p in passed and p not in from_above for i in ids[p]]
        take_or_spread = lambda p: [(later_spread if p in passed else take)(i) for i in ids[p]]
        first.append(w_far)
        for p in after_hot:
            first += [own_spread(i) for i in ids[p]]
        for p in far_cold:
            first += take_or_spread(p) if distance[p] == 1 else []
        first += [corner(p) for p in order_hot]
        first += [from_mate(p) for p in order_hot]
        timed = [(73.0, event) for p in far_cold if distance[p] > 1 for event in take_or_spread(p)]
        order = at_once + after_hot + far_cold
        timed += [((110.0, 120.8, 137.0, 145.0)[min(k, 3)], beside(p)) for k, p in enumerate(order)]
        timed += [((142.4, 150.5, 200.0)[min(k, 2)], corner(p)) for k, p in enumerate(order)]
        return first, sorted(timed, key=lambda entry: entry[0])

    plans = [lists(zv) for zv in range(depth)]

    def each_plane(events_of):
        for zv in range(depth):
            events = events_of(zv)
            if events:

                @pl.when(z == zv)
                def _():
                    for event in events:
                        event(zv)

    w_copy(1 + 2 * core, 0, mate).start()
    fill = pltpu.make_async_copy(block_ref, stage_ref, local_sem)
    fill.start()
    fill.wait()
    keep = pltpu.make_async_copy(stage_ref, out_ref.at[me], local_sem)
    keep.start()
    each_plane(lambda zv: plans[zv][0])
    keep.wait()

    near_sem = x_sem
    def service(stop):
        low = stops[stop - 1] if stop else -1.0
        high = stops[stop] if stop < len(stops) else 1e9
        each_plane(lambda zv: [event for time, event in plans[zv][1] if low < time <= high])

    rows = q_ref.shape[0]
    window = k_ref.shape[0]
    loads = [copies(where, name, out_ref, w_ref.at[i], sem.at[i]) for i, name in enumerate(("w_query", "w_key", "w_value"))]
    vecs = copies(where, "vec1", out_ref, vec1_ref, vec_sem) + copies(where, "vec2", out_ref, vec2_ref, vec_sem)
    start(vecs)
    for made in loads:
        start(made)

    def slot_rows(slot):
        return pl.ds(pl.multiple_of(slot * rows, rows), rows)

    def bring(slot, there=None):
        at = x_ref.at[slot_rows(slot)]
        if there is None:
            pltpu.make_async_copy(x_got_ref.at[slot], at, near_sem).start()
            return

        @pl.when(there)
        def _():
            pltpu.make_async_copy(x_got_ref.at[slot], at, near_sem).start()

        @pl.when(jnp.logical_not(there))
        def _():
            pltpu.make_async_copy(x_in_ref, at, near_sem).start()

    def brought(many):
        for _ in range(many):
            pltpu.make_async_copy(x_in_ref, x_ref.at[slot_rows(0)], near_sem).wait()

    mate_slot, far_slot = 3 - 2 * core, 1 + 2 * core
    w_wait(mate_slot)
    pltpu.make_async_copy(x_in_ref, x_ref.at[slot_rows(2)], near_sem).start()
    bring(mate_slot)
    brought(2)
    wait(vecs)
    vec = vector_rows(vec1_ref)
    gain, shift = as_row(vec, 0, DC), as_row(vec, DC, DC)
    biases = vector_rows(vec2_ref)
    zero = jnp.zeros((1, D), F32)
    step = rows // 3

    @pl.loop(0, rows // 8)
    def _(i):
        at = pl.ds(i * 8, 8)
        bias_ref[at] = jnp.where(segq_ref[at] == segk_ref[...], 0.0, NEG)

    def norm_slots(slots):
        for slot in slots:

            @pl.loop(0, rows // step)
            def _(i):
                at = pl.ds(pl.multiple_of(slot * rows + i * step, step), step)
                normed, _ = norm_rows(x_ref[at].astype(F32))
                turned_ref[:, at] = normed.astype(BF).T
                normed_ref[at] = (normed * gain + shift).astype(BF)

    def project(i, out, add, slots):
        for c in range(0, DC, 2):
            many = min(2, DC - c)
            lanes = slice(c * LANES, (c + many) * LANES)
            weights = panels(w_ref.at[i], c, many, D // ROWS)
            for slot in slots:
                at = slot_rows(slot)
                value = (nn(normed_ref[at], weights) + add[:, lanes]).astype(BF)
                if i == 0:
                    out[:, lanes] = value
                else:
                    out[at, lanes] = value

    norm_slots([2, mate_slot])
    service(0)
    for made in loads:
        wait(made)
    v_add = as_row(biases, DC, DC)
    project(0, q_ref, as_row(biases, 0, DC), [2])
    service(1)
    project(1, k_ref, zero, [2, mate_slot])
    service(2)
    project(2, v_ref, v_add, [2, mate_slot])
    service(3)
    w_middle(None)

    @pl.when((core == 0) & has_before)
    def _():
        w_wait(1)

    @pl.when((core == 1) & has_after)
    def _():
        w_wait(3)

    bring(0, has_before)
    bring(4, has_after)
    bring(far_slot, jnp.where(core == 0, has_before, has_after))
    brought(3)
    others = [0, 4, far_slot]
    norm_slots(others)
    saves = [pltpu.make_async_copy(x_ref, x_out_ref, local_sem), pltpu.make_async_copy(turned_ref, turned_out_ref, local_sem)]
    start(saves)
    service(4)
    project(1, k_ref, zero, others)
    service(5)
    k_save = pltpu.make_async_copy(k_ref, k_out_ref, keys_sem.at[0])
    k_save.start()
    project(2, v_ref, v_add, others)
    v_save = pltpu.make_async_copy(v_ref, v_out_ref, keys_sem.at[1])
    v_save.start()
    wait(saves)

    @pl.loop(0, window // LANES)
    def _(i):
        at = pl.ds(pl.multiple_of(i * LANES, LANES), LANES)
        turned_ref[:, at] = k_ref[at].T

    keys_save = pltpu.make_async_copy(turned_ref, keys_out_ref, keys_sem.at[2])
    keys_save.start()
    attended_ref[...] = jnp.zeros_like(attended_ref)
    rest_ref[...] = jnp.zeros_like(rest_ref)
    logs_ref[...] = jnp.zeros_like(logs_ref)
    lane_l = lax.broadcasted_iota(jnp.int32, logs_ref.shape, 1)

    @pl.loop(0, HEADS)
    def _(h):
        for at_head in range(HEADS):

            @pl.when(h == at_head)
            def _():
                service(6 + at_head)

        lane, offset = head_window(h)
        mask = head_mask(rows, offset)
        lanes = pl.ds(lane, PAIR)
        query = jnp.where(mask, q_ref[:, lanes], jnp.zeros((), BF))
        score_ref[...] = nt(query, k_ref[:, lanes]) * SCALE + bias_ref[...]
        top = jnp.max(score_ref[...], axis=-1, keepdims=True)
        powers = jnp.exp(score_ref[...] - top)
        total = jnp.sum(powers, axis=-1, keepdims=True)
        prob_ref[...] = powers.astype(BF)
        out = nn(prob_ref[...], v_ref[:, lanes]) / total
        rounded = out.astype(BF)
        attended_ref[:, lanes] = jnp.where(mask, rounded, attended_ref[:, lanes])
        rest_ref[:, lanes] = jnp.where(mask, (out - rounded.astype(F32)).astype(BF), rest_ref[:, lanes])
        logs_ref[...] = jnp.where(lane_l == h, top + jnp.log(total), logs_ref[...])

    service(len(stops))
    each_plane(lambda zv: [from_mate(p) for p in cold])

    def sent(zv):
        for i, (p, piece) in enumerate(chunk_list):
            for copy in plane_copies(i):
                copy.wait_send()
            level = piece[0]
            if zv < depth - 1 and level <= zv:
                z_copy(i, True).wait_send()
            if zv > 0 and level >= zv:
                z_copy(i, False).wait_send()
        for p in range(len(pieces)):
            for copy in mate_copies(p) + (corner_copies(p) if by_plane(p, zv) else ()):
                copy.wait_send()
            for copy in sum(corner_along_z(p, zv), []) if not by_plane(p, zv) else []:
                copy.wait_send()

    each_plane(lambda zv: [sent])
    w_copy(0, 0, mate).wait_send()

    @pl.when(has_after)
    def _():
        w_copy(0, 1, after).wait_send()

    @pl.when(has_before)
    def _():
        w_copy(4, 2, before).wait_send()

    @pl.when(jnp.where(core == 1, has_before, has_after))
    def _():
        w_forward(0).wait_send()

    wait([k_save, v_save, keys_save])


def gather_front(block, block_input, seg_query, seg_keys, plan):
    where = plan[0]
    count = lax.axis_size("fsdp")
    depth = count // 8
    rows, window = block_input.shape[0], seg_keys.shape[1]
    early, whole = transfer_pieces(plan, depth)
    late = whole
    shape = lambda n, d=D, t=BF: jax.ShapeDtypeStruct((n, d), t)
    dma = pltpu.SemaphoreType.DMA
    units = D // ROWS
    many = len(early) + len(late)
    chunks = many + 3 * sum(1 for piece in early if piece[0] == 0)
    got = jax.ShapeDtypeStruct((5, rows, D), BF)
    return pl.pallas_call(
        functools.partial(gather_front_kernel, depth, where, early, late),
        out_shape=(
            jax.ShapeDtypeStruct((count, *block.shape), BF), shape(window), shape(D, window), shape(D, window), shape(window), shape(window), got,
            shape(rows), shape(rows), shape(rows), shape(rows, LANES, F32),
        ),
        in_specs=[ANY, ANY, VM, VM],
        out_specs=[ANY] * 7 + [VM] * 4,
        scratch_shapes=[
            dma((chunks, 2)), dma((chunks,)), dma((chunks,)), dma((chunks,)), dma((chunks,)), dma((chunks,)),
            dma((many, 2)), dma((many, 2)), dma((many, 4)), dma((many, 2)), dma((5, chunks)), dma((5, chunks)), dma((4,)), dma((5,)),
            dma, pltpu.VMEM(block.shape, BF), pltpu.VMEM((window, D), BF), pltpu.VMEM((window, D), BF),
            pltpu.VMEM((window, D), BF), pltpu.VMEM((D, window), BF), pltpu.VMEM((window, D), BF),
            pltpu.VMEM((3, units, DC, ROWS, LANES), BF), pltpu.VMEM((2, ROWS, LANES), BF), pltpu.VMEM((2, ROWS, LANES), BF),
            pltpu.VMEM((rows, window), F32), pltpu.VMEM((rows, window), F32), pltpu.VMEM((rows, window), BF), dma((3,)), dma, dma, dma((3,)),
        ],
        compiler_params=pltpu.CompilerParams(collective_id=0, has_side_effects=True, vmem_limit_bytes=VMEM_LIMIT),
        name="gather_front",
    )(block, block_input, seg_query, seg_keys)


def back_scatter_kernel(
    depth, where, early, late,
    x_hbm_ref, turned_hbm_ref, keys_hbm_ref, segq_ref, segk_ref, blocks_ref, q_ref, k_hbm_ref, v_hbm_ref, grad_ref, logs_ref, delta_ref, mid_hbm_ref, parts_in_ref,
    parts_ref, out_ref, in_grad_ref, mates, sums, halfs, fulls, lines, near_ref, near_got,
    w_ref, g_ref, vec1_ref, vec2_ref, score_ref, prob_ref, turned_ref, k_ref, v_ref, dq_ref, part_ref, logs_t_ref, x_ref,
    block_ref, mid_ref, g_value_ref, gain_acc, shift_acc, stage, total,
    mate_send, mate_recv, half_send, half_recv, full_send, full_recv, line_send, line_recv, near_send, near_recv,
    load_sem, store_sem, sem, vec_sem, out_sem, x_sem,
):
    me = lax.axis_index("fsdp")
    count = 8 * depth
    core, x, y, z = place(me)
    mate, x_near, y_near = index_of(1 - core, x, y, z), index_of(core, 1 - x, y, z), index_of(core, x, 1 - y, z)
    after, before = me + 2, me - 2
    has_after, has_before = after < count, before >= 0
    greet(
        [(mate, None), (x_near, None), (y_near, None), (me - 8, z > 0), (me + 8, z < depth - 1), (after, has_after), (before, has_before)]
    )
    pieces = early + late
    block_tiles = parts_ref.shape[1]
    early_ids, late_ids = range(len(early)), range(len(early), len(pieces))

    def remote(source, target, send, recv, device):
        return pltpu.make_async_remote_copy(
            src_ref=source, dst_ref=target, send_sem=send, recv_sem=recv, device_id=(device,), device_id_type=MESH
        )

    def owner(level, slot, which_core):
        return index_of(which_core, 1 - x if slot in (1, 3) else x, 1 - y if slot in (2, 3) else y, level)

    def at_plane(zv, run):
        @pl.when(z == zv)
        def _():
            run()

    def span(p, lo=0, many=None):
        _, first, tiles = pieces[p]
        return pl.ds(first + lo, tiles if many is None else many)

    def half_of(p):
        return pieces[p][2] // 2

    def to_mate(p, slot):
        level = pieces[p][0]
        return remote(
            parts_ref.at[owner(level, slot, 1 - core), span(p)], mates.at[level, slot, span(p)],
            mate_send.at[p, slot], mate_recv.at[p, slot], mate,
        )

    def half_out(p, side):
        level, _, tiles = pieces[p]
        part = span(p, half_of(p), tiles - half_of(p)) if side else span(p, 0, half_of(p))
        return remote(
            sums.at[level, 3, part], halfs.at[level, side, part], half_send.at[p, side], half_recv.at[p, side],
            x_near if side else y_near,
        )

    def full_out(p, side):
        level = pieces[p][0]
        return remote(
            sums.at[level, 1 + side, span(p)], fulls.at[level, side, span(p)], full_send.at[p, side], full_recv.at[p, side],
            y_near if side else x_near,
        )

    def subs(p):
        tiles = pieces[p][2]
        if p in early_ids or tiles < block_tiles // 3:
            return [(0, tiles)]
        return [(0, tiles // 2), (tiles // 2, tiles - tiles // 2)]

    def line_out(p, zv, sub):
        level = pieces[p][0]
        part = span(p, *subs(p)[sub])
        upward = level > zv
        slot = depth if not upward and level == zv - 1 else level
        side = 1 if slot == depth else 0
        return remote(
            sums.at[level, 0, part], lines.at[slot, part], line_send.at[p, sub], line_recv.at[p, 2 * sub + side],
            me + 8 if upward else me - 8,
        )

    def line_in(p, side, sub):
        level = pieces[p][0]
        slot = depth if side else level
        part = span(p, *subs(p)[sub])
        return remote(sums.at[level, 0, part], lines.at[slot, part], line_send.at[p, sub], line_recv.at[p, 2 * sub + side], me)

    def line_sides(p, zv):
        level = pieces[p][0]
        if level > zv:
            return [0] if zv > 0 else []
        if level < zv:
            return [0] if zv < depth - 1 else []
        return ([0] if zv > 0 else []) + ([1] if zv < depth - 1 else [])

    def extent(job):
        kind, p, sub = job
        return subs(p)[sub] if kind == 0 else (0, pieces[p][2])

    def sources(job, zv):
        kind, p, sub = job
        level, _, tiles = pieces[p]
        h = half_of(p)
        if kind == 0:
            lo, many = extent(job)
            part = span(p, lo, many)
            refs = [parts_ref.at[owner(level, 0, core), part], mates.at[level, 0, part]]
            refs += [fulls.at[level, side, part] for side in (0, 1)]
            refs += [lines.at[depth if side else level, part] for side in line_sides(p, zv)]
            return [(ref, 0, many) for ref in refs]
        found = [(parts_ref.at[owner(level, kind, core), span(p)], 0, tiles), (mates.at[level, kind, span(p)], 0, tiles)]
        if kind == 1:
            found.append((halfs.at[level, 0, span(p, 0, h)], 0, h))
        if kind == 2:
            found.append((halfs.at[level, 1, span(p, h, tiles - h)], h, tiles - h))
        return found

    def loads(job, zv, base):
        return [
            pltpu.make_async_copy(ref, stage.at[i, pl.ds(base + lo, many)], load_sem.at[1 if base else 0])
            for i, (ref, lo, many) in enumerate(sources(job, zv))
        ]

    def store(job, base):
        kind, p, sub = job
        lo, many = extent(job)
        return pltpu.make_async_copy(
            total.at[pl.ds(base, many)], sums.at[pieces[p][0], kind, span(p, lo, many)], store_sem.at[1 if base else 0]
        )

    def load(job, zv, base=0):
        kind, p, sub = job
        if sub == 0:
            to_mate(p, kind).wait_recv()
        if kind in (1, 2):
            half_out(p, kind - 1).wait_recv()
        made = loads(job, zv, base)
        if kind == 0:
            if sub == 0:
                for side in (0, 1):
                    full_out(p, side).wait_recv()
            start(made[:4])
            for copy, side in zip(made[4:], line_sides(p, zv)):
                line_in(p, side, sub).wait_recv()
                copy.start()
        else:
            start(made)

    def add(base, lo, many, slots, target, shift):
        def some(first, tiles):
            value = stage[slots[0], pl.ds(first, tiles)].astype(F32)
            for slot in slots[1:]:
                value = value + stage[slot, pl.ds(first, tiles)].astype(F32)
            target[pl.ds(first + shift, tiles)] = value.astype(target.dtype)

        group = 8

        @pl.loop(0, many // group)
        def _(i):
            some(base + lo + i * group, group)

        if many % group:
            some(base + lo + many // group * group, many % group)

    def finish(job, zv, base=0):
        kind, p, sub = job
        level, first, tiles = pieces[p]
        found = sources(job, zv)
        wait(loads(job, zv, base))
        final = kind == 0 and level == zv
        target, shift = (out_ref, first + extent(job)[0] - base) if final else (total, 0)
        edges = sorted({e for _, lo, many in found for e in (lo, lo + many)})
        for lo, hi in zip(edges[:-1], edges[1:]):
            slots = [i for i, (_, a, many) in enumerate(found) if a <= lo and hi <= a + many]
            add(base, lo, hi - lo, slots, target, shift)
        if not final:
            store(job, base).start()

    def send(job, zv, base=0):
        kind, p, sub = job
        if kind == 0 and pieces[p][0] == zv:
            return
        store(job, base).wait()
        if kind == 3:
            half_out(p, 0).start()
            half_out(p, 1).start()
        elif kind == 0:
            line_out(p, zv, sub).start()
        else:
            full_out(p, kind - 1).start()

    second = block_tiles // 2

    def run(jobs, zv):
        for job in jobs:
            load(job, zv)
            finish(job, zv)
            send(job, zv)

    def run_ahead(jobs, zv):
        bases = [second * (k % 2) for k in range(len(jobs))]
        for k, job in enumerate(jobs):
            if k == 0:
                load(job, zv, bases[k])
            if k + 1 < len(jobs):
                load(jobs[k + 1], zv, bases[k + 1])
            finish(job, zv, bases[k])
            if k:
                send(jobs[k - 1], zv, bases[k - 1])
        send(jobs[-1], zv, bases[-1])

    def along(p):
        return [(0, p, sub) for sub in range(len(subs(p)))]

    for p in early_ids:
        for slot in (3, 1, 2, 0):
            to_mate(p, slot).start()

    window, rows = k_ref.shape[0], q_ref.shape[0]
    margin = (window - rows) // 2
    names = ("w_query", "w_key", "w_value")
    k_load = [
        pltpu.make_async_copy(a, b, vec_sem)
        for a, b in ((k_hbm_ref, k_ref), (v_hbm_ref, v_ref), (keys_hbm_ref, turned_ref))
    ]
    start(k_load)
    weight_loads = [copies(where, name, blocks_ref, w_ref.at[i], sem.at[i]) for i, name in enumerate(names)]
    vecs = copies(where, "vec1", blocks_ref, vec1_ref, sem.at[3])
    start(vecs)
    for made in weight_loads:
        start(made)
    x_load = [pltpu.make_async_copy(x_hbm_ref, x_ref, x_sem)]
    start(x_load)
    logs_t_ref[...] = logs_ref[...].T * LOG2E
    g_value_ref[...] = jnp.zeros_like(g_value_ref)

    by_level = {pieces[p][0]: p for p in early_ids}
    a, b, c_ = (by_level[level] for level in sorted(by_level, reverse=True)[:3])
    table = [
        (-1, 0, 3, a, None), (0, 1, 3, b, None), (3, 4, 1, a, None), (4, 5, 2, a, None), (5, 6, 3, c_, None),
        (6, 7, 1, b, None), (7, 8, 2, b, None), (11, 12, 0, a, 0), (12, 13, 1, c_, None), (13, 14, 2, c_, None),
    ]

    def beside(h, which, action):
        for entry in table:
            if entry[which] < 0:
                continue
            kind, p, zv = entry[2:]
            job = (kind, p, 0)
            there = h == entry[which]
            if zv is not None:
                there = there & (z == zv)

            @pl.when(there)
            def _():
                action(job, zv)

    wait(k_load)
    load((3, a, 0), None)

    @pl.loop(0, HEADS)
    def _(h):
        beside(h, 1, finish)
        lane, offset = head_window(h)
        mask = head_mask(rows, offset)
        lanes = pl.ds(lane, PAIR)
        query = jnp.where(mask, q_ref[:, lanes], jnp.zeros((), BF))
        grad = jnp.where(mask, grad_ref[:, lanes], jnp.zeros((), BF))
        log_row, delta_row = logs_t_ref[pl.ds(h, 1)], delta_ref[pl.ds(h, 1)]
        blocks = [pl.ds(n * rows, rows) for n in range(window // rows)]
        for keys in blocks:
            together = jnp.concatenate([segk_ref[keys]] * (rows // LANES), axis=1) == segq_ref[...]
            probs = jnp.exp2(jnp.where(together, nt(k_ref[keys, lanes], query) * (SCALE * LOG2E) - log_row, NEG))
            prob_ref[keys] = probs.astype(BF)
            score_ref[keys] = (probs * (nt(v_ref[keys, lanes], grad) - delta_row)).astype(BF)
        beside(h, 1, send)
        beside(h, 0, load)
        side = head_mask(rows, offset)
        for keys in blocks:
            dv = nn(prob_ref[keys], grad)
            g_value_ref[:, lanes] += column_sums(dv)
            v_ref[keys, lanes] = jnp.where(side, dv.astype(BF), v_ref[keys, lanes])
            dk = nn(score_ref[keys], query) * SCALE
            k_ref[keys, lanes] = jnp.where(side, dk.astype(BF), k_ref[keys, lanes])
        tile = (h * HEAD_DIM) // ROWS * ROWS
        part_ref[...] = nn(turned_ref[pl.ds(pl.multiple_of(tile, ROWS), part_ref.shape[0])], score_ref[...])
        at = pl.ds(pl.multiple_of(h * HEAD_DIM, 8), HEAD_DIM)
        dq_ref[at] = part_ref[pl.ds(pl.multiple_of(h * HEAD_DIM - tile, 8), HEAD_DIM)]

    turned_load = pltpu.make_async_copy(turned_hbm_ref, turned_ref, vec_sem)
    turned_load.start()
    dq = dq_ref[...].T * SCALE
    put_vectors(vec2_ref, [column_sums(dq), g_value_ref[...]])
    saves = copies(where, "vec2", parts_ref, vec2_ref, out_sem.at[3], out=True)
    dq_b = dq.astype(BF)
    wait(vecs)
    vec = vector_rows(vec1_ref)
    gain, shift = as_row(vec, 0, DC), as_row(vec, DC, DC)
    gain_t, shift_t = (jnp.broadcast_to(v, (8, D)).T[:, :1] for v in (gain, shift))
    wait(x_load)
    step = rows // 3

    turned_load.wait()
    for made in weight_loads:
        wait(made)
    gain_acc[...] = jnp.zeros_like(gain_acc)
    shift_acc[...] = jnp.zeros_like(shift_acc)

    later = {
        (1, 0): [("load", [(1, a), (0, b), (3, b)])], (1, 1): [("end", [(1, a), (0, b), (3, b)])],
        (2, 0): [("load", [(0, c_), (3, c_)])],
    }

    def plane_job(what, entries):
        for zv, p in entries:

            def go():
                job = (0, p, 0)
                if what == "load":
                    load(job, zv)
                else:
                    finish(job, zv)
                    send(job, zv)

            at_plane(zv, go)

    own = turned_ref[:, pl.ds(margin, rows)]
    made = []
    for i, (left, right_ref) in enumerate(((own, None), (turned_ref, k_ref), (turned_ref, v_ref))):
        if i == 2:
            wait(made[0])
        for pair, c in enumerate(range(0, DC, 2)):
            for what, entries in later.get((i, pair), []):
                plane_job(what, entries)
            many = min(2, DC - c)
            lanes = slice(c * LANES, (c + many) * LANES)
            right = dq_b[:, lanes] if right_ref is None else right_ref[:, lanes]
            raw = nn(left[...], right)
            summed = column_sums(right.astype(F32))
            put_panels(g_ref.at[i % 2], c, gain_t * raw + shift_t * summed)
            weights = panels(w_ref.at[i], c, many, D // ROWS).astype(F32)
            scaled, shifted = weights * raw, weights * summed
            for j in range(many):
                part = slice(j * LANES, (j + 1) * LANES)
                gain_acc[...] += scaled[:, part]
                shift_acc[...] += shifted[:, part]
        made.append(copies(where, names[i], parts_ref, g_ref.at[i % 2], out_sem.at[i], out=True))
        start(made[i])
    put_vectors(vec1_ref, [column_sums(gain_acc[...].T), column_sums(shift_acc[...].T)])
    saves = saves + copies(where, "vec1", parts_ref, vec1_ref, out_sem.at[3], out=True)
    start(saves)
    plane_job("end", [(0, c_), (3, c_)])
    wait(saves + made[1] + made[2])
    for slots in ((3,), (1, 2), (0,)):
        for p in late_ids:
            for slot in slots:
                to_mate(p, slot).start()

    def row_block(n):
        first = n * rows
        own = n == window // rows // 2
        for c in range(0, DC, 2):
            many = min(2, DC - c)
            lanes = slice(c * LANES, (c + many) * LANES)
            part = lambda i: panels(w_ref.at[i], 0, DC, many * LANES // ROWS, c * LANES // ROWS)
            value = nt(k_ref[first : first + rows], part(1)) + nt(v_ref[first : first + rows], part(2))
            if own:
                value = value + nt(dq_b, part(0))
            block_ref[:, lanes] = value

        @pl.loop(0, rows // step)
        def _(i):
            here = pl.ds(pl.multiple_of(i * step, step), step)
            there = pl.ds(pl.multiple_of(first + i * step, step), step)
            normed, inverse = norm_rows(x_ref[there].astype(F32))
            result = norm_rows_back(block_ref[here], normed, inverse, gain)
            if own:
                block_ref[here] = result
            else:
                x_ref[there] = result.astype(BF)

    def near_rows(slot):
        return x_ref.at[pl.ds(slot * rows, rows)]

    def near_save(slot):
        return pltpu.make_async_copy(near_rows(slot), near_ref.at[slot], x_sem)

    def near_copy(slot, which, device):
        return remote(near_ref.at[slot], near_got.at[which], near_send.at[which], near_recv.at[which], device)

    row_block(0)
    run_ahead([(3, p, 0) for p in late_ids], None)
    row_block(4)
    ends = [near_save(0), near_save(4)]
    start(ends)
    at_plane(1, lambda: run([(0, b, 0)], 1))
    at_plane(2, lambda: run([(0, a, 0), (0, c_, 0)], 2))
    for p in late_ids:
        run_ahead([(1, p, 0), (2, p, 0)], None)
    row_block(1)
    row_block(3)
    wait(ends)
    sides = [near_save(1), near_save(3)]
    start(sides)
    wait(sides)
    to_mate_itself, to_mate_shared = (3 - 2 * core), (1 + 2 * core)
    near_copy(to_mate_itself, 0, mate).start()
    near_copy(to_mate_shared, 1, mate).start()

    @pl.when((core == 0) & has_before)
    def _():
        near_copy(0, 2, before).start()

    @pl.when((core == 1) & has_after)
    def _():
        near_copy(4, 3, after).start()

    row_block(2)
    near_copy(0, 1, me).wait_recv()
    shared_slot = 4 - 4 * core
    fetch = pltpu.make_async_copy(near_got.at[1], k_ref.at[pl.ds(0, rows)], x_sem)
    fetch.start()
    fetch.wait()

    @pl.loop(0, rows // step)
    def _(i):
        here = pl.ds(pl.multiple_of(i * step, step), step)
        there = pl.ds(pl.multiple_of(shared_slot * rows + i * step, step), step)
        x_ref[there] = (x_ref[there].astype(F32) + k_ref[here].astype(F32)).astype(BF)

    shared_save = near_save(shared_slot)
    shared_save.start()
    shared_save.wait()

    @pl.when((core == 0) & has_after)
    def _():
        near_copy(4, 3, after).start()

    @pl.when((core == 1) & has_before)
    def _():
        near_copy(0, 2, before).start()

    def tail(zv):
        out = [p for p in late_ids if pieces[p][0] != zv]
        hops = lambda p: zv if pieces[p][0] > zv else depth - 1 - zv
        moving = [job for p in sorted(out, key=lambda p: (hops(p), p)) for job in along(p)]
        own = [p for ids in (early_ids, late_ids) for p in ids if pieces[p][0] == zv]
        return moving + [job for p in own for job in along(p)]

    for zv in range(depth):
        at_plane(zv, lambda: run(tail(zv), zv))

    near_copy(0, 0, me).wait_recv()

    @pl.when(has_after)
    def _():
        near_copy(0, 2, me).wait_recv()

    @pl.when(has_before)
    def _():
        near_copy(0, 3, me).wait_recv()

    for i, (which, there) in enumerate(((0, None), (2, has_after), (3, has_before))):
        target = k_ref.at[pl.ds(i * rows, rows)]
        if there is None:
            pltpu.make_async_copy(near_got.at[which], target, x_sem).start()
            continue

        @pl.when(there)
        def _():
            pltpu.make_async_copy(near_got.at[which], target, x_sem).start()

        @pl.when(jnp.logical_not(there))
        def _():
            pltpu.make_async_copy(near_ref.at[0], target, x_sem).start()

    for i in range(3):
        pltpu.make_async_copy(near_got.at[0], k_ref.at[pl.ds(i * rows, rows)], x_sem).wait()
    near_after, near_before = (jnp.where(there, 1.0, 0.0) for there in (has_after, has_before))

    @pl.loop(0, rows // step)
    def _(i):
        here = pl.ds(pl.multiple_of(i * step, step), step)
        fetch_mid = pltpu.make_async_copy(mid_hbm_ref.at[here], mid_ref, x_sem)
        fetch_mid.start()
        fetch_mid.wait()
        value = mid_ref[...] + block_ref[here] + k_ref[here].astype(F32)
        value = value + near_after * k_ref[pl.ds(pl.multiple_of(rows + i * step, step), step)].astype(F32)
        value = value + near_before * k_ref[pl.ds(pl.multiple_of(2 * rows + i * step, step), step)].astype(F32)
        in_grad_ref[here] = value.astype(BF)

    for p in range(len(pieces)):
        for slot in range(4):
            to_mate(p, slot).wait_send()
        for side in (0, 1):
            half_out(p, side).wait_send()
            full_out(p, side).wait_send()
        for zv in range(depth):
            if pieces[p][0] != zv:
                at_plane(zv, lambda: [line_out(p, zv, sub).wait_send() for sub in range(len(subs(p)))])
    near_copy(0, 0, mate).wait_send()
    near_copy(0, 1, mate).wait_send()

    @pl.when(has_before)
    def _():
        near_copy(0, 2, before).wait_send()

    @pl.when(has_after)
    def _():
        near_copy(4, 3, after).wait_send()


def back_scatter(x_win, turned, turned_keys, seg_query, seg_keys, gathered, queries, key_win, value_win, att_grad, logs, delta, mid_grad, parts, plan):
    where, block = plan[:2]
    window, rows = x_win.shape[0], queries.shape[0]
    seg_keys = jnp.broadcast_to(seg_keys, (window, LANES))
    count = lax.axis_size("fsdp")
    depth = count // 8
    hot, cold = transfer_pieces(plan, depth)
    early = sorted(cold, reverse=True)
    late = []
    for piece in sorted(hot, reverse=True):
        late += cut(piece, 2) if piece[2] > block // 2 else [piece]
    many = len(early) + len(late)
    dma = pltpu.SemaphoreType.DMA
    tiles = lambda *n: pltpu.VMEM((*n, ROWS, LANES), BF)
    vm = lambda a, b, t: pltpu.VMEM((a, b), t)
    hbm = lambda *n: jax.ShapeDtypeStruct((*n, ROWS, LANES), BF)
    return pl.pallas_call(
        functools.partial(back_scatter_kernel, depth, where, early, late),
        out_shape=(
            jax.ShapeDtypeStruct(parts.shape, BF), jax.ShapeDtypeStruct((block, ROWS, LANES), F32), jax.ShapeDtypeStruct((rows, D), BF),
            hbm(depth, 4, block), hbm(depth, 4, block), hbm(depth, 2, block), hbm(depth, 2, block), hbm(depth + 1, block),
            jax.ShapeDtypeStruct((5, rows, D), BF), jax.ShapeDtypeStruct((4, rows, D), BF),
        ),
        in_specs=[ANY, ANY, ANY, VM, VM, ANY, VM, ANY, ANY, VM, VM, VM, ANY, ANY],
        out_specs=[ANY, VM, VM] + [ANY] * 7,
        scratch_shapes=[
            tiles(3, D // ROWS, DC), tiles(2, D // ROWS, DC), tiles(2), tiles(2),
            vm(window, rows, BF), vm(window, rows, BF), vm(D, window, BF), vm(window, D, BF), vm(window, D, BF),
            vm(D, rows, F32), vm(ROWS * pl.cdiv(HEAD_DIM + 8, ROWS), rows, F32), vm(LANES, rows, F32), vm(window, D, BF), vm(rows, D, F32), vm(rows // 3, D, F32),
            vm(1, D, F32), vm(D, LANES, F32), vm(D, LANES, F32), tiles(6, block), tiles(block),
            dma((many, 4)), dma((many, 4)), dma((many, 2)), dma((many, 2)), dma((many, 2)), dma((many, 2)), dma((many, 2)), dma((many, 4)),
            dma((4,)), dma((4,)), dma((2,)), dma((2,)), dma((4,)), dma, dma((4,)), dma,
        ],
        input_output_aliases={13: 0},
        compiler_params=pltpu.CompilerParams(collective_id=1, has_side_effects=True, vmem_limit_bytes=VMEM_LIMIT),
        name="back_scatter",
    )(x_win, turned, turned_keys, seg_query, seg_keys, gathered, queries, key_win, value_win, att_grad, logs, delta, mid_grad, parts)[1:3]


def passed_along(value, steps):
    count = lax.axis_size("fsdp")
    first, last = (max(0, -steps), min(count, count - steps))
    return lax.ppermute(value, "fsdp", [(source, source + steps) for source in range(first, last)])


def window_of(rows):
    near = [rows if k == 0 else passed_along(rows, -k) for k in range(-REACH, REACH + 1)]
    return jnp.concatenate(near, axis=0)


def shards(kernels, block_input, params, cotangent, segment_ids):
    count = lax.axis_size("fsdp")
    me = lax.axis_index("fsdp")
    rows = block_input.shape[0]
    margin = REACH * rows
    seg_pad = jnp.pad(segment_ids, (margin, margin), constant_values=-1)
    seg_query = lax.dynamic_slice_in_dim(segment_ids, me * rows, rows, 0)
    seg_keys = lax.dynamic_slice_in_dim(seg_pad, me * rows, 2 * margin + rows, 0)
    plan = wire_plan(count, params.shape[1])
    where = plan[0]
    block = to_tiles(params, plan)
    if kernels:
        gathered, x_win, turned, turned_keys, key_win, value_win, _, queries, attended, rest, logs = gather_front(
            block, block_input, seg_query[:, None], seg_keys[None, :], plan
        )
    else:
        x_win = window_of(block_input)
        gathered = lax.all_gather(block, "fsdp", axis=0, tiled=False)
        queries, key_win, value_win, attended, rest, logs = front(
            x_win, seg_query[:, None], seg_keys[None, :], gathered, where, rows
        )
    activations, mid_grad, att_grad, delta, parts = middle(block_input, cotangent, attended, rest, gathered, where)
    sides = (seg_query[None, :], seg_keys[:, None], gathered, queries, key_win, value_win, att_grad, logs)
    if kernels:
        summed, input_grad = back_scatter(x_win, turned, turned_keys, *sides, delta, mid_grad, parts, plan)
    else:
        near, own, parts = back(x_win, *sides, parts, where)
        input_grad = mid_grad + own
        for k in range(-REACH, REACH + 1):
            if k != 0:
                part = near[(k + REACH) * rows : (k + REACH + 1) * rows]
                input_grad = input_grad + passed_along(part, k).astype(jnp.float32)
        input_grad = input_grad.astype(jnp.bfloat16)
        received = lax.all_to_all(parts, "fsdp", split_axis=0, concat_axis=0, tiled=True)
        summed = jnp.sum(received.astype(jnp.float32), axis=0)
    param_grads = to_flat(summed, plan, params.shape[1])
    return (activations, input_grad, param_grads)


def two_by_two(mesh):
    spans = np.array([device.coords for device in mesh.devices.flat])
    return tuple(spans.max(axis=0) - spans.min(axis=0))[:2] == (1, 1)


def solution(mesh):
    return jax.shard_map(
        functools.partial(shards, two_by_two(mesh)),
        mesh=mesh,
        in_specs=(P("fsdp", None), P(None, "fsdp"), P("fsdp", None), P()),
        out_specs=(P("fsdp", None), P("fsdp", None), P(None, "fsdp")),
        check_vma=False,
    )
```

```python
import functools
import math

import jax
import jax.numpy as jnp
import numpy as np
from jax import lax
from jax.experimental import pallas as pl
from jax.experimental.pallas import tpu as pltpu
from jax.sharding import PartitionSpec as P

D = 1152
HEADS = 16
HEAD_DIM = 72
FF = 4304
REACH = 2


EPS = 1e-06
NEG = -1e30
LANES = 128
ROWS = 16
DC = D // LANES
FC = -(-FF // LANES)
WIDE = FF * ROWS // LANES
HEAD = 544
KIND_A, KIND_D, KIND_L2, KIND_L3, KIND_B = 1, 2, 3, 4, 5
MESH = pl.DeviceIdType.MESH


def units():
    found = []
    offset = 0

    def matrix(name, kind, rows, width, tiles):
        nonlocal offset
        for row in range(0, rows, ROWS):
            found.append((name, kind, offset + row * width, tiles))
        offset += rows * width

    def vectors(name, kind, length, tiles):
        nonlocal offset
        found.append((name, kind, offset, tiles))
        offset += length

    vectors("vec1", KIND_L2, 2 * D, 2)
    matrix("w_query", KIND_A, D, D, DC)
    matrix("w_key", KIND_A, D, D, DC)
    matrix("w_value", KIND_A, D, D, DC)
    vectors("vec2", KIND_L2, 2 * D, 2)
    matrix("w_out", KIND_A, D, D, DC)
    vectors("vec3", KIND_L2, 3 * D, 2)
    matrix("w_up", KIND_B, D, FF, FC)
    vectors("vec4", KIND_L3, FF, 3)
    matrix("w_down", KIND_D, FF, D, DC)
    vectors("vec5", KIND_D, D, DC)
    return found


def unit_width(name):
    return {"vec1": 2 * D, "vec2": 2 * D, "vec3": 3 * D, "vec4": FF, "vec5": D, "w_up": ROWS * FF}.get(
        name, ROWS * D
    )


def wire_plan(count, shard):
    blocks = [[] for _ in range(count)]
    where = {}
    used = [0] * count
    tails = [0] * count
    for name, kind, first, tiles in units():
        owner = first // shard
        where.setdefault(name, []).append((owner, used[owner], tiles))
        blocks[owner].append((kind, (first - owner * shard) // LANES, used[owner]))
        used[owner] += tiles
        tails[owner] = max(0, first + unit_width(name) - (owner + 1) * shard)
    block = max(used)
    block += block % 2
    most = max(len(b) for b in blocks)
    table = np.zeros((count, 3 * most), np.int32)
    for owner, entries in enumerate(blocks):
        for i, entry in enumerate(entries):
            table[owner, 3 * i : 3 * i + 3] = entry
    return where, block, table, np.array(tails, np.int32)


def lane_iota(rows):
    return lax.broadcasted_iota(jnp.int32, (rows, LANES), 1)


def wide_rows():
    return [divmod(row * FF, LANES) for row in range(ROWS)]


SKEW = (D * 0 + 80) % LANES


def rows_from_line(line_ref, flat_ref, first, rows):
    step = 8 * LANES

    @pl.loop(0, rows // 8)
    def _(i):
        part = line_ref[:, pl.ds(pl.multiple_of(i * step, step), step)].astype(jnp.float32)
        flat_ref[pl.ds(first + i * 8, 8)] = part.reshape(8, LANES)

    for row in range(rows // 8 * 8, rows):
        flat_ref[pl.ds(first + row, 1)] = line_ref[:, row * LANES : (row + 1) * LANES].astype(jnp.float32)


def line_from_rows(flat_ref, line_ref, first, rows):
    step = 8 * LANES

    @pl.loop(0, rows // 8)
    def _(i):
        part = flat_ref[pl.ds(first + i * 8, 8)]
        line_ref[:, pl.ds(pl.multiple_of(i * step, step), step)] = part.reshape(1, step)

    for row in range(rows // 8 * 8, rows):
        line_ref[:, row * LANES : (row + 1) * LANES] = flat_ref[pl.ds(first + row, 1)]


def to_tiles_kernel(entries, table_ref, line_ref, head_ref, tile_ref, stage_ref, flat_ref):
    rows = line_ref.shape[1] // LANES
    rows_from_line(line_ref, flat_ref, 0, rows)
    rows_from_line(head_ref, flat_ref, rows, HEAD)

    def unit(i, _):
        kind, src, dst = (table_ref[3 * i + j] for j in range(3))

        @pl.when(kind == KIND_A)
        def _():
            for c in range(DC):
                tile_ref[dst + c] = flat_ref[pl.ds(src + c, ROWS, stride=DC), :].astype(jnp.bfloat16)

        @pl.when(kind == KIND_D)
        def _():
            lane = lane_iota(ROWS)
            for c in range(DC):
                here = flat_ref[pl.ds(src + c, ROWS, stride=DC), :]
                after = flat_ref[pl.ds(src + c + 1, ROWS, stride=DC), :]
                both = jnp.where(lane >= SKEW, here, after)
                tile_ref[dst + c] = pltpu.roll(both, LANES - SKEW, 1).astype(jnp.bfloat16)

        for code, tiles in ((KIND_L2, 2), (KIND_L3, 3)):

            @pl.when(kind == code)
            def _():
                for j in range(tiles):
                    tile_ref[dst + j] = flat_ref[pl.ds(src + ROWS * j, ROWS), :].astype(jnp.bfloat16)

        @pl.when(kind == KIND_B)
        def _():
            tall = 8 * pl.cdiv(FC, 8)
            lane = lane_iota(tall)
            row = lax.broadcasted_iota(jnp.int32, (tall, LANES), 0)
            keep = (row < FC - 1) | (lane < FF % LANES)
            for r, (base, skew) in enumerate(wide_rows()):
                part = flat_ref[pl.ds(src + base, tall), :]
                if skew:
                    after = flat_ref[pl.ds(src + base + 1, tall), :]
                    part = pltpu.roll(jnp.where(lane >= skew, part, after), LANES - skew, 1)
                stage_ref[pl.ds(r, tall, stride=ROWS), :] = jnp.where(keep, part, 0.0)
            for c in range(FC):
                tile_ref[dst + c] = stage_ref[pl.ds(ROWS * c, ROWS), :].astype(jnp.bfloat16)

        return 0

    lax.fori_loop(0, entries, unit, 0)


def to_flat_kernel(entries, rows, table_ref, tile_ref, *refs):
    if len(refs) == 5:
        tail_ref, line_ref, stage_ref, flat_ref, first_ref = refs
    else:
        line_ref, stage_ref, flat_ref = refs
    if len(refs) == 5:
        flat_ref[...] = jnp.zeros_like(flat_ref)

    def unit(i, _):
        kind, src, dst = (table_ref[3 * i + j] for j in range(3))

        @pl.when(kind == KIND_A)
        def _():
            for c in range(DC):
                flat_ref[pl.ds(src + c, ROWS, stride=DC), :] = tile_ref[dst + c]

        @pl.when(kind == KIND_D)
        def _():
            lane = lane_iota(ROWS)
            for c in range(DC):
                turned = pltpu.roll(tile_ref[dst + c], SKEW, 1)
                for step, keep in ((0, lane >= SKEW), (1, lane < SKEW)):
                    at = pl.ds(src + c + step, ROWS, stride=DC)
                    flat_ref[at, :] = jnp.where(keep, turned, flat_ref[at, :])

        for code, tiles in ((KIND_L2, 2), (KIND_L3, 3)):

            @pl.when(kind == code)
            def _():
                for j in range(tiles):
                    flat_ref[pl.ds(src + ROWS * j, ROWS), :] = tile_ref[dst + j]

        @pl.when(kind == KIND_B)
        def _():
            tall = 8 * pl.cdiv(FC, 8)
            lane = lane_iota(tall)
            row = lax.broadcasted_iota(jnp.int32, (tall, LANES), 0)
            for c in range(FC):
                stage_ref[pl.ds(ROWS * c, ROWS), :] = tile_ref[dst + c]
            for r, (base, skew) in enumerate(wide_rows()):
                turned = stage_ref[pl.ds(r, tall, stride=ROWS), :]
                if skew:
                    turned = pltpu.roll(turned, skew, 1)
                for step in range(2 if skew else 1):
                    entry = row * LANES + lane + (step * LANES - skew)
                    keep = (lane < skew if step else lane >= skew) & (entry < FF)
                    at = pl.ds(src + base + step, tall)
                    flat_ref[at, :] = jnp.where(keep, turned, flat_ref[at, :])

        return 0

    lax.fori_loop(0, entries, unit, 0)
    if len(refs) == 3:
        line_from_rows(flat_ref, line_ref, rows, HEAD)
        return
    rows_from_line(tail_ref, first_ref, 0, HEAD)
    entry = lax.broadcasted_iota(jnp.int32, (HEAD, LANES), 0) * LANES + lane_iota(HEAD)
    flat_ref[:HEAD] = jnp.where(entry < table_ref[3 * entries], first_ref[...], flat_ref[:HEAD])
    line_from_rows(flat_ref, line_ref, 0, rows)


def my_row(table):
    return lax.dynamic_index_in_dim(jnp.asarray(table), lax.axis_index("fsdp"), 0, keepdims=False)


def relayout_scratch(rows):
    return [
        pltpu.VMEM((ROWS * 8 * pl.cdiv(FC, 8), LANES), jnp.float32),
        pltpu.VMEM((8 * pl.cdiv(rows + HEAD + 8, 8), LANES), jnp.float32),
    ]


def to_tiles(line, plan):
    where, block, table, tails = plan
    count = lax.axis_size("fsdp")
    head = lax.ppermute(line[:, : HEAD * LANES], "fsdp", [(i, (i - 1) % count) for i in range(count)])
    vmem = pl.BlockSpec(memory_space=pltpu.VMEM)
    return pl.pallas_call(
        functools.partial(to_tiles_kernel, table.shape[1] // 3),
        out_shape=jax.ShapeDtypeStruct((block, ROWS, LANES), jnp.bfloat16),
        grid_spec=pltpu.PrefetchScalarGridSpec(
            num_scalar_prefetch=1, grid=(1,), in_specs=[vmem, vmem], out_specs=vmem,
            scratch_shapes=relayout_scratch(line.shape[1] // LANES),
        ),
        name="to_tiles",
    )(my_row(table), line, head)


def to_flat(tiles, plan, length):
    where, block, table, tails = plan
    count = lax.axis_size("fsdp")
    rows = length // LANES
    vmem = pl.BlockSpec(memory_space=pltpu.VMEM)
    last = [max(i for i in range(table.shape[1] // 3) if row[3 * i]) for row in table]
    last = np.stack([row[3 * i : 3 * i + 3] for row, i in zip(table, last)])
    whole = np.concatenate([table, np.roll(tails, 1)[:, None]], axis=1)

    def call(entries, mine, inputs, width, scratch, name):
        return pl.pallas_call(
            functools.partial(to_flat_kernel, entries, rows),
            out_shape=jax.ShapeDtypeStruct((1, width), jnp.float32),
            grid_spec=pltpu.PrefetchScalarGridSpec(
                num_scalar_prefetch=1, grid=(1,), in_specs=[vmem] * len(inputs), out_specs=vmem,
                scratch_shapes=relayout_scratch(rows) + scratch,
            ),
            name=name,
        )(my_row(mine), *inputs)

    tail = call(1, last, (tiles,), HEAD * LANES, [], "tail")
    tail = lax.ppermute(tail, "fsdp", [(i, (i + 1) % count) for i in range(count)])
    return call(table.shape[1] // 3, whole, (tiles, tail), length, [pltpu.VMEM((HEAD, LANES), jnp.float32)], "to_flat")


def place(me):
    return lax.rem(me, 2), lax.rem(me // 2, 2), lax.rem(me // 4, 2), me // 8


def index_of(core, x, y, z):
    return ((z * 2 + y) * 2 + x) * 2 + core


def greet(devices_and_conditions):
    barrier = pltpu.get_barrier_semaphore()
    for device, present in devices_and_conditions:
        if present is None:
            pl.semaphore_signal(barrier, inc=1, device_id=(device,), device_id_type=MESH)
        else:

            @pl.when(present)
            def _():
                pl.semaphore_signal(barrier, inc=1, device_id=(device,), device_id_type=MESH)

    present = [1 if p is None else p.astype(jnp.int32) for _, p in devices_and_conditions]
    pl.semaphore_wait(barrier, sum(present))


BF = jnp.bfloat16
F32 = jnp.float32
PAIR = 2 * LANES
SCALE = HEAD_DIM**-0.5
GELU_A = math.sqrt(2.0 / math.pi)
GELU_B = 0.044715
LOG2E = math.log2(math.e)
ANY = pl.BlockSpec(memory_space=pl.ANY)
VM = pl.BlockSpec(memory_space=pltpu.VMEM)
VMEM_LIMIT = 63 << 20


def nn(left, right):
    return lax.dot_general(left, right, (((1,), (0,)), ((), ())), preferred_element_type=F32)


def nt(left, right):
    return lax.dot_general(left, right, (((1,), (1,)), ((), ())), preferred_element_type=F32)


def runs_of(where, name):
    runs, done = [], 0
    for owner, at, tiles in where[name]:
        if runs and runs[-1][0] == owner and runs[-1][1] + runs[-1][2] == at:
            runs[-1][2] += tiles
        else:
            runs.append([owner, at, tiles, done])
        done += tiles
    return runs


def copies(where, name, blocks_ref, tiles_ref, sem, out=False):
    made = []
    flat_tiles = tiles_ref if len(tiles_ref.shape) == 3 else tiles_ref.reshape(-1, ROWS, LANES)
    for owner, at, tiles, done in runs_of(where, name):
        there, here = blocks_ref.at[owner, pl.ds(at, tiles)], flat_tiles.at[pl.ds(done, tiles)]
        made.append(pltpu.make_async_copy(here, there, sem) if out else pltpu.make_async_copy(there, here, sem))
    return made


def start(made):
    for copy in made:
        copy.start()


def wait(made):
    for copy in made:
        copy.wait()


def panel(tiles_ref, c, units, first=0):
    return tiles_ref[pl.ds(first, units), pl.ds(c, 1)].reshape(units * ROWS, LANES)


def panels(tiles_ref, c, many, units, first=0):
    return jnp.concatenate([panel(tiles_ref, c + i, units, first) for i in range(many)], axis=1)


def put_panel(tiles_ref, c, value, first=0):
    units = value.shape[0] // ROWS
    tiles_ref[pl.ds(first, units), pl.ds(c, 1)] = value.astype(BF).reshape(units, 1, ROWS, LANES)


def put_panels(tiles_ref, c, value, first=0):
    for i in range(value.shape[1] // LANES):
        put_panel(tiles_ref, c + i, value[:, i * LANES : (i + 1) * LANES], first)


def over_pairs(body):
    @pl.loop(0, DC // 2)
    def _(pair):
        body(2 * pair, 2)

    if DC % 2:
        body(DC - 1, 1)


def lanes_of(c, many):
    return pl.ds(c * LANES if isinstance(c, int) else pl.multiple_of(c * LANES, LANES), many * LANES)


def vector_rows(tiles_ref):
    return jnp.concatenate([tiles_ref[i].astype(F32) for i in range(tiles_ref.shape[0])], axis=0)


def as_row(rows, first, many):
    return jnp.concatenate([rows[first + i : first + i + 1] for i in range(many)], axis=1)


def put_vectors(tiles_ref, rows_list):
    parts = [row[:, i * LANES : (i + 1) * LANES] for row in rows_list for i in range(row.shape[1] // LANES)]
    missing = tiles_ref.shape[0] * ROWS - len(parts)
    whole = jnp.concatenate(parts + [jnp.zeros((missing, LANES), F32)] if missing else parts, axis=0)
    for i in range(tiles_ref.shape[0]):
        tiles_ref[i] = whole[i * ROWS : (i + 1) * ROWS].astype(BF)


def norm_rows(values):
    centre = values - jnp.mean(values, axis=-1, keepdims=True)
    inverse = lax.rsqrt(jnp.mean(centre * centre, axis=-1, keepdims=True) + EPS)
    return centre * inverse, inverse


def norm_rows_back(grad, normed, inverse, gain):
    scaled = grad * gain
    return inverse * (
        scaled - jnp.mean(scaled, axis=-1, keepdims=True) - normed * jnp.mean(scaled * normed, axis=-1, keepdims=True)
    )


def column_sums(values):
    return jnp.sum(values, axis=0, keepdims=True)


def head_window(h):
    block = jnp.minimum((h * HEAD_DIM) // LANES, DC - 2)
    lane = pl.multiple_of(block * LANES, LANES)
    return lane, h * HEAD_DIM - lane


def head_mask(rows, offset):
    lane = lax.broadcasted_iota(jnp.int32, (rows, PAIR), 1)
    return (lane >= offset) & (lane < offset + HEAD_DIM)


def front_kernel(
    where, x_ref, segq_ref, segk_ref, blocks_ref, q_ref, k_ref, v_ref, attended_ref, rest_ref, logs_ref,
    normed_ref, w_ref, vec1_ref, vec2_ref, bias_ref, score_ref, prob_ref, sem, vec_sem,
):
    window, rows = x_ref.shape[0], q_ref.shape[0]
    margin = (window - rows) // 2
    loads = [copies(where, name, blocks_ref, w_ref.at[i], sem.at[i]) for i, name in enumerate(("w_query", "w_key", "w_value"))]
    vecs = copies(where, "vec1", blocks_ref, vec1_ref, vec_sem) + copies(where, "vec2", blocks_ref, vec2_ref, vec_sem)
    start(vecs)
    for made in loads:
        start(made)
    wait(vecs)
    vec = vector_rows(vec1_ref)
    gain, shift = as_row(vec, 0, DC), as_row(vec, DC, DC)
    step = rows // 3

    @pl.loop(0, window // step)
    def _(i):
        at = pl.ds(i * step, step)
        normed, _ = norm_rows(x_ref[at].astype(F32))
        normed_ref[at] = (normed * gain + shift).astype(BF)

    @pl.loop(0, rows // 8)
    def _(i):
        at = pl.ds(i * 8, 8)
        bias_ref[at] = jnp.where(segq_ref[at] == segk_ref[...], 0.0, NEG)

    biases = vector_rows(vec2_ref)
    zero = jnp.zeros((1, D), F32)
    for made in loads:
        wait(made)
    for i, (out, add) in enumerate(((q_ref, as_row(biases, 0, DC)), (k_ref, zero), (v_ref, as_row(biases, DC, DC)))):
        for c in range(0, DC, 2):
            many = min(2, DC - c)
            lanes = slice(c * LANES, (c + many) * LANES)
            weights = panels(w_ref.at[i], c, many, D // ROWS)
            if i == 0:
                out[:, lanes] = (nn(normed_ref[pl.ds(margin, rows)], weights) + add[:, lanes]).astype(BF)
            else:

                @pl.loop(0, window // rows)
                def _(b):
                    at = pl.ds(b * rows, rows)
                    out[at, lanes] = (nn(normed_ref[at], weights) + add[:, lanes]).astype(BF)

    attended_ref[...] = jnp.zeros_like(attended_ref)
    rest_ref[...] = jnp.zeros_like(rest_ref)
    logs_ref[...] = jnp.zeros_like(logs_ref)
    lane_l = lax.broadcasted_iota(jnp.int32, logs_ref.shape, 1)

    @pl.loop(0, HEADS)
    def _(h):
        lane, offset = head_window(h)
        mask = head_mask(rows, offset)
        lanes = pl.ds(lane, PAIR)
        query = jnp.where(mask, q_ref[:, lanes], jnp.zeros((), BF))
        score_ref[...] = nt(query, k_ref[:, lanes]) * SCALE + bias_ref[...]
        top = jnp.max(score_ref[...], axis=-1, keepdims=True)
        powers = jnp.exp(score_ref[...] - top)
        total = jnp.sum(powers, axis=-1, keepdims=True)
        prob_ref[...] = powers.astype(BF)
        out = nn(prob_ref[...], v_ref[:, lanes]) / total
        rounded = out.astype(BF)
        attended_ref[:, lanes] = jnp.where(mask, rounded, attended_ref[:, lanes])
        rest_ref[:, lanes] = jnp.where(mask, (out - rounded.astype(F32)).astype(BF), rest_ref[:, lanes])
        logs_ref[...] = jnp.where(lane_l == h, top + jnp.log(total), logs_ref[...])


def front(x_win, seg_query, seg_keys, gathered, where, rows):
    window = x_win.shape[0]
    shape = lambda n, d=D, t=BF: jax.ShapeDtypeStruct((n, d), t)
    dma = pltpu.SemaphoreType.DMA
    units = D // ROWS
    return pl.pallas_call(
        functools.partial(front_kernel, where),
        out_shape=(shape(rows), shape(window), shape(window), shape(rows), shape(rows), shape(rows, LANES, F32)),
        in_specs=[VM, VM, VM, ANY],
        out_specs=[VM] * 6,
        scratch_shapes=[
            pltpu.VMEM((window, D), BF),
            pltpu.VMEM((3, units, DC, ROWS, LANES), BF), pltpu.VMEM((2, ROWS, LANES), BF), pltpu.VMEM((2, ROWS, LANES), BF),
            pltpu.VMEM((rows, window), F32), pltpu.VMEM((rows, window), F32), pltpu.VMEM((rows, window), BF), dma((3,)), dma,
        ],
        compiler_params=pltpu.CompilerParams(vmem_limit_bytes=VMEM_LIMIT),
        name="front",
    )(x_win, seg_query, seg_keys, gathered)


def middle_kernel(
    where, x_ref, cot_ref, attended_ref, rest_ref, blocks_ref, act_ref, mid_grad_ref, att_grad_ref, delta_ref, parts_ref,
    wo_ref, wu_ref, wd_ref, vec3_ref, vec4_ref, vec5_ref, b_up_ref, hidden_ref, slope_ref, pre_ref, normed_ref, normed_b_ref,
    mid_ref, g_up_ref, mid_b_ref, sem, out_sem,
):
    rows = x_ref.shape[0]
    units, f_units = D // ROWS, FF // ROWS
    names = ("w_out", "w_up", "w_down", "vec3", "vec4", "vec5")
    refs = (wo_ref, wu_ref, wd_ref, vec3_ref, vec4_ref, vec5_ref)
    loads = {n: copies(where, n, blocks_ref, r, sem.at[i]) for i, (n, r) in enumerate(zip(names, refs))}
    saves = {n: copies(where, n, parts_ref, r, out_sem, out=True) for n, r in zip(names, refs)}
    for n in ("vec3", "vec4", "vec5", "w_out", "w_up", "w_down"):
        start(loads[n])
    f_wide = FC * LANES
    pads = f_wide // ROWS - f_units
    wd_ref[pl.ds(f_units, pads)] = jnp.zeros((pads, DC, ROWS, LANES), BF)
    for n in ("vec3", "vec4", "vec5", "w_out"):
        wait(loads[n])
    vec = vector_rows(vec3_ref)
    b_out, gain, shift = (as_row(vec, i * DC, DC) for i in range(3))
    vec = vector_rows(vec4_ref)
    entry = lax.broadcasted_iota(jnp.int32, vec.shape, 0) * LANES + lax.broadcasted_iota(jnp.int32, vec.shape, 1)
    b_up_ref[...] = jnp.where(entry < FF, vec, 0.0)
    b_down = jnp.concatenate([vec5_ref[c].astype(F32)[0:1] for c in range(DC)], axis=1)

    for c in range(0, DC, 2):
        many = min(2, DC - c)
        lanes = slice(c * LANES, (c + many) * LANES)
        mid_ref[:, lanes] = (
            x_ref[:, lanes].astype(F32) + nn(attended_ref[...], panels(wo_ref, c, many, units)) + b_out[:, lanes]
        )
    normed, inverse = norm_rows(mid_ref[...])
    normed_ref[...] = normed
    normed_b_ref[...] = (normed * gain + shift).astype(BF)

    wait(loads["w_up"])

    @pl.loop(0, FC // 2)
    def _(p):
        at = pl.ds(pl.multiple_of(p * PAIR, PAIR), PAIR)
        bias = jnp.concatenate([b_up_ref[pl.ds(2 * p, 1)], b_up_ref[pl.ds(2 * p + 1, 1)]], axis=1)
        v = nn(normed_b_ref[...], panels(wu_ref, 2 * p, 2, units)) + bias
        square = v * v
        bent = jnp.tanh(GELU_A * v * (1.0 + GELU_B * square))
        hidden_ref[:, at] = (0.5 * v * (1.0 + bent)).astype(BF)
        slope_ref[:, at] = 0.5 * (1.0 + bent) + 0.5 * v * (1.0 - bent * bent) * (
            GELU_A * (1.0 + 3.0 * GELU_B * square)
        )

    wait(loads["w_down"])
    for c in range(0, DC, 2):
        many = min(2, DC - c)
        lanes = slice(c * LANES, (c + many) * LANES)
        act_ref[:, lanes] = (
            mid_ref[:, lanes] + nn(hidden_ref[...], panels(wd_ref, c, many, f_wide // ROWS)) + b_down[:, lanes]
        ).astype(BF)

    @pl.loop(0, FC // 2)
    def _(p):
        at = pl.ds(pl.multiple_of(p * PAIR, PAIR), PAIR)
        first = p * (PAIR // ROWS)
        grad = nt(cot_ref[...], panels(wd_ref, 0, DC, PAIR // ROWS, first)) * slope_ref[:, at]
        pre_ref[:, at] = grad.astype(BF)
        sums = column_sums(grad)
        g_up_ref[pl.ds(2 * p, 1)] = sums[:, :LANES]
        g_up_ref[pl.ds(2 * p + 1, 1)] = sums[:, LANES:]
        put_panels(wd_ref, 0, nn(hidden_ref[:, at].T, cot_ref[...]), first)

    start(saves["w_down"])
    put_vectors(vec4_ref, [b_up_row for b_up_row in [g_up_ref[i : i + 1] for i in range(FC)]])
    start(saves["vec4"])
    cot = cot_ref[...].astype(F32)
    sums = column_sums(cot)
    row0 = lax.broadcasted_iota(jnp.int32, (ROWS, LANES), 0) == 0
    for c in range(DC):
        vec5_ref[c] = jnp.where(row0, sums[:, c * LANES : (c + 1) * LANES], 0.0).astype(BF)
    start(saves["vec5"])

    for c in range(0, DC, 2):
        many = min(2, DC - c)
        weights = panels(wu_ref, 0, FC, many * LANES // ROWS, c * LANES // ROWS)
        mid_ref[:, c * LANES : (c + many) * LANES] = nt(pre_ref[...], weights)
    turned_b = normed_b_ref[...].T

    @pl.loop(0, FC // 2)
    def _(p):
        at = pl.ds(pl.multiple_of(p * PAIR, PAIR), PAIR)
        put_panels(wu_ref, 2 * p, nn(turned_b, pre_ref[:, at]))

    start(saves["w_up"])
    e = mid_ref[...]
    normed = normed_ref[...]
    g_gain, g_shift = column_sums(e * normed), column_sums(e)
    mid_grad = cot + norm_rows_back(e, normed, inverse, gain)
    mid_grad_ref[...] = mid_grad
    put_vectors(vec3_ref, [column_sums(mid_grad), g_gain, g_shift])
    start(saves["vec3"])
    mid_b = mid_grad.astype(BF)
    mid_b_ref[...] = mid_b

    def attended_grad(c, many):
        weights = panels(wo_ref, 0, DC, many * LANES // ROWS, c * (LANES // ROWS))
        att_grad_ref[:, lanes_of(c, many)] = nt(mid_b_ref[...], weights).astype(BF)

    over_pairs(attended_grad)
    product = att_grad_ref[...].astype(F32) * (attended_ref[...].astype(F32) + rest_ref[...].astype(F32))
    delta_ref[...] = jnp.sum(product.T.reshape(HEADS, HEAD_DIM, rows), axis=1)
    turned = attended_ref[...].T
    over_pairs(lambda c, many: put_panels(wo_ref, c, nn(turned, mid_b_ref[:, lanes_of(c, many)])))
    start(saves["w_out"])
    for n in names:
        wait(saves[n])


def middle(block_input, cotangent, attended, rest, gathered, where):
    rows = block_input.shape[0]
    shape = lambda t: jax.ShapeDtypeStruct((rows, D), t)
    dma = pltpu.SemaphoreType.DMA
    tiles = lambda *n: pltpu.VMEM((*n, ROWS, LANES), BF)
    units, f_wide = D // ROWS, FC * LANES
    return pl.pallas_call(
        functools.partial(middle_kernel, where),
        out_shape=(shape(BF), shape(F32), shape(BF), jax.ShapeDtypeStruct((HEADS, rows), F32), jax.ShapeDtypeStruct(gathered.shape, BF)),
        in_specs=[VM, VM, VM, VM, ANY],
        out_specs=[VM, VM, VM, VM, ANY],
        scratch_shapes=[
            tiles(units, DC), tiles(units, FC), tiles(f_wide // ROWS, DC), tiles(2), tiles(3), tiles(DC),
            pltpu.VMEM((3 * ROWS, LANES), F32), pltpu.VMEM((rows, f_wide), BF), pltpu.VMEM((rows, f_wide), F32),
            pltpu.VMEM((rows, f_wide), BF), pltpu.VMEM((rows, D), F32), pltpu.VMEM((rows, D), BF), pltpu.VMEM((rows, D), F32),
            pltpu.VMEM((3 * ROWS, LANES), F32), pltpu.VMEM((rows, D), BF), dma((6,)), dma,
        ],
        compiler_params=pltpu.CompilerParams(vmem_limit_bytes=VMEM_LIMIT),
        name="middle",
    )(block_input, cotangent, attended, rest, gathered)


def back_kernel(
    where, x_hbm_ref, segq_ref, segk_ref, blocks_ref, q_ref, k_ref, v_ref, grad_ref, logs_ref, parts_in_ref,
    near_ref, own_ref, parts_ref,
    w_ref, vec1_ref, vec2_ref, bias_ref, score_ref, prob_ref, turned_ref, dk_ref, dv_ref, dq_ref, part_ref, logs_t_ref, x_ref,
    sem, vec_sem, out_sem, x_sem,
):
    window, rows = x_ref.shape[0], q_ref.shape[0]
    margin = (window - rows) // 2
    units = D // ROWS
    names = ("w_query", "w_key", "w_value")
    loads = [copies(where, name, blocks_ref, w_ref.at[i], sem.at[i]) for i, name in enumerate(names)]
    vecs = copies(where, "vec1", blocks_ref, vec1_ref, vec_sem)
    start(vecs)
    for made in loads:
        start(made)
    x_load = pltpu.make_async_copy(x_hbm_ref, x_ref, x_sem)
    x_load.start()

    @pl.loop(0, window // LANES)
    def _(i):
        at = pl.ds(pl.multiple_of(i * LANES, LANES), LANES)
        bias_ref[at] = jnp.where(segk_ref[at] == segq_ref[...], 0.0, NEG)
        turned_ref[:, at] = k_ref[at].T
        dk_ref[at] = jnp.zeros((LANES, D), F32)
        dv_ref[at] = jnp.zeros((LANES, D), F32)

    logs_t_ref[...] = logs_ref[...].T

    @pl.loop(0, HEADS)
    def _(h):
        lane, offset = head_window(h)
        mask = head_mask(rows, offset)
        lanes = pl.ds(lane, PAIR)
        query = jnp.where(mask, q_ref[:, lanes], jnp.zeros((), BF))
        grad = jnp.where(mask, grad_ref[:, lanes], jnp.zeros((), BF))
        probs = jnp.exp(nt(k_ref[:, lanes], query) * SCALE + bias_ref[...] - logs_t_ref[pl.ds(h, 1)])
        score_ref[...] = probs
        prob_ref[...] = probs.astype(BF)
        prob_grad = nt(v_ref[:, lanes], grad)
        row_total = jnp.sum(score_ref[...] * prob_grad, axis=0, keepdims=True)
        dv_ref[:, lanes] += nn(prob_ref[...], grad)
        prob_ref[...] = (score_ref[...] * (prob_grad - row_total)).astype(BF)
        dk_ref[:, lanes] += nn(prob_ref[...], query)
        part_ref[...] = nn(turned_ref[lanes], prob_ref[...])
        at = pl.ds(pl.multiple_of(h * HEAD_DIM, 8), HEAD_DIM)
        dq_ref[at] = part_ref[pl.ds(pl.multiple_of(offset, 8), HEAD_DIM)]

    dq = dq_ref[...].T * SCALE
    g_query = column_sums(dq)
    dq_b = dq.astype(BF)
    wait(vecs)
    vec = vector_rows(vec1_ref)
    gain, shift = as_row(vec, 0, DC), as_row(vec, DC, DC)
    dk_b_ref, dv_b_ref = k_ref, v_ref
    x_load.wait()
    g_value = jnp.zeros((1, D), F32)
    step = rows // 3

    def rounded(i, total):
        at = pl.ds(pl.multiple_of(i * step, step), step)
        dk_b_ref[at] = (dk_ref[at] * SCALE).astype(BF)
        dv = dv_ref[at]
        dv_b_ref[at] = dv.astype(BF)
        normed, _ = norm_rows(x_ref[at].astype(F32))
        turned_ref[:, at] = (normed * gain + shift).astype(BF).T
        return total + column_sums(dv)

    g_value = lax.fori_loop(0, window // step, rounded, g_value)
    put_vectors(vec2_ref, [g_query, g_value])
    save = copies(where, "vec2", parts_ref, vec2_ref, out_sem, out=True)
    for made in loads:
        wait(made)
    for c in range(0, DC, 2):
        many = min(2, DC - c)
        lanes = slice(c * LANES, (c + many) * LANES)
        part = [panels(w_ref.at[i], 0, DC, many * LANES // ROWS, c * LANES // ROWS) for i in range(3)]

        @pl.loop(0, window // rows)
        def _(b):
            at = pl.ds(b * rows, rows)
            dk_ref[at, lanes] = nt(dk_b_ref[at], part[1]) + nt(dv_b_ref[at], part[2])

        dk_ref[pl.ds(margin, rows), lanes] += nt(dq_b, part[0])
    turned_own = turned_ref[:, pl.ds(margin, rows)]
    for c in range(0, DC, 2):
        many = min(2, DC - c)
        lanes = slice(c * LANES, (c + many) * LANES)
        put_panels(w_ref.at[0], c, nn(turned_own, dq_b[:, lanes]))
        put_panels(w_ref.at[1], c, nn(turned_ref[...], dk_b_ref[:, lanes]))
        put_panels(w_ref.at[2], c, nn(turned_ref[...], dv_b_ref[:, lanes]))
    for i, name in enumerate(names):
        save = save + copies(where, name, parts_ref, w_ref.at[i], out_sem, out=True)
    start(save)

    def norm_block(i, totals):
        at = pl.ds(pl.multiple_of(i * step, step), step)
        normed, inverse = norm_rows(x_ref[at].astype(F32))
        e = dk_ref[at]
        part = norm_rows_back(e, normed, inverse, gain)
        x_ref[at] = part.astype(BF)

        @pl.when((i >= margin // step) & (i < (margin + rows) // step))
        def _():
            own_ref[pl.ds(pl.multiple_of(i * step - margin, step), step)] = part

        return totals[0] + column_sums(e * normed), totals[1] + column_sums(e)

    zero = jnp.zeros((1, D), F32)
    g_gain, g_shift = lax.fori_loop(0, window // step, norm_block, (zero, zero))
    put_vectors(vec1_ref, [g_gain, g_shift])
    last = copies(where, "vec1", parts_ref, vec1_ref, out_sem, out=True)
    last = last + [pltpu.make_async_copy(x_ref, near_ref, x_sem)]
    start(last)
    wait(save + last)


def back(x_win, seg_query, seg_keys, gathered, queries, key_win, value_win, att_grad, logs, parts, where):
    window, rows = x_win.shape[0], queries.shape[0]
    dma = pltpu.SemaphoreType.DMA
    tiles = lambda *n: pltpu.VMEM((*n, ROWS, LANES), BF)
    vm = lambda a, b, t: pltpu.VMEM((a, b), t)
    return pl.pallas_call(
        functools.partial(back_kernel, where),
        out_shape=(
            jax.ShapeDtypeStruct((window, D), BF), jax.ShapeDtypeStruct((rows, D), F32), jax.ShapeDtypeStruct(parts.shape, BF),
        ),
        in_specs=[ANY, VM, VM, ANY, VM, VM, VM, VM, VM, ANY],
        out_specs=[ANY, VM, ANY],
        scratch_shapes=[
            tiles(3, D // ROWS, DC), tiles(2), tiles(2), vm(window, rows, F32), vm(window, rows, F32), vm(window, rows, BF),
            vm(D, window, BF), vm(window, D, F32), vm(window, D, F32), vm(D, rows, F32), vm(PAIR, rows, F32), vm(LANES, rows, F32),
            vm(window, D, BF), dma((3,)), dma, dma, dma,
        ],
        input_output_aliases={9: 2},
        compiler_params=pltpu.CompilerParams(vmem_limit_bytes=VMEM_LIMIT),
        name="back",
    )(x_win, seg_query, seg_keys, gathered, queries, key_win, value_win, att_grad, logs, parts)


HOT_NAMES = ("vec1", "w_query", "w_key", "w_value", "vec2")


def transfer_pieces(plan, depth):
    where = plan[0]
    count = plan[2].shape[0]
    hot, used = [0] * depth, [0] * depth
    for name in where:
        for owner, at, tiles in where[name]:
            level = owner * depth // count
            used[level] = max(used[level], at + tiles)
            if name in HOT_NAMES:
                hot[level] = max(hot[level], at + tiles)
    early = [(level, 0, h) for level, h in enumerate(hot) if h]
    late = [(level, h, u - h) for level, (h, u) in enumerate(zip(hot, used)) if h < u]
    return early, late


def cut(piece, many):
    level, first, tiles = piece
    half = tiles // 2
    edges = [half * i // (many // 2) for i in range(many // 2)] + [
        half + (tiles - half) * i // (many // 2) for i in range(many // 2 + 1)
    ]
    return [(level, first + a, b - a) for a, b in zip(edges[:-1], edges[1:])]


def gather_front_kernel(
    depth, where, early, late,
    block_ref, x_in_ref, segq_ref, segk_ref,
    out_ref, x_out_ref, turned_out_ref, keys_out_ref, k_out_ref, v_out_ref, x_got_ref, q_ref, attended_ref, rest_ref, logs_ref,
    z_send, z_recv, x_send, x_recv, y_send, y_recv, corner_send, corner_recv, line_send, line_recv, mate_send, mate_recv, w_send, w_recv,
    local_sem, stage_ref, both_ref, x_ref, turned_ref, normed_ref, w_ref, vec1_ref, vec2_ref, bias_ref, score_ref, prob_ref, add_ref, sem, vec_sem, x_sem, keys_sem,
):
    me = lax.axis_index("fsdp")
    count = 8 * depth
    core, x, y, z = place(me)
    mate, x_near, y_near = index_of(1 - core, x, y, z), index_of(core, 1 - x, y, z), index_of(core, x, 1 - y, z)
    up, down = me + 8, me - 8
    after, before = me + 2, me - 2
    has_after, has_before = after < count, before >= 0
    greet(
        [(mate, None), (x_near, None), (y_near, None), (down, z > 0), (up, z < depth - 1), (after, has_after), (before, has_before)]
    )
    pieces = early + late
    chunks = {p: cut(piece, 4) if piece[0] == 0 and p < len(early) else [piece] for p, piece in enumerate(pieces)}
    chunk_list = [(p, chunk) for p in chunks for chunk in chunks[p]]
    ids = {p: [i for i, (q, _) in enumerate(chunk_list) if q == p] for p in chunks}
    hot, cold = range(len(early)), range(len(early), len(pieces))
    hot_levels = {level for level, _, _ in early}

    def remote(source, target, send, recv, device):
        return pltpu.make_async_remote_copy(
            src_ref=source, dst_ref=target, send_sem=send, recv_sem=recv, device_id=(device,), device_id_type=MESH
        )

    def span(piece):
        return pl.ds(piece[1], piece[2])

    def halves(p):
        level, first, tiles = pieces[p]
        part = tiles // 2 if p in hot else tiles * 2 // 3
        return (level, first, part), (level, first + part, tiles - part)

    def column(level):
        return index_of(core, x, y, level)

    def from_x(level):
        return index_of(core, 1 - x, y, level)

    def from_y(level):
        return index_of(core, x, 1 - y, level)

    def across(level):
        return index_of(core, 1 - x, 1 - y, level)

    def pass_on(block, piece, send, recv, device, own=False):
        there = out_ref.at[block, span(piece)]
        return remote(block_ref.at[span(piece)] if own else there, there, send, recv, device)

    def z_copy(i, upward, own=False):
        piece = chunk_list[i][1]
        return pass_on(column(piece[0]), piece, z_send.at[i, 0 if upward else 1], z_recv.at[i], up if upward else down, own)

    def plane_copies(i, own=False):
        piece = chunk_list[i][1]
        block = column(piece[0])
        return (
            pass_on(block, piece, x_send.at[i], x_recv.at[i], x_near, own),
            pass_on(block, piece, y_send.at[i], y_recv.at[i], y_near, own),
            pass_on(block, piece, mate_send.at[0, i], mate_recv.at[0, i], mate, own),
        )

    def got(block, i, recv):
        piece = chunk_list[i][1]
        pass_on(block, piece, x_send.at[i], recv, me).wait_recv()

    def spread(i, own=False):
        for copy in plane_copies(i, own):
            copy.start()

    def z_pass(i):
        def run(zv):
            level = chunk_list[i][1][0]
            got(column(level), i, z_recv.at[i])
            if level < zv < depth - 1:
                z_copy(i, True).start()
            if 0 < zv < level:
                z_copy(i, False).start()

        return run

    def take(i):
        def run(zv):
            z_pass(i)(zv)
            spread(i)

        return run

    def later_spread(i):
        return lambda zv: spread(i)

    def by_plane(p, zv):
        return True

    def corner_copies(p):
        level = pieces[p][0]
        first, second = halves(p)
        return (
            pass_on(from_x(level), first, corner_send.at[p, 0], corner_recv.at[p, 0], y_near),
            pass_on(from_y(level), second, corner_send.at[p, 1], corner_recv.at[p, 1], x_near),
        )

    def corner_along_z(p, zv):
        level = pieces[p][0]
        ways = [up] * (level <= zv < depth - 1) + [down] * (0 < zv <= level)
        return [
            [
                pass_on(across(level), part, line_send.at[p, 2 * side + (way is up)], line_recv.at[p, side], way)
                for way in ways
            ]
            for side, part in enumerate(halves(p))
        ]

    def mate_copies(p):
        level = pieces[p][0]
        first, second = halves(p)
        return (
            pass_on(from_x(level), pieces[p], mate_send.at[1, p], mate_recv.at[1, p], mate),
            pass_on(from_y(level), pieces[p], mate_send.at[2, p], mate_recv.at[2, p], mate),
            pass_on(across(level), first, mate_send.at[3, p], mate_recv.at[3, p], mate),
            pass_on(across(level), second, mate_send.at[4, p], mate_recv.at[4, p], mate),
        )

    def beside(p):
        def run(zv):
            level = pieces[p][0]
            for i in ids[p]:
                got(from_x(level), i, x_recv.at[i])
            if by_plane(p, zv):
                corner_copies(p)[0].start()
            mate_copies(p)[0].start()
            for i in ids[p]:
                got(from_y(level), i, y_recv.at[i])
            if by_plane(p, zv):
                corner_copies(p)[1].start()
            mate_copies(p)[1].start()

        return run

    def corner(p):
        def run(zv):
            level = pieces[p][0]
            for side, part in enumerate(halves(p)):
                recv = corner_recv if by_plane(p, zv) else line_recv
                pass_on(across(level), part, corner_send.at[p, side], recv.at[p, side], me).wait_recv()
                if not by_plane(p, zv):
                    for copy in corner_along_z(p, zv)[side]:
                        copy.start()
                mate_copies(p)[2 + side].start()

        return run

    def from_mate(p):
        def run(zv):
            level = pieces[p][0]
            other = 1 - 2 * core
            for i in ids[p]:
                pass_on(column(level) + other, chunk_list[i][1], mate_send.at[0, i], mate_recv.at[0, i], me).wait_recv()
            first, second = halves(p)
            for slot, (block, piece) in enumerate(
                ((from_x(level), pieces[p]), (from_y(level), pieces[p]), (across(level), first), (across(level), second))
            ):
                pass_on(block + other, piece, mate_send.at[slot + 1, p], mate_recv.at[slot + 1, p], me).wait_recv()

        return run

    def own_spread(i):
        return lambda zv: spread(i, True)

    def own_up(i):
        return lambda zv: z_copy(i, True, True).start() if zv < depth - 1 else None

    def own_down(i):
        return lambda zv: z_copy(i, False, True).start() if zv > 0 else None

    def w_copy(slot, which, device, source=None):
        return remote(x_in_ref if source is None else source, x_got_ref.at[slot], w_send.at[which], w_recv.at[slot], device)

    def w_far(zv):
        @pl.when(has_after)
        def _():
            w_copy(0, 1, after).start()

        @pl.when(has_before)
        def _():
            w_copy(4, 2, before).start()

    def w_forward(core_index):
        slot = 0 if core_index else 4
        return w_copy(1 if core_index else 3, 3, mate, x_got_ref.at[slot])

    def w_wait(slot):
        w_copy(slot, 0, me).wait_recv()

    def w_middle(zv):
        @pl.when(has_before)
        def _():
            w_wait(0)

        @pl.when(has_after)
        def _():
            w_wait(4)

        @pl.when((core == 1) & has_before)
        def _():
            w_forward(1).start()

        @pl.when((core == 0) & has_after)
        def _():
            w_forward(0).start()

    stops = [61.0, 63.0, 68.0, 73.0, 95.0, 102.0, 110.0] + [110.0 + 2.7 * h for h in range(1, HEADS)]

    def lists(zv):
        own_hot = [p for p in hot if pieces[p][0] == zv]
        own_cold = [p for p in cold if pieces[p][0] == zv]
        far_hot = sorted((p for p in hot if pieces[p][0] != zv), key=lambda p: abs(pieces[p][0] - zv))
        far_cold = sorted((p for p in cold if pieces[p][0] != zv), key=lambda p: (abs(pieces[p][0] - zv), -pieces[p][0]))
        distance = {p: abs(pieces[p][0] - zv) for p in cold}
        at_once = own_cold if zv > depth // 2 else []
        after_hot = [p for p in own_cold if p not in at_once]
        first = []
        for p in own_hot:
            for i in ids[p]:
                first += [own_up(i), own_down(i), own_spread(i)]
        for p in own_cold:
            first += [own_down(i) for i in ids[p]]
        for p in at_once:
            first += [own_spread(i) for i in ids[p]]
        for p in far_hot:
            first += [take(i) for i in ids[p]]
        passed = {p for p in far_cold if distance[p] < 3 and (0 < zv < pieces[p][0] or pieces[p][0] < zv < depth - 1)}
        from_above = [p for p in far_cold if p in passed and pieces[p][0] == zv + 1]
        first += [z_pass(i) for p in from_above for i in ids[p]]
        for p in own_cold:
            first += [own_up(i) for i in ids[p]]
        order_hot = own_hot + far_hot
        first += [beside(p) for p in order_hot]
        first += [z_pass(i) for p in far_cold if p in passed and p not in from_above for i in ids[p]]
        take_or_spread = lambda p: [(later_spread if p in passed else take)(i) for i in ids[p]]
        first.append(w_far)
        for p in after_hot:
            first += [own_spread(i) for i in ids[p]]
        for p in far_cold:
            first += take_or_spread(p) if distance[p] == 1 else []
        first += [corner(p) for p in order_hot]
        first += [from_mate(p) for p in order_hot]
        timed = [(73.0, event) for p in far_cold if distance[p] > 1 for event in take_or_spread(p)]
        order = at_once + after_hot + far_cold
        timed += [((110.0, 120.8, 137.0, 145.0)[min(k, 3)], beside(p)) for k, p in enumerate(order)]
        timed += [((142.4, 150.5, 200.0)[min(k, 2)], corner(p)) for k, p in enumerate(order)]
        return first, sorted(timed, key=lambda entry: entry[0])

    plans = [lists(zv) for zv in range(depth)]

    def each_plane(events_of):
        for zv in range(depth):
            events = events_of(zv)
            if events:

                @pl.when(z == zv)
                def _():
                    for event in events:
                        event(zv)

    w_copy(1 + 2 * core, 0, mate).start()
    fill = pltpu.make_async_copy(block_ref, stage_ref, local_sem)
    fill.start()
    fill.wait()
    keep = pltpu.make_async_copy(stage_ref, out_ref.at[me], local_sem)
    keep.start()
    each_plane(lambda zv: plans[zv][0])
    keep.wait()

    near_sem = x_sem
    def service(stop):
        low = stops[stop - 1] if stop else -1.0
        high = stops[stop] if stop < len(stops) else 1e9
        each_plane(lambda zv: [event for time, event in plans[zv][1] if low < time <= high])

    rows, window = q_ref.shape[0], x_ref.shape[0]
    k_ref, v_ref = both_ref.at[0], both_ref.at[1]
    loads = [copies(where, name, out_ref, w_ref.at[i], sem.at[i]) for i, name in enumerate(("w_query", "w_key", "w_value"))]
    vecs = copies(where, "vec1", out_ref, vec1_ref, vec_sem) + copies(where, "vec2", out_ref, vec2_ref, vec_sem)
    start(vecs)
    for made in loads:
        start(made)

    def slot_rows(slot):
        return pl.ds(pl.multiple_of(slot * rows, rows), rows)

    def bring(slot, there=None):
        at = x_ref.at[slot_rows(slot)]
        if there is None:
            pltpu.make_async_copy(x_got_ref.at[slot], at, near_sem).start()
            return

        @pl.when(there)
        def _():
            pltpu.make_async_copy(x_got_ref.at[slot], at, near_sem).start()

        @pl.when(jnp.logical_not(there))
        def _():
            pltpu.make_async_copy(x_in_ref, at, near_sem).start()

    def brought(many):
        for _ in range(many):
            pltpu.make_async_copy(x_in_ref, x_ref.at[slot_rows(0)], near_sem).wait()

    mate_slot, far_slot = 3 - 2 * core, 1 + 2 * core
    w_wait(mate_slot)
    pltpu.make_async_copy(x_in_ref, x_ref.at[slot_rows(2)], near_sem).start()
    bring(mate_slot)
    brought(2)
    wait(vecs)
    vec = vector_rows(vec1_ref)
    gain, shift = as_row(vec, 0, DC), as_row(vec, DC, DC)
    biases = vector_rows(vec2_ref)
    step = rows // 3

    @pl.loop(0, rows // 8)
    def _(i):
        at = pl.ds(i * 8, 8)
        bias_ref[at] = jnp.where(segq_ref[at] == segk_ref[...], 0.0, NEG)

    def over_slots(slots, body):
        @pl.loop(0, len(slots))
        def _(i):
            slot = slots[-1]
            for k, other in enumerate(slots[:-1]):
                slot = jnp.where(i == k, other, slot)
            body(slot)

    def norm_slots(slots):
        def norm_slot(slot):
            @pl.loop(0, rows // step)
            def _(i):
                at = pl.ds(pl.multiple_of(slot * rows + i * step, step), step)
                normed, _ = norm_rows(x_ref[at].astype(F32))
                turned_ref[:, at] = normed.astype(BF).T
                normed_ref[at] = (normed * gain + shift).astype(BF)

        over_slots(slots, norm_slot)

    def project(i, slots):
        def some(c, many):
            lanes = lanes_of(c, many)
            weights = panels(w_ref.at[i], c, many, D // ROWS)

            def rows_of(slot):
                value = (nn(normed_ref[slot_rows(slot)], weights) + add_ref[i, 0:1, lanes]).astype(BF)
                if isinstance(i, int):
                    q_ref[:, lanes] = value
                else:
                    both_ref[i - 1, slot_rows(slot), lanes] = value

            over_slots(slots, rows_of)

        over_pairs(some)

    def keys_and_values(slots, between):
        @pl.loop(0, 2)
        def _(i):
            project(i + 1, slots)
            for k, action in enumerate(between):

                @pl.when(i == k)
                def _():
                    action()

    norm_slots([2, mate_slot])
    service(0)
    for made in loads:
        wait(made)
    for i, row in enumerate((as_row(biases, 0, DC), jnp.zeros((1, D), F32), as_row(biases, DC, DC))):
        add_ref[i, 0:1] = row
    project(0, [2])
    service(1)
    keys_and_values([2, mate_slot], [lambda: service(2), lambda: service(3)])
    w_middle(None)

    @pl.when((core == 0) & has_before)
    def _():
        w_wait(1)

    @pl.when((core == 1) & has_after)
    def _():
        w_wait(3)

    bring(0, has_before)
    bring(4, has_after)
    bring(far_slot, jnp.where(core == 0, has_before, has_after))
    brought(3)
    others = [0, 4, far_slot]
    norm_slots(others)
    saves = [pltpu.make_async_copy(x_ref, x_out_ref, local_sem), pltpu.make_async_copy(turned_ref, turned_out_ref, local_sem)]
    start(saves)
    service(4)
    k_save = pltpu.make_async_copy(k_ref, k_out_ref, keys_sem.at[0])

    def keys_done():
        service(5)
        k_save.start()

    keys_and_values(others, [keys_done])
    v_save = pltpu.make_async_copy(v_ref, v_out_ref, keys_sem.at[1])
    v_save.start()
    wait(saves)

    @pl.loop(0, window // LANES)
    def _(i):
        at = pl.ds(pl.multiple_of(i * LANES, LANES), LANES)
        turned_ref[:, at] = k_ref[at].T

    keys_save = pltpu.make_async_copy(turned_ref, keys_out_ref, keys_sem.at[2])
    keys_save.start()
    attended_ref[...] = jnp.zeros_like(attended_ref)
    rest_ref[...] = jnp.zeros_like(rest_ref)
    logs_ref[...] = jnp.zeros_like(logs_ref)
    lane_l = lax.broadcasted_iota(jnp.int32, logs_ref.shape, 1)

    @pl.loop(0, HEADS)
    def _(h):
        for at_head in range(HEADS):

            @pl.when(h == at_head)
            def _():
                service(6 + at_head)

        lane, offset = head_window(h)
        mask = head_mask(rows, offset)
        lanes = pl.ds(lane, PAIR)
        query = jnp.where(mask, q_ref[:, lanes], jnp.zeros((), BF))
        score_ref[...] = nt(query, k_ref[:, lanes]) * SCALE + bias_ref[...]
        top = jnp.max(score_ref[...], axis=-1, keepdims=True)
        powers = jnp.exp(score_ref[...] - top)
        total = jnp.sum(powers, axis=-1, keepdims=True)
        prob_ref[...] = powers.astype(BF)
        out = nn(prob_ref[...], v_ref[:, lanes]) / total
        rounded = out.astype(BF)
        attended_ref[:, lanes] = jnp.where(mask, rounded, attended_ref[:, lanes])
        rest_ref[:, lanes] = jnp.where(mask, (out - rounded.astype(F32)).astype(BF), rest_ref[:, lanes])
        logs_ref[...] = jnp.where(lane_l == h, top + jnp.log(total), logs_ref[...])

    service(len(stops))
    each_plane(lambda zv: [from_mate(p) for p in cold])

    def sent(zv):
        for i, (p, piece) in enumerate(chunk_list):
            for copy in plane_copies(i):
                copy.wait_send()
            level = piece[0]
            if zv < depth - 1 and level <= zv:
                z_copy(i, True).wait_send()
            if zv > 0 and level >= zv:
                z_copy(i, False).wait_send()
        for p in range(len(pieces)):
            for copy in mate_copies(p) + (corner_copies(p) if by_plane(p, zv) else ()):
                copy.wait_send()
            for copy in sum(corner_along_z(p, zv), []) if not by_plane(p, zv) else []:
                copy.wait_send()

    each_plane(lambda zv: [sent])
    w_copy(0, 0, mate).wait_send()

    @pl.when(has_after)
    def _():
        w_copy(0, 1, after).wait_send()

    @pl.when(has_before)
    def _():
        w_copy(4, 2, before).wait_send()

    @pl.when(jnp.where(core == 1, has_before, has_after))
    def _():
        w_forward(0).wait_send()

    wait([k_save, v_save, keys_save])


def gather_front(block, block_input, seg_query, seg_keys, plan):
    where = plan[0]
    count = lax.axis_size("fsdp")
    depth = count // 8
    rows, window = block_input.shape[0], seg_keys.shape[1]
    early, whole = transfer_pieces(plan, depth)
    late = whole
    shape = lambda n, d=D, t=BF: jax.ShapeDtypeStruct((n, d), t)
    dma = pltpu.SemaphoreType.DMA
    units = D // ROWS
    many = len(early) + len(late)
    chunks = many + 3 * sum(1 for piece in early if piece[0] == 0)
    got = jax.ShapeDtypeStruct((5, rows, D), BF)
    return pl.pallas_call(
        functools.partial(gather_front_kernel, depth, where, early, late),
        out_shape=(
            jax.ShapeDtypeStruct((count, *block.shape), BF), shape(window), shape(D, window), shape(D, window), shape(window), shape(window), got,
            shape(rows), shape(rows), shape(rows), shape(rows, LANES, F32),
        ),
        in_specs=[ANY, ANY, VM, VM],
        out_specs=[ANY] * 7 + [VM] * 4,
        scratch_shapes=[
            dma((chunks, 2)), dma((chunks,)), dma((chunks,)), dma((chunks,)), dma((chunks,)), dma((chunks,)),
            dma((many, 2)), dma((many, 2)), dma((many, 4)), dma((many, 2)), dma((5, chunks)), dma((5, chunks)), dma((4,)), dma((5,)),
            dma, pltpu.VMEM(block.shape, BF), pltpu.VMEM((2, window, D), BF),
            pltpu.VMEM((window, D), BF), pltpu.VMEM((D, window), BF), pltpu.VMEM((window, D), BF),
            pltpu.VMEM((3, units, DC, ROWS, LANES), BF), pltpu.VMEM((2, ROWS, LANES), BF), pltpu.VMEM((2, ROWS, LANES), BF),
            pltpu.VMEM((rows, window), F32), pltpu.VMEM((rows, window), F32), pltpu.VMEM((rows, window), BF), pltpu.VMEM((3, 8, D), F32),
            dma((3,)), dma, dma, dma((3,)),
        ],
        compiler_params=pltpu.CompilerParams(collective_id=0, has_side_effects=True, vmem_limit_bytes=VMEM_LIMIT),
        name="gather_front",
    )(block, block_input, seg_query, seg_keys)


def back_scatter_kernel(
    depth, where, early, late,
    x_hbm_ref, turned_hbm_ref, keys_hbm_ref, segq_ref, segk_ref, blocks_ref, q_ref, k_hbm_ref, v_hbm_ref, grad_ref, logs_ref, delta_ref, mid_hbm_ref, parts_in_ref,
    parts_ref, out_ref, in_grad_ref, mates, sums, halfs, fulls, lines, near_ref, near_got,
    w_ref, g_ref, vec1_ref, vec2_ref, score_ref, prob_ref, turned_ref, k_ref, v_ref, dq_ref, part_ref, logs_t_ref, x_ref, dq_b_ref,
    block_ref, mid_ref, g_value_ref, gain_acc, shift_acc, stage, total,
    mate_send, mate_recv, half_send, half_recv, full_send, full_recv, line_send, line_recv, near_send, near_recv,
    load_sem, store_sem, sem, vec_sem, out_sem, x_sem,
):
    me = lax.axis_index("fsdp")
    count = 8 * depth
    core, x, y, z = place(me)
    mate, x_near, y_near = index_of(1 - core, x, y, z), index_of(core, 1 - x, y, z), index_of(core, x, 1 - y, z)
    after, before = me + 2, me - 2
    has_after, has_before = after < count, before >= 0
    greet(
        [(mate, None), (x_near, None), (y_near, None), (me - 8, z > 0), (me + 8, z < depth - 1), (after, has_after), (before, has_before)]
    )
    pieces = early + late
    block_tiles = parts_ref.shape[1]
    early_ids, late_ids = range(len(early)), range(len(early), len(pieces))

    def remote(source, target, send, recv, device):
        return pltpu.make_async_remote_copy(
            src_ref=source, dst_ref=target, send_sem=send, recv_sem=recv, device_id=(device,), device_id_type=MESH
        )

    def owner(level, slot, which_core):
        return index_of(which_core, 1 - x if slot in (1, 3) else x, 1 - y if slot in (2, 3) else y, level)

    def at_plane(zv, run):
        @pl.when(z == zv)
        def _():
            run()

    def span(p, lo=0, many=None):
        _, first, tiles = pieces[p]
        return pl.ds(first + lo, tiles if many is None else many)

    def half_of(p):
        return pieces[p][2] // 2

    def to_mate(p, slot):
        level = pieces[p][0]
        return remote(
            parts_ref.at[owner(level, slot, 1 - core), span(p)], mates.at[level, slot, span(p)],
            mate_send.at[p, slot], mate_recv.at[p, slot], mate,
        )

    def half_out(p, side):
        level, _, tiles = pieces[p]
        part = span(p, half_of(p), tiles - half_of(p)) if side else span(p, 0, half_of(p))
        return remote(
            sums.at[level, 3, part], halfs.at[level, side, part], half_send.at[p, side], half_recv.at[p, side],
            x_near if side else y_near,
        )

    def full_out(p, side):
        level = pieces[p][0]
        return remote(
            sums.at[level, 1 + side, span(p)], fulls.at[level, side, span(p)], full_send.at[p, side], full_recv.at[p, side],
            y_near if side else x_near,
        )

    def subs(p):
        tiles = pieces[p][2]
        if p in early_ids or tiles < block_tiles // 3:
            return [(0, tiles)]
        return [(0, tiles // 2), (tiles // 2, tiles - tiles // 2)]

    def line_out(p, zv, sub):
        level = pieces[p][0]
        part = span(p, *subs(p)[sub])
        upward = level > zv
        slot = depth if not upward and level == zv - 1 else level
        side = 1 if slot == depth else 0
        return remote(
            sums.at[level, 0, part], lines.at[slot, part], line_send.at[p, sub], line_recv.at[p, 2 * sub + side],
            me + 8 if upward else me - 8,
        )

    def line_in(p, side, sub):
        level = pieces[p][0]
        slot = depth if side else level
        part = span(p, *subs(p)[sub])
        return remote(sums.at[level, 0, part], lines.at[slot, part], line_send.at[p, sub], line_recv.at[p, 2 * sub + side], me)

    def line_sides(p, zv):
        level = pieces[p][0]
        if level > zv:
            return [0] if zv > 0 else []
        if level < zv:
            return [0] if zv < depth - 1 else []
        return ([0] if zv > 0 else []) + ([1] if zv < depth - 1 else [])

    def extent(job):
        kind, p, sub = job
        return subs(p)[sub] if kind == 0 else (0, pieces[p][2])

    def sources(job, zv):
        kind, p, sub = job
        level, _, tiles = pieces[p]
        h = half_of(p)
        if kind == 0:
            lo, many = extent(job)
            part = span(p, lo, many)
            refs = [parts_ref.at[owner(level, 0, core), part], mates.at[level, 0, part]]
            refs += [fulls.at[level, side, part] for side in (0, 1)]
            refs += [lines.at[depth if side else level, part] for side in line_sides(p, zv)]
            return [(ref, 0, many) for ref in refs]
        found = [(parts_ref.at[owner(level, kind, core), span(p)], 0, tiles), (mates.at[level, kind, span(p)], 0, tiles)]
        if kind == 1:
            found.append((halfs.at[level, 0, span(p, 0, h)], 0, h))
        if kind == 2:
            found.append((halfs.at[level, 1, span(p, h, tiles - h)], h, tiles - h))
        return found

    def loads(job, zv, base):
        return [
            pltpu.make_async_copy(ref, stage.at[i, pl.ds(base + lo, many)], load_sem.at[1 if base else 0])
            for i, (ref, lo, many) in enumerate(sources(job, zv))
        ]

    def store(job, base):
        kind, p, sub = job
        lo, many = extent(job)
        return pltpu.make_async_copy(
            total.at[pl.ds(base, many)], sums.at[pieces[p][0], kind, span(p, lo, many)], store_sem.at[1 if base else 0]
        )

    def load(job, zv, base=0):
        kind, p, sub = job
        if sub == 0:
            to_mate(p, kind).wait_recv()
        if kind in (1, 2):
            half_out(p, kind - 1).wait_recv()
        made = loads(job, zv, base)
        if kind == 0:
            if sub == 0:
                for side in (0, 1):
                    full_out(p, side).wait_recv()
            start(made[:4])
            for copy, side in zip(made[4:], line_sides(p, zv)):
                line_in(p, side, sub).wait_recv()
                copy.start()
        else:
            start(made)

    def add(base, lo, many, slots, target, shift):
        def some(first, tiles):
            value = stage[slots[0], pl.ds(first, tiles)].astype(F32)
            for slot in slots[1:]:
                value = value + stage[slot, pl.ds(first, tiles)].astype(F32)
            target[pl.ds(first + shift, tiles)] = value.astype(target.dtype)

        group = 8

        @pl.loop(0, many // group)
        def _(i):
            some(base + lo + i * group, group)

        if many % group:
            some(base + lo + many // group * group, many % group)

    def finish(job, zv, base=0):
        kind, p, sub = job
        level, first, tiles = pieces[p]
        found = sources(job, zv)
        wait(loads(job, zv, base))
        final = kind == 0 and level == zv
        target, shift = (out_ref, first + extent(job)[0] - base) if final else (total, 0)
        edges = sorted({e for _, lo, many in found for e in (lo, lo + many)})
        for lo, hi in zip(edges[:-1], edges[1:]):
            slots = [i for i, (_, a, many) in enumerate(found) if a <= lo and hi <= a + many]
            add(base, lo, hi - lo, slots, target, shift)
        if not final:
            store(job, base).start()

    def send(job, zv, base=0):
        kind, p, sub = job
        if kind == 0 and pieces[p][0] == zv:
            return
        store(job, base).wait()
        if kind == 3:
            half_out(p, 0).start()
            half_out(p, 1).start()
        elif kind == 0:
            line_out(p, zv, sub).start()
        else:
            full_out(p, kind - 1).start()

    second = block_tiles // 2

    def run(jobs, zv):
        for job in jobs:
            load(job, zv)
            finish(job, zv)
            send(job, zv)

    def run_ahead(jobs, zv):
        bases = [second * (k % 2) for k in range(len(jobs))]
        for k, job in enumerate(jobs):
            if k == 0:
                load(job, zv, bases[k])
            if k + 1 < len(jobs):
                load(jobs[k + 1], zv, bases[k + 1])
            finish(job, zv, bases[k])
            if k:
                send(jobs[k - 1], zv, bases[k - 1])
        send(jobs[-1], zv, bases[-1])

    def along(p):
        return [(0, p, sub) for sub in range(len(subs(p)))]

    for p in early_ids:
        for slot in (3, 1, 2, 0):
            to_mate(p, slot).start()

    window, rows = k_ref.shape[0], q_ref.shape[0]
    margin = (window - rows) // 2
    names = ("w_query", "w_key", "w_value")
    k_load = [
        pltpu.make_async_copy(a, b, vec_sem)
        for a, b in ((k_hbm_ref, k_ref), (v_hbm_ref, v_ref), (keys_hbm_ref, turned_ref))
    ]
    start(k_load)
    weight_loads = [copies(where, name, blocks_ref, w_ref.at[i], sem.at[i]) for i, name in enumerate(names)]
    vecs = copies(where, "vec1", blocks_ref, vec1_ref, sem.at[3])
    start(vecs)
    for made in weight_loads:
        start(made)
    x_load = [pltpu.make_async_copy(x_hbm_ref, x_ref, x_sem)]
    start(x_load)
    logs_t_ref[...] = logs_ref[...].T * LOG2E
    g_value_ref[...] = jnp.zeros_like(g_value_ref)

    by_level = {pieces[p][0]: p for p in early_ids}
    a, b, c_ = (by_level[level] for level in sorted(by_level, reverse=True)[:3])
    table = [
        (-1, 0, 3, a, None), (0, 1, 3, b, None), (3, 4, 1, a, None), (4, 5, 2, a, None), (5, 6, 3, c_, None),
        (6, 7, 1, b, None), (7, 8, 2, b, None), (11, 12, 0, a, 0), (12, 13, 1, c_, None), (13, 14, 2, c_, None),
    ]

    def beside(h, which, action):
        for entry in table:
            if entry[which] < 0:
                continue
            kind, p, zv = entry[2:]
            job = (kind, p, 0)
            there = h == entry[which]
            if zv is not None:
                there = there & (z == zv)

            @pl.when(there)
            def _():
                action(job, zv)

    wait(k_load)
    load((3, a, 0), None)

    @pl.loop(0, HEADS)
    def _(h):
        beside(h, 1, finish)
        lane, offset = head_window(h)
        mask = head_mask(rows, offset)
        lanes = pl.ds(lane, PAIR)
        query = jnp.where(mask, q_ref[:, lanes], jnp.zeros((), BF))
        grad = jnp.where(mask, grad_ref[:, lanes], jnp.zeros((), BF))
        log_row, delta_row = logs_t_ref[pl.ds(h, 1)], delta_ref[pl.ds(h, 1)]
        blocks = [pl.ds(n * rows, rows) for n in range(window // rows)]
        for keys in blocks:
            together = jnp.concatenate([segk_ref[keys]] * (rows // LANES), axis=1) == segq_ref[...]
            probs = jnp.exp2(jnp.where(together, nt(k_ref[keys, lanes], query) * (SCALE * LOG2E) - log_row, NEG))
            prob_ref[keys] = probs.astype(BF)
            score_ref[keys] = (probs * (nt(v_ref[keys, lanes], grad) - delta_row)).astype(BF)
        beside(h, 1, send)
        beside(h, 0, load)
        side = head_mask(rows, offset)

        @pl.loop(0, window // rows)
        def _(n):
            keys = pl.ds(pl.multiple_of(n * rows, rows), rows)
            dv = nn(prob_ref[keys], grad)
            g_value_ref[:, lanes] += column_sums(dv)
            v_ref[keys, lanes] = jnp.where(side, dv.astype(BF), v_ref[keys, lanes])
            dk = nn(score_ref[keys], query) * SCALE
            k_ref[keys, lanes] = jnp.where(side, dk.astype(BF), k_ref[keys, lanes])
        tile = (h * HEAD_DIM) // ROWS * ROWS
        part_ref[...] = nn(turned_ref[pl.ds(pl.multiple_of(tile, ROWS), part_ref.shape[0])], score_ref[...])
        at = pl.ds(pl.multiple_of(h * HEAD_DIM, 8), HEAD_DIM)
        dq_ref[at] = part_ref[pl.ds(pl.multiple_of(h * HEAD_DIM - tile, 8), HEAD_DIM)]

    turned_load = pltpu.make_async_copy(turned_hbm_ref, turned_ref, vec_sem)
    turned_load.start()
    dq = dq_ref[...].T * SCALE
    put_vectors(vec2_ref, [column_sums(dq), g_value_ref[...]])
    saves = copies(where, "vec2", parts_ref, vec2_ref, out_sem.at[3], out=True)
    dq_b_ref[...] = dq.astype(BF)
    wait(vecs)
    vec = vector_rows(vec1_ref)
    gain, shift = as_row(vec, 0, DC), as_row(vec, DC, DC)
    gain_t, shift_t = (jnp.broadcast_to(v, (8, D)).T[:, :1] for v in (gain, shift))
    wait(x_load)
    step = rows // 3

    turned_load.wait()
    for made in weight_loads:
        wait(made)
    gain_acc[...] = jnp.zeros_like(gain_acc)
    shift_acc[...] = jnp.zeros_like(shift_acc)

    def plane_job(what, entries):
        for zv, p in entries:

            def go():
                job = (0, p, 0)
                if what == "load":
                    load(job, zv)
                else:
                    finish(job, zv)
                    send(job, zv)

            at_plane(zv, go)

    own = turned_ref[:, pl.ds(margin, rows)]
    made = []
    first_jobs, last_jobs = [(1, a), (0, b), (3, b)], [(0, c_), (3, c_)]
    for i, (left, right_ref) in enumerate(((own, dq_b_ref), (turned_ref, k_ref), (turned_ref, v_ref))):
        if i == 1:
            plane_job("load", first_jobs)
        if i == 2:
            plane_job("end", first_jobs)
            plane_job("load", last_jobs)
            wait(made[0])

        def project_back(c, many):
            right = right_ref[:, lanes_of(c, many)]
            raw = nn(left[...], right)
            summed = column_sums(right.astype(F32))
            put_panels(g_ref.at[i % 2], c, gain_t * raw + shift_t * summed)
            weights = panels(w_ref.at[i], c, many, D // ROWS).astype(F32)
            scaled, shifted = weights * raw, weights * summed
            for j in range(many):
                part = slice(j * LANES, (j + 1) * LANES)
                gain_acc[...] += scaled[:, part]
                shift_acc[...] += shifted[:, part]

        over_pairs(project_back)
        made.append(copies(where, names[i], parts_ref, g_ref.at[i % 2], out_sem.at[i], out=True))
        start(made[i])
    put_vectors(vec1_ref, [column_sums(gain_acc[...].T), column_sums(shift_acc[...].T)])
    saves = saves + copies(where, "vec1", parts_ref, vec1_ref, out_sem.at[3], out=True)
    start(saves)
    plane_job("end", last_jobs)
    wait(saves + made[1] + made[2])
    for slots in ((3,), (1, 2), (0,)):
        for p in late_ids:
            for slot in slots:
                to_mate(p, slot).start()

    def slot_rows(n):
        return pl.ds(pl.multiple_of(n * rows, rows), rows)

    def row_block(n, own=False):
        first = n * rows

        def project_back(c, many):
            part = lambda i: panels(w_ref.at[i], 0, DC, many * LANES // ROWS, c * (LANES // ROWS))
            value = nt(k_ref[slot_rows(n)], part(1)) + nt(v_ref[slot_rows(n)], part(2))
            if own:
                value = value + nt(dq_b_ref[...], part(0))
            block_ref[:, lanes_of(c, many)] = value

        over_pairs(project_back)

        @pl.loop(0, rows // step)
        def _(i):
            here = pl.ds(pl.multiple_of(i * step, step), step)
            there = pl.ds(pl.multiple_of(first + i * step, step), step)
            normed, inverse = norm_rows(x_ref[there].astype(F32))
            result = norm_rows_back(block_ref[here], normed, inverse, gain)
            if own:
                block_ref[here] = result
            else:
                x_ref[there] = result.astype(BF)

    def near_rows(slot):
        return x_ref.at[pl.ds(slot * rows, rows)]

    def near_save(slot):
        return pltpu.make_async_copy(near_rows(slot), near_ref.at[slot], x_sem)

    def near_copy(slot, which, device):
        return remote(near_ref.at[slot], near_got.at[which], near_send.at[which], near_recv.at[which], device)


    @pl.loop(0, 4)
    def _(i):
        row_block(jnp.where(i == 0, 0, jnp.where(i == 1, 4, 2 * i - 3)))

        @pl.when(i == 0)
        def _():
            run_ahead([(3, p, 0) for p in late_ids], None)

        @pl.when(i == 1)
        def _():
            at_plane(1, lambda: run([(0, b, 0)], 1))
            at_plane(2, lambda: run([(0, a, 0), (0, c_, 0)], 2))
            for p in late_ids:
                run_ahead([(1, p, 0), (2, p, 0)], None)

    sides = [near_save(slot) for slot in (0, 4, 1, 3)]
    start(sides)
    wait(sides)
    to_mate_itself, to_mate_shared = (3 - 2 * core), (1 + 2 * core)
    near_copy(to_mate_itself, 0, mate).start()
    near_copy(to_mate_shared, 1, mate).start()

    @pl.when((core == 0) & has_before)
    def _():
        near_copy(0, 2, before).start()

    @pl.when((core == 1) & has_after)
    def _():
        near_copy(4, 3, after).start()

    row_block(2, True)
    near_copy(0, 1, me).wait_recv()
    shared_slot = 4 - 4 * core
    fetch = pltpu.make_async_copy(near_got.at[1], k_ref.at[pl.ds(0, rows)], x_sem)
    fetch.start()
    fetch.wait()

    @pl.loop(0, rows // step)
    def _(i):
        here = pl.ds(pl.multiple_of(i * step, step), step)
        there = pl.ds(pl.multiple_of(shared_slot * rows + i * step, step), step)
        x_ref[there] = (x_ref[there].astype(F32) + k_ref[here].astype(F32)).astype(BF)

    shared_save = near_save(shared_slot)
    shared_save.start()
    shared_save.wait()

    @pl.when((core == 0) & has_after)
    def _():
        near_copy(4, 3, after).start()

    @pl.when((core == 1) & has_before)
    def _():
        near_copy(0, 2, before).start()

    def tail(zv):
        out = [p for p in late_ids if pieces[p][0] != zv]
        hops = lambda p: zv if pieces[p][0] > zv else depth - 1 - zv
        moving = [job for p in sorted(out, key=lambda p: (hops(p), p)) for job in along(p)]
        own = [p for ids in (early_ids, late_ids) for p in ids if pieces[p][0] == zv]
        return moving + [job for p in own for job in along(p)]

    for zv in range(depth):
        at_plane(zv, lambda: run(tail(zv), zv))

    near_copy(0, 0, me).wait_recv()

    @pl.when(has_after)
    def _():
        near_copy(0, 2, me).wait_recv()

    @pl.when(has_before)
    def _():
        near_copy(0, 3, me).wait_recv()

    for i, (which, there) in enumerate(((0, None), (2, has_after), (3, has_before))):
        target = k_ref.at[pl.ds(i * rows, rows)]
        if there is None:
            pltpu.make_async_copy(near_got.at[which], target, x_sem).start()
            continue

        @pl.when(there)
        def _():
            pltpu.make_async_copy(near_got.at[which], target, x_sem).start()

        @pl.when(jnp.logical_not(there))
        def _():
            pltpu.make_async_copy(near_ref.at[0], target, x_sem).start()

    for i in range(3):
        pltpu.make_async_copy(near_got.at[0], k_ref.at[pl.ds(i * rows, rows)], x_sem).wait()
    near_after, near_before = (jnp.where(there, 1.0, 0.0) for there in (has_after, has_before))

    @pl.loop(0, rows // step)
    def _(i):
        here = pl.ds(pl.multiple_of(i * step, step), step)
        fetch_mid = pltpu.make_async_copy(mid_hbm_ref.at[here], mid_ref, x_sem)
        fetch_mid.start()
        fetch_mid.wait()
        value = mid_ref[...] + block_ref[here] + k_ref[here].astype(F32)
        value = value + near_after * k_ref[pl.ds(pl.multiple_of(rows + i * step, step), step)].astype(F32)
        value = value + near_before * k_ref[pl.ds(pl.multiple_of(2 * rows + i * step, step), step)].astype(F32)
        in_grad_ref[here] = value.astype(BF)

    for p in range(len(pieces)):
        for slot in range(4):
            to_mate(p, slot).wait_send()
        for side in (0, 1):
            half_out(p, side).wait_send()
            full_out(p, side).wait_send()
        for zv in range(depth):
            if pieces[p][0] != zv:
                at_plane(zv, lambda: [line_out(p, zv, sub).wait_send() for sub in range(len(subs(p)))])
    near_copy(0, 0, mate).wait_send()
    near_copy(0, 1, mate).wait_send()

    @pl.when(has_before)
    def _():
        near_copy(0, 2, before).wait_send()

    @pl.when(has_after)
    def _():
        near_copy(4, 3, after).wait_send()


def back_scatter(x_win, turned, turned_keys, seg_query, seg_keys, gathered, queries, key_win, value_win, att_grad, logs, delta, mid_grad, parts, plan):
    where, block = plan[:2]
    window, rows = x_win.shape[0], queries.shape[0]
    seg_keys = jnp.broadcast_to(seg_keys, (window, LANES))
    count = lax.axis_size("fsdp")
    depth = count // 8
    hot, cold = transfer_pieces(plan, depth)
    early = sorted(cold, reverse=True)
    late = []
    for piece in sorted(hot, reverse=True):
        late += cut(piece, 2) if piece[2] > block // 2 else [piece]
    many = len(early) + len(late)
    dma = pltpu.SemaphoreType.DMA
    tiles = lambda *n: pltpu.VMEM((*n, ROWS, LANES), BF)
    vm = lambda a, b, t: pltpu.VMEM((a, b), t)
    hbm = lambda *n: jax.ShapeDtypeStruct((*n, ROWS, LANES), BF)
    return pl.pallas_call(
        functools.partial(back_scatter_kernel, depth, where, early, late),
        out_shape=(
            jax.ShapeDtypeStruct(parts.shape, BF), jax.ShapeDtypeStruct((block, ROWS, LANES), F32), jax.ShapeDtypeStruct((rows, D), BF),
            hbm(depth, 4, block), hbm(depth, 4, block), hbm(depth, 2, block), hbm(depth, 2, block), hbm(depth + 1, block),
            jax.ShapeDtypeStruct((5, rows, D), BF), jax.ShapeDtypeStruct((4, rows, D), BF),
        ),
        in_specs=[ANY, ANY, ANY, VM, VM, ANY, VM, ANY, ANY, VM, VM, VM, ANY, ANY],
        out_specs=[ANY, VM, VM] + [ANY] * 7,
        scratch_shapes=[
            tiles(3, D // ROWS, DC), tiles(2, D // ROWS, DC), tiles(2), tiles(2),
            vm(window, rows, BF), vm(window, rows, BF), vm(D, window, BF), vm(window, D, BF), vm(window, D, BF),
            vm(D, rows, F32), vm(ROWS * pl.cdiv(HEAD_DIM + 8, ROWS), rows, F32), vm(LANES, rows, F32), vm(window, D, BF), vm(rows, D, BF), vm(rows, D, F32), vm(rows // 3, D, F32),
            vm(1, D, F32), vm(D, LANES, F32), vm(D, LANES, F32), tiles(6, block), tiles(block),
            dma((many, 4)), dma((many, 4)), dma((many, 2)), dma((many, 2)), dma((many, 2)), dma((many, 2)), dma((many, 2)), dma((many, 4)),
            dma((4,)), dma((4,)), dma((2,)), dma((2,)), dma((4,)), dma, dma((4,)), dma,
        ],
        input_output_aliases={13: 0},
        compiler_params=pltpu.CompilerParams(collective_id=1, has_side_effects=True, vmem_limit_bytes=VMEM_LIMIT),
        name="back_scatter",
    )(x_win, turned, turned_keys, seg_query, seg_keys, gathered, queries, key_win, value_win, att_grad, logs, delta, mid_grad, parts)[1:3]


def passed_along(value, steps):
    count = lax.axis_size("fsdp")
    first, last = (max(0, -steps), min(count, count - steps))
    return lax.ppermute(value, "fsdp", [(source, source + steps) for source in range(first, last)])


def window_of(rows):
    near = [rows if k == 0 else passed_along(rows, -k) for k in range(-REACH, REACH + 1)]
    return jnp.concatenate(near, axis=0)


def shards(kernels, block_input, params, cotangent, segment_ids):
    count = lax.axis_size("fsdp")
    me = lax.axis_index("fsdp")
    rows = block_input.shape[0]
    margin = REACH * rows
    seg_pad = jnp.pad(segment_ids, (margin, margin), constant_values=-1)
    seg_query = lax.dynamic_slice_in_dim(segment_ids, me * rows, rows, 0)
    seg_keys = lax.dynamic_slice_in_dim(seg_pad, me * rows, 2 * margin + rows, 0)
    plan = wire_plan(count, params.shape[1])
    where = plan[0]
    block = to_tiles(params, plan)
    if kernels:
        gathered, x_win, turned, turned_keys, key_win, value_win, _, queries, attended, rest, logs = gather_front(
            block, block_input, seg_query[:, None], seg_keys[None, :], plan
        )
    else:
        x_win = window_of(block_input)
        gathered = lax.all_gather(block, "fsdp", axis=0, tiled=False)
        queries, key_win, value_win, attended, rest, logs = front(
            x_win, seg_query[:, None], seg_keys[None, :], gathered, where, rows
        )
    activations, mid_grad, att_grad, delta, parts = middle(block_input, cotangent, attended, rest, gathered, where)
    sides = (seg_query[None, :], seg_keys[:, None], gathered, queries, key_win, value_win, att_grad, logs)
    if kernels:
        summed, input_grad = back_scatter(x_win, turned, turned_keys, *sides, delta, mid_grad, parts, plan)
    else:
        near, own, parts = back(x_win, *sides, parts, where)
        input_grad = mid_grad + own
        for k in range(-REACH, REACH + 1):
            if k != 0:
                part = near[(k + REACH) * rows : (k + REACH + 1) * rows]
                input_grad = input_grad + passed_along(part, k).astype(jnp.float32)
        input_grad = input_grad.astype(jnp.bfloat16)
        received = lax.all_to_all(parts, "fsdp", split_axis=0, concat_axis=0, tiled=True)
        summed = jnp.sum(received.astype(jnp.float32), axis=0)
    param_grads = to_flat(summed, plan, params.shape[1])
    return (activations, input_grad, param_grads)


def two_by_two(mesh):
    spans = np.array([device.coords for device in mesh.devices.flat])
    return tuple(spans.max(axis=0) - spans.min(axis=0))[:2] == (1, 1)


def solution(mesh):
    return jax.shard_map(
        functools.partial(shards, two_by_two(mesh)),
        mesh=mesh,
        in_specs=(P("fsdp", None), P(None, "fsdp"), P("fsdp", None), P()),
        out_specs=(P("fsdp", None), P("fsdp", None), P(None, "fsdp")),
        check_vma=False,
    )
```

```python
import functools
import math

import jax
import jax.numpy as jnp
import numpy as np
from jax import lax
from jax.experimental import pallas as pl
from jax.experimental.pallas import tpu as pltpu
from jax.sharding import PartitionSpec as P

D = 1152
HEADS = 16
HEAD_DIM = 72
FF = 4304
REACH = 2


EPS = 1e-06
NEG = -1e30
LANES = 128
ROWS = 16
DC = D // LANES
FC = -(-FF // LANES)
WIDE = FF * ROWS // LANES
HEAD = 544
KIND_A, KIND_D, KIND_L2, KIND_L3, KIND_B = 1, 2, 3, 4, 5
MESH = pl.DeviceIdType.MESH


def units():
    found = []
    offset = 0

    def matrix(name, kind, rows, width, tiles):
        nonlocal offset
        for row in range(0, rows, ROWS):
            found.append((name, kind, offset + row * width, tiles))
        offset += rows * width

    def vectors(name, kind, length, tiles):
        nonlocal offset
        found.append((name, kind, offset, tiles))
        offset += length

    vectors("vec1", KIND_L2, 2 * D, 2)
    matrix("w_query", KIND_A, D, D, DC)
    matrix("w_key", KIND_A, D, D, DC)
    matrix("w_value", KIND_A, D, D, DC)
    vectors("vec2", KIND_L2, 2 * D, 2)
    matrix("w_out", KIND_A, D, D, DC)
    vectors("vec3", KIND_L2, 3 * D, 2)
    matrix("w_up", KIND_B, D, FF, FC)
    vectors("vec4", KIND_L3, FF, 3)
    matrix("w_down", KIND_D, FF, D, DC)
    vectors("vec5", KIND_D, D, DC)
    return found


def unit_width(name):
    return {"vec1": 2 * D, "vec2": 2 * D, "vec3": 3 * D, "vec4": FF, "vec5": D, "w_up": ROWS * FF}.get(
        name, ROWS * D
    )


def wire_plan(count, shard):
    blocks = [[] for _ in range(count)]
    where = {}
    used = [0] * count
    tails = [0] * count
    for name, kind, first, tiles in units():
        owner = first // shard
        where.setdefault(name, []).append((owner, used[owner], tiles))
        blocks[owner].append((kind, (first - owner * shard) // LANES, used[owner]))
        used[owner] += tiles
        tails[owner] = max(0, first + unit_width(name) - (owner + 1) * shard)
    block = max(used)
    block += block % 2
    most = max(len(b) for b in blocks)
    table = np.zeros((count, 3 * most), np.int32)
    for owner, entries in enumerate(blocks):
        for i, entry in enumerate(entries):
            table[owner, 3 * i : 3 * i + 3] = entry
    return where, block, table, np.array(tails, np.int32)


def lane_iota(rows):
    return lax.broadcasted_iota(jnp.int32, (rows, LANES), 1)


def wide_rows():
    return [divmod(row * FF, LANES) for row in range(ROWS)]


SKEW = (D * 0 + 80) % LANES


def rows_from_line(line_ref, flat_ref, first, rows):
    step = 8 * LANES

    @pl.loop(0, rows // 8)
    def _(i):
        part = line_ref[:, pl.ds(pl.multiple_of(i * step, step), step)].astype(jnp.float32)
        flat_ref[pl.ds(first + i * 8, 8)] = part.reshape(8, LANES)

    for row in range(rows // 8 * 8, rows):
        flat_ref[pl.ds(first + row, 1)] = line_ref[:, row * LANES : (row + 1) * LANES].astype(jnp.float32)


def line_from_rows(flat_ref, line_ref, first, rows):
    step = 8 * LANES

    @pl.loop(0, rows // 8)
    def _(i):
        part = flat_ref[pl.ds(first + i * 8, 8)]
        line_ref[:, pl.ds(pl.multiple_of(i * step, step), step)] = part.reshape(1, step)

    for row in range(rows // 8 * 8, rows):
        line_ref[:, row * LANES : (row + 1) * LANES] = flat_ref[pl.ds(first + row, 1)]


def to_tiles_kernel(entries, table_ref, line_ref, head_ref, tile_ref, stage_ref, flat_ref):
    rows = line_ref.shape[1] // LANES
    rows_from_line(line_ref, flat_ref, 0, rows)
    rows_from_line(head_ref, flat_ref, rows, HEAD)

    def unit(i, _):
        kind, src, dst = (table_ref[3 * i + j] for j in range(3))

        @pl.when(kind == KIND_A)
        def _():
            for c in range(DC):
                tile_ref[dst + c] = flat_ref[pl.ds(src + c, ROWS, stride=DC), :].astype(jnp.bfloat16)

        @pl.when(kind == KIND_D)
        def _():
            lane = lane_iota(ROWS)
            for c in range(DC):
                here = flat_ref[pl.ds(src + c, ROWS, stride=DC), :]
                after = flat_ref[pl.ds(src + c + 1, ROWS, stride=DC), :]
                both = jnp.where(lane >= SKEW, here, after)
                tile_ref[dst + c] = pltpu.roll(both, LANES - SKEW, 1).astype(jnp.bfloat16)

        for code, tiles in ((KIND_L2, 2), (KIND_L3, 3)):

            @pl.when(kind == code)
            def _():
                for j in range(tiles):
                    tile_ref[dst + j] = flat_ref[pl.ds(src + ROWS * j, ROWS), :].astype(jnp.bfloat16)

        @pl.when(kind == KIND_B)
        def _():
            tall = 8 * pl.cdiv(FC, 8)
            lane = lane_iota(tall)
            row = lax.broadcasted_iota(jnp.int32, (tall, LANES), 0)
            keep = (row < FC - 1) | (lane < FF % LANES)
            for r, (base, skew) in enumerate(wide_rows()):
                part = flat_ref[pl.ds(src + base, tall), :]
                if skew:
                    after = flat_ref[pl.ds(src + base + 1, tall), :]
                    part = pltpu.roll(jnp.where(lane >= skew, part, after), LANES - skew, 1)
                stage_ref[pl.ds(r, tall, stride=ROWS), :] = jnp.where(keep, part, 0.0)
            for c in range(FC):
                tile_ref[dst + c] = stage_ref[pl.ds(ROWS * c, ROWS), :].astype(jnp.bfloat16)

        return 0

    lax.fori_loop(0, entries, unit, 0)


def to_flat_kernel(entries, rows, table_ref, tile_ref, *refs):
    if len(refs) == 5:
        tail_ref, line_ref, stage_ref, flat_ref, first_ref = refs
    else:
        line_ref, stage_ref, flat_ref = refs
    if len(refs) == 5:
        flat_ref[...] = jnp.zeros_like(flat_ref)

    def unit(i, _):
        kind, src, dst = (table_ref[3 * i + j] for j in range(3))

        @pl.when(kind == KIND_A)
        def _():
            for c in range(DC):
                flat_ref[pl.ds(src + c, ROWS, stride=DC), :] = tile_ref[dst + c]

        @pl.when(kind == KIND_D)
        def _():
            lane = lane_iota(ROWS)
            for c in range(DC):
                turned = pltpu.roll(tile_ref[dst + c], SKEW, 1)
                for step, keep in ((0, lane >= SKEW), (1, lane < SKEW)):
                    at = pl.ds(src + c + step, ROWS, stride=DC)
                    flat_ref[at, :] = jnp.where(keep, turned, flat_ref[at, :])

        for code, tiles in ((KIND_L2, 2), (KIND_L3, 3)):

            @pl.when(kind == code)
            def _():
                for j in range(tiles):
                    flat_ref[pl.ds(src + ROWS * j, ROWS), :] = tile_ref[dst + j]

        @pl.when(kind == KIND_B)
        def _():
            tall = 8 * pl.cdiv(FC, 8)
            lane = lane_iota(tall)
            row = lax.broadcasted_iota(jnp.int32, (tall, LANES), 0)
            for c in range(FC):
                stage_ref[pl.ds(ROWS * c, ROWS), :] = tile_ref[dst + c]
            for r, (base, skew) in enumerate(wide_rows()):
                turned = stage_ref[pl.ds(r, tall, stride=ROWS), :]
                if skew:
                    turned = pltpu.roll(turned, skew, 1)
                for step in range(2 if skew else 1):
                    entry = row * LANES + lane + (step * LANES - skew)
                    keep = (lane < skew if step else lane >= skew) & (entry < FF)
                    at = pl.ds(src + base + step, tall)
                    flat_ref[at, :] = jnp.where(keep, turned, flat_ref[at, :])

        return 0

    lax.fori_loop(0, entries, unit, 0)
    if len(refs) == 3:
        line_from_rows(flat_ref, line_ref, rows, HEAD)
        return
    rows_from_line(tail_ref, first_ref, 0, HEAD)
    entry = lax.broadcasted_iota(jnp.int32, (HEAD, LANES), 0) * LANES + lane_iota(HEAD)
    flat_ref[:HEAD] = jnp.where(entry < table_ref[3 * entries], first_ref[...], flat_ref[:HEAD])
    line_from_rows(flat_ref, line_ref, 0, rows)


def my_row(table):
    return lax.dynamic_index_in_dim(jnp.asarray(table), lax.axis_index("fsdp"), 0, keepdims=False)


def relayout_scratch(rows):
    return [
        pltpu.VMEM((ROWS * 8 * pl.cdiv(FC, 8), LANES), jnp.float32),
        pltpu.VMEM((8 * pl.cdiv(rows + HEAD + 8, 8), LANES), jnp.float32),
    ]


def to_tiles(line, plan):
    where, block, table, tails = plan
    count = lax.axis_size("fsdp")
    head = lax.ppermute(line[:, : HEAD * LANES], "fsdp", [(i, (i - 1) % count) for i in range(count)])
    vmem = pl.BlockSpec(memory_space=pltpu.VMEM)
    return pl.pallas_call(
        functools.partial(to_tiles_kernel, table.shape[1] // 3),
        out_shape=jax.ShapeDtypeStruct((block, ROWS, LANES), jnp.bfloat16),
        grid_spec=pltpu.PrefetchScalarGridSpec(
            num_scalar_prefetch=1, grid=(1,), in_specs=[vmem, vmem], out_specs=vmem,
            scratch_shapes=relayout_scratch(line.shape[1] // LANES),
        ),
        name="to_tiles",
    )(my_row(table), line, head)


def to_flat(tiles, plan, length):
    where, block, table, tails = plan
    count = lax.axis_size("fsdp")
    rows = length // LANES
    vmem = pl.BlockSpec(memory_space=pltpu.VMEM)
    last = [max(i for i in range(table.shape[1] // 3) if row[3 * i]) for row in table]
    last = np.stack([row[3 * i : 3 * i + 3] for row, i in zip(table, last)])
    whole = np.concatenate([table, np.roll(tails, 1)[:, None]], axis=1)

    def call(entries, mine, inputs, width, scratch, name):
        return pl.pallas_call(
            functools.partial(to_flat_kernel, entries, rows),
            out_shape=jax.ShapeDtypeStruct((1, width), jnp.float32),
            grid_spec=pltpu.PrefetchScalarGridSpec(
                num_scalar_prefetch=1, grid=(1,), in_specs=[vmem] * len(inputs), out_specs=vmem,
                scratch_shapes=relayout_scratch(rows) + scratch,
            ),
            name=name,
        )(my_row(mine), *inputs)

    tail = call(1, last, (tiles,), HEAD * LANES, [], "tail")
    tail = lax.ppermute(tail, "fsdp", [(i, (i + 1) % count) for i in range(count)])
    return call(table.shape[1] // 3, whole, (tiles, tail), length, [pltpu.VMEM((HEAD, LANES), jnp.float32)], "to_flat")


def place(me):
    return lax.rem(me, 2), lax.rem(me // 2, 2), lax.rem(me // 4, 2), me // 8


def index_of(core, x, y, z):
    return ((z * 2 + y) * 2 + x) * 2 + core


def greet(devices_and_conditions):
    barrier = pltpu.get_barrier_semaphore()
    for device, present in devices_and_conditions:
        if present is None:
            pl.semaphore_signal(barrier, inc=1, device_id=(device,), device_id_type=MESH)
        else:

            @pl.when(present)
            def _():
                pl.semaphore_signal(barrier, inc=1, device_id=(device,), device_id_type=MESH)

    present = [1 if p is None else p.astype(jnp.int32) for _, p in devices_and_conditions]
    pl.semaphore_wait(barrier, sum(present))


BF = jnp.bfloat16
F32 = jnp.float32
PAIR = 2 * LANES
SCALE = HEAD_DIM**-0.5
GELU_A = math.sqrt(2.0 / math.pi)
GELU_B = 0.044715
LOG2E = math.log2(math.e)
ANY = pl.BlockSpec(memory_space=pl.ANY)
VM = pl.BlockSpec(memory_space=pltpu.VMEM)
VMEM_LIMIT = 63 << 20


def nn(left, right):
    return lax.dot_general(left, right, (((1,), (0,)), ((), ())), preferred_element_type=F32)


def nt(left, right):
    return lax.dot_general(left, right, (((1,), (1,)), ((), ())), preferred_element_type=F32)


def runs_of(where, name):
    runs, done = [], 0
    for owner, at, tiles in where[name]:
        if runs and runs[-1][0] == owner and runs[-1][1] + runs[-1][2] == at:
            runs[-1][2] += tiles
        else:
            runs.append([owner, at, tiles, done])
        done += tiles
    return runs


def copies(where, name, blocks_ref, tiles_ref, sem, out=False):
    made = []
    flat_tiles = tiles_ref if len(tiles_ref.shape) == 3 else tiles_ref.reshape(-1, ROWS, LANES)
    for owner, at, tiles, done in runs_of(where, name):
        there, here = blocks_ref.at[owner, pl.ds(at, tiles)], flat_tiles.at[pl.ds(done, tiles)]
        made.append(pltpu.make_async_copy(here, there, sem) if out else pltpu.make_async_copy(there, here, sem))
    return made


def start(made):
    for copy in made:
        copy.start()


def wait(made):
    for copy in made:
        copy.wait()


def panel(tiles_ref, c, units, first=0):
    return tiles_ref[pl.ds(first, units), pl.ds(c, 1)].reshape(units * ROWS, LANES)


def panels(tiles_ref, c, many, units, first=0):
    return jnp.concatenate([panel(tiles_ref, c + i, units, first) for i in range(many)], axis=1)


def put_panel(tiles_ref, c, value, first=0):
    units = value.shape[0] // ROWS
    tiles_ref[pl.ds(first, units), pl.ds(c, 1)] = value.astype(BF).reshape(units, 1, ROWS, LANES)


def put_panels(tiles_ref, c, value, first=0):
    for i in range(value.shape[1] // LANES):
        put_panel(tiles_ref, c + i, value[:, i * LANES : (i + 1) * LANES], first)


def over_pairs(body):
    @pl.loop(0, DC // 2)
    def _(pair):
        body(2 * pair, 2)

    if DC % 2:
        body(DC - 1, 1)


def lanes_of(c, many):
    return pl.ds(c * LANES if isinstance(c, int) else pl.multiple_of(c * LANES, LANES), many * LANES)


def vector_rows(tiles_ref):
    return jnp.concatenate([tiles_ref[i].astype(F32) for i in range(tiles_ref.shape[0])], axis=0)


def as_row(rows, first, many):
    return jnp.concatenate([rows[first + i : first + i + 1] for i in range(many)], axis=1)


def put_vectors(tiles_ref, rows_list):
    parts = [row[:, i * LANES : (i + 1) * LANES] for row in rows_list for i in range(row.shape[1] // LANES)]
    missing = tiles_ref.shape[0] * ROWS - len(parts)
    whole = jnp.concatenate(parts + [jnp.zeros((missing, LANES), F32)] if missing else parts, axis=0)
    for i in range(tiles_ref.shape[0]):
        tiles_ref[i] = whole[i * ROWS : (i + 1) * ROWS].astype(BF)


def norm_rows(values):
    centre = values - jnp.mean(values, axis=-1, keepdims=True)
    inverse = lax.rsqrt(jnp.mean(centre * centre, axis=-1, keepdims=True) + EPS)
    return centre * inverse, inverse


def norm_rows_back(grad, normed, inverse, gain):
    scaled = grad * gain
    return inverse * (
        scaled - jnp.mean(scaled, axis=-1, keepdims=True) - normed * jnp.mean(scaled * normed, axis=-1, keepdims=True)
    )


def column_sums(values):
    return jnp.sum(values, axis=0, keepdims=True)


def head_window(h):
    block = jnp.minimum((h * HEAD_DIM) // LANES, DC - 2)
    lane = pl.multiple_of(block * LANES, LANES)
    return lane, h * HEAD_DIM - lane


def head_mask(rows, offset):
    lane = lax.broadcasted_iota(jnp.int32, (rows, PAIR), 1)
    return (lane >= offset) & (lane < offset + HEAD_DIM)


def front_kernel(
    where, x_ref, segq_ref, segk_ref, blocks_ref, q_ref, k_ref, v_ref, attended_ref, rest_ref, logs_ref,
    normed_ref, w_ref, vec1_ref, vec2_ref, bias_ref, score_ref, prob_ref, sem, vec_sem,
):
    window, rows = x_ref.shape[0], q_ref.shape[0]
    margin = (window - rows) // 2
    loads = [copies(where, name, blocks_ref, w_ref.at[i], sem.at[i]) for i, name in enumerate(("w_query", "w_key", "w_value"))]
    vecs = copies(where, "vec1", blocks_ref, vec1_ref, vec_sem) + copies(where, "vec2", blocks_ref, vec2_ref, vec_sem)
    start(vecs)
    for made in loads:
        start(made)
    wait(vecs)
    vec = vector_rows(vec1_ref)
    gain, shift = as_row(vec, 0, DC), as_row(vec, DC, DC)
    step = rows // 3

    @pl.loop(0, window // step)
    def _(i):
        at = pl.ds(i * step, step)
        normed, _ = norm_rows(x_ref[at].astype(F32))
        normed_ref[at] = (normed * gain + shift).astype(BF)

    @pl.loop(0, rows // 8)
    def _(i):
        at = pl.ds(i * 8, 8)
        bias_ref[at] = jnp.where(segq_ref[at] == segk_ref[...], 0.0, NEG)

    biases = vector_rows(vec2_ref)
    zero = jnp.zeros((1, D), F32)
    for made in loads:
        wait(made)
    for i, (out, add) in enumerate(((q_ref, as_row(biases, 0, DC)), (k_ref, zero), (v_ref, as_row(biases, DC, DC)))):
        for c in range(0, DC, 2):
            many = min(2, DC - c)
            lanes = slice(c * LANES, (c + many) * LANES)
            weights = panels(w_ref.at[i], c, many, D // ROWS)
            if i == 0:
                out[:, lanes] = (nn(normed_ref[pl.ds(margin, rows)], weights) + add[:, lanes]).astype(BF)
            else:

                @pl.loop(0, window // rows)
                def _(b):
                    at = pl.ds(b * rows, rows)
                    out[at, lanes] = (nn(normed_ref[at], weights) + add[:, lanes]).astype(BF)

    attended_ref[...] = jnp.zeros_like(attended_ref)
    rest_ref[...] = jnp.zeros_like(rest_ref)
    logs_ref[...] = jnp.zeros_like(logs_ref)
    lane_l = lax.broadcasted_iota(jnp.int32, logs_ref.shape, 1)

    @pl.loop(0, HEADS)
    def _(h):
        lane, offset = head_window(h)
        mask = head_mask(rows, offset)
        lanes = pl.ds(lane, PAIR)
        query = jnp.where(mask, q_ref[:, lanes], jnp.zeros((), BF))
        score_ref[...] = nt(query, k_ref[:, lanes]) * SCALE + bias_ref[...]
        top = jnp.max(score_ref[...], axis=-1, keepdims=True)
        powers = jnp.exp(score_ref[...] - top)
        total = jnp.sum(powers, axis=-1, keepdims=True)
        prob_ref[...] = powers.astype(BF)
        out = nn(prob_ref[...], v_ref[:, lanes]) / total
        rounded = out.astype(BF)
        attended_ref[:, lanes] = jnp.where(mask, rounded, attended_ref[:, lanes])
        rest_ref[:, lanes] = jnp.where(mask, (out - rounded.astype(F32)).astype(BF), rest_ref[:, lanes])
        logs_ref[...] = jnp.where(lane_l == h, top + jnp.log(total), logs_ref[...])


def front(x_win, seg_query, seg_keys, gathered, where, rows):
    window = x_win.shape[0]
    shape = lambda n, d=D, t=BF: jax.ShapeDtypeStruct((n, d), t)
    dma = pltpu.SemaphoreType.DMA
    units = D // ROWS
    return pl.pallas_call(
        functools.partial(front_kernel, where),
        out_shape=(shape(rows), shape(window), shape(window), shape(rows), shape(rows), shape(rows, LANES, F32)),
        in_specs=[VM, VM, VM, ANY],
        out_specs=[VM] * 6,
        scratch_shapes=[
            pltpu.VMEM((window, D), BF),
            pltpu.VMEM((3, units, DC, ROWS, LANES), BF), pltpu.VMEM((2, ROWS, LANES), BF), pltpu.VMEM((2, ROWS, LANES), BF),
            pltpu.VMEM((rows, window), F32), pltpu.VMEM((rows, window), F32), pltpu.VMEM((rows, window), BF), dma((3,)), dma,
        ],
        compiler_params=pltpu.CompilerParams(vmem_limit_bytes=VMEM_LIMIT),
        name="front",
    )(x_win, seg_query, seg_keys, gathered)


def middle_kernel(
    where, x_ref, cot_ref, attended_ref, rest_ref, blocks_ref, act_ref, mid_grad_ref, att_grad_ref, delta_ref, parts_ref,
    wo_ref, wu_ref, wd_ref, vec3_ref, vec4_ref, vec5_ref, b_up_ref, hidden_ref, slope_ref, pre_ref, normed_ref, normed_b_ref,
    mid_ref, g_up_ref, mid_b_ref, sem, out_sem,
):
    rows = x_ref.shape[0]
    units, f_units = D // ROWS, FF // ROWS
    names = ("w_out", "w_up", "w_down", "vec3", "vec4", "vec5")
    refs = (wo_ref, wu_ref, wd_ref, vec3_ref, vec4_ref, vec5_ref)
    loads = {n: copies(where, n, blocks_ref, r, sem.at[i]) for i, (n, r) in enumerate(zip(names, refs))}
    saves = {n: copies(where, n, parts_ref, r, out_sem, out=True) for n, r in zip(names, refs)}
    for n in ("vec3", "vec4", "vec5", "w_out", "w_up", "w_down"):
        start(loads[n])
    f_wide = FC * LANES
    pads = f_wide // ROWS - f_units
    wd_ref[pl.ds(f_units, pads)] = jnp.zeros((pads, DC, ROWS, LANES), BF)
    for n in ("vec3", "vec4", "vec5", "w_out"):
        wait(loads[n])
    vec = vector_rows(vec3_ref)
    b_out, gain, shift = (as_row(vec, i * DC, DC) for i in range(3))
    vec = vector_rows(vec4_ref)
    entry = lax.broadcasted_iota(jnp.int32, vec.shape, 0) * LANES + lax.broadcasted_iota(jnp.int32, vec.shape, 1)
    b_up_ref[...] = jnp.where(entry < FF, vec, 0.0)
    b_down = jnp.concatenate([vec5_ref[c].astype(F32)[0:1] for c in range(DC)], axis=1)

    for c in range(0, DC, 2):
        many = min(2, DC - c)
        lanes = slice(c * LANES, (c + many) * LANES)
        mid_ref[:, lanes] = (
            x_ref[:, lanes].astype(F32) + nn(attended_ref[...], panels(wo_ref, c, many, units)) + b_out[:, lanes]
        )
    normed, inverse = norm_rows(mid_ref[...])
    normed_ref[...] = normed
    normed_b_ref[...] = (normed * gain + shift).astype(BF)

    wait(loads["w_up"])

    @pl.loop(0, FC // 2)
    def _(p):
        at = pl.ds(pl.multiple_of(p * PAIR, PAIR), PAIR)
        bias = jnp.concatenate([b_up_ref[pl.ds(2 * p, 1)], b_up_ref[pl.ds(2 * p + 1, 1)]], axis=1)
        v = nn(normed_b_ref[...], panels(wu_ref, 2 * p, 2, units)) + bias
        square = v * v
        bent = jnp.tanh(GELU_A * v * (1.0 + GELU_B * square))
        hidden_ref[:, at] = (0.5 * v * (1.0 + bent)).astype(BF)
        slope_ref[:, at] = 0.5 * (1.0 + bent) + 0.5 * v * (1.0 - bent * bent) * (
            GELU_A * (1.0 + 3.0 * GELU_B * square)
        )

    wait(loads["w_down"])
    for c in range(0, DC, 2):
        many = min(2, DC - c)
        lanes = slice(c * LANES, (c + many) * LANES)
        act_ref[:, lanes] = (
            mid_ref[:, lanes] + nn(hidden_ref[...], panels(wd_ref, c, many, f_wide // ROWS)) + b_down[:, lanes]
        ).astype(BF)

    @pl.loop(0, FC // 2)
    def _(p):
        at = pl.ds(pl.multiple_of(p * PAIR, PAIR), PAIR)
        first = p * (PAIR // ROWS)
        grad = nt(cot_ref[...], panels(wd_ref, 0, DC, PAIR // ROWS, first)) * slope_ref[:, at]
        pre_ref[:, at] = grad.astype(BF)
        sums = column_sums(grad)
        g_up_ref[pl.ds(2 * p, 1)] = sums[:, :LANES]
        g_up_ref[pl.ds(2 * p + 1, 1)] = sums[:, LANES:]
        put_panels(wd_ref, 0, nn(hidden_ref[:, at].T, cot_ref[...]), first)

    start(saves["w_down"])
    put_vectors(vec4_ref, [b_up_row for b_up_row in [g_up_ref[i : i + 1] for i in range(FC)]])
    start(saves["vec4"])
    cot = cot_ref[...].astype(F32)
    sums = column_sums(cot)
    row0 = lax.broadcasted_iota(jnp.int32, (ROWS, LANES), 0) == 0
    for c in range(DC):
        vec5_ref[c] = jnp.where(row0, sums[:, c * LANES : (c + 1) * LANES], 0.0).astype(BF)
    start(saves["vec5"])

    for c in range(0, DC, 2):
        many = min(2, DC - c)
        weights = panels(wu_ref, 0, FC, many * LANES // ROWS, c * LANES // ROWS)
        mid_ref[:, c * LANES : (c + many) * LANES] = nt(pre_ref[...], weights)
    turned_b = normed_b_ref[...].T

    @pl.loop(0, FC // 2)
    def _(p):
        at = pl.ds(pl.multiple_of(p * PAIR, PAIR), PAIR)
        put_panels(wu_ref, 2 * p, nn(turned_b, pre_ref[:, at]))

    start(saves["w_up"])
    e = mid_ref[...]
    normed = normed_ref[...]
    g_gain, g_shift = column_sums(e * normed), column_sums(e)
    mid_grad = cot + norm_rows_back(e, normed, inverse, gain)
    mid_grad_ref[...] = mid_grad
    put_vectors(vec3_ref, [column_sums(mid_grad), g_gain, g_shift])
    start(saves["vec3"])
    mid_b = mid_grad.astype(BF)
    mid_b_ref[...] = mid_b

    def attended_grad(c, many):
        weights = panels(wo_ref, 0, DC, many * LANES // ROWS, c * (LANES // ROWS))
        att_grad_ref[:, lanes_of(c, many)] = nt(mid_b_ref[...], weights).astype(BF)

    over_pairs(attended_grad)
    product = att_grad_ref[...].astype(F32) * (attended_ref[...].astype(F32) + rest_ref[...].astype(F32))
    delta_ref[...] = jnp.sum(product.T.reshape(HEADS, HEAD_DIM, rows), axis=1)
    turned = attended_ref[...].T
    over_pairs(lambda c, many: put_panels(wo_ref, c, nn(turned, mid_b_ref[:, lanes_of(c, many)])))
    start(saves["w_out"])
    for n in names:
        wait(saves[n])


def middle(block_input, cotangent, attended, rest, gathered, where):
    rows = block_input.shape[0]
    shape = lambda t: jax.ShapeDtypeStruct((rows, D), t)
    dma = pltpu.SemaphoreType.DMA
    tiles = lambda *n: pltpu.VMEM((*n, ROWS, LANES), BF)
    units, f_wide = D // ROWS, FC * LANES
    return pl.pallas_call(
        functools.partial(middle_kernel, where),
        out_shape=(shape(BF), shape(F32), shape(BF), jax.ShapeDtypeStruct((HEADS, rows), F32), jax.ShapeDtypeStruct(gathered.shape, BF)),
        in_specs=[VM, VM, VM, VM, ANY],
        out_specs=[VM, VM, VM, VM, ANY],
        scratch_shapes=[
            tiles(units, DC), tiles(units, FC), tiles(f_wide // ROWS, DC), tiles(2), tiles(3), tiles(DC),
            pltpu.VMEM((3 * ROWS, LANES), F32), pltpu.VMEM((rows, f_wide), BF), pltpu.VMEM((rows, f_wide), F32),
            pltpu.VMEM((rows, f_wide), BF), pltpu.VMEM((rows, D), F32), pltpu.VMEM((rows, D), BF), pltpu.VMEM((rows, D), F32),
            pltpu.VMEM((3 * ROWS, LANES), F32), pltpu.VMEM((rows, D), BF), dma((6,)), dma,
        ],
        compiler_params=pltpu.CompilerParams(vmem_limit_bytes=VMEM_LIMIT),
        name="middle",
    )(block_input, cotangent, attended, rest, gathered)


def back_kernel(
    where, x_hbm_ref, segq_ref, segk_ref, blocks_ref, q_ref, k_ref, v_ref, grad_ref, logs_ref, parts_in_ref,
    near_ref, own_ref, parts_ref,
    w_ref, vec1_ref, vec2_ref, bias_ref, score_ref, prob_ref, turned_ref, dk_ref, dv_ref, dq_ref, part_ref, logs_t_ref, x_ref,
    sem, vec_sem, out_sem, x_sem,
):
    window, rows = x_ref.shape[0], q_ref.shape[0]
    margin = (window - rows) // 2
    units = D // ROWS
    names = ("w_query", "w_key", "w_value")
    loads = [copies(where, name, blocks_ref, w_ref.at[i], sem.at[i]) for i, name in enumerate(names)]
    vecs = copies(where, "vec1", blocks_ref, vec1_ref, vec_sem)
    start(vecs)
    for made in loads:
        start(made)
    x_load = pltpu.make_async_copy(x_hbm_ref, x_ref, x_sem)
    x_load.start()

    @pl.loop(0, window // LANES)
    def _(i):
        at = pl.ds(pl.multiple_of(i * LANES, LANES), LANES)
        bias_ref[at] = jnp.where(segk_ref[at] == segq_ref[...], 0.0, NEG)
        turned_ref[:, at] = k_ref[at].T
        dk_ref[at] = jnp.zeros((LANES, D), F32)
        dv_ref[at] = jnp.zeros((LANES, D), F32)

    logs_t_ref[...] = logs_ref[...].T

    @pl.loop(0, HEADS)
    def _(h):
        lane, offset = head_window(h)
        mask = head_mask(rows, offset)
        lanes = pl.ds(lane, PAIR)
        query = jnp.where(mask, q_ref[:, lanes], jnp.zeros((), BF))
        grad = jnp.where(mask, grad_ref[:, lanes], jnp.zeros((), BF))
        probs = jnp.exp(nt(k_ref[:, lanes], query) * SCALE + bias_ref[...] - logs_t_ref[pl.ds(h, 1)])
        score_ref[...] = probs
        prob_ref[...] = probs.astype(BF)
        prob_grad = nt(v_ref[:, lanes], grad)
        row_total = jnp.sum(score_ref[...] * prob_grad, axis=0, keepdims=True)
        dv_ref[:, lanes] += nn(prob_ref[...], grad)
        prob_ref[...] = (score_ref[...] * (prob_grad - row_total)).astype(BF)
        dk_ref[:, lanes] += nn(prob_ref[...], query)
        part_ref[...] = nn(turned_ref[lanes], prob_ref[...])
        at = pl.ds(pl.multiple_of(h * HEAD_DIM, 8), HEAD_DIM)
        dq_ref[at] = part_ref[pl.ds(pl.multiple_of(offset, 8), HEAD_DIM)]

    dq = dq_ref[...].T * SCALE
    g_query = column_sums(dq)
    dq_b = dq.astype(BF)
    wait(vecs)
    vec = vector_rows(vec1_ref)
    gain, shift = as_row(vec, 0, DC), as_row(vec, DC, DC)
    dk_b_ref, dv_b_ref = k_ref, v_ref
    x_load.wait()
    g_value = jnp.zeros((1, D), F32)
    step = rows // 3

    def rounded(i, total):
        at = pl.ds(pl.multiple_of(i * step, step), step)
        dk_b_ref[at] = (dk_ref[at] * SCALE).astype(BF)
        dv = dv_ref[at]
        dv_b_ref[at] = dv.astype(BF)
        normed, _ = norm_rows(x_ref[at].astype(F32))
        turned_ref[:, at] = (normed * gain + shift).astype(BF).T
        return total + column_sums(dv)

    g_value = lax.fori_loop(0, window // step, rounded, g_value)
    put_vectors(vec2_ref, [g_query, g_value])
    save = copies(where, "vec2", parts_ref, vec2_ref, out_sem, out=True)
    for made in loads:
        wait(made)
    for c in range(0, DC, 2):
        many = min(2, DC - c)
        lanes = slice(c * LANES, (c + many) * LANES)
        part = [panels(w_ref.at[i], 0, DC, many * LANES // ROWS, c * LANES // ROWS) for i in range(3)]

        @pl.loop(0, window // rows)
        def _(b):
            at = pl.ds(b * rows, rows)
            dk_ref[at, lanes] = nt(dk_b_ref[at], part[1]) + nt(dv_b_ref[at], part[2])

        dk_ref[pl.ds(margin, rows), lanes] += nt(dq_b, part[0])
    turned_own = turned_ref[:, pl.ds(margin, rows)]
    for c in range(0, DC, 2):
        many = min(2, DC - c)
        lanes = slice(c * LANES, (c + many) * LANES)
        put_panels(w_ref.at[0], c, nn(turned_own, dq_b[:, lanes]))
        put_panels(w_ref.at[1], c, nn(turned_ref[...], dk_b_ref[:, lanes]))
        put_panels(w_ref.at[2], c, nn(turned_ref[...], dv_b_ref[:, lanes]))
    for i, name in enumerate(names):
        save = save + copies(where, name, parts_ref, w_ref.at[i], out_sem, out=True)
    start(save)

    def norm_block(i, totals):
        at = pl.ds(pl.multiple_of(i * step, step), step)
        normed, inverse = norm_rows(x_ref[at].astype(F32))
        e = dk_ref[at]
        part = norm_rows_back(e, normed, inverse, gain)
        x_ref[at] = part.astype(BF)

        @pl.when((i >= margin // step) & (i < (margin + rows) // step))
        def _():
            own_ref[pl.ds(pl.multiple_of(i * step - margin, step), step)] = part

        return totals[0] + column_sums(e * normed), totals[1] + column_sums(e)

    zero = jnp.zeros((1, D), F32)
    g_gain, g_shift = lax.fori_loop(0, window // step, norm_block, (zero, zero))
    put_vectors(vec1_ref, [g_gain, g_shift])
    last = copies(where, "vec1", parts_ref, vec1_ref, out_sem, out=True)
    last = last + [pltpu.make_async_copy(x_ref, near_ref, x_sem)]
    start(last)
    wait(save + last)


def back(x_win, seg_query, seg_keys, gathered, queries, key_win, value_win, att_grad, logs, parts, where):
    window, rows = x_win.shape[0], queries.shape[0]
    dma = pltpu.SemaphoreType.DMA
    tiles = lambda *n: pltpu.VMEM((*n, ROWS, LANES), BF)
    vm = lambda a, b, t: pltpu.VMEM((a, b), t)
    return pl.pallas_call(
        functools.partial(back_kernel, where),
        out_shape=(
            jax.ShapeDtypeStruct((window, D), BF), jax.ShapeDtypeStruct((rows, D), F32), jax.ShapeDtypeStruct(parts.shape, BF),
        ),
        in_specs=[ANY, VM, VM, ANY, VM, VM, VM, VM, VM, ANY],
        out_specs=[ANY, VM, ANY],
        scratch_shapes=[
            tiles(3, D // ROWS, DC), tiles(2), tiles(2), vm(window, rows, F32), vm(window, rows, F32), vm(window, rows, BF),
            vm(D, window, BF), vm(window, D, F32), vm(window, D, F32), vm(D, rows, F32), vm(PAIR, rows, F32), vm(LANES, rows, F32),
            vm(window, D, BF), dma((3,)), dma, dma, dma,
        ],
        input_output_aliases={9: 2},
        compiler_params=pltpu.CompilerParams(vmem_limit_bytes=VMEM_LIMIT),
        name="back",
    )(x_win, seg_query, seg_keys, gathered, queries, key_win, value_win, att_grad, logs, parts)


HOT_NAMES = ("vec1", "w_query", "w_key", "w_value", "vec2")


def transfer_pieces(plan, depth):
    where = plan[0]
    count = plan[2].shape[0]
    hot, used = [0] * depth, [0] * depth
    for name in where:
        for owner, at, tiles in where[name]:
            level = owner * depth // count
            used[level] = max(used[level], at + tiles)
            if name in HOT_NAMES:
                hot[level] = max(hot[level], at + tiles)
    early = [(level, 0, h) for level, h in enumerate(hot) if h]
    late = [(level, h, u - h) for level, (h, u) in enumerate(zip(hot, used)) if h < u]
    return early, late


def cut(piece, many):
    level, first, tiles = piece
    half = tiles // 2
    edges = [half * i // (many // 2) for i in range(many // 2)] + [
        half + (tiles - half) * i // (many // 2) for i in range(many // 2 + 1)
    ]
    return [(level, first + a, b - a) for a, b in zip(edges[:-1], edges[1:])]


def gather_front_kernel(
    depth, where, early, late,
    block_ref, x_in_ref, segq_ref, segk_ref,
    out_ref, x_out_ref, turned_out_ref, keys_out_ref, k_out_ref, v_out_ref, x_got_ref, q_ref, attended_ref, rest_ref, logs_ref,
    z_send, z_recv, x_send, x_recv, y_send, y_recv, corner_send, corner_recv, line_send, line_recv, mate_send, mate_recv, w_send, w_recv,
    local_sem, stage_ref, both_ref, x_ref, turned_ref, normed_ref, w_ref, vec1_ref, vec2_ref, bias_ref, score_ref, prob_ref, add_ref, sem, vec_sem, x_sem, keys_sem,
):
    me = lax.axis_index("fsdp")
    count = 8 * depth
    core, x, y, z = place(me)
    mate, x_near, y_near = index_of(1 - core, x, y, z), index_of(core, 1 - x, y, z), index_of(core, x, 1 - y, z)
    up, down = me + 8, me - 8
    after, before = me + 2, me - 2
    has_after, has_before = after < count, before >= 0
    greet(
        [(mate, None), (x_near, None), (y_near, None), (down, z > 0), (up, z < depth - 1), (after, has_after), (before, has_before)]
    )
    pieces = early + late
    chunks = {p: cut(piece, 4) if piece[0] == 0 and p < len(early) else [piece] for p, piece in enumerate(pieces)}
    chunk_list = [(p, chunk) for p in chunks for chunk in chunks[p]]
    ids = {p: [i for i, (q, _) in enumerate(chunk_list) if q == p] for p in chunks}
    hot, cold = range(len(early)), range(len(early), len(pieces))
    hot_levels = {level for level, _, _ in early}

    def remote(source, target, send, recv, device):
        return pltpu.make_async_remote_copy(
            src_ref=source, dst_ref=target, send_sem=send, recv_sem=recv, device_id=(device,), device_id_type=MESH
        )

    def span(piece):
        return pl.ds(piece[1], piece[2])

    def halves(p):
        level, first, tiles = pieces[p]
        part = tiles // 2 if p in hot else tiles * 2 // 3
        return (level, first, part), (level, first + part, tiles - part)

    def column(level):
        return index_of(core, x, y, level)

    def from_x(level):
        return index_of(core, 1 - x, y, level)

    def from_y(level):
        return index_of(core, x, 1 - y, level)

    def across(level):
        return index_of(core, 1 - x, 1 - y, level)

    def pass_on(block, piece, send, recv, device, own=False):
        there = out_ref.at[block, span(piece)]
        return remote(block_ref.at[span(piece)] if own else there, there, send, recv, device)

    def z_copy(i, upward, own=False):
        piece = chunk_list[i][1]
        return pass_on(column(piece[0]), piece, z_send.at[i, 0 if upward else 1], z_recv.at[i], up if upward else down, own)

    def plane_copies(i, own=False):
        piece = chunk_list[i][1]
        block = column(piece[0])
        return (
            pass_on(block, piece, x_send.at[i], x_recv.at[i], x_near, own),
            pass_on(block, piece, y_send.at[i], y_recv.at[i], y_near, own),
            pass_on(block, piece, mate_send.at[0, i], mate_recv.at[0, i], mate, own),
        )

    def got(block, i, recv):
        piece = chunk_list[i][1]
        pass_on(block, piece, x_send.at[i], recv, me).wait_recv()

    def spread(i, own=False):
        for copy in plane_copies(i, own):
            copy.start()

    def z_pass(i):
        def run(zv):
            level = chunk_list[i][1][0]
            got(column(level), i, z_recv.at[i])
            if level < zv < depth - 1:
                z_copy(i, True).start()
            if 0 < zv < level:
                z_copy(i, False).start()

        return run

    def take(i):
        def run(zv):
            z_pass(i)(zv)
            spread(i)

        return run

    def later_spread(i):
        return lambda zv: spread(i)

    def by_plane(p, zv):
        return True

    def corner_copies(p):
        level = pieces[p][0]
        first, second = halves(p)
        return (
            pass_on(from_x(level), first, corner_send.at[p, 0], corner_recv.at[p, 0], y_near),
            pass_on(from_y(level), second, corner_send.at[p, 1], corner_recv.at[p, 1], x_near),
        )

    def corner_along_z(p, zv):
        level = pieces[p][0]
        ways = [up] * (level <= zv < depth - 1) + [down] * (0 < zv <= level)
        return [
            [
                pass_on(across(level), part, line_send.at[p, 2 * side + (way is up)], line_recv.at[p, side], way)
                for way in ways
            ]
            for side, part in enumerate(halves(p))
        ]

    def mate_copies(p):
        level = pieces[p][0]
        first, second = halves(p)
        return (
            pass_on(from_x(level), pieces[p], mate_send.at[1, p], mate_recv.at[1, p], mate),
            pass_on(from_y(level), pieces[p], mate_send.at[2, p], mate_recv.at[2, p], mate),
            pass_on(across(level), first, mate_send.at[3, p], mate_recv.at[3, p], mate),
            pass_on(across(level), second, mate_send.at[4, p], mate_recv.at[4, p], mate),
        )

    def beside(p):
        def run(zv):
            level = pieces[p][0]
            for i in ids[p]:
                got(from_x(level), i, x_recv.at[i])
            if by_plane(p, zv):
                corner_copies(p)[0].start()
            mate_copies(p)[0].start()
            for i in ids[p]:
                got(from_y(level), i, y_recv.at[i])
            if by_plane(p, zv):
                corner_copies(p)[1].start()
            mate_copies(p)[1].start()

        return run

    def corner(p):
        def run(zv):
            level = pieces[p][0]
            for side, part in enumerate(halves(p)):
                recv = corner_recv if by_plane(p, zv) else line_recv
                pass_on(across(level), part, corner_send.at[p, side], recv.at[p, side], me).wait_recv()
                if not by_plane(p, zv):
                    for copy in corner_along_z(p, zv)[side]:
                        copy.start()
                mate_copies(p)[2 + side].start()

        return run

    def from_mate(p):
        def run(zv):
            level = pieces[p][0]
            other = 1 - 2 * core
            for i in ids[p]:
                pass_on(column(level) + other, chunk_list[i][1], mate_send.at[0, i], mate_recv.at[0, i], me).wait_recv()
            first, second = halves(p)
            for slot, (block, piece) in enumerate(
                ((from_x(level), pieces[p]), (from_y(level), pieces[p]), (across(level), first), (across(level), second))
            ):
                pass_on(block + other, piece, mate_send.at[slot + 1, p], mate_recv.at[slot + 1, p], me).wait_recv()

        return run

    def own_spread(i):
        return lambda zv: spread(i, True)

    def own_up(i):
        return lambda zv: z_copy(i, True, True).start() if zv < depth - 1 else None

    def own_down(i):
        return lambda zv: z_copy(i, False, True).start() if zv > 0 else None

    def w_copy(slot, which, device, source=None):
        return remote(x_in_ref if source is None else source, x_got_ref.at[slot], w_send.at[which], w_recv.at[slot], device)

    def w_far(zv):
        @pl.when(has_after)
        def _():
            w_copy(0, 1, after).start()

        @pl.when(has_before)
        def _():
            w_copy(4, 2, before).start()

    def w_forward(core_index):
        slot = 0 if core_index else 4
        return w_copy(1 if core_index else 3, 3, mate, x_got_ref.at[slot])

    def w_wait(slot):
        w_copy(slot, 0, me).wait_recv()

    def w_middle(zv):
        @pl.when(has_before)
        def _():
            w_wait(0)

        @pl.when(has_after)
        def _():
            w_wait(4)

        @pl.when((core == 1) & has_before)
        def _():
            w_forward(1).start()

        @pl.when((core == 0) & has_after)
        def _():
            w_forward(0).start()

    stops = [61.0, 63.0, 68.0, 73.0, 95.0, 102.0, 110.0] + [110.0 + 2.7 * h for h in range(1, HEADS)]

    def lists(zv):
        own_hot = [p for p in hot if pieces[p][0] == zv]
        own_cold = [p for p in cold if pieces[p][0] == zv]
        far_hot = sorted((p for p in hot if pieces[p][0] != zv), key=lambda p: abs(pieces[p][0] - zv))
        far_cold = sorted((p for p in cold if pieces[p][0] != zv), key=lambda p: (abs(pieces[p][0] - zv), -pieces[p][0]))
        distance = {p: abs(pieces[p][0] - zv) for p in cold}
        at_once = own_cold if zv > depth // 2 else []
        after_hot = [p for p in own_cold if p not in at_once]
        first = []
        for p in own_hot:
            for i in ids[p]:
                first += [own_up(i), own_down(i), own_spread(i)]
        for p in own_cold:
            first += [own_down(i) for i in ids[p]]
        for p in at_once:
            first += [own_spread(i) for i in ids[p]]
        for p in far_hot:
            first += [take(i) for i in ids[p]]
        passed = {p for p in far_cold if distance[p] < 3 and (0 < zv < pieces[p][0] or pieces[p][0] < zv < depth - 1)}
        from_above = [p for p in far_cold if p in passed and pieces[p][0] == zv + 1]
        first += [z_pass(i) for p in from_above for i in ids[p]]
        for p in own_cold:
            first += [own_up(i) for i in ids[p]]
        order_hot = own_hot + far_hot
        first += [beside(p) for p in order_hot]
        first += [z_pass(i) for p in far_cold if p in passed and p not in from_above for i in ids[p]]
        take_or_spread = lambda p: [(later_spread if p in passed else take)(i) for i in ids[p]]
        first.append(w_far)
        for p in after_hot:
            first += [own_spread(i) for i in ids[p]]
        for p in far_cold:
            first += take_or_spread(p) if distance[p] == 1 else []
        first += [corner(p) for p in order_hot]
        first += [from_mate(p) for p in order_hot]
        timed = [(73.0, event) for p in far_cold if distance[p] > 1 for event in take_or_spread(p)]
        order = at_once + after_hot + far_cold
        timed += [((110.0, 120.8, 137.0, 145.0)[min(k, 3)], beside(p)) for k, p in enumerate(order)]
        timed += [((142.4, 150.5, 200.0)[min(k, 2)], corner(p)) for k, p in enumerate(order)]
        return first, sorted(timed, key=lambda entry: entry[0])

    plans = [lists(zv) for zv in range(depth)]

    def each_plane(events_of):
        for zv in range(depth):
            events = events_of(zv)
            if events:

                @pl.when(z == zv)
                def _():
                    for event in events:
                        event(zv)

    w_copy(1 + 2 * core, 0, mate).start()
    fill = pltpu.make_async_copy(block_ref, stage_ref, local_sem)
    fill.start()
    fill.wait()
    keep = pltpu.make_async_copy(stage_ref, out_ref.at[me], local_sem)
    keep.start()
    each_plane(lambda zv: plans[zv][0])
    keep.wait()

    near_sem = x_sem
    def service(stop):
        low = stops[stop - 1] if stop else -1.0
        high = stops[stop] if stop < len(stops) else 1e9
        each_plane(lambda zv: [event for time, event in plans[zv][1] if low < time <= high])

    rows, window = q_ref.shape[0], x_ref.shape[0]
    k_ref, v_ref = both_ref.at[0], both_ref.at[1]
    loads = [copies(where, name, out_ref, w_ref.at[i], sem.at[i]) for i, name in enumerate(("w_query", "w_key", "w_value"))]
    vecs = copies(where, "vec1", out_ref, vec1_ref, vec_sem) + copies(where, "vec2", out_ref, vec2_ref, vec_sem)
    start(vecs)
    for made in loads:
        start(made)

    def slot_rows(slot):
        return pl.ds(pl.multiple_of(slot * rows, rows), rows)

    def bring(slot, there=None):
        at = x_ref.at[slot_rows(slot)]
        if there is None:
            pltpu.make_async_copy(x_got_ref.at[slot], at, near_sem).start()
            return

        @pl.when(there)
        def _():
            pltpu.make_async_copy(x_got_ref.at[slot], at, near_sem).start()

        @pl.when(jnp.logical_not(there))
        def _():
            pltpu.make_async_copy(x_in_ref, at, near_sem).start()

    def brought(many):
        for _ in range(many):
            pltpu.make_async_copy(x_in_ref, x_ref.at[slot_rows(0)], near_sem).wait()

    mate_slot, far_slot = 3 - 2 * core, 1 + 2 * core
    w_wait(mate_slot)
    pltpu.make_async_copy(x_in_ref, x_ref.at[slot_rows(2)], near_sem).start()
    bring(mate_slot)
    brought(2)
    wait(vecs)
    vec = vector_rows(vec1_ref)
    gain, shift = as_row(vec, 0, DC), as_row(vec, DC, DC)
    biases = vector_rows(vec2_ref)
    step = rows // 3

    @pl.loop(0, rows // 8)
    def _(i):
        at = pl.ds(i * 8, 8)
        bias_ref[at] = jnp.where(segq_ref[at] == segk_ref[...], 0.0, NEG)

    def over_slots(slots, body):
        @pl.loop(0, len(slots))
        def _(i):
            slot = slots[-1]
            for k, other in enumerate(slots[:-1]):
                slot = jnp.where(i == k, other, slot)
            body(slot)

    def norm_slots(slots):
        def norm_slot(slot):
            @pl.loop(0, rows // step)
            def _(i):
                at = pl.ds(pl.multiple_of(slot * rows + i * step, step), step)
                normed, _ = norm_rows(x_ref[at].astype(F32))
                turned_ref[:, at] = normed.astype(BF).T
                normed_ref[at] = (normed * gain + shift).astype(BF)

        over_slots(slots, norm_slot)

    def project(i, slots):
        def some(c, many):
            lanes = lanes_of(c, many)
            weights = panels(w_ref.at[i], c, many, D // ROWS)

            def rows_of(slot):
                value = (nn(normed_ref[slot_rows(slot)], weights) + add_ref[i, 0:1, lanes]).astype(BF)
                if isinstance(i, int):
                    q_ref[:, lanes] = value
                else:
                    both_ref[i - 1, slot_rows(slot), lanes] = value

            over_slots(slots, rows_of)

        over_pairs(some)

    def keys_and_values(slots, between):
        @pl.loop(0, 2)
        def _(i):
            project(i + 1, slots)
            for k, action in enumerate(between):

                @pl.when(i == k)
                def _():
                    action()

    norm_slots([2, mate_slot])
    service(0)
    for made in loads:
        wait(made)
    for i, row in enumerate((as_row(biases, 0, DC), jnp.zeros((1, D), F32), as_row(biases, DC, DC))):
        add_ref[i, 0:1] = row
    project(0, [2])
    service(1)
    keys_and_values([2, mate_slot], [lambda: service(2), lambda: service(3)])
    w_middle(None)

    @pl.when((core == 0) & has_before)
    def _():
        w_wait(1)

    @pl.when((core == 1) & has_after)
    def _():
        w_wait(3)

    bring(0, has_before)
    bring(4, has_after)
    bring(far_slot, jnp.where(core == 0, has_before, has_after))
    brought(3)
    others = [0, 4, far_slot]
    norm_slots(others)
    saves = [pltpu.make_async_copy(x_ref, x_out_ref, local_sem), pltpu.make_async_copy(turned_ref, turned_out_ref, local_sem)]
    start(saves)
    service(4)
    k_save = pltpu.make_async_copy(k_ref, k_out_ref, keys_sem.at[0])

    def keys_done():
        service(5)
        k_save.start()

    keys_and_values(others, [keys_done])
    v_save = pltpu.make_async_copy(v_ref, v_out_ref, keys_sem.at[1])
    v_save.start()
    wait(saves)

    @pl.loop(0, window // LANES)
    def _(i):
        at = pl.ds(pl.multiple_of(i * LANES, LANES), LANES)
        turned_ref[:, at] = k_ref[at].T

    keys_save = pltpu.make_async_copy(turned_ref, keys_out_ref, keys_sem.at[2])
    keys_save.start()
    attended_ref[...] = jnp.zeros_like(attended_ref)
    rest_ref[...] = jnp.zeros_like(rest_ref)
    logs_ref[...] = jnp.zeros_like(logs_ref)
    lane_l = lax.broadcasted_iota(jnp.int32, logs_ref.shape, 1)

    @pl.loop(0, HEADS)
    def _(h):
        for at_head in range(HEADS):

            @pl.when(h == at_head)
            def _():
                service(6 + at_head)

        lane, offset = head_window(h)
        mask = head_mask(rows, offset)
        lanes = pl.ds(lane, PAIR)
        query = jnp.where(mask, q_ref[:, lanes], jnp.zeros((), BF))
        score_ref[...] = nt(query, k_ref[:, lanes]) * SCALE + bias_ref[...]
        top = jnp.max(score_ref[...], axis=-1, keepdims=True)
        powers = jnp.exp(score_ref[...] - top)
        total = jnp.sum(powers, axis=-1, keepdims=True)
        prob_ref[...] = powers.astype(BF)
        out = nn(prob_ref[...], v_ref[:, lanes]) / total
        rounded = out.astype(BF)
        attended_ref[:, lanes] = jnp.where(mask, rounded, attended_ref[:, lanes])
        rest_ref[:, lanes] = jnp.where(mask, (out - rounded.astype(F32)).astype(BF), rest_ref[:, lanes])
        logs_ref[...] = jnp.where(lane_l == h, top + jnp.log(total), logs_ref[...])

    service(len(stops))
    each_plane(lambda zv: [from_mate(p) for p in cold])

    def sent(zv):
        for i, (p, piece) in enumerate(chunk_list):
            for copy in plane_copies(i):
                copy.wait_send()
            level = piece[0]
            if zv < depth - 1 and level <= zv:
                z_copy(i, True).wait_send()
            if zv > 0 and level >= zv:
                z_copy(i, False).wait_send()
        for p in range(len(pieces)):
            for copy in mate_copies(p) + (corner_copies(p) if by_plane(p, zv) else ()):
                copy.wait_send()
            for copy in sum(corner_along_z(p, zv), []) if not by_plane(p, zv) else []:
                copy.wait_send()

    each_plane(lambda zv: [sent])
    w_copy(0, 0, mate).wait_send()

    @pl.when(has_after)
    def _():
        w_copy(0, 1, after).wait_send()

    @pl.when(has_before)
    def _():
        w_copy(4, 2, before).wait_send()

    @pl.when(jnp.where(core == 1, has_before, has_after))
    def _():
        w_forward(0).wait_send()

    wait([k_save, v_save, keys_save])


def gather_front(block, block_input, seg_query, seg_keys, plan):
    where = plan[0]
    count = lax.axis_size("fsdp")
    depth = count // 8
    rows, window = block_input.shape[0], seg_keys.shape[1]
    early, whole = transfer_pieces(plan, depth)
    late = whole
    shape = lambda n, d=D, t=BF: jax.ShapeDtypeStruct((n, d), t)
    dma = pltpu.SemaphoreType.DMA
    units = D // ROWS
    many = len(early) + len(late)
    chunks = many + 3 * sum(1 for piece in early if piece[0] == 0)
    got = jax.ShapeDtypeStruct((5, rows, D), BF)
    return pl.pallas_call(
        functools.partial(gather_front_kernel, depth, where, early, late),
        out_shape=(
            jax.ShapeDtypeStruct((count, *block.shape), BF), shape(window), shape(D, window), shape(D, window), shape(window), shape(window), got,
            shape(rows), shape(rows), shape(rows), shape(rows, LANES, F32),
        ),
        in_specs=[ANY, ANY, VM, VM],
        out_specs=[ANY] * 7 + [VM] * 4,
        scratch_shapes=[
            dma((chunks, 2)), dma((chunks,)), dma((chunks,)), dma((chunks,)), dma((chunks,)), dma((chunks,)),
            dma((many, 2)), dma((many, 2)), dma((many, 4)), dma((many, 2)), dma((5, chunks)), dma((5, chunks)), dma((4,)), dma((5,)),
            dma, pltpu.VMEM(block.shape, BF), pltpu.VMEM((2, window, D), BF),
            pltpu.VMEM((window, D), BF), pltpu.VMEM((D, window), BF), pltpu.VMEM((window, D), BF),
            pltpu.VMEM((3, units, DC, ROWS, LANES), BF), pltpu.VMEM((2, ROWS, LANES), BF), pltpu.VMEM((2, ROWS, LANES), BF),
            pltpu.VMEM((rows, window), F32), pltpu.VMEM((rows, window), F32), pltpu.VMEM((rows, window), BF), pltpu.VMEM((3, 8, D), F32),
            dma((3,)), dma, dma, dma((3,)),
        ],
        compiler_params=pltpu.CompilerParams(collective_id=0, has_side_effects=True, vmem_limit_bytes=VMEM_LIMIT),
        name="gather_front",
    )(block, block_input, seg_query, seg_keys)


def back_scatter_kernel(
    depth, where, early, late,
    x_hbm_ref, turned_hbm_ref, keys_hbm_ref, segq_ref, segk_ref, blocks_ref, q_ref, k_hbm_ref, v_hbm_ref, grad_ref, logs_ref, delta_ref, mid_hbm_ref, parts_in_ref,
    parts_ref, out_ref, in_grad_ref, mates, sums, halfs, fulls, lines, near_ref, near_got,
    w_ref, g_ref, vec1_ref, vec2_ref, score_ref, prob_ref, turned_ref, k_ref, v_ref, dq_ref, part_ref, logs_t_ref, x_ref, dq_b_ref,
    block_ref, mid_ref, g_value_ref, gain_acc, shift_acc, stage, total,
    mate_send, mate_recv, half_send, half_recv, full_send, full_recv, line_send, line_recv, near_send, near_recv,
    load_sem, store_sem, sem, vec_sem, out_sem, x_sem,
):
    me = lax.axis_index("fsdp")
    count = 8 * depth
    core, x, y, z = place(me)
    mate, x_near, y_near = index_of(1 - core, x, y, z), index_of(core, 1 - x, y, z), index_of(core, x, 1 - y, z)
    after, before = me + 2, me - 2
    has_after, has_before = after < count, before >= 0
    greet(
        [(mate, None), (x_near, None), (y_near, None), (me - 8, z > 0), (me + 8, z < depth - 1), (after, has_after), (before, has_before)]
    )
    pieces = early + late
    block_tiles = parts_ref.shape[1]
    early_ids, late_ids = range(len(early)), range(len(early), len(pieces))

    def remote(source, target, send, recv, device):
        return pltpu.make_async_remote_copy(
            src_ref=source, dst_ref=target, send_sem=send, recv_sem=recv, device_id=(device,), device_id_type=MESH
        )

    def owner(level, slot, which_core):
        return index_of(which_core, 1 - x if slot in (1, 3) else x, 1 - y if slot in (2, 3) else y, level)

    def at_plane(zv, run):
        @pl.when(z == zv)
        def _():
            run()

    def span(p, lo=0, many=None):
        _, first, tiles = pieces[p]
        return pl.ds(first + lo, tiles if many is None else many)

    def half_of(p):
        return pieces[p][2] // 2

    def to_mate(p, slot):
        level = pieces[p][0]
        return remote(
            parts_ref.at[owner(level, slot, 1 - core), span(p)], mates.at[level, slot, span(p)],
            mate_send.at[p, slot], mate_recv.at[p, slot], mate,
        )

    def half_out(p, side):
        level, _, tiles = pieces[p]
        part = span(p, half_of(p), tiles - half_of(p)) if side else span(p, 0, half_of(p))
        return remote(
            sums.at[level, 3, part], halfs.at[level, side, part], half_send.at[p, side], half_recv.at[p, side],
            x_near if side else y_near,
        )

    def full_out(p, side):
        level = pieces[p][0]
        return remote(
            sums.at[level, 1 + side, span(p)], fulls.at[level, side, span(p)], full_send.at[p, side], full_recv.at[p, side],
            y_near if side else x_near,
        )

    def subs(p):
        tiles = pieces[p][2]
        if p in early_ids or tiles < block_tiles // 3:
            return [(0, tiles)]
        return [(0, tiles // 2), (tiles // 2, tiles - tiles // 2)]

    def line_out(p, zv, sub):
        level = pieces[p][0]
        part = span(p, *subs(p)[sub])
        upward = level > zv
        slot = depth if not upward and level == zv - 1 else level
        side = 1 if slot == depth else 0
        return remote(
            sums.at[level, 0, part], lines.at[slot, part], line_send.at[p, sub], line_recv.at[p, 2 * sub + side],
            me + 8 if upward else me - 8,
        )

    def line_in(p, side, sub):
        level = pieces[p][0]
        slot = depth if side else level
        part = span(p, *subs(p)[sub])
        return remote(sums.at[level, 0, part], lines.at[slot, part], line_send.at[p, sub], line_recv.at[p, 2 * sub + side], me)

    def line_sides(p, zv):
        level = pieces[p][0]
        if level > zv:
            return [0] if zv > 0 else []
        if level < zv:
            return [0] if zv < depth - 1 else []
        return ([0] if zv > 0 else []) + ([1] if zv < depth - 1 else [])

    def extent(job):
        kind, p, sub = job
        return subs(p)[sub] if kind == 0 else (0, pieces[p][2])

    def sources(job, zv):
        kind, p, sub = job
        level, _, tiles = pieces[p]
        h = half_of(p)
        if kind == 0:
            lo, many = extent(job)
            part = span(p, lo, many)
            refs = [parts_ref.at[owner(level, 0, core), part], mates.at[level, 0, part]]
            refs += [fulls.at[level, side, part] for side in (0, 1)]
            refs += [lines.at[depth if side else level, part] for side in line_sides(p, zv)]
            return [(ref, 0, many) for ref in refs]
        found = [(parts_ref.at[owner(level, kind, core), span(p)], 0, tiles), (mates.at[level, kind, span(p)], 0, tiles)]
        if kind == 1:
            found.append((halfs.at[level, 0, span(p, 0, h)], 0, h))
        if kind == 2:
            found.append((halfs.at[level, 1, span(p, h, tiles - h)], h, tiles - h))
        return found

    def loads(job, zv, base):
        return [
            pltpu.make_async_copy(ref, stage.at[i, pl.ds(base + lo, many)], load_sem.at[1 if base else 0])
            for i, (ref, lo, many) in enumerate(sources(job, zv))
        ]

    def store(job, base):
        kind, p, sub = job
        lo, many = extent(job)
        return pltpu.make_async_copy(
            total.at[pl.ds(base, many)], sums.at[pieces[p][0], kind, span(p, lo, many)], store_sem.at[1 if base else 0]
        )

    def load(job, zv, base=0):
        kind, p, sub = job
        if sub == 0:
            to_mate(p, kind).wait_recv()
        if kind in (1, 2):
            half_out(p, kind - 1).wait_recv()
        made = loads(job, zv, base)
        if kind == 0:
            if sub == 0:
                for side in (0, 1):
                    full_out(p, side).wait_recv()
            start(made[:4])
            for copy, side in zip(made[4:], line_sides(p, zv)):
                line_in(p, side, sub).wait_recv()
                copy.start()
        else:
            start(made)

    def add(base, lo, many, slots, target, shift):
        def some(first, tiles):
            value = stage[slots[0], pl.ds(first, tiles)].astype(F32)
            for slot in slots[1:]:
                value = value + stage[slot, pl.ds(first, tiles)].astype(F32)
            target[pl.ds(first + shift, tiles)] = value.astype(target.dtype)

        group = 8

        @pl.loop(0, many // group)
        def _(i):
            some(base + lo + i * group, group)

        if many % group:
            some(base + lo + many // group * group, many % group)

    def finish(job, zv, base=0):
        kind, p, sub = job
        level, first, tiles = pieces[p]
        found = sources(job, zv)
        wait(loads(job, zv, base))
        final = kind == 0 and level == zv
        target, shift = (out_ref, first + extent(job)[0] - base) if final else (total, 0)
        edges = sorted({e for _, lo, many in found for e in (lo, lo + many)})
        for lo, hi in zip(edges[:-1], edges[1:]):
            slots = [i for i, (_, a, many) in enumerate(found) if a <= lo and hi <= a + many]
            add(base, lo, hi - lo, slots, target, shift)
        if not final:
            store(job, base).start()

    def send(job, zv, base=0):
        kind, p, sub = job
        if kind == 0 and pieces[p][0] == zv:
            return
        store(job, base).wait()
        if kind == 3:
            half_out(p, 0).start()
            half_out(p, 1).start()
        elif kind == 0:
            line_out(p, zv, sub).start()
        else:
            full_out(p, kind - 1).start()

    second = block_tiles // 2

    def run(jobs, zv):
        for job in jobs:
            load(job, zv)
            finish(job, zv)
            send(job, zv)

    def run_ahead(jobs, zv):
        bases = [second * (k % 2) for k in range(len(jobs))]
        for k, job in enumerate(jobs):
            if k == 0:
                load(job, zv, bases[k])
            if k + 1 < len(jobs):
                load(jobs[k + 1], zv, bases[k + 1])
            finish(job, zv, bases[k])
            if k:
                send(jobs[k - 1], zv, bases[k - 1])
        send(jobs[-1], zv, bases[-1])

    def along(p):
        return [(0, p, sub) for sub in range(len(subs(p)))]

    for p in early_ids:
        for slot in (3, 1, 2, 0):
            to_mate(p, slot).start()

    window, rows = k_ref.shape[0], q_ref.shape[0]
    margin = (window - rows) // 2
    names = ("w_query", "w_key", "w_value")
    k_load = [
        pltpu.make_async_copy(a, b, vec_sem)
        for a, b in ((k_hbm_ref, k_ref), (v_hbm_ref, v_ref), (keys_hbm_ref, turned_ref))
    ]
    start(k_load)
    weight_loads = [copies(where, name, blocks_ref, w_ref.at[i], sem.at[i]) for i, name in enumerate(names)]
    vecs = copies(where, "vec1", blocks_ref, vec1_ref, sem.at[3])
    start(vecs)
    for made in weight_loads:
        start(made)
    x_load = [pltpu.make_async_copy(x_hbm_ref, x_ref, x_sem)]
    start(x_load)
    logs_t_ref[...] = logs_ref[...].T * LOG2E
    g_value_ref[...] = jnp.zeros_like(g_value_ref)

    by_level = {pieces[p][0]: p for p in early_ids}
    a, b, c_ = (by_level[level] for level in sorted(by_level, reverse=True)[:3])
    table = [
        (-1, 0, 3, a, None), (0, 1, 3, b, None), (3, 4, 1, a, None), (4, 5, 2, a, None), (5, 6, 3, c_, None),
        (6, 7, 1, b, None), (7, 8, 2, b, None), (11, 12, 0, a, 0), (12, 13, 1, c_, None), (13, 14, 2, c_, None),
    ]

    def beside(h, which, action):
        for entry in table:
            if entry[which] < 0:
                continue
            kind, p, zv = entry[2:]
            job = (kind, p, 0)
            there = h == entry[which]
            if zv is not None:
                there = there & (z == zv)

            @pl.when(there)
            def _():
                action(job, zv)

    wait(k_load)
    load((3, a, 0), None)

    @pl.loop(0, HEADS)
    def _(h):
        beside(h, 1, finish)
        lane, offset = head_window(h)
        mask = head_mask(rows, offset)
        lanes = pl.ds(lane, PAIR)
        query = jnp.where(mask, q_ref[:, lanes], jnp.zeros((), BF))
        grad = jnp.where(mask, grad_ref[:, lanes], jnp.zeros((), BF))
        log_row, delta_row = logs_t_ref[pl.ds(h, 1)], delta_ref[pl.ds(h, 1)]
        blocks = [pl.ds(n * rows, rows) for n in range(window // rows)]
        for keys in blocks:
            together = jnp.concatenate([segk_ref[keys]] * (rows // LANES), axis=1) == segq_ref[...]
            probs = jnp.exp2(jnp.where(together, nt(k_ref[keys, lanes], query) * (SCALE * LOG2E) - log_row, NEG))
            prob_ref[keys] = probs.astype(BF)
            score_ref[keys] = (probs * (nt(v_ref[keys, lanes], grad) - delta_row)).astype(BF)
        beside(h, 1, send)
        beside(h, 0, load)
        side = head_mask(rows, offset)

        @pl.loop(0, window // rows)
        def _(n):
            keys = pl.ds(pl.multiple_of(n * rows, rows), rows)
            dv = nn(prob_ref[keys], grad)
            g_value_ref[:, lanes] += column_sums(dv)
            v_ref[keys, lanes] = jnp.where(side, dv.astype(BF), v_ref[keys, lanes])
            dk = nn(score_ref[keys], query) * SCALE
            k_ref[keys, lanes] = jnp.where(side, dk.astype(BF), k_ref[keys, lanes])
        tile = (h * HEAD_DIM) // ROWS * ROWS
        part_ref[...] = nn(turned_ref[pl.ds(pl.multiple_of(tile, ROWS), part_ref.shape[0])], score_ref[...])
        at = pl.ds(pl.multiple_of(h * HEAD_DIM, 8), HEAD_DIM)
        dq_ref[at] = part_ref[pl.ds(pl.multiple_of(h * HEAD_DIM - tile, 8), HEAD_DIM)]

    turned_load = pltpu.make_async_copy(turned_hbm_ref, turned_ref, vec_sem)
    turned_load.start()
    dq = dq_ref[...].T * SCALE
    put_vectors(vec2_ref, [column_sums(dq), g_value_ref[...]])
    saves = copies(where, "vec2", parts_ref, vec2_ref, out_sem.at[3], out=True)
    dq_b_ref[...] = dq.astype(BF)
    wait(vecs)
    vec = vector_rows(vec1_ref)
    gain, shift = as_row(vec, 0, DC), as_row(vec, DC, DC)
    gain_t, shift_t = (jnp.broadcast_to(v, (8, D)).T[:, :1] for v in (gain, shift))
    wait(x_load)
    step = rows // 3

    turned_load.wait()
    for made in weight_loads:
        wait(made)
    gain_acc[...] = jnp.zeros_like(gain_acc)
    shift_acc[...] = jnp.zeros_like(shift_acc)

    def plane_job(what, entries):
        for zv, p in entries:

            def go():
                job = (0, p, 0)
                if what == "load":
                    load(job, zv)
                else:
                    finish(job, zv)
                    send(job, zv)

            at_plane(zv, go)

    own = turned_ref[:, pl.ds(margin, rows)]
    made = []
    first_jobs, last_jobs = [(1, a), (0, b), (3, b)], [(0, c_), (3, c_)]
    for i, (left, right_ref) in enumerate(((own, dq_b_ref), (turned_ref, k_ref), (turned_ref, v_ref))):
        if i == 1:
            plane_job("load", first_jobs)
        if i == 2:
            plane_job("end", first_jobs)
            plane_job("load", last_jobs)
            wait(made[0])

        def project_back(c, many):
            right = right_ref[:, lanes_of(c, many)]
            raw = nn(left[...], right)
            summed = column_sums(right.astype(F32))
            put_panels(g_ref.at[i % 2], c, gain_t * raw + shift_t * summed)
            weights = panels(w_ref.at[i], c, many, D // ROWS).astype(F32)
            scaled, shifted = weights * raw, weights * summed
            for j in range(many):
                part = slice(j * LANES, (j + 1) * LANES)
                gain_acc[...] += scaled[:, part]
                shift_acc[...] += shifted[:, part]

        over_pairs(project_back)
        made.append(copies(where, names[i], parts_ref, g_ref.at[i % 2], out_sem.at[i], out=True))
        start(made[i])
    put_vectors(vec1_ref, [column_sums(gain_acc[...].T), column_sums(shift_acc[...].T)])
    saves = saves + copies(where, "vec1", parts_ref, vec1_ref, out_sem.at[3], out=True)
    start(saves)
    plane_job("end", last_jobs)
    wait(saves + made[1] + made[2])
    for slots in ((3,), (1, 2), (0,)):
        for p in late_ids:
            for slot in slots:
                to_mate(p, slot).start()

    def slot_rows(n):
        return pl.ds(pl.multiple_of(n * rows, rows), rows)

    def row_block(n, own=False):
        first = n * rows

        def project_back(c, many):
            part = lambda i: panels(w_ref.at[i], 0, DC, many * LANES // ROWS, c * (LANES // ROWS))
            value = nt(k_ref[slot_rows(n)], part(1)) + nt(v_ref[slot_rows(n)], part(2))
            if own:
                value = value + nt(dq_b_ref[...], part(0))
            block_ref[:, lanes_of(c, many)] = value

        over_pairs(project_back)

        @pl.loop(0, rows // step)
        def _(i):
            here = pl.ds(pl.multiple_of(i * step, step), step)
            there = pl.ds(pl.multiple_of(first + i * step, step), step)
            normed, inverse = norm_rows(x_ref[there].astype(F32))
            result = norm_rows_back(block_ref[here], normed, inverse, gain)
            if own:
                block_ref[here] = result
            else:
                x_ref[there] = result.astype(BF)

    def near_rows(slot):
        return x_ref.at[pl.ds(slot * rows, rows)]

    def near_save(slot):
        return pltpu.make_async_copy(near_rows(slot), near_ref.at[slot], x_sem)

    def near_copy(slot, which, device):
        return remote(near_ref.at[slot], near_got.at[which], near_send.at[which], near_recv.at[which], device)


    @pl.loop(0, 4)
    def _(i):
        row_block(jnp.where(i == 0, 0, jnp.where(i == 1, 4, 2 * i - 3)))

        @pl.when(i == 0)
        def _():
            run_ahead([(3, p, 0) for p in late_ids], None)

        @pl.when(i == 1)
        def _():
            at_plane(1, lambda: run([(0, b, 0)], 1))
            at_plane(2, lambda: run([(0, a, 0), (0, c_, 0)], 2))
            for p in late_ids:
                run_ahead([(1, p, 0), (2, p, 0)], None)

    sides = [near_save(slot) for slot in (0, 4, 1, 3)]
    start(sides)
    wait(sides)
    to_mate_itself, to_mate_shared = (3 - 2 * core), (1 + 2 * core)
    near_copy(to_mate_itself, 0, mate).start()
    near_copy(to_mate_shared, 1, mate).start()

    @pl.when((core == 0) & has_before)
    def _():
        near_copy(0, 2, before).start()

    @pl.when((core == 1) & has_after)
    def _():
        near_copy(4, 3, after).start()

    near_copy(0, 1, me).wait_recv()
    shared_slot = 4 - 4 * core
    fetch = pltpu.make_async_copy(near_got.at[1], k_ref.at[pl.ds(0, rows)], x_sem)
    fetch.start()
    fetch.wait()

    @pl.loop(0, rows // step)
    def _(i):
        here = pl.ds(pl.multiple_of(i * step, step), step)
        there = pl.ds(pl.multiple_of(shared_slot * rows + i * step, step), step)
        x_ref[there] = (x_ref[there].astype(F32) + k_ref[here].astype(F32)).astype(BF)

    shared_save = near_save(shared_slot)
    shared_save.start()
    shared_save.wait()

    @pl.when((core == 0) & has_after)
    def _():
        near_copy(4, 3, after).start()

    @pl.when((core == 1) & has_before)
    def _():
        near_copy(0, 2, before).start()

    def hops(p, zv):
        return zv if pieces[p][0] > zv else depth - 1 - zv

    def tail(zv, at_end):
        out = sorted((p for p in late_ids if pieces[p][0] != zv), key=lambda p: (hops(p, zv), p))
        if not at_end:
            return [job for p in out if hops(p, zv) == 0 for job in along(p)]
        own = [p for ids in (early_ids, late_ids) for p in ids if pieces[p][0] == zv]
        return [job for p in out + own if p in own or hops(p, zv) for job in along(p)]

    for zv in (0, depth - 1):
        at_plane(zv, lambda: run(tail(zv, False), zv))
    row_block(2, True)

    @pl.loop(0, rows // step)
    def _(i):
        here = pl.ds(pl.multiple_of(i * step, step), step)
        fetch_mid = pltpu.make_async_copy(mid_hbm_ref.at[here], mid_ref, x_sem)
        fetch_mid.start()
        fetch_mid.wait()
        block_ref[here] += mid_ref[...]

    for zv in range(depth):
        at_plane(zv, lambda: run(tail(zv, True), zv))

    near_copy(0, 0, me).wait_recv()

    @pl.when(has_after)
    def _():
        near_copy(0, 2, me).wait_recv()

    @pl.when(has_before)
    def _():
        near_copy(0, 3, me).wait_recv()

    for i, (which, there) in enumerate(((0, None), (2, has_after), (3, has_before))):
        target = k_ref.at[pl.ds(i * rows, rows)]
        if there is None:
            pltpu.make_async_copy(near_got.at[which], target, x_sem).start()
            continue

        @pl.when(there)
        def _():
            pltpu.make_async_copy(near_got.at[which], target, x_sem).start()

        @pl.when(jnp.logical_not(there))
        def _():
            pltpu.make_async_copy(near_ref.at[0], target, x_sem).start()

    for i in range(3):
        pltpu.make_async_copy(near_got.at[0], k_ref.at[pl.ds(i * rows, rows)], x_sem).wait()
    near_after, near_before = (jnp.where(there, 1.0, 0.0) for there in (has_after, has_before))

    @pl.loop(0, rows // step)
    def _(i):
        here = pl.ds(pl.multiple_of(i * step, step), step)
        value = block_ref[here] + k_ref[here].astype(F32)
        value = value + near_after * k_ref[pl.ds(pl.multiple_of(rows + i * step, step), step)].astype(F32)
        value = value + near_before * k_ref[pl.ds(pl.multiple_of(2 * rows + i * step, step), step)].astype(F32)
        in_grad_ref[here] = value.astype(BF)

    for p in range(len(pieces)):
        for slot in range(4):
            to_mate(p, slot).wait_send()
        for side in (0, 1):
            half_out(p, side).wait_send()
            full_out(p, side).wait_send()
        for zv in range(depth):
            if pieces[p][0] != zv:
                at_plane(zv, lambda: [line_out(p, zv, sub).wait_send() for sub in range(len(subs(p)))])
    near_copy(0, 0, mate).wait_send()
    near_copy(0, 1, mate).wait_send()

    @pl.when(has_before)
    def _():
        near_copy(0, 2, before).wait_send()

    @pl.when(has_after)
    def _():
        near_copy(4, 3, after).wait_send()


def back_scatter(x_win, turned, turned_keys, seg_query, seg_keys, gathered, queries, key_win, value_win, att_grad, logs, delta, mid_grad, parts, plan):
    where, block = plan[:2]
    window, rows = x_win.shape[0], queries.shape[0]
    seg_keys = jnp.broadcast_to(seg_keys, (window, LANES))
    count = lax.axis_size("fsdp")
    depth = count // 8
    hot, cold = transfer_pieces(plan, depth)
    early = sorted(cold, reverse=True)
    late = []
    for piece in sorted(hot, reverse=True):
        late += cut(piece, 2) if piece[2] > block // 2 else [piece]
    many = len(early) + len(late)
    dma = pltpu.SemaphoreType.DMA
    tiles = lambda *n: pltpu.VMEM((*n, ROWS, LANES), BF)
    vm = lambda a, b, t: pltpu.VMEM((a, b), t)
    hbm = lambda *n: jax.ShapeDtypeStruct((*n, ROWS, LANES), BF)
    return pl.pallas_call(
        functools.partial(back_scatter_kernel, depth, where, early, late),
        out_shape=(
            jax.ShapeDtypeStruct(parts.shape, BF), jax.ShapeDtypeStruct((block, ROWS, LANES), F32), jax.ShapeDtypeStruct((rows, D), BF),
            hbm(depth, 4, block), hbm(depth, 4, block), hbm(depth, 2, block), hbm(depth, 2, block), hbm(depth + 1, block),
            jax.ShapeDtypeStruct((5, rows, D), BF), jax.ShapeDtypeStruct((4, rows, D), BF),
        ),
        in_specs=[ANY, ANY, ANY, VM, VM, ANY, VM, ANY, ANY, VM, VM, VM, ANY, ANY],
        out_specs=[ANY, VM, VM] + [ANY] * 7,
        scratch_shapes=[
            tiles(3, D // ROWS, DC), tiles(2, D // ROWS, DC), tiles(2), tiles(2),
            vm(window, rows, BF), vm(window, rows, BF), vm(D, window, BF), vm(window, D, BF), vm(window, D, BF),
            vm(D, rows, F32), vm(ROWS * pl.cdiv(HEAD_DIM + 8, ROWS), rows, F32), vm(LANES, rows, F32), vm(window, D, BF), vm(rows, D, BF), vm(rows, D, F32), vm(rows // 3, D, F32),
            vm(1, D, F32), vm(D, LANES, F32), vm(D, LANES, F32), tiles(6, block), tiles(block),
            dma((many, 4)), dma((many, 4)), dma((many, 2)), dma((many, 2)), dma((many, 2)), dma((many, 2)), dma((many, 2)), dma((many, 4)),
            dma((4,)), dma((4,)), dma((2,)), dma((2,)), dma((4,)), dma, dma((4,)), dma,
        ],
        input_output_aliases={13: 0},
        compiler_params=pltpu.CompilerParams(collective_id=1, has_side_effects=True, vmem_limit_bytes=VMEM_LIMIT),
        name="back_scatter",
    )(x_win, turned, turned_keys, seg_query, seg_keys, gathered, queries, key_win, value_win, att_grad, logs, delta, mid_grad, parts)[1:3]


def passed_along(value, steps):
    count = lax.axis_size("fsdp")
    first, last = (max(0, -steps), min(count, count - steps))
    return lax.ppermute(value, "fsdp", [(source, source + steps) for source in range(first, last)])


def window_of(rows):
    near = [rows if k == 0 else passed_along(rows, -k) for k in range(-REACH, REACH + 1)]
    return jnp.concatenate(near, axis=0)


def shards(kernels, block_input, params, cotangent, segment_ids):
    count = lax.axis_size("fsdp")
    me = lax.axis_index("fsdp")
    rows = block_input.shape[0]
    margin = REACH * rows
    seg_pad = jnp.pad(segment_ids, (margin, margin), constant_values=-1)
    seg_query = lax.dynamic_slice_in_dim(segment_ids, me * rows, rows, 0)
    seg_keys = lax.dynamic_slice_in_dim(seg_pad, me * rows, 2 * margin + rows, 0)
    plan = wire_plan(count, params.shape[1])
    where = plan[0]
    block = to_tiles(params, plan)
    if kernels:
        gathered, x_win, turned, turned_keys, key_win, value_win, _, queries, attended, rest, logs = gather_front(
            block, block_input, seg_query[:, None], seg_keys[None, :], plan
        )
    else:
        x_win = window_of(block_input)
        gathered = lax.all_gather(block, "fsdp", axis=0, tiled=False)
        queries, key_win, value_win, attended, rest, logs = front(
            x_win, seg_query[:, None], seg_keys[None, :], gathered, where, rows
        )
    activations, mid_grad, att_grad, delta, parts = middle(block_input, cotangent, attended, rest, gathered, where)
    sides = (seg_query[None, :], seg_keys[:, None], gathered, queries, key_win, value_win, att_grad, logs)
    if kernels:
        summed, input_grad = back_scatter(x_win, turned, turned_keys, *sides, delta, mid_grad, parts, plan)
    else:
        near, own, parts = back(x_win, *sides, parts, where)
        input_grad = mid_grad + own
        for k in range(-REACH, REACH + 1):
            if k != 0:
                part = near[(k + REACH) * rows : (k + REACH + 1) * rows]
                input_grad = input_grad + passed_along(part, k).astype(jnp.float32)
        input_grad = input_grad.astype(jnp.bfloat16)
        received = lax.all_to_all(parts, "fsdp", split_axis=0, concat_axis=0, tiled=True)
        summed = jnp.sum(received.astype(jnp.float32), axis=0)
    param_grads = to_flat(summed, plan, params.shape[1])
    return (activations, input_grad, param_grads)


def two_by_two(mesh):
    spans = np.array([device.coords for device in mesh.devices.flat])
    return tuple(spans.max(axis=0) - spans.min(axis=0))[:2] == (1, 1)


def solution(mesh):
    return jax.shard_map(
        functools.partial(shards, two_by_two(mesh)),
        mesh=mesh,
        in_specs=(P("fsdp", None), P(None, "fsdp"), P("fsdp", None), P()),
        out_specs=(P("fsdp", None), P("fsdp", None), P(None, "fsdp")),
        check_vma=False,
    )
```

```python
import functools
import math

import jax
import jax.numpy as jnp
import numpy as np
from jax import lax
from jax.experimental import pallas as pl
from jax.experimental.pallas import tpu as pltpu
from jax.sharding import PartitionSpec as P

D = 1152
HEADS = 16
HEAD_DIM = 72
FF = 4304
REACH = 2


EPS = 1e-06
NEG = -1e30
LANES = 128
ROWS = 16
DC = D // LANES
FC = -(-FF // LANES)
WIDE = FF * ROWS // LANES
HEAD = 544
KIND_A, KIND_D, KIND_L2, KIND_L3, KIND_B = 1, 2, 3, 4, 5
MESH = pl.DeviceIdType.MESH


def units():
    found = []
    offset = 0

    def matrix(name, kind, rows, width, tiles):
        nonlocal offset
        for row in range(0, rows, ROWS):
            found.append((name, kind, offset + row * width, tiles))
        offset += rows * width

    def vectors(name, kind, length, tiles):
        nonlocal offset
        found.append((name, kind, offset, tiles))
        offset += length

    vectors("vec1", KIND_L2, 2 * D, 2)
    matrix("w_query", KIND_A, D, D, DC)
    matrix("w_key", KIND_A, D, D, DC)
    matrix("w_value", KIND_A, D, D, DC)
    vectors("vec2", KIND_L2, 2 * D, 2)
    matrix("w_out", KIND_A, D, D, DC)
    vectors("vec3", KIND_L2, 3 * D, 2)
    matrix("w_up", KIND_B, D, FF, FC)
    vectors("vec4", KIND_L3, FF, 3)
    matrix("w_down", KIND_D, FF, D, DC)
    vectors("vec5", KIND_D, D, DC)
    return found


def unit_width(name):
    return {"vec1": 2 * D, "vec2": 2 * D, "vec3": 3 * D, "vec4": FF, "vec5": D, "w_up": ROWS * FF}.get(
        name, ROWS * D
    )


def wire_plan(count, shard):
    blocks = [[] for _ in range(count)]
    where = {}
    used = [0] * count
    tails = [0] * count
    for name, kind, first, tiles in units():
        owner = first // shard
        where.setdefault(name, []).append((owner, used[owner], tiles))
        blocks[owner].append((kind, (first - owner * shard) // LANES, used[owner]))
        used[owner] += tiles
        tails[owner] = max(0, first + unit_width(name) - (owner + 1) * shard)
    block = max(used)
    block += block % 2
    most = max(len(b) for b in blocks)
    table = np.zeros((count, 3 * most), np.int32)
    for owner, entries in enumerate(blocks):
        for i, entry in enumerate(entries):
            table[owner, 3 * i : 3 * i + 3] = entry
    return where, block, table, np.array(tails, np.int32)


def lane_iota(rows):
    return lax.broadcasted_iota(jnp.int32, (rows, LANES), 1)


def wide_rows():
    return [divmod(row * FF, LANES) for row in range(ROWS)]


SKEW = (D * 0 + 80) % LANES


def rows_from_line(line_ref, flat_ref, first, rows):
    step = 8 * LANES

    @pl.loop(0, rows // 8)
    def _(i):
        part = line_ref[:, pl.ds(pl.multiple_of(i * step, step), step)].astype(jnp.float32)
        flat_ref[pl.ds(first + i * 8, 8)] = part.reshape(8, LANES)

    for row in range(rows // 8 * 8, rows):
        flat_ref[pl.ds(first + row, 1)] = line_ref[:, row * LANES : (row + 1) * LANES].astype(jnp.float32)


def line_from_rows(flat_ref, line_ref, first, rows):
    step = 8 * LANES

    @pl.loop(0, rows // 8)
    def _(i):
        part = flat_ref[pl.ds(first + i * 8, 8)]
        line_ref[:, pl.ds(pl.multiple_of(i * step, step), step)] = part.reshape(1, step)

    for row in range(rows // 8 * 8, rows):
        line_ref[:, row * LANES : (row + 1) * LANES] = flat_ref[pl.ds(first + row, 1)]


def to_tiles_kernel(entries, table_ref, line_ref, head_ref, tile_ref, stage_ref, flat_ref):
    rows = line_ref.shape[1] // LANES
    rows_from_line(line_ref, flat_ref, 0, rows)
    rows_from_line(head_ref, flat_ref, rows, HEAD)

    def unit(i, _):
        kind, src, dst = (table_ref[3 * i + j] for j in range(3))

        @pl.when(kind == KIND_A)
        def _():
            for c in range(DC):
                tile_ref[dst + c] = flat_ref[pl.ds(src + c, ROWS, stride=DC), :].astype(jnp.bfloat16)

        @pl.when(kind == KIND_D)
        def _():
            lane = lane_iota(ROWS)
            for c in range(DC):
                here = flat_ref[pl.ds(src + c, ROWS, stride=DC), :]
                after = flat_ref[pl.ds(src + c + 1, ROWS, stride=DC), :]
                both = jnp.where(lane >= SKEW, here, after)
                tile_ref[dst + c] = pltpu.roll(both, LANES - SKEW, 1).astype(jnp.bfloat16)

        for code, tiles in ((KIND_L2, 2), (KIND_L3, 3)):

            @pl.when(kind == code)
            def _():
                for j in range(tiles):
                    tile_ref[dst + j] = flat_ref[pl.ds(src + ROWS * j, ROWS), :].astype(jnp.bfloat16)

        @pl.when(kind == KIND_B)
        def _():
            tall = 8 * pl.cdiv(FC, 8)
            lane = lane_iota(tall)
            row = lax.broadcasted_iota(jnp.int32, (tall, LANES), 0)
            keep = (row < FC - 1) | (lane < FF % LANES)
            for r, (base, skew) in enumerate(wide_rows()):
                part = flat_ref[pl.ds(src + base, tall), :]
                if skew:
                    after = flat_ref[pl.ds(src + base + 1, tall), :]
                    part = pltpu.roll(jnp.where(lane >= skew, part, after), LANES - skew, 1)
                stage_ref[pl.ds(r, tall, stride=ROWS), :] = jnp.where(keep, part, 0.0)
            for c in range(FC):
                tile_ref[dst + c] = stage_ref[pl.ds(ROWS * c, ROWS), :].astype(jnp.bfloat16)

        return 0

    lax.fori_loop(0, entries, unit, 0)


def to_flat_kernel(entries, rows, table_ref, tile_ref, *refs):
    if len(refs) == 5:
        tail_ref, line_ref, stage_ref, flat_ref, first_ref = refs
    else:
        line_ref, stage_ref, flat_ref = refs
    if len(refs) == 5:
        flat_ref[...] = jnp.zeros_like(flat_ref)

    def unit(i, _):
        kind, src, dst = (table_ref[3 * i + j] for j in range(3))

        @pl.when(kind == KIND_A)
        def _():
            for c in range(DC):
                flat_ref[pl.ds(src + c, ROWS, stride=DC), :] = tile_ref[dst + c]

        @pl.when(kind == KIND_D)
        def _():
            lane = lane_iota(ROWS)
            for c in range(DC):
                turned = pltpu.roll(tile_ref[dst + c], SKEW, 1)
                for step, keep in ((0, lane >= SKEW), (1, lane < SKEW)):
                    at = pl.ds(src + c + step, ROWS, stride=DC)
                    flat_ref[at, :] = jnp.where(keep, turned, flat_ref[at, :])

        for code, tiles in ((KIND_L2, 2), (KIND_L3, 3)):

            @pl.when(kind == code)
            def _():
                for j in range(tiles):
                    flat_ref[pl.ds(src + ROWS * j, ROWS), :] = tile_ref[dst + j]

        @pl.when(kind == KIND_B)
        def _():
            tall = 8 * pl.cdiv(FC, 8)
            lane = lane_iota(tall)
            row = lax.broadcasted_iota(jnp.int32, (tall, LANES), 0)
            for c in range(FC):
                stage_ref[pl.ds(ROWS * c, ROWS), :] = tile_ref[dst + c]
            for r, (base, skew) in enumerate(wide_rows()):
                turned = stage_ref[pl.ds(r, tall, stride=ROWS), :]
                if skew:
                    turned = pltpu.roll(turned, skew, 1)
                for step in range(2 if skew else 1):
                    entry = row * LANES + lane + (step * LANES - skew)
                    keep = (lane < skew if step else lane >= skew) & (entry < FF)
                    at = pl.ds(src + base + step, tall)
                    flat_ref[at, :] = jnp.where(keep, turned, flat_ref[at, :])

        return 0

    lax.fori_loop(0, entries, unit, 0)
    if len(refs) == 3:
        line_from_rows(flat_ref, line_ref, rows, HEAD)
        return
    rows_from_line(tail_ref, first_ref, 0, HEAD)
    entry = lax.broadcasted_iota(jnp.int32, (HEAD, LANES), 0) * LANES + lane_iota(HEAD)
    flat_ref[:HEAD] = jnp.where(entry < table_ref[3 * entries], first_ref[...], flat_ref[:HEAD])
    line_from_rows(flat_ref, line_ref, 0, rows)


def my_row(table):
    return lax.dynamic_index_in_dim(jnp.asarray(table), lax.axis_index("fsdp"), 0, keepdims=False)


def relayout_scratch(rows):
    return [
        pltpu.VMEM((ROWS * 8 * pl.cdiv(FC, 8), LANES), jnp.float32),
        pltpu.VMEM((8 * pl.cdiv(rows + HEAD + 8, 8), LANES), jnp.float32),
    ]


def to_tiles(line, plan):
    where, block, table, tails = plan
    count = lax.axis_size("fsdp")
    head = lax.ppermute(line[:, : HEAD * LANES], "fsdp", [(i, (i - 1) % count) for i in range(count)])
    vmem = pl.BlockSpec(memory_space=pltpu.VMEM)
    return pl.pallas_call(
        functools.partial(to_tiles_kernel, table.shape[1] // 3),
        out_shape=jax.ShapeDtypeStruct((block, ROWS, LANES), jnp.bfloat16),
        grid_spec=pltpu.PrefetchScalarGridSpec(
            num_scalar_prefetch=1, grid=(1,), in_specs=[vmem, vmem], out_specs=vmem,
            scratch_shapes=relayout_scratch(line.shape[1] // LANES),
        ),
        name="to_tiles",
    )(my_row(table), line, head)


def to_flat(tiles, plan, length):
    where, block, table, tails = plan
    count = lax.axis_size("fsdp")
    rows = length // LANES
    vmem = pl.BlockSpec(memory_space=pltpu.VMEM)
    last = [max(i for i in range(table.shape[1] // 3) if row[3 * i]) for row in table]
    last = np.stack([row[3 * i : 3 * i + 3] for row, i in zip(table, last)])
    whole = np.concatenate([table, np.roll(tails, 1)[:, None]], axis=1)

    def call(entries, mine, inputs, width, scratch, name):
        return pl.pallas_call(
            functools.partial(to_flat_kernel, entries, rows),
            out_shape=jax.ShapeDtypeStruct((1, width), jnp.float32),
            grid_spec=pltpu.PrefetchScalarGridSpec(
                num_scalar_prefetch=1, grid=(1,), in_specs=[vmem] * len(inputs), out_specs=vmem,
                scratch_shapes=relayout_scratch(rows) + scratch,
            ),
            name=name,
        )(my_row(mine), *inputs)

    tail = call(1, last, (tiles,), HEAD * LANES, [], "tail")
    tail = lax.ppermute(tail, "fsdp", [(i, (i + 1) % count) for i in range(count)])
    return call(table.shape[1] // 3, whole, (tiles, tail), length, [pltpu.VMEM((HEAD, LANES), jnp.float32)], "to_flat")


def place(me):
    return lax.rem(me, 2), lax.rem(me // 2, 2), lax.rem(me // 4, 2), me // 8


def index_of(core, x, y, z):
    return ((z * 2 + y) * 2 + x) * 2 + core


def greet(devices_and_conditions):
    barrier = pltpu.get_barrier_semaphore()
    for device, present in devices_and_conditions:
        if present is None:
            pl.semaphore_signal(barrier, inc=1, device_id=(device,), device_id_type=MESH)
        else:

            @pl.when(present)
            def _():
                pl.semaphore_signal(barrier, inc=1, device_id=(device,), device_id_type=MESH)

    present = [1 if p is None else p.astype(jnp.int32) for _, p in devices_and_conditions]
    pl.semaphore_wait(barrier, sum(present))


BF = jnp.bfloat16
F32 = jnp.float32
PAIR = 2 * LANES
SCALE = HEAD_DIM**-0.5
GELU_A = math.sqrt(2.0 / math.pi)
GELU_B = 0.044715
LOG2E = math.log2(math.e)
ANY = pl.BlockSpec(memory_space=pl.ANY)
VM = pl.BlockSpec(memory_space=pltpu.VMEM)
VMEM_LIMIT = 63 << 20


def nn(left, right):
    return lax.dot_general(left, right, (((1,), (0,)), ((), ())), preferred_element_type=F32)


def nt(left, right):
    return lax.dot_general(left, right, (((1,), (1,)), ((), ())), preferred_element_type=F32)


def runs_of(where, name):
    runs, done = [], 0
    for owner, at, tiles in where[name]:
        if runs and runs[-1][0] == owner and runs[-1][1] + runs[-1][2] == at:
            runs[-1][2] += tiles
        else:
            runs.append([owner, at, tiles, done])
        done += tiles
    return runs


def copies(where, name, blocks_ref, tiles_ref, sem, out=False):
    made = []
    flat_tiles = tiles_ref if len(tiles_ref.shape) == 3 else tiles_ref.reshape(-1, ROWS, LANES)
    for owner, at, tiles, done in runs_of(where, name):
        there, here = blocks_ref.at[owner, pl.ds(at, tiles)], flat_tiles.at[pl.ds(done, tiles)]
        made.append(pltpu.make_async_copy(here, there, sem) if out else pltpu.make_async_copy(there, here, sem))
    return made


def start(made):
    for copy in made:
        copy.start()


def wait(made):
    for copy in made:
        copy.wait()


def panel(tiles_ref, c, units, first=0):
    return tiles_ref[pl.ds(first, units), pl.ds(c, 1)].reshape(units * ROWS, LANES)


def panels(tiles_ref, c, many, units, first=0):
    return jnp.concatenate([panel(tiles_ref, c + i, units, first) for i in range(many)], axis=1)


def put_panel(tiles_ref, c, value, first=0):
    units = value.shape[0] // ROWS
    tiles_ref[pl.ds(first, units), pl.ds(c, 1)] = value.astype(BF).reshape(units, 1, ROWS, LANES)


def put_panels(tiles_ref, c, value, first=0):
    for i in range(value.shape[1] // LANES):
        put_panel(tiles_ref, c + i, value[:, i * LANES : (i + 1) * LANES], first)


def over_pairs(body):
    @pl.loop(0, DC // 2)
    def _(pair):
        body(2 * pair, 2)

    if DC % 2:
        body(DC - 1, 1)


def lanes_of(c, many):
    return pl.ds(c * LANES if isinstance(c, int) else pl.multiple_of(c * LANES, LANES), many * LANES)


def vector_rows(tiles_ref):
    return jnp.concatenate([tiles_ref[i].astype(F32) for i in range(tiles_ref.shape[0])], axis=0)


def as_row(rows, first, many):
    return jnp.concatenate([rows[first + i : first + i + 1] for i in range(many)], axis=1)


def put_vectors(tiles_ref, rows_list):
    parts = [row[:, i * LANES : (i + 1) * LANES] for row in rows_list for i in range(row.shape[1] // LANES)]
    missing = tiles_ref.shape[0] * ROWS - len(parts)
    whole = jnp.concatenate(parts + [jnp.zeros((missing, LANES), F32)] if missing else parts, axis=0)
    for i in range(tiles_ref.shape[0]):
        tiles_ref[i] = whole[i * ROWS : (i + 1) * ROWS].astype(BF)


def norm_rows(values):
    centre = values - jnp.mean(values, axis=-1, keepdims=True)
    inverse = lax.rsqrt(jnp.mean(centre * centre, axis=-1, keepdims=True) + EPS)
    return centre * inverse, inverse


def norm_rows_back(grad, normed, inverse, gain):
    scaled = grad * gain
    return inverse * (
        scaled - jnp.mean(scaled, axis=-1, keepdims=True) - normed * jnp.mean(scaled * normed, axis=-1, keepdims=True)
    )


def column_sums(values):
    return jnp.sum(values, axis=0, keepdims=True)


def head_window(h):
    block = jnp.minimum((h * HEAD_DIM) // LANES, DC - 2)
    lane = pl.multiple_of(block * LANES, LANES)
    return lane, h * HEAD_DIM - lane


def head_mask(rows, offset):
    lane = lax.broadcasted_iota(jnp.int32, (rows, PAIR), 1)
    return (lane >= offset) & (lane < offset + HEAD_DIM)


def front_kernel(
    where, x_ref, segq_ref, segk_ref, blocks_ref, q_ref, k_ref, v_ref, attended_ref, rest_ref, logs_ref,
    normed_ref, w_ref, vec1_ref, vec2_ref, bias_ref, score_ref, prob_ref, sem, vec_sem,
):
    window, rows = x_ref.shape[0], q_ref.shape[0]
    margin = (window - rows) // 2
    loads = [copies(where, name, blocks_ref, w_ref.at[i], sem.at[i]) for i, name in enumerate(("w_query", "w_key", "w_value"))]
    vecs = copies(where, "vec1", blocks_ref, vec1_ref, vec_sem) + copies(where, "vec2", blocks_ref, vec2_ref, vec_sem)
    start(vecs)
    for made in loads:
        start(made)
    wait(vecs)
    vec = vector_rows(vec1_ref)
    gain, shift = as_row(vec, 0, DC), as_row(vec, DC, DC)
    step = rows // 3

    @pl.loop(0, window // step)
    def _(i):
        at = pl.ds(i * step, step)
        normed, _ = norm_rows(x_ref[at].astype(F32))
        normed_ref[at] = (normed * gain + shift).astype(BF)

    @pl.loop(0, rows // 8)
    def _(i):
        at = pl.ds(i * 8, 8)
        bias_ref[at] = jnp.where(segq_ref[at] == segk_ref[...], 0.0, NEG)

    biases = vector_rows(vec2_ref)
    zero = jnp.zeros((1, D), F32)
    for made in loads:
        wait(made)
    for i, (out, add) in enumerate(((q_ref, as_row(biases, 0, DC)), (k_ref, zero), (v_ref, as_row(biases, DC, DC)))):
        for c in range(0, DC, 2):
            many = min(2, DC - c)
            lanes = slice(c * LANES, (c + many) * LANES)
            weights = panels(w_ref.at[i], c, many, D // ROWS)
            if i == 0:
                out[:, lanes] = (nn(normed_ref[pl.ds(margin, rows)], weights) + add[:, lanes]).astype(BF)
            else:

                @pl.loop(0, window // rows)
                def _(b):
                    at = pl.ds(b * rows, rows)
                    out[at, lanes] = (nn(normed_ref[at], weights) + add[:, lanes]).astype(BF)

    attended_ref[...] = jnp.zeros_like(attended_ref)
    rest_ref[...] = jnp.zeros_like(rest_ref)
    logs_ref[...] = jnp.zeros_like(logs_ref)
    lane_l = lax.broadcasted_iota(jnp.int32, logs_ref.shape, 1)

    @pl.loop(0, HEADS)
    def _(h):
        lane, offset = head_window(h)
        mask = head_mask(rows, offset)
        lanes = pl.ds(lane, PAIR)
        query = jnp.where(mask, q_ref[:, lanes], jnp.zeros((), BF))
        score_ref[...] = nt(query, k_ref[:, lanes]) * SCALE + bias_ref[...]
        top = jnp.max(score_ref[...], axis=-1, keepdims=True)
        powers = jnp.exp(score_ref[...] - top)
        total = jnp.sum(powers, axis=-1, keepdims=True)
        prob_ref[...] = powers.astype(BF)
        out = nn(prob_ref[...], v_ref[:, lanes]) / total
        rounded = out.astype(BF)
        attended_ref[:, lanes] = jnp.where(mask, rounded, attended_ref[:, lanes])
        rest_ref[:, lanes] = jnp.where(mask, (out - rounded.astype(F32)).astype(BF), rest_ref[:, lanes])
        logs_ref[...] = jnp.where(lane_l == h, top + jnp.log(total), logs_ref[...])


def front(x_win, seg_query, seg_keys, gathered, where, rows):
    window = x_win.shape[0]
    shape = lambda n, d=D, t=BF: jax.ShapeDtypeStruct((n, d), t)
    dma = pltpu.SemaphoreType.DMA
    units = D // ROWS
    return pl.pallas_call(
        functools.partial(front_kernel, where),
        out_shape=(shape(rows), shape(window), shape(window), shape(rows), shape(rows), shape(rows, LANES, F32)),
        in_specs=[VM, VM, VM, ANY],
        out_specs=[VM] * 6,
        scratch_shapes=[
            pltpu.VMEM((window, D), BF),
            pltpu.VMEM((3, units, DC, ROWS, LANES), BF), pltpu.VMEM((2, ROWS, LANES), BF), pltpu.VMEM((2, ROWS, LANES), BF),
            pltpu.VMEM((rows, window), F32), pltpu.VMEM((rows, window), F32), pltpu.VMEM((rows, window), BF), dma((3,)), dma,
        ],
        compiler_params=pltpu.CompilerParams(vmem_limit_bytes=VMEM_LIMIT),
        name="front",
    )(x_win, seg_query, seg_keys, gathered)


def middle_kernel(
    where, x_ref, cot_ref, attended_ref, rest_ref, blocks_ref, act_ref, mid_grad_ref, att_grad_ref, delta_ref, parts_ref,
    wo_ref, wu_ref, wd_ref, vec3_ref, vec4_ref, vec5_ref, b_up_ref, hidden_ref, slope_ref, pre_ref, normed_ref, normed_b_ref,
    mid_ref, g_up_ref, mid_b_ref, sem, out_sem,
):
    rows = x_ref.shape[0]
    units, f_units = D // ROWS, FF // ROWS
    names = ("w_out", "w_up", "w_down", "vec3", "vec4", "vec5")
    refs = (wo_ref, wu_ref, wd_ref, vec3_ref, vec4_ref, vec5_ref)
    loads = {n: copies(where, n, blocks_ref, r, sem.at[i]) for i, (n, r) in enumerate(zip(names, refs))}
    saves = {n: copies(where, n, parts_ref, r, out_sem, out=True) for n, r in zip(names, refs)}
    for n in ("vec3", "vec4", "vec5", "w_out", "w_up", "w_down"):
        start(loads[n])
    f_wide = FC * LANES
    pads = f_wide // ROWS - f_units
    wd_ref[pl.ds(f_units, pads)] = jnp.zeros((pads, DC, ROWS, LANES), BF)
    for n in ("vec3", "vec4", "vec5", "w_out"):
        wait(loads[n])
    vec = vector_rows(vec3_ref)
    b_out, gain, shift = (as_row(vec, i * DC, DC) for i in range(3))
    vec = vector_rows(vec4_ref)
    entry = lax.broadcasted_iota(jnp.int32, vec.shape, 0) * LANES + lax.broadcasted_iota(jnp.int32, vec.shape, 1)
    b_up_ref[...] = jnp.where(entry < FF, vec, 0.0)
    b_down = jnp.concatenate([vec5_ref[c].astype(F32)[0:1] for c in range(DC)], axis=1)

    for c in range(0, DC, 2):
        many = min(2, DC - c)
        lanes = slice(c * LANES, (c + many) * LANES)
        mid_ref[:, lanes] = (
            x_ref[:, lanes].astype(F32) + nn(attended_ref[...], panels(wo_ref, c, many, units)) + b_out[:, lanes]
        )
    normed, inverse = norm_rows(mid_ref[...])
    normed_ref[...] = normed
    normed_b_ref[...] = (normed * gain + shift).astype(BF)

    wait(loads["w_up"])

    @pl.loop(0, FC // 2)
    def _(p):
        at = pl.ds(pl.multiple_of(p * PAIR, PAIR), PAIR)
        bias = jnp.concatenate([b_up_ref[pl.ds(2 * p, 1)], b_up_ref[pl.ds(2 * p + 1, 1)]], axis=1)
        v = nn(normed_b_ref[...], panels(wu_ref, 2 * p, 2, units)) + bias
        square = v * v
        bent = jnp.tanh(GELU_A * v * (1.0 + GELU_B * square))
        hidden_ref[:, at] = (0.5 * v * (1.0 + bent)).astype(BF)
        slope_ref[:, at] = 0.5 * (1.0 + bent) + 0.5 * v * (1.0 - bent * bent) * (
            GELU_A * (1.0 + 3.0 * GELU_B * square)
        )

    wait(loads["w_down"])
    for c in range(0, DC, 2):
        many = min(2, DC - c)
        lanes = slice(c * LANES, (c + many) * LANES)
        act_ref[:, lanes] = (
            mid_ref[:, lanes] + nn(hidden_ref[...], panels(wd_ref, c, many, f_wide // ROWS)) + b_down[:, lanes]
        ).astype(BF)

    @pl.loop(0, FC // 2)
    def _(p):
        at = pl.ds(pl.multiple_of(p * PAIR, PAIR), PAIR)
        first = p * (PAIR // ROWS)
        grad = nt(cot_ref[...], panels(wd_ref, 0, DC, PAIR // ROWS, first)) * slope_ref[:, at]
        pre_ref[:, at] = grad.astype(BF)
        sums = column_sums(grad)
        g_up_ref[pl.ds(2 * p, 1)] = sums[:, :LANES]
        g_up_ref[pl.ds(2 * p + 1, 1)] = sums[:, LANES:]
        put_panels(wd_ref, 0, nn(hidden_ref[:, at].T, cot_ref[...]), first)

    start(saves["w_down"])
    put_vectors(vec4_ref, [b_up_row for b_up_row in [g_up_ref[i : i + 1] for i in range(FC)]])
    start(saves["vec4"])
    cot = cot_ref[...].astype(F32)
    sums = column_sums(cot)
    row0 = lax.broadcasted_iota(jnp.int32, (ROWS, LANES), 0) == 0
    for c in range(DC):
        vec5_ref[c] = jnp.where(row0, sums[:, c * LANES : (c + 1) * LANES], 0.0).astype(BF)
    start(saves["vec5"])

    for c in range(0, DC, 2):
        many = min(2, DC - c)
        weights = panels(wu_ref, 0, FC, many * LANES // ROWS, c * LANES // ROWS)
        mid_ref[:, c * LANES : (c + many) * LANES] = nt(pre_ref[...], weights)
    turned_b = normed_b_ref[...].T

    @pl.loop(0, FC // 2)
    def _(p):
        at = pl.ds(pl.multiple_of(p * PAIR, PAIR), PAIR)
        put_panels(wu_ref, 2 * p, nn(turned_b, pre_ref[:, at]))

    start(saves["w_up"])
    e = mid_ref[...]
    normed = normed_ref[...]
    g_gain, g_shift = column_sums(e * normed), column_sums(e)
    mid_grad = cot + norm_rows_back(e, normed, inverse, gain)
    mid_grad_ref[...] = mid_grad
    put_vectors(vec3_ref, [column_sums(mid_grad), g_gain, g_shift])
    start(saves["vec3"])
    mid_b = mid_grad.astype(BF)
    mid_b_ref[...] = mid_b

    def attended_grad(c, many):
        weights = panels(wo_ref, 0, DC, many * LANES // ROWS, c * (LANES // ROWS))
        att_grad_ref[:, lanes_of(c, many)] = nt(mid_b_ref[...], weights).astype(BF)

    over_pairs(attended_grad)
    product = att_grad_ref[...].astype(F32) * (attended_ref[...].astype(F32) + rest_ref[...].astype(F32))
    delta_ref[...] = jnp.sum(product.T.reshape(HEADS, HEAD_DIM, rows), axis=1)
    turned = attended_ref[...].T
    over_pairs(lambda c, many: put_panels(wo_ref, c, nn(turned, mid_b_ref[:, lanes_of(c, many)])))
    start(saves["w_out"])
    for n in names:
        wait(saves[n])


def middle(block_input, cotangent, attended, rest, gathered, where):
    rows = block_input.shape[0]
    shape = lambda t: jax.ShapeDtypeStruct((rows, D), t)
    dma = pltpu.SemaphoreType.DMA
    tiles = lambda *n: pltpu.VMEM((*n, ROWS, LANES), BF)
    units, f_wide = D // ROWS, FC * LANES
    return pl.pallas_call(
        functools.partial(middle_kernel, where),
        out_shape=(shape(BF), shape(F32), shape(BF), jax.ShapeDtypeStruct((HEADS, rows), F32), jax.ShapeDtypeStruct(gathered.shape, BF)),
        in_specs=[VM, VM, VM, VM, ANY],
        out_specs=[VM, VM, VM, VM, ANY],
        scratch_shapes=[
            tiles(units, DC), tiles(units, FC), tiles(f_wide // ROWS, DC), tiles(2), tiles(3), tiles(DC),
            pltpu.VMEM((3 * ROWS, LANES), F32), pltpu.VMEM((rows, f_wide), BF), pltpu.VMEM((rows, f_wide), F32),
            pltpu.VMEM((rows, f_wide), BF), pltpu.VMEM((rows, D), F32), pltpu.VMEM((rows, D), BF), pltpu.VMEM((rows, D), F32),
            pltpu.VMEM((3 * ROWS, LANES), F32), pltpu.VMEM((rows, D), BF), dma((6,)), dma,
        ],
        compiler_params=pltpu.CompilerParams(vmem_limit_bytes=VMEM_LIMIT),
        name="middle",
    )(block_input, cotangent, attended, rest, gathered)


def back_kernel(
    where, x_hbm_ref, segq_ref, segk_ref, blocks_ref, q_ref, k_ref, v_ref, grad_ref, logs_ref, parts_in_ref,
    near_ref, own_ref, parts_ref,
    w_ref, vec1_ref, vec2_ref, bias_ref, score_ref, prob_ref, turned_ref, dk_ref, dv_ref, dq_ref, part_ref, logs_t_ref, x_ref,
    sem, vec_sem, out_sem, x_sem,
):
    window, rows = x_ref.shape[0], q_ref.shape[0]
    margin = (window - rows) // 2
    units = D // ROWS
    names = ("w_query", "w_key", "w_value")
    loads = [copies(where, name, blocks_ref, w_ref.at[i], sem.at[i]) for i, name in enumerate(names)]
    vecs = copies(where, "vec1", blocks_ref, vec1_ref, vec_sem)
    start(vecs)
    for made in loads:
        start(made)
    x_load = pltpu.make_async_copy(x_hbm_ref, x_ref, x_sem)
    x_load.start()

    @pl.loop(0, window // LANES)
    def _(i):
        at = pl.ds(pl.multiple_of(i * LANES, LANES), LANES)
        bias_ref[at] = jnp.where(segk_ref[at] == segq_ref[...], 0.0, NEG)
        turned_ref[:, at] = k_ref[at].T
        dk_ref[at] = jnp.zeros((LANES, D), F32)
        dv_ref[at] = jnp.zeros((LANES, D), F32)

    logs_t_ref[...] = logs_ref[...].T

    @pl.loop(0, HEADS)
    def _(h):
        lane, offset = head_window(h)
        mask = head_mask(rows, offset)
        lanes = pl.ds(lane, PAIR)
        query = jnp.where(mask, q_ref[:, lanes], jnp.zeros((), BF))
        grad = jnp.where(mask, grad_ref[:, lanes], jnp.zeros((), BF))
        probs = jnp.exp(nt(k_ref[:, lanes], query) * SCALE + bias_ref[...] - logs_t_ref[pl.ds(h, 1)])
        score_ref[...] = probs
        prob_ref[...] = probs.astype(BF)
        prob_grad = nt(v_ref[:, lanes], grad)
        row_total = jnp.sum(score_ref[...] * prob_grad, axis=0, keepdims=True)
        dv_ref[:, lanes] += nn(prob_ref[...], grad)
        prob_ref[...] = (score_ref[...] * (prob_grad - row_total)).astype(BF)
        dk_ref[:, lanes] += nn(prob_ref[...], query)
        part_ref[...] = nn(turned_ref[lanes], prob_ref[...])
        at = pl.ds(pl.multiple_of(h * HEAD_DIM, 8), HEAD_DIM)
        dq_ref[at] = part_ref[pl.ds(pl.multiple_of(offset, 8), HEAD_DIM)]

    dq = dq_ref[...].T * SCALE
    g_query = column_sums(dq)
    dq_b = dq.astype(BF)
    wait(vecs)
    vec = vector_rows(vec1_ref)
    gain, shift = as_row(vec, 0, DC), as_row(vec, DC, DC)
    dk_b_ref, dv_b_ref = k_ref, v_ref
    x_load.wait()
    g_value = jnp.zeros((1, D), F32)
    step = rows // 3

    def rounded(i, total):
        at = pl.ds(pl.multiple_of(i * step, step), step)
        dk_b_ref[at] = (dk_ref[at] * SCALE).astype(BF)
        dv = dv_ref[at]
        dv_b_ref[at] = dv.astype(BF)
        normed, _ = norm_rows(x_ref[at].astype(F32))
        turned_ref[:, at] = (normed * gain + shift).astype(BF).T
        return total + column_sums(dv)

    g_value = lax.fori_loop(0, window // step, rounded, g_value)
    put_vectors(vec2_ref, [g_query, g_value])
    save = copies(where, "vec2", parts_ref, vec2_ref, out_sem, out=True)
    for made in loads:
        wait(made)
    for c in range(0, DC, 2):
        many = min(2, DC - c)
        lanes = slice(c * LANES, (c + many) * LANES)
        part = [panels(w_ref.at[i], 0, DC, many * LANES // ROWS, c * LANES // ROWS) for i in range(3)]

        @pl.loop(0, window // rows)
        def _(b):
            at = pl.ds(b * rows, rows)
            dk_ref[at, lanes] = nt(dk_b_ref[at], part[1]) + nt(dv_b_ref[at], part[2])

        dk_ref[pl.ds(margin, rows), lanes] += nt(dq_b, part[0])
    turned_own = turned_ref[:, pl.ds(margin, rows)]
    for c in range(0, DC, 2):
        many = min(2, DC - c)
        lanes = slice(c * LANES, (c + many) * LANES)
        put_panels(w_ref.at[0], c, nn(turned_own, dq_b[:, lanes]))
        put_panels(w_ref.at[1], c, nn(turned_ref[...], dk_b_ref[:, lanes]))
        put_panels(w_ref.at[2], c, nn(turned_ref[...], dv_b_ref[:, lanes]))
    for i, name in enumerate(names):
        save = save + copies(where, name, parts_ref, w_ref.at[i], out_sem, out=True)
    start(save)

    def norm_block(i, totals):
        at = pl.ds(pl.multiple_of(i * step, step), step)
        normed, inverse = norm_rows(x_ref[at].astype(F32))
        e = dk_ref[at]
        part = norm_rows_back(e, normed, inverse, gain)
        x_ref[at] = part.astype(BF)

        @pl.when((i >= margin // step) & (i < (margin + rows) // step))
        def _():
            own_ref[pl.ds(pl.multiple_of(i * step - margin, step), step)] = part

        return totals[0] + column_sums(e * normed), totals[1] + column_sums(e)

    zero = jnp.zeros((1, D), F32)
    g_gain, g_shift = lax.fori_loop(0, window // step, norm_block, (zero, zero))
    put_vectors(vec1_ref, [g_gain, g_shift])
    last = copies(where, "vec1", parts_ref, vec1_ref, out_sem, out=True)
    last = last + [pltpu.make_async_copy(x_ref, near_ref, x_sem)]
    start(last)
    wait(save + last)


def back(x_win, seg_query, seg_keys, gathered, queries, key_win, value_win, att_grad, logs, parts, where):
    window, rows = x_win.shape[0], queries.shape[0]
    dma = pltpu.SemaphoreType.DMA
    tiles = lambda *n: pltpu.VMEM((*n, ROWS, LANES), BF)
    vm = lambda a, b, t: pltpu.VMEM((a, b), t)
    return pl.pallas_call(
        functools.partial(back_kernel, where),
        out_shape=(
            jax.ShapeDtypeStruct((window, D), BF), jax.ShapeDtypeStruct((rows, D), F32), jax.ShapeDtypeStruct(parts.shape, BF),
        ),
        in_specs=[ANY, VM, VM, ANY, VM, VM, VM, VM, VM, ANY],
        out_specs=[ANY, VM, ANY],
        scratch_shapes=[
            tiles(3, D // ROWS, DC), tiles(2), tiles(2), vm(window, rows, F32), vm(window, rows, F32), vm(window, rows, BF),
            vm(D, window, BF), vm(window, D, F32), vm(window, D, F32), vm(D, rows, F32), vm(PAIR, rows, F32), vm(LANES, rows, F32),
            vm(window, D, BF), dma((3,)), dma, dma, dma,
        ],
        input_output_aliases={9: 2},
        compiler_params=pltpu.CompilerParams(vmem_limit_bytes=VMEM_LIMIT),
        name="back",
    )(x_win, seg_query, seg_keys, gathered, queries, key_win, value_win, att_grad, logs, parts)


HOT_NAMES = ("vec1", "w_query", "w_key", "w_value", "vec2")


def transfer_pieces(plan, depth):
    where = plan[0]
    count = plan[2].shape[0]
    hot, used = [0] * depth, [0] * depth
    for name in where:
        for owner, at, tiles in where[name]:
            level = owner * depth // count
            used[level] = max(used[level], at + tiles)
            if name in HOT_NAMES:
                hot[level] = max(hot[level], at + tiles)
    early = [(level, 0, h) for level, h in enumerate(hot) if h]
    late = [(level, h, u - h) for level, (h, u) in enumerate(zip(hot, used)) if h < u]
    return early, late


def cut(piece, many):
    level, first, tiles = piece
    half = tiles // 2
    edges = [half * i // (many // 2) for i in range(many // 2)] + [
        half + (tiles - half) * i // (many // 2) for i in range(many // 2 + 1)
    ]
    return [(level, first + a, b - a) for a, b in zip(edges[:-1], edges[1:])]


def gather_front_kernel(
    depth, where, early, late,
    block_ref, x_in_ref, segq_ref, segk_ref,
    out_ref, x_out_ref, turned_out_ref, keys_out_ref, k_out_ref, v_out_ref, x_got_ref, q_ref, attended_ref, rest_ref, logs_ref,
    z_send, z_recv, x_send, x_recv, y_send, y_recv, corner_send, corner_recv, line_send, line_recv, mate_send, mate_recv, w_send, w_recv,
    local_sem, stage_ref, both_ref, x_ref, turned_ref, normed_ref, w_ref, vec1_ref, vec2_ref, bias_ref, score_ref, prob_ref, add_ref, sem, vec_sem, x_sem, keys_sem,
):
    me = lax.axis_index("fsdp")
    count = 8 * depth
    core, x, y, z = place(me)
    mate, x_near, y_near = index_of(1 - core, x, y, z), index_of(core, 1 - x, y, z), index_of(core, x, 1 - y, z)
    up, down = me + 8, me - 8
    after, before = me + 2, me - 2
    has_after, has_before = after < count, before >= 0
    greet(
        [(mate, None), (x_near, None), (y_near, None), (down, z > 0), (up, z < depth - 1), (after, has_after), (before, has_before)]
    )
    pieces = early + late
    chunks = {p: cut(piece, 4) if piece[0] == 0 and p < len(early) else [piece] for p, piece in enumerate(pieces)}
    chunk_list = [(p, chunk) for p in chunks for chunk in chunks[p]]
    ids = {p: [i for i, (q, _) in enumerate(chunk_list) if q == p] for p in chunks}
    hot, cold = range(len(early)), range(len(early), len(pieces))
    hot_levels = {level for level, _, _ in early}

    def remote(source, target, send, recv, device):
        return pltpu.make_async_remote_copy(
            src_ref=source, dst_ref=target, send_sem=send, recv_sem=recv, device_id=(device,), device_id_type=MESH
        )

    def span(piece):
        return pl.ds(piece[1], piece[2])

    def halves(p):
        level, first, tiles = pieces[p]
        part = tiles // 2 if p in hot else tiles * 2 // 3
        return (level, first, part), (level, first + part, tiles - part)

    def column(level):
        return index_of(core, x, y, level)

    def from_x(level):
        return index_of(core, 1 - x, y, level)

    def from_y(level):
        return index_of(core, x, 1 - y, level)

    def across(level):
        return index_of(core, 1 - x, 1 - y, level)

    def pass_on(block, piece, send, recv, device, own=False):
        there = out_ref.at[block, span(piece)]
        return remote(block_ref.at[span(piece)] if own else there, there, send, recv, device)

    def z_copy(i, upward, own=False):
        piece = chunk_list[i][1]
        return pass_on(column(piece[0]), piece, z_send.at[i, 0 if upward else 1], z_recv.at[i], up if upward else down, own)

    def plane_copies(i, own=False):
        piece = chunk_list[i][1]
        block = column(piece[0])
        return (
            pass_on(block, piece, x_send.at[i], x_recv.at[i], x_near, own),
            pass_on(block, piece, y_send.at[i], y_recv.at[i], y_near, own),
            pass_on(block, piece, mate_send.at[0, i], mate_recv.at[0, i], mate, own),
        )

    def got(block, i, recv):
        piece = chunk_list[i][1]
        pass_on(block, piece, x_send.at[i], recv, me).wait_recv()

    def spread(i, own=False):
        for copy in plane_copies(i, own):
            copy.start()

    def z_pass(i):
        def run(zv):
            level = chunk_list[i][1][0]
            got(column(level), i, z_recv.at[i])
            if level < zv < depth - 1:
                z_copy(i, True).start()
            if 0 < zv < level:
                z_copy(i, False).start()

        return run

    def take(i):
        def run(zv):
            z_pass(i)(zv)
            spread(i)

        return run

    def later_spread(i):
        return lambda zv: spread(i)

    def by_plane(p, zv):
        return True

    def corner_copies(p):
        level = pieces[p][0]
        first, second = halves(p)
        return (
            pass_on(from_x(level), first, corner_send.at[p, 0], corner_recv.at[p, 0], y_near),
            pass_on(from_y(level), second, corner_send.at[p, 1], corner_recv.at[p, 1], x_near),
        )

    def corner_along_z(p, zv):
        level = pieces[p][0]
        ways = [up] * (level <= zv < depth - 1) + [down] * (0 < zv <= level)
        return [
            [
                pass_on(across(level), part, line_send.at[p, 2 * side + (way is up)], line_recv.at[p, side], way)
                for way in ways
            ]
            for side, part in enumerate(halves(p))
        ]

    def mate_copies(p):
        level = pieces[p][0]
        first, second = halves(p)
        return (
            pass_on(from_x(level), pieces[p], mate_send.at[1, p], mate_recv.at[1, p], mate),
            pass_on(from_y(level), pieces[p], mate_send.at[2, p], mate_recv.at[2, p], mate),
            pass_on(across(level), first, mate_send.at[3, p], mate_recv.at[3, p], mate),
            pass_on(across(level), second, mate_send.at[4, p], mate_recv.at[4, p], mate),
        )

    def beside(p):
        def run(zv):
            level = pieces[p][0]
            for i in ids[p]:
                got(from_x(level), i, x_recv.at[i])
            if by_plane(p, zv):
                corner_copies(p)[0].start()
            mate_copies(p)[0].start()
            for i in ids[p]:
                got(from_y(level), i, y_recv.at[i])
            if by_plane(p, zv):
                corner_copies(p)[1].start()
            mate_copies(p)[1].start()

        return run

    def corner(p):
        def run(zv):
            level = pieces[p][0]
            for side, part in enumerate(halves(p)):
                recv = corner_recv if by_plane(p, zv) else line_recv
                pass_on(across(level), part, corner_send.at[p, side], recv.at[p, side], me).wait_recv()
                if not by_plane(p, zv):
                    for copy in corner_along_z(p, zv)[side]:
                        copy.start()
                mate_copies(p)[2 + side].start()

        return run

    def from_mate(p):
        def run(zv):
            level = pieces[p][0]
            other = 1 - 2 * core
            for i in ids[p]:
                pass_on(column(level) + other, chunk_list[i][1], mate_send.at[0, i], mate_recv.at[0, i], me).wait_recv()
            first, second = halves(p)
            for slot, (block, piece) in enumerate(
                ((from_x(level), pieces[p]), (from_y(level), pieces[p]), (across(level), first), (across(level), second))
            ):
                pass_on(block + other, piece, mate_send.at[slot + 1, p], mate_recv.at[slot + 1, p], me).wait_recv()

        return run

    def own_spread(i):
        return lambda zv: spread(i, True)

    def own_up(i):
        return lambda zv: z_copy(i, True, True).start() if zv < depth - 1 else None

    def own_down(i):
        return lambda zv: z_copy(i, False, True).start() if zv > 0 else None

    def w_copy(slot, which, device, source=None):
        return remote(x_in_ref if source is None else source, x_got_ref.at[slot], w_send.at[which], w_recv.at[slot], device)

    def w_far(zv):
        @pl.when(has_after)
        def _():
            w_copy(0, 1, after).start()

        @pl.when(has_before)
        def _():
            w_copy(4, 2, before).start()

    def w_forward(core_index):
        slot = 0 if core_index else 4
        return w_copy(1 if core_index else 3, 3, mate, x_got_ref.at[slot])

    def w_wait(slot):
        w_copy(slot, 0, me).wait_recv()

    def w_middle(zv):
        @pl.when(has_before)
        def _():
            w_wait(0)

        @pl.when(has_after)
        def _():
            w_wait(4)

        @pl.when((core == 1) & has_before)
        def _():
            w_forward(1).start()

        @pl.when((core == 0) & has_after)
        def _():
            w_forward(0).start()

    stops = [61.0, 63.0, 68.0, 73.0, 95.0, 102.0, 110.0] + [110.0 + 2.7 * h for h in range(1, HEADS)]

    def lists(zv):
        own_hot = [p for p in hot if pieces[p][0] == zv]
        own_cold = [p for p in cold if pieces[p][0] == zv]
        far_hot = sorted((p for p in hot if pieces[p][0] != zv), key=lambda p: abs(pieces[p][0] - zv))
        far_cold = sorted((p for p in cold if pieces[p][0] != zv), key=lambda p: (abs(pieces[p][0] - zv), -pieces[p][0]))
        distance = {p: abs(pieces[p][0] - zv) for p in cold}
        at_once = own_cold if zv > depth // 2 else []
        after_hot = [p for p in own_cold if p not in at_once]
        first = []
        for p in own_hot:
            for i in ids[p]:
                first += [own_up(i), own_down(i), own_spread(i)]
        for p in own_cold:
            first += [own_down(i) for i in ids[p]]
        for p in at_once:
            first += [own_spread(i) for i in ids[p]]
        for p in far_hot:
            first += [take(i) for i in ids[p]]
        passed = {p for p in far_cold if distance[p] < 3 and (0 < zv < pieces[p][0] or pieces[p][0] < zv < depth - 1)}
        from_above = [p for p in far_cold if p in passed and pieces[p][0] == zv + 1]
        first += [z_pass(i) for p in from_above for i in ids[p]]
        for p in own_cold:
            first += [own_up(i) for i in ids[p]]
        order_hot = own_hot + far_hot
        first += [beside(p) for p in order_hot]
        first += [z_pass(i) for p in far_cold if p in passed and p not in from_above for i in ids[p]]
        take_or_spread = lambda p: [(later_spread if p in passed else take)(i) for i in ids[p]]
        first.append(w_far)
        for p in after_hot:
            first += [own_spread(i) for i in ids[p]]
        for p in far_cold:
            first += take_or_spread(p) if distance[p] == 1 else []
        first += [corner(p) for p in order_hot]
        first += [from_mate(p) for p in order_hot]
        timed = [(73.0, event) for p in far_cold if distance[p] > 1 for event in take_or_spread(p)]
        order = at_once + after_hot + far_cold
        timed += [((110.0, 120.8, 137.0, 145.0)[min(k, 3)], beside(p)) for k, p in enumerate(order)]
        timed += [((142.4, 150.5, 200.0)[min(k, 2)], corner(p)) for k, p in enumerate(order)]
        return first, sorted(timed, key=lambda entry: entry[0])

    plans = [lists(zv) for zv in range(depth)]

    def each_plane(events_of):
        for zv in range(depth):
            events = events_of(zv)
            if events:

                @pl.when(z == zv)
                def _():
                    for event in events:
                        event(zv)

    w_copy(1 + 2 * core, 0, mate).start()
    fill = pltpu.make_async_copy(block_ref, stage_ref, local_sem)
    fill.start()
    fill.wait()
    keep = pltpu.make_async_copy(stage_ref, out_ref.at[me], local_sem)
    keep.start()
    each_plane(lambda zv: plans[zv][0])
    keep.wait()

    near_sem = x_sem
    def service(stop):
        low = stops[stop - 1] if stop else -1.0
        high = stops[stop] if stop < len(stops) else 1e9
        each_plane(lambda zv: [event for time, event in plans[zv][1] if low < time <= high])

    rows, window = q_ref.shape[0], x_ref.shape[0]
    k_ref, v_ref = both_ref.at[0], both_ref.at[1]
    loads = [copies(where, name, out_ref, w_ref.at[i], sem.at[i]) for i, name in enumerate(("w_query", "w_key", "w_value"))]
    vecs = copies(where, "vec1", out_ref, vec1_ref, vec_sem) + copies(where, "vec2", out_ref, vec2_ref, vec_sem)
    start(vecs)
    for made in loads:
        start(made)

    def slot_rows(slot):
        return pl.ds(pl.multiple_of(slot * rows, rows), rows)

    def bring(slot, there=None):
        at = x_ref.at[slot_rows(slot)]
        if there is None:
            pltpu.make_async_copy(x_got_ref.at[slot], at, near_sem).start()
            return

        @pl.when(there)
        def _():
            pltpu.make_async_copy(x_got_ref.at[slot], at, near_sem).start()

        @pl.when(jnp.logical_not(there))
        def _():
            pltpu.make_async_copy(x_in_ref, at, near_sem).start()

    def brought(many):
        for _ in range(many):
            pltpu.make_async_copy(x_in_ref, x_ref.at[slot_rows(0)], near_sem).wait()

    mate_slot, far_slot = 3 - 2 * core, 1 + 2 * core
    w_wait(mate_slot)
    pltpu.make_async_copy(x_in_ref, x_ref.at[slot_rows(2)], near_sem).start()
    bring(mate_slot)
    brought(2)
    wait(vecs)
    vec = vector_rows(vec1_ref)
    gain, shift = as_row(vec, 0, DC), as_row(vec, DC, DC)
    biases = vector_rows(vec2_ref)
    step = rows // 3

    @pl.loop(0, rows // 8)
    def _(i):
        at = pl.ds(i * 8, 8)
        bias_ref[at] = jnp.where(segq_ref[at] == segk_ref[...], 0.0, NEG)

    def over_slots(slots, body):
        @pl.loop(0, len(slots))
        def _(i):
            slot = slots[-1]
            for k, other in enumerate(slots[:-1]):
                slot = jnp.where(i == k, other, slot)
            body(slot)

    def norm_slots(slots):
        def norm_slot(slot):
            @pl.loop(0, rows // step)
            def _(i):
                at = pl.ds(pl.multiple_of(slot * rows + i * step, step), step)
                normed, _ = norm_rows(x_ref[at].astype(F32))
                turned_ref[:, at] = normed.astype(BF).T
                normed_ref[at] = (normed * gain + shift).astype(BF)

        over_slots(slots, norm_slot)

    def project(i, slots):
        def some(c, many):
            lanes = lanes_of(c, many)
            weights = panels(w_ref.at[i], c, many, D // ROWS)

            def rows_of(slot):
                value = (nn(normed_ref[slot_rows(slot)], weights) + add_ref[i, 0:1, lanes]).astype(BF)
                if isinstance(i, int):
                    q_ref[:, lanes] = value
                else:
                    both_ref[i - 1, slot_rows(slot), lanes] = value

            over_slots(slots, rows_of)

        over_pairs(some)

    def keys_and_values(slots, between):
        @pl.loop(0, 2)
        def _(i):
            project(i + 1, slots)
            for k, action in enumerate(between):

                @pl.when(i == k)
                def _():
                    action()

    norm_slots([2, mate_slot])
    service(0)
    for made in loads:
        wait(made)
    for i, row in enumerate((as_row(biases, 0, DC), jnp.zeros((1, D), F32), as_row(biases, DC, DC))):
        add_ref[i, 0:1] = row
    project(0, [2])
    service(1)
    keys_and_values([2, mate_slot], [lambda: service(2), lambda: service(3)])
    w_middle(None)

    @pl.when((core == 0) & has_before)
    def _():
        w_wait(1)

    @pl.when((core == 1) & has_after)
    def _():
        w_wait(3)

    bring(0, has_before)
    bring(4, has_after)
    bring(far_slot, jnp.where(core == 0, has_before, has_after))
    brought(3)
    others = [0, 4, far_slot]
    norm_slots(others)
    saves = [pltpu.make_async_copy(x_ref, x_out_ref, local_sem), pltpu.make_async_copy(turned_ref, turned_out_ref, local_sem)]
    start(saves)
    service(4)
    k_save = pltpu.make_async_copy(k_ref, k_out_ref, keys_sem.at[0])

    def keys_done():
        service(5)
        k_save.start()

    keys_and_values(others, [keys_done])
    v_save = pltpu.make_async_copy(v_ref, v_out_ref, keys_sem.at[1])
    v_save.start()
    wait(saves)

    @pl.loop(0, window // LANES)
    def _(i):
        at = pl.ds(pl.multiple_of(i * LANES, LANES), LANES)
        turned_ref[:, at] = k_ref[at].T

    keys_save = pltpu.make_async_copy(turned_ref, keys_out_ref, keys_sem.at[2])
    keys_save.start()
    attended_ref[...] = jnp.zeros_like(attended_ref)
    rest_ref[...] = jnp.zeros_like(rest_ref)
    logs_ref[...] = jnp.zeros_like(logs_ref)
    lane_l = lax.broadcasted_iota(jnp.int32, logs_ref.shape, 1)

    @pl.loop(0, HEADS)
    def _(h):
        for at_head in range(HEADS):

            @pl.when(h == at_head)
            def _():
                service(6 + at_head)

        lane, offset = head_window(h)
        mask = head_mask(rows, offset)
        lanes = pl.ds(lane, PAIR)
        query = jnp.where(mask, q_ref[:, lanes], jnp.zeros((), BF))
        score_ref[...] = nt(query, k_ref[:, lanes]) * SCALE + bias_ref[...]
        top = jnp.max(score_ref[...], axis=-1, keepdims=True)
        powers = jnp.exp(score_ref[...] - top)
        total = jnp.sum(powers, axis=-1, keepdims=True)
        prob_ref[...] = powers.astype(BF)
        out = nn(prob_ref[...], v_ref[:, lanes]) / total
        rounded = out.astype(BF)
        attended_ref[:, lanes] = jnp.where(mask, rounded, attended_ref[:, lanes])
        rest_ref[:, lanes] = jnp.where(mask, (out - rounded.astype(F32)).astype(BF), rest_ref[:, lanes])
        logs_ref[...] = jnp.where(lane_l == h, top + jnp.log(total), logs_ref[...])

    service(len(stops))
    each_plane(lambda zv: [from_mate(p) for p in cold])

    def sent(zv):
        for i, (p, piece) in enumerate(chunk_list):
            for copy in plane_copies(i):
                copy.wait_send()
            level = piece[0]
            if zv < depth - 1 and level <= zv:
                z_copy(i, True).wait_send()
            if zv > 0 and level >= zv:
                z_copy(i, False).wait_send()
        for p in range(len(pieces)):
            for copy in mate_copies(p) + (corner_copies(p) if by_plane(p, zv) else ()):
                copy.wait_send()
            for copy in sum(corner_along_z(p, zv), []) if not by_plane(p, zv) else []:
                copy.wait_send()

    each_plane(lambda zv: [sent])
    w_copy(0, 0, mate).wait_send()

    @pl.when(has_after)
    def _():
        w_copy(0, 1, after).wait_send()

    @pl.when(has_before)
    def _():
        w_copy(4, 2, before).wait_send()

    @pl.when(jnp.where(core == 1, has_before, has_after))
    def _():
        w_forward(0).wait_send()

    wait([k_save, v_save, keys_save])


def gather_front(block, block_input, seg_query, seg_keys, plan):
    where = plan[0]
    count = lax.axis_size("fsdp")
    depth = count // 8
    rows, window = block_input.shape[0], seg_keys.shape[1]
    early, whole = transfer_pieces(plan, depth)
    late = whole
    shape = lambda n, d=D, t=BF: jax.ShapeDtypeStruct((n, d), t)
    dma = pltpu.SemaphoreType.DMA
    units = D // ROWS
    many = len(early) + len(late)
    chunks = many + 3 * sum(1 for piece in early if piece[0] == 0)
    got = jax.ShapeDtypeStruct((5, rows, D), BF)
    return pl.pallas_call(
        functools.partial(gather_front_kernel, depth, where, early, late),
        out_shape=(
            jax.ShapeDtypeStruct((count, *block.shape), BF), shape(window), shape(D, window), shape(D, window), shape(window), shape(window), got,
            shape(rows), shape(rows), shape(rows), shape(rows, LANES, F32),
        ),
        in_specs=[ANY, ANY, VM, VM],
        out_specs=[ANY] * 7 + [VM] * 4,
        scratch_shapes=[
            dma((chunks, 2)), dma((chunks,)), dma((chunks,)), dma((chunks,)), dma((chunks,)), dma((chunks,)),
            dma((many, 2)), dma((many, 2)), dma((many, 4)), dma((many, 2)), dma((5, chunks)), dma((5, chunks)), dma((4,)), dma((5,)),
            dma, pltpu.VMEM(block.shape, BF), pltpu.VMEM((2, window, D), BF),
            pltpu.VMEM((window, D), BF), pltpu.VMEM((D, window), BF), pltpu.VMEM((window, D), BF),
            pltpu.VMEM((3, units, DC, ROWS, LANES), BF), pltpu.VMEM((2, ROWS, LANES), BF), pltpu.VMEM((2, ROWS, LANES), BF),
            pltpu.VMEM((rows, window), F32), pltpu.VMEM((rows, window), F32), pltpu.VMEM((rows, window), BF), pltpu.VMEM((3, 8, D), F32),
            dma((3,)), dma, dma, dma((3,)),
        ],
        compiler_params=pltpu.CompilerParams(collective_id=0, has_side_effects=True, vmem_limit_bytes=VMEM_LIMIT),
        name="gather_front",
    )(block, block_input, seg_query, seg_keys)


def back_scatter_kernel(
    depth, where, early, late,
    x_hbm_ref, turned_hbm_ref, keys_hbm_ref, segq_ref, segk_ref, blocks_ref, q_ref, k_hbm_ref, v_hbm_ref, grad_ref, logs_ref, delta_ref, mid_hbm_ref, parts_in_ref,
    parts_ref, out_ref, in_grad_ref, mates, sums, halfs, fulls, lines, near_ref, near_got,
    w_ref, g_ref, vec1_ref, vec2_ref, score_ref, prob_ref, turned_ref, k_ref, v_ref, dq_ref, part_ref, logs_t_ref, x_ref, dq_b_ref,
    block_ref, mid_ref, g_value_ref, gain_acc, shift_acc, stage, total,
    mate_send, mate_recv, half_send, half_recv, full_send, full_recv, line_send, line_recv, near_send, near_recv,
    load_sem, store_sem, sem, vec_sem, out_sem, x_sem,
):
    me = lax.axis_index("fsdp")
    count = 8 * depth
    core, x, y, z = place(me)
    mate, x_near, y_near = index_of(1 - core, x, y, z), index_of(core, 1 - x, y, z), index_of(core, x, 1 - y, z)
    after, before = me + 2, me - 2
    has_after, has_before = after < count, before >= 0
    greet(
        [(mate, None), (x_near, None), (y_near, None), (me - 8, z > 0), (me + 8, z < depth - 1), (after, has_after), (before, has_before)]
    )
    pieces = early + late
    block_tiles = parts_ref.shape[1]
    early_ids, late_ids = range(len(early)), range(len(early), len(pieces))

    def remote(source, target, send, recv, device):
        return pltpu.make_async_remote_copy(
            src_ref=source, dst_ref=target, send_sem=send, recv_sem=recv, device_id=(device,), device_id_type=MESH
        )

    def owner(level, slot, which_core):
        return index_of(which_core, 1 - x if slot in (1, 3) else x, 1 - y if slot in (2, 3) else y, level)

    def at_plane(zv, run):
        @pl.when(z == zv)
        def _():
            run()

    def span(p, lo=0, many=None):
        _, first, tiles = pieces[p]
        return pl.ds(first + lo, tiles if many is None else many)

    def half_of(p):
        return pieces[p][2] // 2

    def to_mate(p, slot):
        level = pieces[p][0]
        return remote(
            parts_ref.at[owner(level, slot, 1 - core), span(p)], mates.at[level, slot, span(p)],
            mate_send.at[p, slot], mate_recv.at[p, slot], mate,
        )

    def half_out(p, side):
        level, _, tiles = pieces[p]
        part = span(p, half_of(p), tiles - half_of(p)) if side else span(p, 0, half_of(p))
        return remote(
            sums.at[level, 3, part], halfs.at[level, side, part], half_send.at[p, side], half_recv.at[p, side],
            x_near if side else y_near,
        )

    def full_out(p, side):
        level = pieces[p][0]
        return remote(
            sums.at[level, 1 + side, span(p)], fulls.at[level, side, span(p)], full_send.at[p, side], full_recv.at[p, side],
            y_near if side else x_near,
        )

    def subs(p):
        tiles = pieces[p][2]
        if p in early_ids or tiles < block_tiles // 3:
            return [(0, tiles)]
        return [(0, tiles // 2), (tiles // 2, tiles - tiles // 2)]

    def line_out(p, zv, sub):
        level = pieces[p][0]
        part = span(p, *subs(p)[sub])
        upward = level > zv
        slot = depth if not upward and level == zv - 1 else level
        side = 1 if slot == depth else 0
        return remote(
            sums.at[level, 0, part], lines.at[slot, part], line_send.at[p, sub], line_recv.at[p, 2 * sub + side],
            me + 8 if upward else me - 8,
        )

    def line_in(p, side, sub):
        level = pieces[p][0]
        slot = depth if side else level
        part = span(p, *subs(p)[sub])
        return remote(sums.at[level, 0, part], lines.at[slot, part], line_send.at[p, sub], line_recv.at[p, 2 * sub + side], me)

    def line_sides(p, zv):
        level = pieces[p][0]
        if level > zv:
            return [0] if zv > 0 else []
        if level < zv:
            return [0] if zv < depth - 1 else []
        return ([0] if zv > 0 else []) + ([1] if zv < depth - 1 else [])

    def extent(job):
        kind, p, sub = job
        return subs(p)[sub] if kind == 0 else (0, pieces[p][2])

    def sources(job, zv):
        kind, p, sub = job
        level, _, tiles = pieces[p]
        h = half_of(p)
        if kind == 0:
            lo, many = extent(job)
            part = span(p, lo, many)
            refs = [parts_ref.at[owner(level, 0, core), part], mates.at[level, 0, part]]
            refs += [fulls.at[level, side, part] for side in (0, 1)]
            refs += [lines.at[depth if side else level, part] for side in line_sides(p, zv)]
            return [(ref, 0, many) for ref in refs]
        found = [(parts_ref.at[owner(level, kind, core), span(p)], 0, tiles), (mates.at[level, kind, span(p)], 0, tiles)]
        if kind == 1:
            found.append((halfs.at[level, 0, span(p, 0, h)], 0, h))
        if kind == 2:
            found.append((halfs.at[level, 1, span(p, h, tiles - h)], h, tiles - h))
        return found

    def loads(job, zv, base):
        return [
            pltpu.make_async_copy(ref, stage.at[i, pl.ds(base + lo, many)], load_sem.at[1 if base else 0])
            for i, (ref, lo, many) in enumerate(sources(job, zv))
        ]

    def store(job, base):
        kind, p, sub = job
        lo, many = extent(job)
        return pltpu.make_async_copy(
            total.at[pl.ds(base, many)], sums.at[pieces[p][0], kind, span(p, lo, many)], store_sem.at[1 if base else 0]
        )

    def load(job, zv, base=0):
        kind, p, sub = job
        if sub == 0:
            to_mate(p, kind).wait_recv()
        if kind in (1, 2):
            half_out(p, kind - 1).wait_recv()
        made = loads(job, zv, base)
        if kind == 0:
            if sub == 0:
                for side in (0, 1):
                    full_out(p, side).wait_recv()
            start(made[:4])
            for copy, side in zip(made[4:], line_sides(p, zv)):
                line_in(p, side, sub).wait_recv()
                copy.start()
        else:
            start(made)

    def add(base, lo, many, slots, target, shift):
        def some(first, tiles):
            value = stage[slots[0], pl.ds(first, tiles)].astype(F32)
            for slot in slots[1:]:
                value = value + stage[slot, pl.ds(first, tiles)].astype(F32)
            target[pl.ds(first + shift, tiles)] = value.astype(target.dtype)

        group = 8

        @pl.loop(0, many // group)
        def _(i):
            some(base + lo + i * group, group)

        if many % group:
            some(base + lo + many // group * group, many % group)

    def finish(job, zv, base=0):
        kind, p, sub = job
        level, first, tiles = pieces[p]
        found = sources(job, zv)
        wait(loads(job, zv, base))
        final = kind == 0 and level == zv
        target, shift = (out_ref, first + extent(job)[0] - base) if final else (total, 0)
        edges = sorted({e for _, lo, many in found for e in (lo, lo + many)})
        for lo, hi in zip(edges[:-1], edges[1:]):
            slots = [i for i, (_, a, many) in enumerate(found) if a <= lo and hi <= a + many]
            add(base, lo, hi - lo, slots, target, shift)
        if not final:
            store(job, base).start()

    def send(job, zv, base=0):
        kind, p, sub = job
        if kind == 0 and pieces[p][0] == zv:
            return
        store(job, base).wait()
        if kind == 3:
            half_out(p, 0).start()
            half_out(p, 1).start()
        elif kind == 0:
            line_out(p, zv, sub).start()
        else:
            full_out(p, kind - 1).start()

    second = block_tiles // 2

    def run(jobs, zv):
        for job in jobs:
            load(job, zv)
            finish(job, zv)
            send(job, zv)

    def run_ahead(jobs, zv):
        bases = [second * (k % 2) for k in range(len(jobs))]
        for k, job in enumerate(jobs):
            if k == 0:
                load(job, zv, bases[k])
            if k + 1 < len(jobs):
                load(jobs[k + 1], zv, bases[k + 1])
            finish(job, zv, bases[k])
            if k:
                send(jobs[k - 1], zv, bases[k - 1])
        send(jobs[-1], zv, bases[-1])

    def along(p):
        return [(0, p, sub) for sub in range(len(subs(p)))]

    for p in early_ids:
        for slot in (3, 1, 2, 0):
            to_mate(p, slot).start()

    window, rows = k_ref.shape[0], q_ref.shape[0]
    margin = (window - rows) // 2
    names = ("w_query", "w_key", "w_value")
    k_load = [
        pltpu.make_async_copy(a, b, vec_sem)
        for a, b in ((k_hbm_ref, k_ref), (v_hbm_ref, v_ref), (keys_hbm_ref, turned_ref))
    ]
    start(k_load)
    weight_loads = [copies(where, name, blocks_ref, w_ref.at[i], sem.at[i]) for i, name in enumerate(names)]
    vecs = copies(where, "vec1", blocks_ref, vec1_ref, sem.at[3])
    start(vecs)
    for made in weight_loads:
        start(made)
    x_load = [pltpu.make_async_copy(x_hbm_ref, x_ref, x_sem)]
    start(x_load)
    logs_t_ref[...] = logs_ref[...].T * LOG2E
    g_value_ref[...] = jnp.zeros_like(g_value_ref)

    by_level = {pieces[p][0]: p for p in early_ids}
    a, b, c_ = (by_level[level] for level in sorted(by_level, reverse=True)[:3])
    table = [
        (-1, 0, 3, a, None), (0, 1, 3, b, None), (3, 4, 1, a, None), (4, 5, 2, a, None), (5, 6, 3, c_, None),
        (6, 7, 1, b, None), (7, 8, 2, b, None), (11, 12, 0, a, 0), (12, 13, 1, c_, None), (13, 14, 2, c_, None),
    ]

    def beside(h, which, action):
        for entry in table:
            if entry[which] < 0:
                continue
            kind, p, zv = entry[2:]
            job = (kind, p, 0)
            there = h == entry[which]
            if zv is not None:
                there = there & (z == zv)

            @pl.when(there)
            def _():
                action(job, zv)

    wait(k_load)
    load((3, a, 0), None)

    @pl.loop(0, HEADS)
    def _(h):
        beside(h, 1, finish)
        lane, offset = head_window(h)
        mask = head_mask(rows, offset)
        lanes = pl.ds(lane, PAIR)
        query = jnp.where(mask, q_ref[:, lanes], jnp.zeros((), BF))
        grad = jnp.where(mask, grad_ref[:, lanes], jnp.zeros((), BF))
        log_row, delta_row = logs_t_ref[pl.ds(h, 1)], delta_ref[pl.ds(h, 1)]
        blocks = [pl.ds(n * rows, rows) for n in range(window // rows)]
        for keys in blocks:
            together = jnp.concatenate([segk_ref[keys]] * (rows // LANES), axis=1) == segq_ref[...]
            probs = jnp.exp2(jnp.where(together, nt(k_ref[keys, lanes], query) * (SCALE * LOG2E) - log_row, NEG))
            prob_ref[keys] = probs.astype(BF)
            score_ref[keys] = (probs * (nt(v_ref[keys, lanes], grad) - delta_row)).astype(BF)
        beside(h, 1, send)
        beside(h, 0, load)
        side = head_mask(rows, offset)

        @pl.loop(0, window // rows)
        def _(n):
            keys = pl.ds(pl.multiple_of(n * rows, rows), rows)
            dv = nn(prob_ref[keys], grad)
            g_value_ref[:, lanes] += column_sums(dv)
            v_ref[keys, lanes] = jnp.where(side, dv.astype(BF), v_ref[keys, lanes])
            dk = nn(score_ref[keys], query) * SCALE
            k_ref[keys, lanes] = jnp.where(side, dk.astype(BF), k_ref[keys, lanes])
        tile = (h * HEAD_DIM) // ROWS * ROWS
        part_ref[...] = nn(turned_ref[pl.ds(pl.multiple_of(tile, ROWS), part_ref.shape[0])], score_ref[...])
        at = pl.ds(pl.multiple_of(h * HEAD_DIM, 8), HEAD_DIM)
        dq_ref[at] = part_ref[pl.ds(pl.multiple_of(h * HEAD_DIM - tile, 8), HEAD_DIM)]

    turned_load = pltpu.make_async_copy(turned_hbm_ref, turned_ref, vec_sem)
    turned_load.start()
    dq = dq_ref[...].T * SCALE
    put_vectors(vec2_ref, [column_sums(dq), g_value_ref[...]])
    saves = copies(where, "vec2", parts_ref, vec2_ref, out_sem.at[3], out=True)
    dq_b_ref[...] = dq.astype(BF)
    wait(vecs)
    vec = vector_rows(vec1_ref)
    gain, shift = as_row(vec, 0, DC), as_row(vec, DC, DC)
    gain_t, shift_t = (jnp.broadcast_to(v, (8, D)).T[:, :1] for v in (gain, shift))
    wait(x_load)
    step = rows // 3

    turned_load.wait()
    for made in weight_loads:
        wait(made)
    gain_acc[...] = jnp.zeros_like(gain_acc)
    shift_acc[...] = jnp.zeros_like(shift_acc)

    def plane_job(what, entries):
        for zv, p in entries:

            def go():
                job = (0, p, 0)
                if what == "load":
                    load(job, zv)
                else:
                    finish(job, zv)
                    send(job, zv)

            at_plane(zv, go)

    own = turned_ref[:, pl.ds(margin, rows)]
    made = []
    first_jobs, last_jobs = [(1, a), (0, b), (3, b)], [(0, c_), (3, c_)]
    for i, (left, right_ref) in enumerate(((own, dq_b_ref), (turned_ref, k_ref), (turned_ref, v_ref))):
        if i == 1:
            plane_job("load", first_jobs)
        if i == 2:
            plane_job("end", first_jobs)
            plane_job("load", last_jobs)
            wait(made[0])

        def project_back(c, many):
            right = right_ref[:, lanes_of(c, many)]
            raw = nn(left[...], right)
            summed = column_sums(right.astype(F32))
            put_panels(g_ref.at[i % 2], c, gain_t * raw + shift_t * summed)
            weights = panels(w_ref.at[i], c, many, D // ROWS).astype(F32)
            scaled, shifted = weights * raw, weights * summed
            for j in range(many):
                part = slice(j * LANES, (j + 1) * LANES)
                gain_acc[...] += scaled[:, part]
                shift_acc[...] += shifted[:, part]

        over_pairs(project_back)
        made.append(copies(where, names[i], parts_ref, g_ref.at[i % 2], out_sem.at[i], out=True))
        start(made[i])
    put_vectors(vec1_ref, [column_sums(gain_acc[...].T), column_sums(shift_acc[...].T)])
    saves = saves + copies(where, "vec1", parts_ref, vec1_ref, out_sem.at[3], out=True)
    start(saves)
    plane_job("end", last_jobs)
    wait(saves + made[1] + made[2])
    for slots in ((3,), (1, 2), (0,)):
        for p in late_ids:
            for slot in slots:
                to_mate(p, slot).start()

    def slot_rows(n):
        return pl.ds(pl.multiple_of(n * rows, rows), rows)

    def row_block(n, own=False):
        first = n * rows

        def project_back(c, many):
            part = lambda i: panels(w_ref.at[i], 0, DC, many * LANES // ROWS, c * (LANES // ROWS))
            value = nt(k_ref[slot_rows(n)], part(1)) + nt(v_ref[slot_rows(n)], part(2))
            if own:
                value = value + nt(dq_b_ref[...], part(0))
            block_ref[:, lanes_of(c, many)] = value

        over_pairs(project_back)

        @pl.loop(0, rows // step)
        def _(i):
            here = pl.ds(pl.multiple_of(i * step, step), step)
            there = pl.ds(pl.multiple_of(first + i * step, step), step)
            normed, inverse = norm_rows(x_ref[there].astype(F32))
            result = norm_rows_back(block_ref[here], normed, inverse, gain)
            if own:
                block_ref[here] = result
            else:
                x_ref[there] = result.astype(BF)

    def near_rows(slot):
        return x_ref.at[pl.ds(slot * rows, rows)]

    def near_save(slot):
        return pltpu.make_async_copy(near_rows(slot), near_ref.at[slot], x_sem)

    def near_copy(slot, which, device):
        return remote(near_ref.at[slot], near_got.at[which], near_send.at[which], near_recv.at[which], device)


    run_ahead([(3, p, 0) for p in late_ids], None)

    @pl.loop(0, 4)
    def _(i):
        row_block(jnp.where(i == 0, 0, jnp.where(i == 1, 4, 2 * i - 3)))

        @pl.when(i == 1)
        def _():
            at_plane(1, lambda: run([(0, b, 0)], 1))
            at_plane(2, lambda: run([(0, a, 0), (0, c_, 0)], 2))
            for p in late_ids:
                run_ahead([(1, p, 0), (2, p, 0)], None)

    sides = [near_save(slot) for slot in (0, 4, 1, 3)]
    start(sides)
    wait(sides)
    to_mate_itself, to_mate_shared = (3 - 2 * core), (1 + 2 * core)
    near_copy(to_mate_itself, 0, mate).start()
    near_copy(to_mate_shared, 1, mate).start()

    @pl.when((core == 0) & has_before)
    def _():
        near_copy(0, 2, before).start()

    @pl.when((core == 1) & has_after)
    def _():
        near_copy(4, 3, after).start()

    near_copy(0, 1, me).wait_recv()
    shared_slot = 4 - 4 * core
    fetch = pltpu.make_async_copy(near_got.at[1], k_ref.at[pl.ds(0, rows)], x_sem)
    fetch.start()
    fetch.wait()

    @pl.loop(0, rows // step)
    def _(i):
        here = pl.ds(pl.multiple_of(i * step, step), step)
        there = pl.ds(pl.multiple_of(shared_slot * rows + i * step, step), step)
        x_ref[there] = (x_ref[there].astype(F32) + k_ref[here].astype(F32)).astype(BF)

    shared_save = near_save(shared_slot)
    shared_save.start()
    shared_save.wait()

    @pl.when((core == 0) & has_after)
    def _():
        near_copy(4, 3, after).start()

    @pl.when((core == 1) & has_before)
    def _():
        near_copy(0, 2, before).start()

    def hops(p, zv):
        return zv if pieces[p][0] > zv else depth - 1 - zv

    def tail(zv, at_end):
        out = sorted((p for p in late_ids if pieces[p][0] != zv), key=lambda p: (hops(p, zv), p))
        if not at_end:
            return [job for p in out if hops(p, zv) == 0 for job in along(p)]
        own = [p for ids in (early_ids, late_ids) for p in ids if pieces[p][0] == zv]
        return [job for p in out + own if p in own or hops(p, zv) for job in along(p)]

    for zv in (0, depth - 1):
        at_plane(zv, lambda: run(tail(zv, False), zv))
    row_block(2, True)

    @pl.loop(0, rows // step)
    def _(i):
        here = pl.ds(pl.multiple_of(i * step, step), step)
        fetch_mid = pltpu.make_async_copy(mid_hbm_ref.at[here], mid_ref, x_sem)
        fetch_mid.start()
        fetch_mid.wait()
        block_ref[here] += mid_ref[...]

    for zv in range(depth):
        at_plane(zv, lambda: run(tail(zv, True), zv))

    near_copy(0, 0, me).wait_recv()

    @pl.when(has_after)
    def _():
        near_copy(0, 2, me).wait_recv()

    @pl.when(has_before)
    def _():
        near_copy(0, 3, me).wait_recv()

    for i, (which, there) in enumerate(((0, None), (2, has_after), (3, has_before))):
        target = k_ref.at[pl.ds(i * rows, rows)]
        if there is None:
            pltpu.make_async_copy(near_got.at[which], target, x_sem).start()
            continue

        @pl.when(there)
        def _():
            pltpu.make_async_copy(near_got.at[which], target, x_sem).start()

        @pl.when(jnp.logical_not(there))
        def _():
            pltpu.make_async_copy(near_ref.at[0], target, x_sem).start()

    for i in range(3):
        pltpu.make_async_copy(near_got.at[0], k_ref.at[pl.ds(i * rows, rows)], x_sem).wait()
    near_after, near_before = (jnp.where(there, 1.0, 0.0) for there in (has_after, has_before))

    @pl.loop(0, rows // step)
    def _(i):
        here = pl.ds(pl.multiple_of(i * step, step), step)
        value = block_ref[here] + k_ref[here].astype(F32)
        value = value + near_after * k_ref[pl.ds(pl.multiple_of(rows + i * step, step), step)].astype(F32)
        value = value + near_before * k_ref[pl.ds(pl.multiple_of(2 * rows + i * step, step), step)].astype(F32)
        in_grad_ref[here] = value.astype(BF)

    for p in range(len(pieces)):
        for slot in range(4):
            to_mate(p, slot).wait_send()
        for side in (0, 1):
            half_out(p, side).wait_send()
            full_out(p, side).wait_send()
        for zv in range(depth):
            if pieces[p][0] != zv:
                at_plane(zv, lambda: [line_out(p, zv, sub).wait_send() for sub in range(len(subs(p)))])
    near_copy(0, 0, mate).wait_send()
    near_copy(0, 1, mate).wait_send()

    @pl.when(has_before)
    def _():
        near_copy(0, 2, before).wait_send()

    @pl.when(has_after)
    def _():
        near_copy(4, 3, after).wait_send()


def back_scatter(x_win, turned, turned_keys, seg_query, seg_keys, gathered, queries, key_win, value_win, att_grad, logs, delta, mid_grad, parts, plan):
    where, block = plan[:2]
    window, rows = x_win.shape[0], queries.shape[0]
    seg_keys = jnp.broadcast_to(seg_keys, (window, LANES))
    count = lax.axis_size("fsdp")
    depth = count // 8
    hot, cold = transfer_pieces(plan, depth)
    early = sorted(cold, reverse=True)
    late = []
    for piece in sorted(hot, reverse=True):
        late += cut(piece, 2) if piece[2] > block // 2 else [piece]
    many = len(early) + len(late)
    dma = pltpu.SemaphoreType.DMA
    tiles = lambda *n: pltpu.VMEM((*n, ROWS, LANES), BF)
    vm = lambda a, b, t: pltpu.VMEM((a, b), t)
    hbm = lambda *n: jax.ShapeDtypeStruct((*n, ROWS, LANES), BF)
    return pl.pallas_call(
        functools.partial(back_scatter_kernel, depth, where, early, late),
        out_shape=(
            jax.ShapeDtypeStruct(parts.shape, BF), jax.ShapeDtypeStruct((block, ROWS, LANES), F32), jax.ShapeDtypeStruct((rows, D), BF),
            hbm(depth, 4, block), hbm(depth, 4, block), hbm(depth, 2, block), hbm(depth, 2, block), hbm(depth + 1, block),
            jax.ShapeDtypeStruct((5, rows, D), BF), jax.ShapeDtypeStruct((4, rows, D), BF),
        ),
        in_specs=[ANY, ANY, ANY, VM, VM, ANY, VM, ANY, ANY, VM, VM, VM, ANY, ANY],
        out_specs=[ANY, VM, VM] + [ANY] * 7,
        scratch_shapes=[
            tiles(3, D // ROWS, DC), tiles(2, D // ROWS, DC), tiles(2), tiles(2),
            vm(window, rows, BF), vm(window, rows, BF), vm(D, window, BF), vm(window, D, BF), vm(window, D, BF),
            vm(D, rows, F32), vm(ROWS * pl.cdiv(HEAD_DIM + 8, ROWS), rows, F32), vm(LANES, rows, F32), vm(window, D, BF), vm(rows, D, BF), vm(rows, D, F32), vm(rows // 3, D, F32),
            vm(1, D, F32), vm(D, LANES, F32), vm(D, LANES, F32), tiles(6, block), tiles(block),
            dma((many, 4)), dma((many, 4)), dma((many, 2)), dma((many, 2)), dma((many, 2)), dma((many, 2)), dma((many, 2)), dma((many, 4)),
            dma((4,)), dma((4,)), dma((2,)), dma((2,)), dma((4,)), dma, dma((4,)), dma,
        ],
        input_output_aliases={13: 0},
        compiler_params=pltpu.CompilerParams(collective_id=1, has_side_effects=True, vmem_limit_bytes=VMEM_LIMIT),
        name="back_scatter",
    )(x_win, turned, turned_keys, seg_query, seg_keys, gathered, queries, key_win, value_win, att_grad, logs, delta, mid_grad, parts)[1:3]


def passed_along(value, steps):
    count = lax.axis_size("fsdp")
    first, last = (max(0, -steps), min(count, count - steps))
    return lax.ppermute(value, "fsdp", [(source, source + steps) for source in range(first, last)])


def window_of(rows):
    near = [rows if k == 0 else passed_along(rows, -k) for k in range(-REACH, REACH + 1)]
    return jnp.concatenate(near, axis=0)


def shards(kernels, block_input, params, cotangent, segment_ids):
    count = lax.axis_size("fsdp")
    me = lax.axis_index("fsdp")
    rows = block_input.shape[0]
    margin = REACH * rows
    seg_pad = jnp.pad(segment_ids, (margin, margin), constant_values=-1)
    seg_query = lax.dynamic_slice_in_dim(segment_ids, me * rows, rows, 0)
    seg_keys = lax.dynamic_slice_in_dim(seg_pad, me * rows, 2 * margin + rows, 0)
    plan = wire_plan(count, params.shape[1])
    where = plan[0]
    block = to_tiles(params, plan)
    if kernels:
        gathered, x_win, turned, turned_keys, key_win, value_win, _, queries, attended, rest, logs = gather_front(
            block, block_input, seg_query[:, None], seg_keys[None, :], plan
        )
    else:
        x_win = window_of(block_input)
        gathered = lax.all_gather(block, "fsdp", axis=0, tiled=False)
        queries, key_win, value_win, attended, rest, logs = front(
            x_win, seg_query[:, None], seg_keys[None, :], gathered, where, rows
        )
    activations, mid_grad, att_grad, delta, parts = middle(block_input, cotangent, attended, rest, gathered, where)
    sides = (seg_query[None, :], seg_keys[:, None], gathered, queries, key_win, value_win, att_grad, logs)
    if kernels:
        summed, input_grad = back_scatter(x_win, turned, turned_keys, *sides, delta, mid_grad, parts, plan)
    else:
        near, own, parts = back(x_win, *sides, parts, where)
        input_grad = mid_grad + own
        for k in range(-REACH, REACH + 1):
            if k != 0:
                part = near[(k + REACH) * rows : (k + REACH + 1) * rows]
                input_grad = input_grad + passed_along(part, k).astype(jnp.float32)
        input_grad = input_grad.astype(jnp.bfloat16)
        received = lax.all_to_all(parts, "fsdp", split_axis=0, concat_axis=0, tiled=True)
        summed = jnp.sum(received.astype(jnp.float32), axis=0)
    param_grads = to_flat(summed, plan, params.shape[1])
    return (activations, input_grad, param_grads)


def two_by_two(mesh):
    spans = np.array([device.coords for device in mesh.devices.flat])
    return tuple(spans.max(axis=0) - spans.min(axis=0))[:2] == (1, 1)


def solution(mesh):
    return jax.shard_map(
        functools.partial(shards, two_by_two(mesh)),
        mesh=mesh,
        in_specs=(P("fsdp", None), P(None, "fsdp"), P("fsdp", None), P()),
        out_specs=(P("fsdp", None), P("fsdp", None), P(None, "fsdp")),
        check_vma=False,
    )
```

```python
import functools
import math

import jax
import jax.numpy as jnp
import numpy as np
from jax import lax
from jax.experimental import pallas as pl
from jax.experimental.pallas import tpu as pltpu
from jax.sharding import PartitionSpec as P

D = 1152
HEADS = 16
HEAD_DIM = 72
FF = 4304
REACH = 2


EPS = 1e-06
NEG = -1e30
LANES = 128
ROWS = 16
DC = D // LANES
FC = -(-FF // LANES)
WIDE = FF * ROWS // LANES
HEAD = 544
KIND_A, KIND_D, KIND_L2, KIND_L3, KIND_B = 1, 2, 3, 4, 5
MESH = pl.DeviceIdType.MESH


def units():
    found = []
    offset = 0

    def matrix(name, kind, rows, width, tiles):
        nonlocal offset
        for row in range(0, rows, ROWS):
            found.append((name, kind, offset + row * width, tiles))
        offset += rows * width

    def vectors(name, kind, length, tiles):
        nonlocal offset
        found.append((name, kind, offset, tiles))
        offset += length

    vectors("vec1", KIND_L2, 2 * D, 2)
    matrix("w_query", KIND_A, D, D, DC)
    matrix("w_key", KIND_A, D, D, DC)
    matrix("w_value", KIND_A, D, D, DC)
    vectors("vec2", KIND_L2, 2 * D, 2)
    matrix("w_out", KIND_A, D, D, DC)
    vectors("vec3", KIND_L2, 3 * D, 2)
    matrix("w_up", KIND_B, D, FF, FC)
    vectors("vec4", KIND_L3, FF, 3)
    matrix("w_down", KIND_D, FF, D, DC)
    vectors("vec5", KIND_D, D, DC)
    return found


def unit_width(name):
    return {"vec1": 2 * D, "vec2": 2 * D, "vec3": 3 * D, "vec4": FF, "vec5": D, "w_up": ROWS * FF}.get(
        name, ROWS * D
    )


def wire_plan(count, shard):
    blocks = [[] for _ in range(count)]
    where = {}
    used = [0] * count
    tails = [0] * count
    for name, kind, first, tiles in units():
        owner = first // shard
        where.setdefault(name, []).append((owner, used[owner], tiles))
        blocks[owner].append((kind, (first - owner * shard) // LANES, used[owner]))
        used[owner] += tiles
        tails[owner] = max(0, first + unit_width(name) - (owner + 1) * shard)
    block = max(used)
    block += block % 2
    most = max(len(b) for b in blocks)
    table = np.zeros((count, 3 * most), np.int32)
    for owner, entries in enumerate(blocks):
        for i, entry in enumerate(entries):
            table[owner, 3 * i : 3 * i + 3] = entry
    return where, block, table, np.array(tails, np.int32)


def lane_iota(rows):
    return lax.broadcasted_iota(jnp.int32, (rows, LANES), 1)


def wide_rows():
    return [divmod(row * FF, LANES) for row in range(ROWS)]


SKEW = (D * 0 + 80) % LANES


def rows_from_line(line_ref, flat_ref, first, rows):
    step = 8 * LANES

    @pl.loop(0, rows // 8)
    def _(i):
        part = line_ref[:, pl.ds(pl.multiple_of(i * step, step), step)].astype(jnp.float32)
        flat_ref[pl.ds(first + i * 8, 8)] = part.reshape(8, LANES)

    for row in range(rows // 8 * 8, rows):
        flat_ref[pl.ds(first + row, 1)] = line_ref[:, row * LANES : (row + 1) * LANES].astype(jnp.float32)


def line_from_rows(flat_ref, line_ref, first, rows):
    step = 8 * LANES

    @pl.loop(0, rows // 8)
    def _(i):
        part = flat_ref[pl.ds(first + i * 8, 8)]
        line_ref[:, pl.ds(pl.multiple_of(i * step, step), step)] = part.reshape(1, step)

    for row in range(rows // 8 * 8, rows):
        line_ref[:, row * LANES : (row + 1) * LANES] = flat_ref[pl.ds(first + row, 1)]


def to_tiles_kernel(entries, table_ref, line_ref, head_ref, tile_ref, stage_ref, flat_ref):
    rows = line_ref.shape[1] // LANES
    rows_from_line(line_ref, flat_ref, 0, rows)
    rows_from_line(head_ref, flat_ref, rows, HEAD)

    def unit(i, _):
        kind, src, dst = (table_ref[3 * i + j] for j in range(3))

        @pl.when(kind == KIND_A)
        def _():
            for c in range(DC):
                tile_ref[dst + c] = flat_ref[pl.ds(src + c, ROWS, stride=DC), :].astype(jnp.bfloat16)

        @pl.when(kind == KIND_D)
        def _():
            lane = lane_iota(ROWS)
            for c in range(DC):
                here = flat_ref[pl.ds(src + c, ROWS, stride=DC), :]
                after = flat_ref[pl.ds(src + c + 1, ROWS, stride=DC), :]
                both = jnp.where(lane >= SKEW, here, after)
                tile_ref[dst + c] = pltpu.roll(both, LANES - SKEW, 1).astype(jnp.bfloat16)

        for code, tiles in ((KIND_L2, 2), (KIND_L3, 3)):

            @pl.when(kind == code)
            def _():
                for j in range(tiles):
                    tile_ref[dst + j] = flat_ref[pl.ds(src + ROWS * j, ROWS), :].astype(jnp.bfloat16)

        @pl.when(kind == KIND_B)
        def _():
            tall = 8 * pl.cdiv(FC, 8)
            lane = lane_iota(tall)
            row = lax.broadcasted_iota(jnp.int32, (tall, LANES), 0)
            keep = (row < FC - 1) | (lane < FF % LANES)
            for r, (base, skew) in enumerate(wide_rows()):
                part = flat_ref[pl.ds(src + base, tall), :]
                if skew:
                    after = flat_ref[pl.ds(src + base + 1, tall), :]
                    part = pltpu.roll(jnp.where(lane >= skew, part, after), LANES - skew, 1)
                stage_ref[pl.ds(r, tall, stride=ROWS), :] = jnp.where(keep, part, 0.0)
            for c in range(FC):
                tile_ref[dst + c] = stage_ref[pl.ds(ROWS * c, ROWS), :].astype(jnp.bfloat16)

        return 0

    lax.fori_loop(0, entries, unit, 0)


def to_flat_kernel(entries, rows, table_ref, tile_ref, *refs):
    if len(refs) == 5:
        tail_ref, line_ref, stage_ref, flat_ref, first_ref = refs
    else:
        line_ref, stage_ref, flat_ref = refs
    if len(refs) == 5:
        flat_ref[...] = jnp.zeros_like(flat_ref)

    def unit(i, _):
        kind, src, dst = (table_ref[3 * i + j] for j in range(3))

        @pl.when(kind == KIND_A)
        def _():
            for c in range(DC):
                flat_ref[pl.ds(src + c, ROWS, stride=DC), :] = tile_ref[dst + c]

        @pl.when(kind == KIND_D)
        def _():
            lane = lane_iota(ROWS)
            for c in range(DC):
                turned = pltpu.roll(tile_ref[dst + c], SKEW, 1)
                for step, keep in ((0, lane >= SKEW), (1, lane < SKEW)):
                    at = pl.ds(src + c + step, ROWS, stride=DC)
                    flat_ref[at, :] = jnp.where(keep, turned, flat_ref[at, :])

        for code, tiles in ((KIND_L2, 2), (KIND_L3, 3)):

            @pl.when(kind == code)
            def _():
                for j in range(tiles):
                    flat_ref[pl.ds(src + ROWS * j, ROWS), :] = tile_ref[dst + j]

        @pl.when(kind == KIND_B)
        def _():
            tall = 8 * pl.cdiv(FC, 8)
            lane = lane_iota(tall)
            row = lax.broadcasted_iota(jnp.int32, (tall, LANES), 0)
            for c in range(FC):
                stage_ref[pl.ds(ROWS * c, ROWS), :] = tile_ref[dst + c]
            for r, (base, skew) in enumerate(wide_rows()):
                turned = stage_ref[pl.ds(r, tall, stride=ROWS), :]
                if skew:
                    turned = pltpu.roll(turned, skew, 1)
                for step in range(2 if skew else 1):
                    entry = row * LANES + lane + (step * LANES - skew)
                    keep = (lane < skew if step else lane >= skew) & (entry < FF)
                    at = pl.ds(src + base + step, tall)
                    flat_ref[at, :] = jnp.where(keep, turned, flat_ref[at, :])

        return 0

    lax.fori_loop(0, entries, unit, 0)
    if len(refs) == 3:
        line_from_rows(flat_ref, line_ref, rows, HEAD)
        return
    rows_from_line(tail_ref, first_ref, 0, HEAD)
    entry = lax.broadcasted_iota(jnp.int32, (HEAD, LANES), 0) * LANES + lane_iota(HEAD)
    flat_ref[:HEAD] = jnp.where(entry < table_ref[3 * entries], first_ref[...], flat_ref[:HEAD])
    line_from_rows(flat_ref, line_ref, 0, rows)


def my_row(table):
    return lax.dynamic_index_in_dim(jnp.asarray(table), lax.axis_index("fsdp"), 0, keepdims=False)


def relayout_scratch(rows):
    return [
        pltpu.VMEM((ROWS * 8 * pl.cdiv(FC, 8), LANES), jnp.float32),
        pltpu.VMEM((8 * pl.cdiv(rows + HEAD + 8, 8), LANES), jnp.float32),
    ]


def to_tiles(line, plan):
    where, block, table, tails = plan
    count = lax.axis_size("fsdp")
    head = lax.ppermute(line[:, : HEAD * LANES], "fsdp", [(i, (i - 1) % count) for i in range(count)])
    vmem = pl.BlockSpec(memory_space=pltpu.VMEM)
    return pl.pallas_call(
        functools.partial(to_tiles_kernel, table.shape[1] // 3),
        out_shape=jax.ShapeDtypeStruct((block, ROWS, LANES), jnp.bfloat16),
        grid_spec=pltpu.PrefetchScalarGridSpec(
            num_scalar_prefetch=1, grid=(1,), in_specs=[vmem, vmem], out_specs=vmem,
            scratch_shapes=relayout_scratch(line.shape[1] // LANES),
        ),
        name="to_tiles",
    )(my_row(table), line, head)


def to_flat(tiles, plan, length):
    where, block, table, tails = plan
    count = lax.axis_size("fsdp")
    rows = length // LANES
    vmem = pl.BlockSpec(memory_space=pltpu.VMEM)
    last = [max(i for i in range(table.shape[1] // 3) if row[3 * i]) for row in table]
    last = np.stack([row[3 * i : 3 * i + 3] for row, i in zip(table, last)])
    whole = np.concatenate([table, np.roll(tails, 1)[:, None]], axis=1)

    def call(entries, mine, inputs, width, scratch, name):
        return pl.pallas_call(
            functools.partial(to_flat_kernel, entries, rows),
            out_shape=jax.ShapeDtypeStruct((1, width), jnp.float32),
            grid_spec=pltpu.PrefetchScalarGridSpec(
                num_scalar_prefetch=1, grid=(1,), in_specs=[vmem] * len(inputs), out_specs=vmem,
                scratch_shapes=relayout_scratch(rows) + scratch,
            ),
            name=name,
        )(my_row(mine), *inputs)

    tail = call(1, last, (tiles,), HEAD * LANES, [], "tail")
    tail = lax.ppermute(tail, "fsdp", [(i, (i + 1) % count) for i in range(count)])
    return call(table.shape[1] // 3, whole, (tiles, tail), length, [pltpu.VMEM((HEAD, LANES), jnp.float32)], "to_flat")


def place(me):
    return lax.rem(me, 2), lax.rem(me // 2, 2), lax.rem(me // 4, 2), me // 8


def index_of(core, x, y, z):
    return ((z * 2 + y) * 2 + x) * 2 + core


def greet(devices_and_conditions):
    barrier = pltpu.get_barrier_semaphore()
    for device, present in devices_and_conditions:
        if present is None:
            pl.semaphore_signal(barrier, inc=1, device_id=(device,), device_id_type=MESH)
        else:

            @pl.when(present)
            def _():
                pl.semaphore_signal(barrier, inc=1, device_id=(device,), device_id_type=MESH)

    present = [1 if p is None else p.astype(jnp.int32) for _, p in devices_and_conditions]
    pl.semaphore_wait(barrier, sum(present))


BF = jnp.bfloat16
F32 = jnp.float32
PAIR = 2 * LANES
SCALE = HEAD_DIM**-0.5
GELU_A = math.sqrt(2.0 / math.pi)
GELU_B = 0.044715
LOG2E = math.log2(math.e)
ANY = pl.BlockSpec(memory_space=pl.ANY)
VM = pl.BlockSpec(memory_space=pltpu.VMEM)
VMEM_LIMIT = 63 << 20


def nn(left, right):
    return lax.dot_general(left, right, (((1,), (0,)), ((), ())), preferred_element_type=F32)


def nt(left, right):
    return lax.dot_general(left, right, (((1,), (1,)), ((), ())), preferred_element_type=F32)


def runs_of(where, name):
    runs, done = [], 0
    for owner, at, tiles in where[name]:
        if runs and runs[-1][0] == owner and runs[-1][1] + runs[-1][2] == at:
            runs[-1][2] += tiles
        else:
            runs.append([owner, at, tiles, done])
        done += tiles
    return runs


def copies(where, name, blocks_ref, tiles_ref, sem, out=False):
    made = []
    flat_tiles = tiles_ref if len(tiles_ref.shape) == 3 else tiles_ref.reshape(-1, ROWS, LANES)
    for owner, at, tiles, done in runs_of(where, name):
        there, here = blocks_ref.at[owner, pl.ds(at, tiles)], flat_tiles.at[pl.ds(done, tiles)]
        made.append(pltpu.make_async_copy(here, there, sem) if out else pltpu.make_async_copy(there, here, sem))
    return made


def start(made):
    for copy in made:
        copy.start()


def wait(made):
    for copy in made:
        copy.wait()


def panel(tiles_ref, c, units, first=0):
    return tiles_ref[pl.ds(first, units), pl.ds(c, 1)].reshape(units * ROWS, LANES)


def panels(tiles_ref, c, many, units, first=0):
    return jnp.concatenate([panel(tiles_ref, c + i, units, first) for i in range(many)], axis=1)


def put_panel(tiles_ref, c, value, first=0):
    units = value.shape[0] // ROWS
    tiles_ref[pl.ds(first, units), pl.ds(c, 1)] = value.astype(BF).reshape(units, 1, ROWS, LANES)


def put_panels(tiles_ref, c, value, first=0):
    for i in range(value.shape[1] // LANES):
        put_panel(tiles_ref, c + i, value[:, i * LANES : (i + 1) * LANES], first)


def over_pairs(body):
    @pl.loop(0, DC // 2)
    def _(pair):
        body(2 * pair, 2)

    if DC % 2:
        body(DC - 1, 1)


def lanes_of(c, many):
    return pl.ds(c * LANES if isinstance(c, int) else pl.multiple_of(c * LANES, LANES), many * LANES)


def vector_rows(tiles_ref):
    return jnp.concatenate([tiles_ref[i].astype(F32) for i in range(tiles_ref.shape[0])], axis=0)


def as_row(rows, first, many):
    return jnp.concatenate([rows[first + i : first + i + 1] for i in range(many)], axis=1)


def put_vectors(tiles_ref, rows_list):
    parts = [row[:, i * LANES : (i + 1) * LANES] for row in rows_list for i in range(row.shape[1] // LANES)]
    missing = tiles_ref.shape[0] * ROWS - len(parts)
    whole = jnp.concatenate(parts + [jnp.zeros((missing, LANES), F32)] if missing else parts, axis=0)
    for i in range(tiles_ref.shape[0]):
        tiles_ref[i] = whole[i * ROWS : (i + 1) * ROWS].astype(BF)


def norm_rows(values):
    centre = values - jnp.mean(values, axis=-1, keepdims=True)
    inverse = lax.rsqrt(jnp.mean(centre * centre, axis=-1, keepdims=True) + EPS)
    return centre * inverse, inverse


def norm_rows_back(grad, normed, inverse, gain):
    scaled = grad * gain
    return inverse * (
        scaled - jnp.mean(scaled, axis=-1, keepdims=True) - normed * jnp.mean(scaled * normed, axis=-1, keepdims=True)
    )


def column_sums(values):
    return jnp.sum(values, axis=0, keepdims=True)


def head_window(h):
    block = jnp.minimum((h * HEAD_DIM) // LANES, DC - 2)
    lane = pl.multiple_of(block * LANES, LANES)
    return lane, h * HEAD_DIM - lane


def head_mask(rows, offset):
    lane = lax.broadcasted_iota(jnp.int32, (rows, PAIR), 1)
    return (lane >= offset) & (lane < offset + HEAD_DIM)


def front_kernel(
    where, x_ref, segq_ref, segk_ref, blocks_ref, q_ref, k_ref, v_ref, attended_ref, rest_ref, logs_ref,
    normed_ref, w_ref, vec1_ref, vec2_ref, bias_ref, score_ref, prob_ref, sem, vec_sem,
):
    window, rows = x_ref.shape[0], q_ref.shape[0]
    margin = (window - rows) // 2
    loads = [copies(where, name, blocks_ref, w_ref.at[i], sem.at[i]) for i, name in enumerate(("w_query", "w_key", "w_value"))]
    vecs = copies(where, "vec1", blocks_ref, vec1_ref, vec_sem) + copies(where, "vec2", blocks_ref, vec2_ref, vec_sem)
    start(vecs)
    for made in loads:
        start(made)
    wait(vecs)
    vec = vector_rows(vec1_ref)
    gain, shift = as_row(vec, 0, DC), as_row(vec, DC, DC)
    step = rows // 3

    @pl.loop(0, window // step)
    def _(i):
        at = pl.ds(i * step, step)
        normed, _ = norm_rows(x_ref[at].astype(F32))
        normed_ref[at] = (normed * gain + shift).astype(BF)

    @pl.loop(0, rows // 8)
    def _(i):
        at = pl.ds(i * 8, 8)
        bias_ref[at] = jnp.where(segq_ref[at] == segk_ref[...], 0.0, NEG)

    biases = vector_rows(vec2_ref)
    zero = jnp.zeros((1, D), F32)
    for made in loads:
        wait(made)
    for i, (out, add) in enumerate(((q_ref, as_row(biases, 0, DC)), (k_ref, zero), (v_ref, as_row(biases, DC, DC)))):
        for c in range(0, DC, 2):
            many = min(2, DC - c)
            lanes = slice(c * LANES, (c + many) * LANES)
            weights = panels(w_ref.at[i], c, many, D // ROWS)
            if i == 0:
                out[:, lanes] = (nn(normed_ref[pl.ds(margin, rows)], weights) + add[:, lanes]).astype(BF)
            else:

                @pl.loop(0, window // rows)
                def _(b):
                    at = pl.ds(b * rows, rows)
                    out[at, lanes] = (nn(normed_ref[at], weights) + add[:, lanes]).astype(BF)

    attended_ref[...] = jnp.zeros_like(attended_ref)
    rest_ref[...] = jnp.zeros_like(rest_ref)
    logs_ref[...] = jnp.zeros_like(logs_ref)
    lane_l = lax.broadcasted_iota(jnp.int32, logs_ref.shape, 1)

    @pl.loop(0, HEADS)
    def _(h):
        lane, offset = head_window(h)
        mask = head_mask(rows, offset)
        lanes = pl.ds(lane, PAIR)
        query = jnp.where(mask, q_ref[:, lanes], jnp.zeros((), BF))
        score_ref[...] = nt(query, k_ref[:, lanes]) * SCALE + bias_ref[...]
        top = jnp.max(score_ref[...], axis=-1, keepdims=True)
        powers = jnp.exp(score_ref[...] - top)
        total = jnp.sum(powers, axis=-1, keepdims=True)
        prob_ref[...] = powers.astype(BF)
        out = nn(prob_ref[...], v_ref[:, lanes]) / total
        rounded = out.astype(BF)
        attended_ref[:, lanes] = jnp.where(mask, rounded, attended_ref[:, lanes])
        rest_ref[:, lanes] = jnp.where(mask, (out - rounded.astype(F32)).astype(BF), rest_ref[:, lanes])
        logs_ref[...] = jnp.where(lane_l == h, top + jnp.log(total), logs_ref[...])


def front(x_win, seg_query, seg_keys, gathered, where, rows):
    window = x_win.shape[0]
    shape = lambda n, d=D, t=BF: jax.ShapeDtypeStruct((n, d), t)
    dma = pltpu.SemaphoreType.DMA
    units = D // ROWS
    return pl.pallas_call(
        functools.partial(front_kernel, where),
        out_shape=(shape(rows), shape(window), shape(window), shape(rows), shape(rows), shape(rows, LANES, F32)),
        in_specs=[VM, VM, VM, ANY],
        out_specs=[VM] * 6,
        scratch_shapes=[
            pltpu.VMEM((window, D), BF),
            pltpu.VMEM((3, units, DC, ROWS, LANES), BF), pltpu.VMEM((2, ROWS, LANES), BF), pltpu.VMEM((2, ROWS, LANES), BF),
            pltpu.VMEM((rows, window), F32), pltpu.VMEM((rows, window), F32), pltpu.VMEM((rows, window), BF), dma((3,)), dma,
        ],
        compiler_params=pltpu.CompilerParams(vmem_limit_bytes=VMEM_LIMIT),
        name="front",
    )(x_win, seg_query, seg_keys, gathered)


def middle_kernel(
    where, x_ref, cot_ref, attended_ref, rest_ref, blocks_ref, act_ref, mid_grad_ref, att_grad_ref, delta_ref, parts_ref,
    wo_ref, wu_ref, wd_ref, vec3_ref, vec4_ref, vec5_ref, b_up_ref, hidden_ref, slope_ref, pre_ref, normed_ref, normed_b_ref,
    mid_ref, g_up_ref, mid_b_ref, sem, out_sem,
):
    rows = x_ref.shape[0]
    units, f_units = D // ROWS, FF // ROWS
    names = ("w_out", "w_up", "w_down", "vec3", "vec4", "vec5")
    refs = (wo_ref, wu_ref, wd_ref, vec3_ref, vec4_ref, vec5_ref)
    loads = {n: copies(where, n, blocks_ref, r, sem.at[i]) for i, (n, r) in enumerate(zip(names, refs))}
    saves = {n: copies(where, n, parts_ref, r, out_sem, out=True) for n, r in zip(names, refs)}
    for n in ("vec3", "vec4", "vec5", "w_out", "w_up", "w_down"):
        start(loads[n])
    f_wide = FC * LANES
    pads = f_wide // ROWS - f_units
    wd_ref[pl.ds(f_units, pads)] = jnp.zeros((pads, DC, ROWS, LANES), BF)
    for n in ("vec3", "vec4", "vec5", "w_out"):
        wait(loads[n])
    vec = vector_rows(vec3_ref)
    b_out, gain, shift = (as_row(vec, i * DC, DC) for i in range(3))
    vec = vector_rows(vec4_ref)
    entry = lax.broadcasted_iota(jnp.int32, vec.shape, 0) * LANES + lax.broadcasted_iota(jnp.int32, vec.shape, 1)
    b_up_ref[...] = jnp.where(entry < FF, vec, 0.0)
    b_down = jnp.concatenate([vec5_ref[c].astype(F32)[0:1] for c in range(DC)], axis=1)

    for c in range(0, DC, 2):
        many = min(2, DC - c)
        lanes = slice(c * LANES, (c + many) * LANES)
        mid_ref[:, lanes] = (
            x_ref[:, lanes].astype(F32) + nn(attended_ref[...], panels(wo_ref, c, many, units)) + b_out[:, lanes]
        )
    normed, inverse = norm_rows(mid_ref[...])
    normed_ref[...] = normed
    normed_b_ref[...] = (normed * gain + shift).astype(BF)

    wait(loads["w_up"])

    @pl.loop(0, FC // 2)
    def _(p):
        at = pl.ds(pl.multiple_of(p * PAIR, PAIR), PAIR)
        bias = jnp.concatenate([b_up_ref[pl.ds(2 * p, 1)], b_up_ref[pl.ds(2 * p + 1, 1)]], axis=1)
        v = nn(normed_b_ref[...], panels(wu_ref, 2 * p, 2, units)) + bias
        square = v * v
        bent = jnp.tanh(GELU_A * v * (1.0 + GELU_B * square))
        hidden_ref[:, at] = (0.5 * v * (1.0 + bent)).astype(BF)
        slope_ref[:, at] = 0.5 * (1.0 + bent) + 0.5 * v * (1.0 - bent * bent) * (
            GELU_A * (1.0 + 3.0 * GELU_B * square)
        )

    wait(loads["w_down"])
    for c in range(0, DC, 2):
        many = min(2, DC - c)
        lanes = slice(c * LANES, (c + many) * LANES)
        act_ref[:, lanes] = (
            mid_ref[:, lanes] + nn(hidden_ref[...], panels(wd_ref, c, many, f_wide // ROWS)) + b_down[:, lanes]
        ).astype(BF)

    @pl.loop(0, FC // 2)
    def _(p):
        at = pl.ds(pl.multiple_of(p * PAIR, PAIR), PAIR)
        first = p * (PAIR // ROWS)
        grad = nt(cot_ref[...], panels(wd_ref, 0, DC, PAIR // ROWS, first)) * slope_ref[:, at]
        pre_ref[:, at] = grad.astype(BF)
        sums = column_sums(grad)
        g_up_ref[pl.ds(2 * p, 1)] = sums[:, :LANES]
        g_up_ref[pl.ds(2 * p + 1, 1)] = sums[:, LANES:]
        put_panels(wd_ref, 0, nn(hidden_ref[:, at].T, cot_ref[...]), first)

    start(saves["w_down"])
    put_vectors(vec4_ref, [b_up_row for b_up_row in [g_up_ref[i : i + 1] for i in range(FC)]])
    start(saves["vec4"])
    cot = cot_ref[...].astype(F32)
    sums = column_sums(cot)
    row0 = lax.broadcasted_iota(jnp.int32, (ROWS, LANES), 0) == 0
    for c in range(DC):
        vec5_ref[c] = jnp.where(row0, sums[:, c * LANES : (c + 1) * LANES], 0.0).astype(BF)
    start(saves["vec5"])

    for c in range(0, DC, 2):
        many = min(2, DC - c)
        weights = panels(wu_ref, 0, FC, many * LANES // ROWS, c * LANES // ROWS)
        mid_ref[:, c * LANES : (c + many) * LANES] = nt(pre_ref[...], weights)
    turned_b = normed_b_ref[...].T

    @pl.loop(0, FC // 2)
    def _(p):
        at = pl.ds(pl.multiple_of(p * PAIR, PAIR), PAIR)
        put_panels(wu_ref, 2 * p, nn(turned_b, pre_ref[:, at]))

    start(saves["w_up"])
    e = mid_ref[...]
    normed = normed_ref[...]
    g_gain, g_shift = column_sums(e * normed), column_sums(e)
    mid_grad = cot + norm_rows_back(e, normed, inverse, gain)
    mid_grad_ref[...] = mid_grad
    put_vectors(vec3_ref, [column_sums(mid_grad), g_gain, g_shift])
    start(saves["vec3"])
    mid_b = mid_grad.astype(BF)
    mid_b_ref[...] = mid_b

    def attended_grad(c, many):
        weights = panels(wo_ref, 0, DC, many * LANES // ROWS, c * (LANES // ROWS))
        att_grad_ref[:, lanes_of(c, many)] = nt(mid_b_ref[...], weights).astype(BF)

    over_pairs(attended_grad)
    product = att_grad_ref[...].astype(F32) * (attended_ref[...].astype(F32) + rest_ref[...].astype(F32))
    delta_ref[...] = jnp.sum(product.T.reshape(HEADS, HEAD_DIM, rows), axis=1)
    turned = attended_ref[...].T
    over_pairs(lambda c, many: put_panels(wo_ref, c, nn(turned, mid_b_ref[:, lanes_of(c, many)])))
    start(saves["w_out"])
    for n in names:
        wait(saves[n])


def middle(block_input, cotangent, attended, rest, gathered, where):
    rows = block_input.shape[0]
    shape = lambda t: jax.ShapeDtypeStruct((rows, D), t)
    dma = pltpu.SemaphoreType.DMA
    tiles = lambda *n: pltpu.VMEM((*n, ROWS, LANES), BF)
    units, f_wide = D // ROWS, FC * LANES
    return pl.pallas_call(
        functools.partial(middle_kernel, where),
        out_shape=(shape(BF), shape(F32), shape(BF), jax.ShapeDtypeStruct((HEADS, rows), F32), jax.ShapeDtypeStruct(gathered.shape, BF)),
        in_specs=[VM, VM, VM, VM, ANY],
        out_specs=[VM, VM, VM, VM, ANY],
        scratch_shapes=[
            tiles(units, DC), tiles(units, FC), tiles(f_wide // ROWS, DC), tiles(2), tiles(3), tiles(DC),
            pltpu.VMEM((3 * ROWS, LANES), F32), pltpu.VMEM((rows, f_wide), BF), pltpu.VMEM((rows, f_wide), F32),
            pltpu.VMEM((rows, f_wide), BF), pltpu.VMEM((rows, D), F32), pltpu.VMEM((rows, D), BF), pltpu.VMEM((rows, D), F32),
            pltpu.VMEM((3 * ROWS, LANES), F32), pltpu.VMEM((rows, D), BF), dma((6,)), dma,
        ],
        compiler_params=pltpu.CompilerParams(vmem_limit_bytes=VMEM_LIMIT),
        name="middle",
    )(block_input, cotangent, attended, rest, gathered)


def back_kernel(
    where, x_hbm_ref, segq_ref, segk_ref, blocks_ref, q_ref, k_ref, v_ref, grad_ref, logs_ref, parts_in_ref,
    near_ref, own_ref, parts_ref,
    w_ref, vec1_ref, vec2_ref, bias_ref, score_ref, prob_ref, turned_ref, dk_ref, dv_ref, dq_ref, part_ref, logs_t_ref, x_ref,
    sem, vec_sem, out_sem, x_sem,
):
    window, rows = x_ref.shape[0], q_ref.shape[0]
    margin = (window - rows) // 2
    units = D // ROWS
    names = ("w_query", "w_key", "w_value")
    loads = [copies(where, name, blocks_ref, w_ref.at[i], sem.at[i]) for i, name in enumerate(names)]
    vecs = copies(where, "vec1", blocks_ref, vec1_ref, vec_sem)
    start(vecs)
    for made in loads:
        start(made)
    x_load = pltpu.make_async_copy(x_hbm_ref, x_ref, x_sem)
    x_load.start()

    @pl.loop(0, window // LANES)
    def _(i):
        at = pl.ds(pl.multiple_of(i * LANES, LANES), LANES)
        bias_ref[at] = jnp.where(segk_ref[at] == segq_ref[...], 0.0, NEG)
        turned_ref[:, at] = k_ref[at].T
        dk_ref[at] = jnp.zeros((LANES, D), F32)
        dv_ref[at] = jnp.zeros((LANES, D), F32)

    logs_t_ref[...] = logs_ref[...].T

    @pl.loop(0, HEADS)
    def _(h):
        lane, offset = head_window(h)
        mask = head_mask(rows, offset)
        lanes = pl.ds(lane, PAIR)
        query = jnp.where(mask, q_ref[:, lanes], jnp.zeros((), BF))
        grad = jnp.where(mask, grad_ref[:, lanes], jnp.zeros((), BF))
        probs = jnp.exp(nt(k_ref[:, lanes], query) * SCALE + bias_ref[...] - logs_t_ref[pl.ds(h, 1)])
        score_ref[...] = probs
        prob_ref[...] = probs.astype(BF)
        prob_grad = nt(v_ref[:, lanes], grad)
        row_total = jnp.sum(score_ref[...] * prob_grad, axis=0, keepdims=True)
        dv_ref[:, lanes] += nn(prob_ref[...], grad)
        prob_ref[...] = (score_ref[...] * (prob_grad - row_total)).astype(BF)
        dk_ref[:, lanes] += nn(prob_ref[...], query)
        part_ref[...] = nn(turned_ref[lanes], prob_ref[...])
        at = pl.ds(pl.multiple_of(h * HEAD_DIM, 8), HEAD_DIM)
        dq_ref[at] = part_ref[pl.ds(pl.multiple_of(offset, 8), HEAD_DIM)]

    dq = dq_ref[...].T * SCALE
    g_query = column_sums(dq)
    dq_b = dq.astype(BF)
    wait(vecs)
    vec = vector_rows(vec1_ref)
    gain, shift = as_row(vec, 0, DC), as_row(vec, DC, DC)
    dk_b_ref, dv_b_ref = k_ref, v_ref
    x_load.wait()
    g_value = jnp.zeros((1, D), F32)
    step = rows // 3

    def rounded(i, total):
        at = pl.ds(pl.multiple_of(i * step, step), step)
        dk_b_ref[at] = (dk_ref[at] * SCALE).astype(BF)
        dv = dv_ref[at]
        dv_b_ref[at] = dv.astype(BF)
        normed, _ = norm_rows(x_ref[at].astype(F32))
        turned_ref[:, at] = (normed * gain + shift).astype(BF).T
        return total + column_sums(dv)

    g_value = lax.fori_loop(0, window // step, rounded, g_value)
    put_vectors(vec2_ref, [g_query, g_value])
    save = copies(where, "vec2", parts_ref, vec2_ref, out_sem, out=True)
    for made in loads:
        wait(made)
    for c in range(0, DC, 2):
        many = min(2, DC - c)
        lanes = slice(c * LANES, (c + many) * LANES)
        part = [panels(w_ref.at[i], 0, DC, many * LANES // ROWS, c * LANES // ROWS) for i in range(3)]

        @pl.loop(0, window // rows)
        def _(b):
            at = pl.ds(b * rows, rows)
            dk_ref[at, lanes] = nt(dk_b_ref[at], part[1]) + nt(dv_b_ref[at], part[2])

        dk_ref[pl.ds(margin, rows), lanes] += nt(dq_b, part[0])
    turned_own = turned_ref[:, pl.ds(margin, rows)]
    for c in range(0, DC, 2):
        many = min(2, DC - c)
        lanes = slice(c * LANES, (c + many) * LANES)
        put_panels(w_ref.at[0], c, nn(turned_own, dq_b[:, lanes]))
        put_panels(w_ref.at[1], c, nn(turned_ref[...], dk_b_ref[:, lanes]))
        put_panels(w_ref.at[2], c, nn(turned_ref[...], dv_b_ref[:, lanes]))
    for i, name in enumerate(names):
        save = save + copies(where, name, parts_ref, w_ref.at[i], out_sem, out=True)
    start(save)

    def norm_block(i, totals):
        at = pl.ds(pl.multiple_of(i * step, step), step)
        normed, inverse = norm_rows(x_ref[at].astype(F32))
        e = dk_ref[at]
        part = norm_rows_back(e, normed, inverse, gain)
        x_ref[at] = part.astype(BF)

        @pl.when((i >= margin // step) & (i < (margin + rows) // step))
        def _():
            own_ref[pl.ds(pl.multiple_of(i * step - margin, step), step)] = part

        return totals[0] + column_sums(e * normed), totals[1] + column_sums(e)

    zero = jnp.zeros((1, D), F32)
    g_gain, g_shift = lax.fori_loop(0, window // step, norm_block, (zero, zero))
    put_vectors(vec1_ref, [g_gain, g_shift])
    last = copies(where, "vec1", parts_ref, vec1_ref, out_sem, out=True)
    last = last + [pltpu.make_async_copy(x_ref, near_ref, x_sem)]
    start(last)
    wait(save + last)


def back(x_win, seg_query, seg_keys, gathered, queries, key_win, value_win, att_grad, logs, parts, where):
    window, rows = x_win.shape[0], queries.shape[0]
    dma = pltpu.SemaphoreType.DMA
    tiles = lambda *n: pltpu.VMEM((*n, ROWS, LANES), BF)
    vm = lambda a, b, t: pltpu.VMEM((a, b), t)
    return pl.pallas_call(
        functools.partial(back_kernel, where),
        out_shape=(
            jax.ShapeDtypeStruct((window, D), BF), jax.ShapeDtypeStruct((rows, D), F32), jax.ShapeDtypeStruct(parts.shape, BF),
        ),
        in_specs=[ANY, VM, VM, ANY, VM, VM, VM, VM, VM, ANY],
        out_specs=[ANY, VM, ANY],
        scratch_shapes=[
            tiles(3, D // ROWS, DC), tiles(2), tiles(2), vm(window, rows, F32), vm(window, rows, F32), vm(window, rows, BF),
            vm(D, window, BF), vm(window, D, F32), vm(window, D, F32), vm(D, rows, F32), vm(PAIR, rows, F32), vm(LANES, rows, F32),
            vm(window, D, BF), dma((3,)), dma, dma, dma,
        ],
        input_output_aliases={9: 2},
        compiler_params=pltpu.CompilerParams(vmem_limit_bytes=VMEM_LIMIT),
        name="back",
    )(x_win, seg_query, seg_keys, gathered, queries, key_win, value_win, att_grad, logs, parts)


HOT_NAMES = ("vec1", "w_query", "w_key", "w_value", "vec2")


def transfer_pieces(plan, depth):
    where = plan[0]
    count = plan[2].shape[0]
    hot, used = [0] * depth, [0] * depth
    for name in where:
        for owner, at, tiles in where[name]:
            level = owner * depth // count
            used[level] = max(used[level], at + tiles)
            if name in HOT_NAMES:
                hot[level] = max(hot[level], at + tiles)
    early = [(level, 0, h) for level, h in enumerate(hot) if h]
    late = [(level, h, u - h) for level, (h, u) in enumerate(zip(hot, used)) if h < u]
    return early, late


def cut(piece, many):
    level, first, tiles = piece
    half = tiles // 2
    edges = [half * i // (many // 2) for i in range(many // 2)] + [
        half + (tiles - half) * i // (many // 2) for i in range(many // 2 + 1)
    ]
    return [(level, first + a, b - a) for a, b in zip(edges[:-1], edges[1:])]


def gather_front_kernel(
    depth, where, early, late,
    block_ref, x_in_ref, segq_ref, segk_ref,
    out_ref, x_out_ref, turned_out_ref, keys_out_ref, k_out_ref, v_out_ref, x_got_ref, q_ref, attended_ref, rest_ref, logs_ref,
    z_send, z_recv, x_send, x_recv, y_send, y_recv, corner_send, corner_recv, line_send, line_recv, mate_send, mate_recv, w_send, w_recv,
    local_sem, stage_ref, both_ref, x_ref, turned_ref, normed_ref, w_ref, vec1_ref, vec2_ref, bias_ref, score_ref, prob_ref, add_ref, sem, vec_sem, x_sem, keys_sem,
):
    me = lax.axis_index("fsdp")
    count = 8 * depth
    core, x, y, z = place(me)
    mate, x_near, y_near = index_of(1 - core, x, y, z), index_of(core, 1 - x, y, z), index_of(core, x, 1 - y, z)
    up, down = me + 8, me - 8
    after, before = me + 2, me - 2
    has_after, has_before = after < count, before >= 0
    greet(
        [(mate, None), (x_near, None), (y_near, None), (down, z > 0), (up, z < depth - 1), (after, has_after), (before, has_before)]
    )
    pieces = early + late
    chunks = {p: cut(piece, 4) if piece[0] == 0 and p < len(early) else [piece] for p, piece in enumerate(pieces)}
    chunk_list = [(p, chunk) for p in chunks for chunk in chunks[p]]
    ids = {p: [i for i, (q, _) in enumerate(chunk_list) if q == p] for p in chunks}
    hot, cold = range(len(early)), range(len(early), len(pieces))
    hot_levels = {level for level, _, _ in early}

    def remote(source, target, send, recv, device):
        return pltpu.make_async_remote_copy(
            src_ref=source, dst_ref=target, send_sem=send, recv_sem=recv, device_id=(device,), device_id_type=MESH
        )

    def span(piece):
        return pl.ds(piece[1], piece[2])

    def halves(p):
        level, first, tiles = pieces[p]
        part = tiles // 2 if p in hot else tiles * 2 // 3
        return (level, first, part), (level, first + part, tiles - part)

    def column(level):
        return index_of(core, x, y, level)

    def from_x(level):
        return index_of(core, 1 - x, y, level)

    def from_y(level):
        return index_of(core, x, 1 - y, level)

    def across(level):
        return index_of(core, 1 - x, 1 - y, level)

    def pass_on(block, piece, send, recv, device, own=False):
        there = out_ref.at[block, span(piece)]
        return remote(block_ref.at[span(piece)] if own else there, there, send, recv, device)

    def z_copy(i, upward, own=False):
        piece = chunk_list[i][1]
        return pass_on(column(piece[0]), piece, z_send.at[i, 0 if upward else 1], z_recv.at[i], up if upward else down, own)

    def plane_copies(i, own=False):
        piece = chunk_list[i][1]
        block = column(piece[0])
        return (
            pass_on(block, piece, x_send.at[i], x_recv.at[i], x_near, own),
            pass_on(block, piece, y_send.at[i], y_recv.at[i], y_near, own),
            pass_on(block, piece, mate_send.at[0, i], mate_recv.at[0, i], mate, own),
        )

    def got(block, i, recv):
        piece = chunk_list[i][1]
        pass_on(block, piece, x_send.at[i], recv, me).wait_recv()

    def spread(i, own=False):
        for copy in plane_copies(i, own):
            copy.start()

    def z_pass(i):
        def run(zv):
            level = chunk_list[i][1][0]
            got(column(level), i, z_recv.at[i])
            if level < zv < depth - 1:
                z_copy(i, True).start()
            if 0 < zv < level:
                z_copy(i, False).start()

        return run

    def take(i):
        def run(zv):
            z_pass(i)(zv)
            spread(i)

        return run

    def later_spread(i):
        return lambda zv: spread(i)

    def by_plane(p, zv):
        return True

    def corner_copies(p):
        level = pieces[p][0]
        first, second = halves(p)
        return (
            pass_on(from_x(level), first, corner_send.at[p, 0], corner_recv.at[p, 0], y_near),
            pass_on(from_y(level), second, corner_send.at[p, 1], corner_recv.at[p, 1], x_near),
        )

    def corner_along_z(p, zv):
        level = pieces[p][0]
        ways = [up] * (level <= zv < depth - 1) + [down] * (0 < zv <= level)
        return [
            [
                pass_on(across(level), part, line_send.at[p, 2 * side + (way is up)], line_recv.at[p, side], way)
                for way in ways
            ]
            for side, part in enumerate(halves(p))
        ]

    def mate_copies(p):
        level = pieces[p][0]
        first, second = halves(p)
        return (
            pass_on(from_x(level), pieces[p], mate_send.at[1, p], mate_recv.at[1, p], mate),
            pass_on(from_y(level), pieces[p], mate_send.at[2, p], mate_recv.at[2, p], mate),
            pass_on(across(level), first, mate_send.at[3, p], mate_recv.at[3, p], mate),
            pass_on(across(level), second, mate_send.at[4, p], mate_recv.at[4, p], mate),
        )

    def beside(p):
        def run(zv):
            level = pieces[p][0]
            for i in ids[p]:
                got(from_x(level), i, x_recv.at[i])
            if by_plane(p, zv):
                corner_copies(p)[0].start()
            mate_copies(p)[0].start()
            for i in ids[p]:
                got(from_y(level), i, y_recv.at[i])
            if by_plane(p, zv):
                corner_copies(p)[1].start()
            mate_copies(p)[1].start()

        return run

    def corner(p):
        def run(zv):
            level = pieces[p][0]
            for side, part in enumerate(halves(p)):
                recv = corner_recv if by_plane(p, zv) else line_recv
                pass_on(across(level), part, corner_send.at[p, side], recv.at[p, side], me).wait_recv()
                if not by_plane(p, zv):
                    for copy in corner_along_z(p, zv)[side]:
                        copy.start()
                mate_copies(p)[2 + side].start()

        return run

    def from_mate(p):
        def run(zv):
            level = pieces[p][0]
            other = 1 - 2 * core
            for i in ids[p]:
                pass_on(column(level) + other, chunk_list[i][1], mate_send.at[0, i], mate_recv.at[0, i], me).wait_recv()
            first, second = halves(p)
            for slot, (block, piece) in enumerate(
                ((from_x(level), pieces[p]), (from_y(level), pieces[p]), (across(level), first), (across(level), second))
            ):
                pass_on(block + other, piece, mate_send.at[slot + 1, p], mate_recv.at[slot + 1, p], me).wait_recv()

        return run

    def own_spread(i):
        return lambda zv: spread(i, True)

    def own_up(i):
        return lambda zv: z_copy(i, True, True).start() if zv < depth - 1 else None

    def own_down(i):
        return lambda zv: z_copy(i, False, True).start() if zv > 0 else None

    def w_copy(slot, which, device, source=None):
        return remote(x_in_ref if source is None else source, x_got_ref.at[slot], w_send.at[which], w_recv.at[slot], device)

    def w_far(zv):
        @pl.when(has_after)
        def _():
            w_copy(0, 1, after).start()

        @pl.when(has_before)
        def _():
            w_copy(4, 2, before).start()

    def w_forward(core_index):
        slot = 0 if core_index else 4
        return w_copy(1 if core_index else 3, 3, mate, x_got_ref.at[slot])

    def w_wait(slot):
        w_copy(slot, 0, me).wait_recv()

    def w_middle(zv):
        @pl.when(has_before)
        def _():
            w_wait(0)

        @pl.when(has_after)
        def _():
            w_wait(4)

        @pl.when((core == 1) & has_before)
        def _():
            w_forward(1).start()

        @pl.when((core == 0) & has_after)
        def _():
            w_forward(0).start()

    stops = [61.0, 63.0, 68.0, 73.0, 95.0, 102.0, 110.0] + [110.0 + 2.7 * h for h in range(1, HEADS)]

    def lists(zv):
        own_hot = [p for p in hot if pieces[p][0] == zv]
        own_cold = [p for p in cold if pieces[p][0] == zv]
        far_hot = sorted((p for p in hot if pieces[p][0] != zv), key=lambda p: abs(pieces[p][0] - zv))
        far_cold = sorted((p for p in cold if pieces[p][0] != zv), key=lambda p: (abs(pieces[p][0] - zv), -pieces[p][0]))
        distance = {p: abs(pieces[p][0] - zv) for p in cold}
        at_once = own_cold if zv > depth // 2 else []
        after_hot = [p for p in own_cold if p not in at_once]
        first = []
        for p in own_hot:
            for i in ids[p]:
                first += [own_up(i), own_down(i), own_spread(i)]
        for p in own_cold:
            first += [own_down(i) for i in ids[p]]
        for p in at_once:
            first += [own_spread(i) for i in ids[p]]
        for p in far_hot:
            first += [take(i) for i in ids[p]]
        passed = {p for p in far_cold if distance[p] < 3 and (0 < zv < pieces[p][0] or pieces[p][0] < zv < depth - 1)}
        from_above = [p for p in far_cold if p in passed and pieces[p][0] == zv + 1]
        first += [z_pass(i) for p in from_above for i in ids[p]]
        for p in own_cold:
            first += [own_up(i) for i in ids[p]]
        order_hot = own_hot + far_hot
        first += [beside(p) for p in order_hot]
        first += [z_pass(i) for p in far_cold if p in passed and p not in from_above for i in ids[p]]
        take_or_spread = lambda p: [(later_spread if p in passed else take)(i) for i in ids[p]]
        first.append(w_far)
        for p in after_hot:
            first += [own_spread(i) for i in ids[p]]
        for p in far_cold:
            first += take_or_spread(p) if distance[p] == 1 else []
        first += [corner(p) for p in order_hot]
        first += [from_mate(p) for p in order_hot]
        timed = [(73.0, event) for p in far_cold if distance[p] > 1 for event in take_or_spread(p)]
        order = at_once + after_hot + far_cold
        timed += [((110.0, 120.8, 137.0, 145.0)[min(k, 3)], beside(p)) for k, p in enumerate(order)]
        timed += [((142.4, 150.5, 200.0)[min(k, 2)], corner(p)) for k, p in enumerate(order)]
        return first, sorted(timed, key=lambda entry: entry[0])

    plans = [lists(zv) for zv in range(depth)]

    def each_plane(events_of):
        for zv in range(depth):
            events = events_of(zv)
            if events:

                @pl.when(z == zv)
                def _():
                    for event in events:
                        event(zv)

    w_copy(1 + 2 * core, 0, mate).start()
    fill = pltpu.make_async_copy(block_ref, stage_ref, local_sem)
    fill.start()
    fill.wait()
    keep = pltpu.make_async_copy(stage_ref, out_ref.at[me], local_sem)
    keep.start()
    each_plane(lambda zv: plans[zv][0])
    keep.wait()

    near_sem = x_sem
    def service(stop):
        low = stops[stop - 1] if stop else -1.0
        high = stops[stop] if stop < len(stops) else 1e9
        each_plane(lambda zv: [event for time, event in plans[zv][1] if low < time <= high])

    rows, window = q_ref.shape[0], x_ref.shape[0]
    k_ref, v_ref = both_ref.at[0], both_ref.at[1]
    loads = [copies(where, name, out_ref, w_ref.at[i], sem.at[i]) for i, name in enumerate(("w_query", "w_key", "w_value"))]
    vecs = copies(where, "vec1", out_ref, vec1_ref, vec_sem) + copies(where, "vec2", out_ref, vec2_ref, vec_sem)
    start(vecs)
    for made in loads:
        start(made)

    def slot_rows(slot):
        return pl.ds(pl.multiple_of(slot * rows, rows), rows)

    def bring(slot, there=None):
        at = x_ref.at[slot_rows(slot)]
        if there is None:
            pltpu.make_async_copy(x_got_ref.at[slot], at, near_sem).start()
            return

        @pl.when(there)
        def _():
            pltpu.make_async_copy(x_got_ref.at[slot], at, near_sem).start()

        @pl.when(jnp.logical_not(there))
        def _():
            pltpu.make_async_copy(x_in_ref, at, near_sem).start()

    def brought(many):
        for _ in range(many):
            pltpu.make_async_copy(x_in_ref, x_ref.at[slot_rows(0)], near_sem).wait()

    mate_slot, far_slot = 3 - 2 * core, 1 + 2 * core
    w_wait(mate_slot)
    pltpu.make_async_copy(x_in_ref, x_ref.at[slot_rows(2)], near_sem).start()
    bring(mate_slot)
    brought(2)
    wait(vecs)
    vec = vector_rows(vec1_ref)
    gain, shift = as_row(vec, 0, DC), as_row(vec, DC, DC)
    biases = vector_rows(vec2_ref)
    step = rows // 3

    @pl.loop(0, rows // 8)
    def _(i):
        at = pl.ds(i * 8, 8)
        bias_ref[at] = jnp.where(segq_ref[at] == segk_ref[...], 0.0, NEG)

    def over_slots(slots, body):
        @pl.loop(0, len(slots))
        def _(i):
            slot = slots[-1]
            for k, other in enumerate(slots[:-1]):
                slot = jnp.where(i == k, other, slot)
            body(slot)

    def norm_slots(slots):
        def norm_slot(slot):
            @pl.loop(0, rows // step)
            def _(i):
                at = pl.ds(pl.multiple_of(slot * rows + i * step, step), step)
                normed, _ = norm_rows(x_ref[at].astype(F32))
                turned_ref[:, at] = normed.astype(BF).T
                normed_ref[at] = (normed * gain + shift).astype(BF)

        over_slots(slots, norm_slot)

    def project(i, slots):
        def some(c, many):
            lanes = lanes_of(c, many)
            weights = panels(w_ref.at[i], c, many, D // ROWS)

            def rows_of(slot):
                value = (nn(normed_ref[slot_rows(slot)], weights) + add_ref[i, 0:1, lanes]).astype(BF)
                if isinstance(i, int):
                    q_ref[:, lanes] = value
                else:
                    both_ref[i - 1, slot_rows(slot), lanes] = value

            over_slots(slots, rows_of)

        over_pairs(some)

    def keys_and_values(slots, between):
        @pl.loop(0, 2)
        def _(i):
            project(i + 1, slots)
            for k, action in enumerate(between):

                @pl.when(i == k)
                def _():
                    action()

    norm_slots([2, mate_slot])
    service(0)
    for made in loads:
        wait(made)
    for i, row in enumerate((as_row(biases, 0, DC), jnp.zeros((1, D), F32), as_row(biases, DC, DC))):
        add_ref[i, 0:1] = row
    project(0, [2])
    service(1)
    keys_and_values([2, mate_slot], [lambda: service(2), lambda: service(3)])
    w_middle(None)

    @pl.when((core == 0) & has_before)
    def _():
        w_wait(1)

    @pl.when((core == 1) & has_after)
    def _():
        w_wait(3)

    bring(0, has_before)
    bring(4, has_after)
    bring(far_slot, jnp.where(core == 0, has_before, has_after))
    brought(3)
    others = [0, 4, far_slot]
    norm_slots(others)
    saves = [pltpu.make_async_copy(x_ref, x_out_ref, local_sem), pltpu.make_async_copy(turned_ref, turned_out_ref, local_sem)]
    start(saves)
    service(4)
    k_save = pltpu.make_async_copy(k_ref, k_out_ref, keys_sem.at[0])

    def keys_done():
        service(5)
        k_save.start()

    keys_and_values(others, [keys_done])
    v_save = pltpu.make_async_copy(v_ref, v_out_ref, keys_sem.at[1])
    v_save.start()
    wait(saves)

    @pl.loop(0, window // LANES)
    def _(i):
        at = pl.ds(pl.multiple_of(i * LANES, LANES), LANES)
        turned_ref[:, at] = k_ref[at].T

    keys_save = pltpu.make_async_copy(turned_ref, keys_out_ref, keys_sem.at[2])
    keys_save.start()
    attended_ref[...] = jnp.zeros_like(attended_ref)
    rest_ref[...] = jnp.zeros_like(rest_ref)
    logs_ref[...] = jnp.zeros_like(logs_ref)
    lane_l = lax.broadcasted_iota(jnp.int32, logs_ref.shape, 1)

    @pl.loop(0, HEADS)
    def _(h):
        for at_head in range(HEADS):

            @pl.when(h == at_head)
            def _():
                service(6 + at_head)

        lane, offset = head_window(h)
        mask = head_mask(rows, offset)
        lanes = pl.ds(lane, PAIR)
        query = jnp.where(mask, q_ref[:, lanes], jnp.zeros((), BF))
        score_ref[...] = nt(query, k_ref[:, lanes]) * SCALE + bias_ref[...]
        top = jnp.max(score_ref[...], axis=-1, keepdims=True)
        powers = jnp.exp(score_ref[...] - top)
        total = jnp.sum(powers, axis=-1, keepdims=True)
        prob_ref[...] = powers.astype(BF)
        out = nn(prob_ref[...], v_ref[:, lanes]) / total
        rounded = out.astype(BF)
        attended_ref[:, lanes] = jnp.where(mask, rounded, attended_ref[:, lanes])
        rest_ref[:, lanes] = jnp.where(mask, (out - rounded.astype(F32)).astype(BF), rest_ref[:, lanes])
        logs_ref[...] = jnp.where(lane_l == h, top + jnp.log(total), logs_ref[...])

    service(len(stops))
    each_plane(lambda zv: [from_mate(p) for p in cold])

    def sent(zv):
        for i, (p, piece) in enumerate(chunk_list):
            for copy in plane_copies(i):
                copy.wait_send()
            level = piece[0]
            if zv < depth - 1 and level <= zv:
                z_copy(i, True).wait_send()
            if zv > 0 and level >= zv:
                z_copy(i, False).wait_send()
        for p in range(len(pieces)):
            for copy in mate_copies(p) + (corner_copies(p) if by_plane(p, zv) else ()):
                copy.wait_send()
            for copy in sum(corner_along_z(p, zv), []) if not by_plane(p, zv) else []:
                copy.wait_send()

    each_plane(lambda zv: [sent])
    w_copy(0, 0, mate).wait_send()

    @pl.when(has_after)
    def _():
        w_copy(0, 1, after).wait_send()

    @pl.when(has_before)
    def _():
        w_copy(4, 2, before).wait_send()

    @pl.when(jnp.where(core == 1, has_before, has_after))
    def _():
        w_forward(0).wait_send()

    wait([k_save, v_save, keys_save])


def gather_front(block, block_input, seg_query, seg_keys, plan):
    where = plan[0]
    count = lax.axis_size("fsdp")
    depth = count // 8
    rows, window = block_input.shape[0], seg_keys.shape[1]
    early, whole = transfer_pieces(plan, depth)
    late = whole
    shape = lambda n, d=D, t=BF: jax.ShapeDtypeStruct((n, d), t)
    dma = pltpu.SemaphoreType.DMA
    units = D // ROWS
    many = len(early) + len(late)
    chunks = many + 3 * sum(1 for piece in early if piece[0] == 0)
    got = jax.ShapeDtypeStruct((5, rows, D), BF)
    return pl.pallas_call(
        functools.partial(gather_front_kernel, depth, where, early, late),
        out_shape=(
            jax.ShapeDtypeStruct((count, *block.shape), BF), shape(window), shape(D, window), shape(D, window), shape(window), shape(window), got,
            shape(rows), shape(rows), shape(rows), shape(rows, LANES, F32),
        ),
        in_specs=[ANY, ANY, VM, VM],
        out_specs=[ANY] * 7 + [VM] * 4,
        scratch_shapes=[
            dma((chunks, 2)), dma((chunks,)), dma((chunks,)), dma((chunks,)), dma((chunks,)), dma((chunks,)),
            dma((many, 2)), dma((many, 2)), dma((many, 4)), dma((many, 2)), dma((5, chunks)), dma((5, chunks)), dma((4,)), dma((5,)),
            dma, pltpu.VMEM(block.shape, BF), pltpu.VMEM((2, window, D), BF),
            pltpu.VMEM((window, D), BF), pltpu.VMEM((D, window), BF), pltpu.VMEM((window, D), BF),
            pltpu.VMEM((3, units, DC, ROWS, LANES), BF), pltpu.VMEM((2, ROWS, LANES), BF), pltpu.VMEM((2, ROWS, LANES), BF),
            pltpu.VMEM((rows, window), F32), pltpu.VMEM((rows, window), F32), pltpu.VMEM((rows, window), BF), pltpu.VMEM((3, 8, D), F32),
            dma((3,)), dma, dma, dma((3,)),
        ],
        compiler_params=pltpu.CompilerParams(collective_id=0, has_side_effects=True, vmem_limit_bytes=VMEM_LIMIT),
        name="gather_front",
    )(block, block_input, seg_query, seg_keys)


def back_scatter_kernel(
    depth, where, early, late,
    x_hbm_ref, turned_hbm_ref, keys_hbm_ref, segq_ref, segk_ref, blocks_ref, q_ref, k_hbm_ref, v_hbm_ref, grad_ref, logs_ref, delta_ref, mid_hbm_ref, parts_in_ref,
    parts_ref, out_ref, in_grad_ref, mates, sums, halfs, fulls, lines, near_ref, near_got,
    w_ref, g_ref, vec1_ref, vec2_ref, score_ref, prob_ref, turned_ref, k_ref, v_ref, dq_ref, part_ref, logs_t_ref, x_ref, dq_b_ref,
    block_ref, mid_ref, g_value_ref, gain_acc, shift_acc, stage, total,
    mate_send, mate_recv, half_send, half_recv, full_send, full_recv, line_send, line_recv, near_send, near_recv,
    load_sem, store_sem, sem, vec_sem, out_sem, x_sem,
):
    me = lax.axis_index("fsdp")
    count = 8 * depth
    core, x, y, z = place(me)
    mate, x_near, y_near = index_of(1 - core, x, y, z), index_of(core, 1 - x, y, z), index_of(core, x, 1 - y, z)
    after, before = me + 2, me - 2
    has_after, has_before = after < count, before >= 0
    greet(
        [(mate, None), (x_near, None), (y_near, None), (me - 8, z > 0), (me + 8, z < depth - 1), (after, has_after), (before, has_before)]
    )
    pieces = early + late
    block_tiles = parts_ref.shape[1]
    early_ids, late_ids = range(len(early)), range(len(early), len(pieces))

    def remote(source, target, send, recv, device):
        return pltpu.make_async_remote_copy(
            src_ref=source, dst_ref=target, send_sem=send, recv_sem=recv, device_id=(device,), device_id_type=MESH
        )

    def owner(level, slot, which_core):
        return index_of(which_core, 1 - x if slot in (1, 3) else x, 1 - y if slot in (2, 3) else y, level)

    def at_plane(zv, run):
        @pl.when(z == zv)
        def _():
            run()

    def span(p, lo=0, many=None):
        _, first, tiles = pieces[p]
        return pl.ds(first + lo, tiles if many is None else many)

    def half_of(p):
        return pieces[p][2] // 2

    def to_mate(p, slot):
        level = pieces[p][0]
        return remote(
            parts_ref.at[owner(level, slot, 1 - core), span(p)], mates.at[level, slot, span(p)],
            mate_send.at[p, slot], mate_recv.at[p, slot], mate,
        )

    def half_out(p, side):
        level, _, tiles = pieces[p]
        part = span(p, half_of(p), tiles - half_of(p)) if side else span(p, 0, half_of(p))
        return remote(
            sums.at[level, 3, part], halfs.at[level, side, part], half_send.at[p, side], half_recv.at[p, side],
            x_near if side else y_near,
        )

    def full_out(p, side):
        level = pieces[p][0]
        return remote(
            sums.at[level, 1 + side, span(p)], fulls.at[level, side, span(p)], full_send.at[p, side], full_recv.at[p, side],
            y_near if side else x_near,
        )

    def subs(p):
        tiles = pieces[p][2]
        if p in early_ids or tiles < block_tiles // 3:
            return [(0, tiles)]
        return [(0, tiles // 2), (tiles // 2, tiles - tiles // 2)]

    def line_out(p, zv, sub):
        level = pieces[p][0]
        part = span(p, *subs(p)[sub])
        upward = level > zv
        slot = depth if not upward and level == zv - 1 else level
        side = 1 if slot == depth else 0
        return remote(
            sums.at[level, 0, part], lines.at[slot, part], line_send.at[p, sub], line_recv.at[p, 2 * sub + side],
            me + 8 if upward else me - 8,
        )

    def line_in(p, side, sub):
        level = pieces[p][0]
        slot = depth if side else level
        part = span(p, *subs(p)[sub])
        return remote(sums.at[level, 0, part], lines.at[slot, part], line_send.at[p, sub], line_recv.at[p, 2 * sub + side], me)

    def line_sides(p, zv):
        level = pieces[p][0]
        if level > zv:
            return [0] if zv > 0 else []
        if level < zv:
            return [0] if zv < depth - 1 else []
        return ([0] if zv > 0 else []) + ([1] if zv < depth - 1 else [])

    def extent(job):
        kind, p, sub = job
        return subs(p)[sub] if kind == 0 else (0, pieces[p][2])

    def sources(job, zv):
        kind, p, sub = job
        level, _, tiles = pieces[p]
        h = half_of(p)
        if kind == 0:
            lo, many = extent(job)
            part = span(p, lo, many)
            refs = [parts_ref.at[owner(level, 0, core), part], mates.at[level, 0, part]]
            refs += [fulls.at[level, side, part] for side in (0, 1)]
            refs += [lines.at[depth if side else level, part] for side in line_sides(p, zv)]
            return [(ref, 0, many) for ref in refs]
        found = [(parts_ref.at[owner(level, kind, core), span(p)], 0, tiles), (mates.at[level, kind, span(p)], 0, tiles)]
        if kind == 1:
            found.append((halfs.at[level, 0, span(p, 0, h)], 0, h))
        if kind == 2:
            found.append((halfs.at[level, 1, span(p, h, tiles - h)], h, tiles - h))
        return found

    def loads(job, zv, base):
        return [
            pltpu.make_async_copy(ref, stage.at[i, pl.ds(base + lo, many)], load_sem.at[1 if base else 0])
            for i, (ref, lo, many) in enumerate(sources(job, zv))
        ]

    def store(job, base):
        kind, p, sub = job
        lo, many = extent(job)
        return pltpu.make_async_copy(
            total.at[pl.ds(base, many)], sums.at[pieces[p][0], kind, span(p, lo, many)], store_sem.at[1 if base else 0]
        )

    def load(job, zv, base=0):
        kind, p, sub = job
        if sub == 0:
            to_mate(p, kind).wait_recv()
        if kind in (1, 2):
            half_out(p, kind - 1).wait_recv()
        made = loads(job, zv, base)
        if kind == 0:
            if sub == 0:
                for side in (0, 1):
                    full_out(p, side).wait_recv()
            start(made[:4])
            for copy, side in zip(made[4:], line_sides(p, zv)):
                line_in(p, side, sub).wait_recv()
                copy.start()
        else:
            start(made)

    def add(base, lo, many, slots, target, shift):
        def some(first, tiles):
            value = stage[slots[0], pl.ds(first, tiles)].astype(F32)
            for slot in slots[1:]:
                value = value + stage[slot, pl.ds(first, tiles)].astype(F32)
            target[pl.ds(first + shift, tiles)] = value.astype(target.dtype)

        group = 8

        @pl.loop(0, many // group)
        def _(i):
            some(base + lo + i * group, group)

        if many % group:
            some(base + lo + many // group * group, many % group)

    def finish(job, zv, base=0):
        kind, p, sub = job
        level, first, tiles = pieces[p]
        found = sources(job, zv)
        wait(loads(job, zv, base))
        final = kind == 0 and level == zv
        target, shift = (out_ref, first + extent(job)[0] - base) if final else (total, 0)
        edges = sorted({e for _, lo, many in found for e in (lo, lo + many)})
        for lo, hi in zip(edges[:-1], edges[1:]):
            slots = [i for i, (_, a, many) in enumerate(found) if a <= lo and hi <= a + many]
            add(base, lo, hi - lo, slots, target, shift)
        if not final:
            store(job, base).start()

    def send(job, zv, base=0):
        kind, p, sub = job
        if kind == 0 and pieces[p][0] == zv:
            return
        store(job, base).wait()
        if kind == 3:
            half_out(p, 0).start()
            half_out(p, 1).start()
        elif kind == 0:
            line_out(p, zv, sub).start()
        else:
            full_out(p, kind - 1).start()

    second = block_tiles // 2

    def run(jobs, zv):
        for job in jobs:
            load(job, zv)
            finish(job, zv)
            send(job, zv)

    def run_ahead(jobs, zv):
        bases = [second * (k % 2) for k in range(len(jobs))]
        for k, job in enumerate(jobs):
            if k == 0:
                load(job, zv, bases[k])
            if k + 1 < len(jobs):
                load(jobs[k + 1], zv, bases[k + 1])
            finish(job, zv, bases[k])
            if k:
                send(jobs[k - 1], zv, bases[k - 1])
        send(jobs[-1], zv, bases[-1])

    def along(p):
        return [(0, p, sub) for sub in range(len(subs(p)))]

    for p in early_ids:
        for slot in (3, 1, 2, 0):
            to_mate(p, slot).start()

    window, rows = k_ref.shape[0], q_ref.shape[0]
    margin = (window - rows) // 2
    names = ("w_query", "w_key", "w_value")
    k_load = [
        pltpu.make_async_copy(a, b, vec_sem)
        for a, b in ((k_hbm_ref, k_ref), (v_hbm_ref, v_ref), (keys_hbm_ref, turned_ref))
    ]
    start(k_load)
    weight_loads = [copies(where, name, blocks_ref, w_ref.at[i], sem.at[i]) for i, name in enumerate(names)]
    vecs = copies(where, "vec1", blocks_ref, vec1_ref, sem.at[3])
    start(vecs)
    for made in weight_loads:
        start(made)
    x_load = [pltpu.make_async_copy(x_hbm_ref, x_ref, x_sem)]
    start(x_load)
    logs_t_ref[...] = logs_ref[...].T * LOG2E
    g_value_ref[...] = jnp.zeros_like(g_value_ref)

    by_level = {pieces[p][0]: p for p in early_ids}
    a, b, c_ = (by_level[level] for level in sorted(by_level, reverse=True)[:3])
    table = [
        (-1, 0, 3, a, None), (0, 1, 3, b, None), (3, 4, 1, a, None), (4, 5, 2, a, None), (5, 6, 3, c_, None),
        (6, 7, 1, b, None), (7, 8, 2, b, None), (11, 12, 0, a, 0), (12, 13, 1, c_, None), (13, 14, 2, c_, None),
    ]

    def beside(h, which, action):
        for entry in table:
            if entry[which] < 0:
                continue
            kind, p, zv = entry[2:]
            job = (kind, p, 0)
            there = h == entry[which]
            if zv is not None:
                there = there & (z == zv)

            @pl.when(there)
            def _():
                action(job, zv)

    wait(k_load)
    load((3, a, 0), None)

    @pl.loop(0, HEADS)
    def _(h):
        beside(h, 1, finish)
        lane, offset = head_window(h)
        mask = head_mask(rows, offset)
        lanes = pl.ds(lane, PAIR)
        query = jnp.where(mask, q_ref[:, lanes], jnp.zeros((), BF))
        grad = jnp.where(mask, grad_ref[:, lanes], jnp.zeros((), BF))
        log_row, delta_row = logs_t_ref[pl.ds(h, 1)], delta_ref[pl.ds(h, 1)]
        blocks = [pl.ds(n * rows, rows) for n in range(window // rows)]
        for keys in blocks:
            together = jnp.concatenate([segk_ref[keys]] * (rows // LANES), axis=1) == segq_ref[...]
            probs = jnp.exp2(jnp.where(together, nt(k_ref[keys, lanes], query) * (SCALE * LOG2E) - log_row, NEG))
            prob_ref[keys] = probs.astype(BF)
            score_ref[keys] = (probs * (nt(v_ref[keys, lanes], grad) - delta_row)).astype(BF)
        beside(h, 1, send)
        beside(h, 0, load)
        side = head_mask(rows, offset)

        @pl.loop(0, window // rows)
        def _(n):
            keys = pl.ds(pl.multiple_of(n * rows, rows), rows)
            dv = nn(prob_ref[keys], grad)
            g_value_ref[:, lanes] += column_sums(dv)
            v_ref[keys, lanes] = jnp.where(side, dv.astype(BF), v_ref[keys, lanes])
            dk = nn(score_ref[keys], query) * SCALE
            k_ref[keys, lanes] = jnp.where(side, dk.astype(BF), k_ref[keys, lanes])
        tile = (h * HEAD_DIM) // ROWS * ROWS
        part_ref[...] = nn(turned_ref[pl.ds(pl.multiple_of(tile, ROWS), part_ref.shape[0])], score_ref[...])
        at = pl.ds(pl.multiple_of(h * HEAD_DIM, 8), HEAD_DIM)
        dq_ref[at] = part_ref[pl.ds(pl.multiple_of(h * HEAD_DIM - tile, 8), HEAD_DIM)]

    turned_load = pltpu.make_async_copy(turned_hbm_ref, turned_ref, vec_sem)
    turned_load.start()
    dq = dq_ref[...].T * SCALE
    put_vectors(vec2_ref, [column_sums(dq), g_value_ref[...]])
    saves = copies(where, "vec2", parts_ref, vec2_ref, out_sem.at[3], out=True)
    dq_b_ref[...] = dq.astype(BF)
    wait(vecs)
    vec = vector_rows(vec1_ref)
    gain, shift = as_row(vec, 0, DC), as_row(vec, DC, DC)
    gain_t, shift_t = (jnp.broadcast_to(v, (8, D)).T[:, :1] for v in (gain, shift))
    wait(x_load)
    step = rows // 3

    turned_load.wait()
    for made in weight_loads:
        wait(made)
    gain_acc[...] = jnp.zeros_like(gain_acc)
    shift_acc[...] = jnp.zeros_like(shift_acc)

    def plane_job(what, entries):
        for zv, p in entries:

            def go():
                job = (0, p, 0)
                if what == "load":
                    load(job, zv)
                else:
                    finish(job, zv)
                    send(job, zv)

            at_plane(zv, go)

    own = turned_ref[:, pl.ds(margin, rows)]
    made = []
    first_jobs, last_jobs = [(1, a), (0, b), (3, b)], [(0, c_), (3, c_)]
    for i, (left, right_ref) in enumerate(((own, dq_b_ref), (turned_ref, k_ref), (turned_ref, v_ref))):
        if i == 1:
            plane_job("load", first_jobs)
        if i == 2:
            plane_job("end", first_jobs)
            plane_job("load", last_jobs)
            wait(made[0])

        def project_back(c, many):
            right = right_ref[:, lanes_of(c, many)]
            raw = nn(left[...], right)
            summed = column_sums(right.astype(F32))
            put_panels(g_ref.at[i % 2], c, gain_t * raw + shift_t * summed)
            weights = panels(w_ref.at[i], c, many, D // ROWS).astype(F32)
            scaled, shifted = weights * raw, weights * summed
            for j in range(many):
                part = slice(j * LANES, (j + 1) * LANES)
                gain_acc[...] += scaled[:, part]
                shift_acc[...] += shifted[:, part]

        over_pairs(project_back)
        made.append(copies(where, names[i], parts_ref, g_ref.at[i % 2], out_sem.at[i], out=True))
        start(made[i])
    put_vectors(vec1_ref, [column_sums(gain_acc[...].T), column_sums(shift_acc[...].T)])
    saves = saves + copies(where, "vec1", parts_ref, vec1_ref, out_sem.at[3], out=True)
    start(saves)
    plane_job("end", last_jobs)
    wait(saves + made[1] + made[2])
    for slots in ((3,), (1, 2), (0,)):
        for p in late_ids:
            for slot in slots:
                to_mate(p, slot).start()

    def slot_rows(n):
        return pl.ds(pl.multiple_of(n * rows, rows), rows)

    def row_block(n, own=False):
        first = n * rows

        def project_back(c, many):
            part = lambda i: panels(w_ref.at[i], 0, DC, many * LANES // ROWS, c * (LANES // ROWS))
            value = nt(k_ref[slot_rows(n)], part(1)) + nt(v_ref[slot_rows(n)], part(2))
            if own:
                value = value + nt(dq_b_ref[...], part(0))
            block_ref[:, lanes_of(c, many)] = value

        over_pairs(project_back)

        @pl.loop(0, rows // step)
        def _(i):
            here = pl.ds(pl.multiple_of(i * step, step), step)
            there = pl.ds(pl.multiple_of(first + i * step, step), step)
            normed, inverse = norm_rows(x_ref[there].astype(F32))
            result = norm_rows_back(block_ref[here], normed, inverse, gain)
            if own:
                block_ref[here] = result
            else:
                x_ref[there] = result.astype(BF)

    def near_rows(slot):
        return x_ref.at[pl.ds(slot * rows, rows)]

    def near_save(slot):
        return pltpu.make_async_copy(near_rows(slot), near_ref.at[slot], x_sem)

    def near_copy(slot, which, device):
        return remote(near_ref.at[slot], near_got.at[which], near_send.at[which], near_recv.at[which], device)


    run_ahead([(3, p, 0) for p in late_ids], None)

    @pl.loop(0, 4)
    def _(i):
        row_block(jnp.where(i == 0, 0, jnp.where(i == 1, 4, 2 * i - 3)))

        @pl.when(i == 1)
        def _():
            for p in late_ids:
                run_ahead([(1, p, 0), (2, p, 0)], None)
            at_plane(1, lambda: run([(0, b, 0)], 1))
            at_plane(2, lambda: run([(0, a, 0), (0, c_, 0)], 2))

    sides = [near_save(slot) for slot in (0, 4, 1, 3)]
    start(sides)
    wait(sides)
    to_mate_itself, to_mate_shared = (3 - 2 * core), (1 + 2 * core)
    near_copy(to_mate_itself, 0, mate).start()
    near_copy(to_mate_shared, 1, mate).start()

    @pl.when((core == 0) & has_before)
    def _():
        near_copy(0, 2, before).start()

    @pl.when((core == 1) & has_after)
    def _():
        near_copy(4, 3, after).start()

    near_copy(0, 1, me).wait_recv()
    shared_slot = 4 - 4 * core
    fetch = pltpu.make_async_copy(near_got.at[1], k_ref.at[pl.ds(0, rows)], x_sem)
    fetch.start()
    fetch.wait()

    @pl.loop(0, rows // step)
    def _(i):
        here = pl.ds(pl.multiple_of(i * step, step), step)
        there = pl.ds(pl.multiple_of(shared_slot * rows + i * step, step), step)
        x_ref[there] = (x_ref[there].astype(F32) + k_ref[here].astype(F32)).astype(BF)

    shared_save = near_save(shared_slot)
    shared_save.start()
    shared_save.wait()

    @pl.when((core == 0) & has_after)
    def _():
        near_copy(4, 3, after).start()

    @pl.when((core == 1) & has_before)
    def _():
        near_copy(0, 2, before).start()

    def hops(p, zv):
        return zv if pieces[p][0] > zv else depth - 1 - zv

    def tail(zv, at_end):
        out = sorted((p for p in late_ids if pieces[p][0] != zv), key=lambda p: (hops(p, zv), p))
        if not at_end:
            return [job for p in out if hops(p, zv) == 0 for job in along(p)]
        own = [p for ids in (early_ids, late_ids) for p in ids if pieces[p][0] == zv]
        return [job for p in out + own if p in own or hops(p, zv) for job in along(p)]

    for zv in (0, depth - 1):
        at_plane(zv, lambda: run(tail(zv, False), zv))
    row_block(2, True)

    @pl.loop(0, rows // step)
    def _(i):
        here = pl.ds(pl.multiple_of(i * step, step), step)
        fetch_mid = pltpu.make_async_copy(mid_hbm_ref.at[here], mid_ref, x_sem)
        fetch_mid.start()
        fetch_mid.wait()
        block_ref[here] += mid_ref[...]

    for zv in range(depth):
        at_plane(zv, lambda: run(tail(zv, True), zv))

    near_copy(0, 0, me).wait_recv()

    @pl.when(has_after)
    def _():
        near_copy(0, 2, me).wait_recv()

    @pl.when(has_before)
    def _():
        near_copy(0, 3, me).wait_recv()

    for i, (which, there) in enumerate(((0, None), (2, has_after), (3, has_before))):
        target = k_ref.at[pl.ds(i * rows, rows)]
        if there is None:
            pltpu.make_async_copy(near_got.at[which], target, x_sem).start()
            continue

        @pl.when(there)
        def _():
            pltpu.make_async_copy(near_got.at[which], target, x_sem).start()

        @pl.when(jnp.logical_not(there))
        def _():
            pltpu.make_async_copy(near_ref.at[0], target, x_sem).start()

    for i in range(3):
        pltpu.make_async_copy(near_got.at[0], k_ref.at[pl.ds(i * rows, rows)], x_sem).wait()
    near_after, near_before = (jnp.where(there, 1.0, 0.0) for there in (has_after, has_before))

    @pl.loop(0, rows // step)
    def _(i):
        here = pl.ds(pl.multiple_of(i * step, step), step)
        value = block_ref[here] + k_ref[here].astype(F32)
        value = value + near_after * k_ref[pl.ds(pl.multiple_of(rows + i * step, step), step)].astype(F32)
        value = value + near_before * k_ref[pl.ds(pl.multiple_of(2 * rows + i * step, step), step)].astype(F32)
        in_grad_ref[here] = value.astype(BF)

    for p in range(len(pieces)):
        for slot in range(4):
            to_mate(p, slot).wait_send()
        for side in (0, 1):
            half_out(p, side).wait_send()
            full_out(p, side).wait_send()
        for zv in range(depth):
            if pieces[p][0] != zv:
                at_plane(zv, lambda: [line_out(p, zv, sub).wait_send() for sub in range(len(subs(p)))])
    near_copy(0, 0, mate).wait_send()
    near_copy(0, 1, mate).wait_send()

    @pl.when(has_before)
    def _():
        near_copy(0, 2, before).wait_send()

    @pl.when(has_after)
    def _():
        near_copy(4, 3, after).wait_send()


def back_scatter(x_win, turned, turned_keys, seg_query, seg_keys, gathered, queries, key_win, value_win, att_grad, logs, delta, mid_grad, parts, plan):
    where, block = plan[:2]
    window, rows = x_win.shape[0], queries.shape[0]
    seg_keys = jnp.broadcast_to(seg_keys, (window, LANES))
    count = lax.axis_size("fsdp")
    depth = count // 8
    hot, cold = transfer_pieces(plan, depth)
    early = sorted(cold, reverse=True)
    late = []
    for piece in sorted(hot, reverse=True):
        late += cut(piece, 2) if piece[2] > block // 2 else [piece]
    many = len(early) + len(late)
    dma = pltpu.SemaphoreType.DMA
    tiles = lambda *n: pltpu.VMEM((*n, ROWS, LANES), BF)
    vm = lambda a, b, t: pltpu.VMEM((a, b), t)
    hbm = lambda *n: jax.ShapeDtypeStruct((*n, ROWS, LANES), BF)
    return pl.pallas_call(
        functools.partial(back_scatter_kernel, depth, where, early, late),
        out_shape=(
            jax.ShapeDtypeStruct(parts.shape, BF), jax.ShapeDtypeStruct((block, ROWS, LANES), F32), jax.ShapeDtypeStruct((rows, D), BF),
            hbm(depth, 4, block), hbm(depth, 4, block), hbm(depth, 2, block), hbm(depth, 2, block), hbm(depth + 1, block),
            jax.ShapeDtypeStruct((5, rows, D), BF), jax.ShapeDtypeStruct((4, rows, D), BF),
        ),
        in_specs=[ANY, ANY, ANY, VM, VM, ANY, VM, ANY, ANY, VM, VM, VM, ANY, ANY],
        out_specs=[ANY, VM, VM] + [ANY] * 7,
        scratch_shapes=[
            tiles(3, D // ROWS, DC), tiles(2, D // ROWS, DC), tiles(2), tiles(2),
            vm(window, rows, BF), vm(window, rows, BF), vm(D, window, BF), vm(window, D, BF), vm(window, D, BF),
            vm(D, rows, F32), vm(ROWS * pl.cdiv(HEAD_DIM + 8, ROWS), rows, F32), vm(LANES, rows, F32), vm(window, D, BF), vm(rows, D, BF), vm(rows, D, F32), vm(rows // 3, D, F32),
            vm(1, D, F32), vm(D, LANES, F32), vm(D, LANES, F32), tiles(6, block), tiles(block),
            dma((many, 4)), dma((many, 4)), dma((many, 2)), dma((many, 2)), dma((many, 2)), dma((many, 2)), dma((many, 2)), dma((many, 4)),
            dma((4,)), dma((4,)), dma((2,)), dma((2,)), dma((4,)), dma, dma((4,)), dma,
        ],
        input_output_aliases={13: 0},
        compiler_params=pltpu.CompilerParams(collective_id=1, has_side_effects=True, vmem_limit_bytes=VMEM_LIMIT),
        name="back_scatter",
    )(x_win, turned, turned_keys, seg_query, seg_keys, gathered, queries, key_win, value_win, att_grad, logs, delta, mid_grad, parts)[1:3]


def passed_along(value, steps):
    count = lax.axis_size("fsdp")
    first, last = (max(0, -steps), min(count, count - steps))
    return lax.ppermute(value, "fsdp", [(source, source + steps) for source in range(first, last)])


def window_of(rows):
    near = [rows if k == 0 else passed_along(rows, -k) for k in range(-REACH, REACH + 1)]
    return jnp.concatenate(near, axis=0)


def shards(kernels, block_input, params, cotangent, segment_ids):
    count = lax.axis_size("fsdp")
    me = lax.axis_index("fsdp")
    rows = block_input.shape[0]
    margin = REACH * rows
    seg_pad = jnp.pad(segment_ids, (margin, margin), constant_values=-1)
    seg_query = lax.dynamic_slice_in_dim(segment_ids, me * rows, rows, 0)
    seg_keys = lax.dynamic_slice_in_dim(seg_pad, me * rows, 2 * margin + rows, 0)
    plan = wire_plan(count, params.shape[1])
    where = plan[0]
    block = to_tiles(params, plan)
    if kernels:
        gathered, x_win, turned, turned_keys, key_win, value_win, _, queries, attended, rest, logs = gather_front(
            block, block_input, seg_query[:, None], seg_keys[None, :], plan
        )
    else:
        x_win = window_of(block_input)
        gathered = lax.all_gather(block, "fsdp", axis=0, tiled=False)
        queries, key_win, value_win, attended, rest, logs = front(
            x_win, seg_query[:, None], seg_keys[None, :], gathered, where, rows
        )
    activations, mid_grad, att_grad, delta, parts = middle(block_input, cotangent, attended, rest, gathered, where)
    sides = (seg_query[None, :], seg_keys[:, None], gathered, queries, key_win, value_win, att_grad, logs)
    if kernels:
        summed, input_grad = back_scatter(x_win, turned, turned_keys, *sides, delta, mid_grad, parts, plan)
    else:
        near, own, parts = back(x_win, *sides, parts, where)
        input_grad = mid_grad + own
        for k in range(-REACH, REACH + 1):
            if k != 0:
                part = near[(k + REACH) * rows : (k + REACH + 1) * rows]
                input_grad = input_grad + passed_along(part, k).astype(jnp.float32)
        input_grad = input_grad.astype(jnp.bfloat16)
        received = lax.all_to_all(parts, "fsdp", split_axis=0, concat_axis=0, tiled=True)
        summed = jnp.sum(received.astype(jnp.float32), axis=0)
    param_grads = to_flat(summed, plan, params.shape[1])
    return (activations, input_grad, param_grads)


def two_by_two(mesh):
    spans = np.array([device.coords for device in mesh.devices.flat])
    return tuple(spans.max(axis=0) - spans.min(axis=0))[:2] == (1, 1)


def solution(mesh):
    return jax.shard_map(
        functools.partial(shards, two_by_two(mesh)),
        mesh=mesh,
        in_specs=(P("fsdp", None), P(None, "fsdp"), P("fsdp", None), P()),
        out_specs=(P("fsdp", None), P("fsdp", None), P(None, "fsdp")),
        check_vma=False,
    )
```
